32 devices in a mesh: data: 32 (over z, y, x, core).
Axes of the slice: x: 2, y: 2, z: 4, core: 2. Of those that a mesh axis runs over, the one named last changes fastest.
Arguments:
- x_act: bfloat16 [256, 196, 768], P('data')
- y_tgt: bfloat16 [256, 196, 768], P('data')
- w_in: float32 [2, 768, 3072], replicated
- w_out: float32 [2, 3072, 768], replicated
Outputs:
- output 1: float32 [2, 768, 3072], replicated
- output 2: float32 [2, 3072, 768], replicated
- output 3: float32 [], replicated
All inputs are finite; a program needn't handle non-finite values.
Results may differ from the reference program's by a relative error of at most 0.001.
Values are sent between devices in bfloat16 or wider.
A program may use at most 1 GiB of HBM per device.

```python
import math
import jax
import jax.numpy as jnp
from jax import lax

D = 768
FF = 3072
SEQ = 196
LAYERS = 2
BATCH_DEV = 4
DEVICES = 32
MICRO_STEPS = 2
BLOCKS = DEVICES * MICRO_STEPS
BATCH_ALL = BLOCKS * BATCH_DEV
BLOCK_ROWS = BATCH_DEV * SEQ
RHO_RADIUS = 0.1 * math.sqrt(LAYERS * (D + FF))
LEARN_RATE = 1.0
TOK_SCALE = 1.0 / (BATCH_ALL * SEQ * D)


def setup_inputs(seed: int = 0) -> dict:
    root_key = jax.random.key(seed)
    k_x, k_y, k_in, k_out, k_gain = jax.random.split(root_key, 5)
    x_act = jax.random.normal(k_x, (BATCH_ALL, SEQ, D), jnp.float32).astype(jnp.bfloat16)
    y_tgt = jax.random.normal(k_y, (BATCH_ALL, SEQ, D), jnp.float32).astype(jnp.bfloat16)
    w_in = jax.random.normal(k_in, (LAYERS, D, FF), jnp.float32) * (D ** -0.5)
    layer_gain = jax.random.uniform(k_gain, (LAYERS, 1, 1), jnp.float32, 0.3, 0.9)
    w_out = jax.random.normal(k_out, (LAYERS, FF, D), jnp.float32) * (FF ** -0.5) * layer_gain
    return {"x_act": x_act, "y_tgt": y_tgt, "w_in": w_in, "w_out": w_out}


def gelu_tanh(z_val):
    return jax.nn.gelu(z_val, approximate=True)


def forward_layer(h_act, wi_cast, wo_cast):
    z_pre = jnp.dot(h_act, wi_cast, preferred_element_type=jnp.float32).astype(jnp.bfloat16)
    gelu_out = gelu_tanh(z_pre.astype(jnp.float32)).astype(jnp.bfloat16)
    u_out = jnp.dot(gelu_out, wo_cast, preferred_element_type=jnp.float32)
    return (h_act.astype(jnp.float32) + u_out).astype(jnp.bfloat16), z_pre


def block_sums(x_blk, y_blk, wi_cast, wo_cast):
    h_list = [x_blk]
    z_list = []
    for layer_idx in range(LAYERS):
        h_next, z_pre = forward_layer(h_list[-1], wi_cast[layer_idx], wo_cast[layer_idx])
        h_list.append(h_next)
        z_list.append(z_pre)
    out_err = h_list[-1].astype(jnp.float32) - y_blk.astype(jnp.float32)
    sq_sum = jnp.sum(out_err * out_err)
    back_grad = out_err.astype(jnp.bfloat16)
    sums_in = [None] * LAYERS
    sums_out = [None] * LAYERS
    for layer_idx in range(LAYERS - 1, -1, -1):
        gelu_out, gelu_vjp = jax.vjp(gelu_tanh, z_list[layer_idx].astype(jnp.float32))
        sums_out[layer_idx] = jnp.dot(gelu_out.astype(jnp.bfloat16).T, back_grad, preferred_element_type=jnp.float32)
        d_act = jnp.dot(back_grad, wo_cast[layer_idx].T, preferred_element_type=jnp.float32)
        d_pre = gelu_vjp(d_act)[0].astype(jnp.bfloat16)
        sums_in[layer_idx] = jnp.dot(h_list[layer_idx].T, d_pre, preferred_element_type=jnp.float32)
        if layer_idx > 0:
            back_in = jnp.dot(d_pre, wi_cast[layer_idx].T, preferred_element_type=jnp.float32)
            back_grad = (back_grad.astype(jnp.float32) + back_in).astype(jnp.bfloat16)
    return jnp.stack(sums_in), jnp.stack(sums_out), sq_sum


def grad_sums(x_blocks, y_blocks, wi_cast, wo_cast):
    def scan_body(acc_state, block_pair):
        acc_in, acc_out, acc_sq = acc_state
        s_in, s_out, s_sq = block_sums(block_pair[0], block_pair[1], wi_cast, wo_cast)
        return (acc_in + s_in, acc_out + s_out, acc_sq + s_sq), None
    init_state = (jnp.zeros((LAYERS, D, FF), jnp.float32), jnp.zeros((LAYERS, FF, D), jnp.float32), jnp.zeros((), jnp.float32))
    final_state, _ = lax.scan(scan_body, init_state, (x_blocks, y_blocks))
    return final_state


def reference(x_act, y_tgt, w_in, w_out):
    x_blocks = x_act.reshape(BLOCKS, BLOCK_ROWS, D)
    y_blocks = y_tgt.reshape(BLOCKS, BLOCK_ROWS, D)
    sum_in, sum_out, _ = grad_sums(x_blocks, y_blocks, w_in.astype(jnp.bfloat16), w_out.astype(jnp.bfloat16))
    grad_in = sum_in * TOK_SCALE
    grad_out = sum_out * TOK_SCALE
    grad_norm = jnp.sqrt(jnp.sum(grad_in * grad_in) + jnp.sum(grad_out * grad_out))
    perturb_coef = RHO_RADIUS / grad_norm
    pert_in = (w_in + perturb_coef * grad_in).astype(jnp.bfloat16)
    pert_out = (w_out + perturb_coef * grad_out).astype(jnp.bfloat16)
    second_in, second_out, second_sq = grad_sums(x_blocks, y_blocks, pert_in, pert_out)
    new_in = w_in - LEARN_RATE * (second_in * TOK_SCALE)
    new_out = w_out - LEARN_RATE * (second_out * TOK_SCALE)
    pert_loss = 0.5 * (second_sq * TOK_SCALE)
    return new_in, new_out, pert_loss
```

```python
import math
import functools
import jax
import jax.numpy as jnp
from jax import lax
from jax.experimental import pallas as pl
from jax.experimental.pallas import tpu as pltpu
from jax.sharding import PartitionSpec as P

RHO_FRAC = 0.1
LEARN_RATE = 1.0
TILE_F = 256
MESH = pl.DeviceIdType.MESH
ANY = pl.BlockSpec(memory_space=pl.ANY)
NN = (((1,), (0,)), ((), ()))
NT = (((1,), (1,)), ((), ()))
GELU_C = math.sqrt(2.0 / math.pi)
GELU_K = 0.044715
VMEM_CAP = 67043328
CORE_SLOTS = 14
RS_LAG = (1, 4, 6, 9, 11)
AG_LAG = (13, 15, 17, 20, 22)
VG_LAG = (0, 2, 4, 6, 8)


def dot(lhs, rhs, dims=NN):
    return lax.dot_general(lhs, rhs, dims, preferred_element_type=jnp.float32)


def gelu_parts(z):
    sq = z * z
    th = jnp.tanh(GELU_C * (z + GELU_K * (sq * z)))
    cdf = 0.5 * (1.0 + th)
    return sq, th, cdf


def gelu(z):
    return z * gelu_parts(z)[2]


def gelu_and_grad(z):
    sq, th, cdf = gelu_parts(z)
    slope = cdf + (0.5 * z) * ((1.0 - th * th) * (GELU_C + (3.0 * GELU_K * GELU_C) * sq))
    return z * cdf, slope


def place(axis="data"):
    me = lax.axis_index(axis)
    bits = [lax.rem(lax.div(me, 1 << k), 2) for k in range(5)]
    peers = [me + (1 << k) * (1 - 2 * bits[k]) for k in range(5)]
    return bits, peers


def route(bits, peers, parity, rows):
    _, bx, by, ba, bb = bits
    _, px, py, pa, pb = peers
    b1 = jnp.where(parity == 0, bx, by)
    b3 = jnp.where(parity == 0, by, bx)
    p1 = jnp.where(parity == 0, px, py)
    p3 = jnp.where(parity == 0, py, px)
    keep, send, base = [0], [], 0
    n = rows
    for bit in (b1, ba, b3, bb):
        n //= 2
        keep.append(pl.multiple_of(base + bit * n, 8))
        send.append(pl.multiple_of(base + (1 - bit) * n, 8))
        base = base + bit * n
    return (p1, pa, p3, pb), keep, send


def enter(peers):
    barrier = pltpu.get_barrier_semaphore()
    for peer in peers:
        pl.semaphore_signal(barrier, inc=1, device_id=(peer,), device_id_type=MESH)
    pl.semaphore_wait(barrier, len(peers))


def remote(src, dst, send_sem, recv_sem, peer):
    return pltpu.make_async_remote_copy(src_ref=src, dst_ref=dst, send_sem=send_sem, recv_sem=recv_sem, device_id=(peer,), device_id_type=MESH)


def local(src, dst, sem):
    return pltpu.make_async_copy(src, dst, sem)


def halves(t):
    return [(0, t // 2), (t // 2, t // 2)] if t % 32 == 0 else [(0, t)]


def transpose_into(dst, src, t):
    full = t // 128
    if full:
        @pl.loop(0, full)
        def _(i):
            lo = pl.multiple_of(i * 128, 128)
            dst[:, pl.ds(lo, 128)] = src[pl.ds(lo, 128), :].T
    if t % 128:
        dst[:, full * 128:t] = src[full * 128:t, :].T


def fwd_unit(h_ref, vin_ref, vout_ref, acc_ref, z_ref, t):
    for lo, n in halves(t):
        z = dot(h_ref[lo:lo + n, :], vin_ref[...]).astype(jnp.bfloat16)
        z_ref[lo:lo + n, :] = z
        a = gelu(z.astype(jnp.float32)).astype(jnp.bfloat16)
        acc_ref[lo:lo + n, :] += dot(a, vout_ref[...], NT)


def fwd_close(h_ref, acc_ref, t):
    for lo, n in halves(t):
        h_ref[lo:lo + n, :] = acc_ref[lo:lo + n, :].astype(jnp.bfloat16)


def fwd_seed(h_ref, acc_ref, t):
    for lo, n in halves(t):
        acc_ref[lo:lo + n, :] = h_ref[lo:lo + n, :].astype(jnp.float32)


def first_forward(dm, x_hbm, y_hbm, wi_hbm, wo_hbm, z_out, v_out, ws_out, h_out, q_out,
                  h, yb, acc, wi, wo, vb, zb, ws, load_sem, z_sem, v_sem, io_sem):
    t, d, f, nf, nl = dm
    nu = nf * nl
    bits, peers = place()
    piece = d // 16

    def loads(u, slot):
        layer, tile = u // nf, u % nf
        lo = pl.multiple_of(tile * f, f)
        return (local(wi_hbm.at[layer, :, pl.ds(lo, f)], wi.at[slot], load_sem.at[slot, 0]),
                local(wo_hbm.at[layer, pl.ds(lo, f), :], wo.at[slot], load_sem.at[slot, 1]))

    def stores(u, slot):
        return local(zb.at[slot], z_out.at[u], z_sem.at[slot]), local(vb.at[slot], v_out.at[u], v_sem.at[slot])

    x_in = local(x_hbm, h, io_sem.at[0])
    y_in = local(y_hbm, yb, io_sem.at[1])
    x_in.start()
    for cp in loads(0, 0):
        cp.start()
    y_in.start()
    x_in.wait()
    fwd_seed(h, acc, t)

    @pl.loop(0, nu)
    def _(u):
        slot = lax.rem(u, 2)
        for cp in loads(u, slot):
            cp.wait()

        @pl.when(u + 1 < nu)
        def _():
            for cp in loads(u + 1, 1 - slot):
                cp.start()

        @pl.when(u >= 2)
        def _():
            for cp in stores(u - 2, slot):
                cp.wait()
        wot = wo[slot].T
        _, keep, _ = route(bits, peers, lax.rem(u, 2), d)
        rows = pl.ds(keep[4], piece)
        vb[slot, 0] = wi[slot].astype(jnp.bfloat16)
        vb[slot, 1] = wot.astype(jnp.bfloat16)

        @pl.when(bits[0] == 0)
        def _():
            ws[u] = wi[slot, rows, :]

        @pl.when(bits[0] == 1)
        def _():
            wi[slot] = wot
            ws[u] = wi[slot, rows, :]

        fwd_unit(h, vb.at[slot, 0], vb.at[slot, 1], acc, zb.at[slot], t)
        for cp in stores(u, slot):
            cp.start()

        @pl.when(u == nf - 1)
        def _():
            fwd_close(h, acc, t)
            fwd_seed(h, acc, t)
            out = local(h, h_out, io_sem.at[0])
            out.start()
            out.wait()

    y_in.wait()
    for lo, n in halves(t):
        hl = acc[lo:lo + n, :].astype(jnp.bfloat16).astype(jnp.float32)
        h[lo:lo + n, :] = (hl - yb[lo:lo + n, :].astype(jnp.float32)).astype(jnp.bfloat16)
    out = local(h, q_out, io_sem.at[0])
    out.start()
    ws_cp = local(ws, ws_out, io_sem.at[1])
    ws_cp.start()
    for u in (nu - 2, nu - 1):
        for cp in stores(u, u % 2):
            cp.wait()
    out.wait()
    ws_cp.wait()


def second_forward(dm, scale, rho, gs_hbm, ws_hbm, x_hbm, y_hbm, z_out, v_out, h_out, q_out, sq_out,
                   h, yb, acc, gs, ws, vb, zb, nb, send_sem, recv_sem, nsend_sem, nrecv_sem, z_sem, v_sem, io_sem):
    t, d, f, nf, nl = dm
    nu = nf * nl
    bits, peers = place()
    core = bits[0]
    piece = d // 16
    enter(peers)
    ins = (local(gs_hbm, gs, io_sem.at[0]), local(ws_hbm, ws, io_sem.at[1]), local(x_hbm, h, io_sem.at[2]), local(y_hbm, yb, io_sem.at[3]))
    for cp in ins:
        cp.start()
    ins[0].wait()

    def square(u, total):
        g = gs[u] * scale
        return total + jnp.sum((g * g).reshape(piece // 8, 8, f // 128, 128), axis=(0, 2))
    nb[0] = lax.fori_loop(0, nu, square, jnp.zeros((8, 128), jnp.float32))
    for k in range(5):
        cp = remote(nb.at[2 * k], nb.at[2 * k + 1], nsend_sem.at[k], nrecv_sem.at[k], peers[k])
        cp.start()
        cp.wait()
        nb[2 * k + 2] = nb[2 * k] + nb[2 * k + 1]
    coef = rho / jnp.sqrt(jnp.sum(nb[10], keepdims=True))
    ins[1].wait()

    def hop(u, k):
        ps, keep, _ = route(bits, peers, lax.rem(u, 2), d)
        if k == 4:
            ref = vb.at[u, core]
            return remote(ref, ref, send_sem.at[u, 4], recv_sem.at[u, 4], peers[0])
        n = piece << k
        ref = vb.at[u, core, pl.ds(pl.multiple_of(keep[4 - k], 16), n), :]
        return remote(ref, ref, send_sem.at[u, k], recv_sem.at[u, k], ps[3 - k])

    @pl.loop(0, nu)
    def _(u):
        _, keep, _ = route(bits, peers, lax.rem(u, 2), d)
        new = ws[u] + coef * (gs[u] * scale)
        vb[u, core, pl.ds(pl.multiple_of(keep[4], 16), piece), :] = new.astype(jnp.bfloat16)
        hop(u, 0).start()

    ins[2].wait()
    fwd_seed(h, acc, t)

    def z_store(u, slot):
        return local(zb.at[slot], z_out.at[u], z_sem.at[slot])

    @pl.loop(0, nu + VG_LAG[4])
    def _(it):
        for k in range(4):
            u = it - VG_LAG[k]

            @pl.when((u >= 0) & (u < nu))
            def _():
                hop(u, k).wait_recv()
                hop(u, k + 1).start()
        u = it - VG_LAG[4]

        @pl.when(u >= 0)
        def _():
            slot = lax.rem(u, 2)
            hop(u, 4).wait_recv()
            local(vb.at[u], v_out.at[u], v_sem.at[u]).start()

            @pl.when(u >= 2)
            def _():
                z_store(u - 2, slot).wait()
            fwd_unit(h, vb.at[u, 0], vb.at[u, 1], acc, zb.at[slot], t)
            z_store(u, slot).start()

            @pl.when(u == nf - 1)
            def _():
                fwd_close(h, acc, t)
                fwd_seed(h, acc, t)
                out = local(h, h_out, io_sem.at[0])
                out.start()
                out.wait()

    ins[3].wait()
    total = jnp.zeros((8, 128), jnp.float32)
    for lo, n in halves(t):
        hl = acc[lo:lo + n, :].astype(jnp.bfloat16).astype(jnp.float32)
        e = hl - yb[lo:lo + n, :].astype(jnp.float32)
        h[lo:lo + n, :] = e.astype(jnp.bfloat16)
        total = total + jnp.sum((e * e).reshape(n // 8, 8, d // 128, 128), axis=(0, 2))
    nb[0] = total
    out = local(h, q_out, io_sem.at[0])
    sq = local(nb.at[0], sq_out, io_sem.at[1])
    out.start()
    sq.start()

    @pl.loop(0, nu)
    def _(u):
        local(vb.at[u], v_out.at[u], v_sem.at[u]).wait()
        for k in range(5):
            hop(u, k).wait_send()
    z_store(nu - 2, nu % 2).wait()
    z_store(nu - 1, (nu - 1) % 2).wait()
    out.wait()
    sq.wait()


def backward(dm, scale, final, *refs):
    t, d, f, nf, nl = dm
    nu = nf * nl
    if final:
        (x_hbm, h_hbm, q_hbm, z_hbm, v_hbm, ws_hbm, sq_hbm, w_out, sq_out, *scr) = refs
    else:
        (x_hbm, h_hbm, q_hbm, z_hbm, v_hbm, g_out, *scr) = refs
    (q, tmp, tb, eb, acc, zb, vb, cbuf, obuf, sbuf, r1, r2, r3, r4, gs,
     load_sem, io_sem, csend_sem, send_sem, recv_sem, credit, *more) = scr
    if final:
        nb, ag_send, ag_recv, ag_loc, nsend_sem, nrecv_sem = more
    rbuf = (r1, r2, r3, r4)
    bits, peers = place()
    core = bits[0]
    piece = d // 16
    slots = cbuf.shape[0]
    enter(peers)

    def unit_of(it):
        return (nl - 1 - it // nf) * nf + lax.rem(it, nf)

    def loads(it, slot):
        u = unit_of(it)
        return local(z_hbm.at[u], zb.at[slot], load_sem.at[slot, 0]), local(v_hbm.at[u], vb.at[slot], load_sem.at[slot, 1])

    q_in = local(q_hbm, q, io_sem.at[0])
    h_in = local(h_hbm, tmp, io_sem.at[1])
    q_in.start()
    for cp in loads(0, 0):
        cp.start()
    h_in.start()
    if final:
        ws_in = local(ws_hbm, gs, io_sem.at[2])
        sq_in = local(sq_hbm, nb.at[0], io_sem.at[3])
        ws_in.start()
        sq_in.start()
        ws_in.wait()
        sq_in.wait()
    q_in.wait()
    fwd_seed(q, acc, t)
    transpose_into(tb.at[1], q, t)
    h_in.wait()
    transpose_into(tb.at[0], tmp, t)
    x_in = local(x_hbm, tmp, io_sem.at[1])
    x_in.start()

    def core_copy(it):
        slot = lax.rem(it, 2)
        return remote(sbuf.at[slot], cbuf.at[lax.rem(it, slots)], csend_sem.at[slot], recv_sem.at[0, it], peers[0])

    def rs_copy(it, k):
        ps, _, send = route(bits, peers, lax.rem(it, 2), d)
        n = d >> (k + 1)
        return remote(cbuf.at[lax.rem(it, slots), pl.ds(send[k], n), :], rbuf[k].at[it], send_sem.at[it, k], recv_sem.at[k + 1, it], ps[k])

    def ag_copy(it, k):
        ps, keep, _ = route(bits, peers, lax.rem(it, 2), d)
        u = unit_of(it)
        if k == 4:
            ref = w_out.at[u, core]
            return remote(ref, ref, ag_send.at[it, 4], ag_recv.at[it, 4], peers[0])
        n = piece << k
        ref = w_out.at[u, core, pl.ds(keep[4 - k], n), :]
        src = gs.at[u] if k == 0 else ref
        return remote(src, ref, ag_send.at[it, k], ag_recv.at[it, k], ps[3 - k])

    def ag_local(it):
        _, keep, _ = route(bits, peers, lax.rem(it, 2), d)
        u = unit_of(it)
        return local(gs.at[u], w_out.at[u, core, pl.ds(keep[4], piece), :], ag_loc.at[it])

    n_it = nu + (AG_LAG[4] if final else RS_LAG[4])

    @pl.loop(0, n_it)
    def _(it):
        @pl.when(it == nf)
        def _():
            fwd_close(q, acc, t)
            transpose_into(tb.at[1], q, t)
            x_in.wait()
            transpose_into(tb.at[0], tmp, t)

        @pl.when(it < nu)
        def _():
            slot = lax.rem(it, 2)
            for cp in loads(it, slot):
                cp.wait()

            @pl.when(it + 1 < nu)
            def _():
                for cp in loads(it + 1, 1 - slot):
                    cp.start()
            for lo, n in halves(t):
                back = dot(q[lo:lo + n, :], vb[slot, 1])
                a, slope = gelu_and_grad(zb[slot, lo:lo + n, :].astype(jnp.float32))
                eb[1, lo:lo + n, :] = a.astype(jnp.bfloat16)
                eb[0, lo:lo + n, :] = (back * slope).astype(jnp.bfloat16)

            @pl.when(it >= 2)
            def _():
                core_copy(it - 2).wait_send()
            other = 1 - core
            sbuf[slot] = dot(tb[other], eb[other])

            @pl.when(it >= slots)
            def _():
                pl.semaphore_wait(credit, 1)
            core_copy(it).start()
            obuf[slot] = dot(tb[core], eb[core])

            @pl.when(it < nf)
            def _():
                for lo, n in halves(t):
                    acc[lo:lo + n, :] += dot(eb[0, lo:lo + n, :], vb[slot, 0], NT)

        j0 = it - RS_LAG[0]

        @pl.when((j0 >= 0) & (j0 < nu))
        def _():
            cs = lax.rem(j0, slots)
            core_copy(j0).wait_recv()
            cbuf[cs] = cbuf[cs] + obuf[lax.rem(j0, 2)]
            rs_copy(j0, 0).start()

        for k in range(4):
            j = it - RS_LAG[k + 1]

            @pl.when((j >= 0) & (j < nu))
            def _():
                cs = lax.rem(j, slots)
                _, keep, _ = route(bits, peers, lax.rem(j, 2), d)
                n = d >> (k + 1)
                rows = pl.ds(keep[k + 1], n)
                rs_copy(j, k).wait_recv()
                if k < 3:
                    cbuf[cs, rows, :] = cbuf[cs, rows, :] + rbuf[k][j]
                    rs_copy(j, k + 1).start()
                else:
                    total = cbuf[cs, rows, :] + rbuf[k][j]
                    u = unit_of(j)
                    gs[u] = gs[u] - LEARN_RATE * (total * scale) if final else total
                    for kk in range(4):
                        rs_copy(j, kk).wait_send()

                    @pl.when(j + slots < nu)
                    def _():
                        pl.semaphore_signal(credit, inc=1, device_id=(peers[0],), device_id_type=MESH)
                    if final:
                        ag_local(j).start()
                        ag_copy(j, 0).start()
        if final:
            for k in range(4):
                j = it - AG_LAG[k]

                @pl.when((j >= 0) & (j < nu))
                def _():
                    ag_copy(j, k).wait_recv()
                    if k == 0:
                        ag_local(j).wait()
                    ag_copy(j, k + 1).start()

            @pl.when(it < 5)
            def _():
                for k in range(5):
                    @pl.when(it == k)
                    def _():
                        cp = remote(nb.at[2 * k], nb.at[2 * k + 1], nsend_sem.at[k], nrecv_sem.at[k], peers[k])
                        cp.start()
                        cp.wait()
                        nb[2 * k + 2] = nb[2 * k] + nb[2 * k + 1]

    core_copy(nu - 2).wait_send()
    core_copy(nu - 1).wait_send()
    if final:
        sq_cp = local(nb.at[10], sq_out, io_sem.at[3])
        sq_cp.start()

        @pl.loop(0, nu)
        def _(it):
            ag_copy(it, 4).wait_recv()
            for k in range(5):
                ag_copy(it, k).wait_send()
        sq_cp.wait()
    else:
        g_cp = local(gs, g_out, io_sem.at[0])
        g_cp.start()
        g_cp.wait()


def sds(shape, dtype):
    return jax.ShapeDtypeStruct(shape, dtype)


def call(kernel, n_in, outs, scratch, name, collective_id=None):
    params = dict(vmem_limit_bytes=VMEM_CAP)
    if collective_id is not None:
        params.update(collective_id=collective_id, has_side_effects=True)
    return pl.pallas_call(
        kernel,
        out_shape=outs,
        in_specs=[ANY] * n_in,
        out_specs=[ANY] * len(outs),
        scratch_shapes=scratch,
        compiler_params=pltpu.CompilerParams(**params),
        name=name,
    )


def local_step(n_dev, tile_f, x_loc, y_loc, w_in, w_out):
    nl, d, ff = w_in.shape
    f = tile_f
    nf = ff // f
    nu = nl * nf
    t = x_loc.shape[0] * x_loc.shape[1]
    piece = d // 16
    dm = (t, d, f, nf, nl)
    scale = 1.0 / (t * n_dev * d)
    rho = RHO_FRAC * math.sqrt(nl * (d + ff))
    bf, f32 = jnp.bfloat16, jnp.float32
    V, DMA = pltpu.VMEM, pltpu.SemaphoreType.DMA
    x = x_loc.reshape(t, d)
    y = y_loc.reshape(t, d)
    z_s, v_s, w_s, a_s = sds((nu, t, f), bf), sds((nu, 2, d, f), bf), sds((nu, piece, f), f32), sds((t, d), bf)

    z, v, ws, h1, q = call(
        functools.partial(first_forward, dm), 4, [z_s, v_s, w_s, a_s, a_s],
        [V((t, d), bf), V((t, d), bf), V((t, d), f32), V((2, d, f), f32), V((2, f, d), f32), V((2, 2, d, f), bf), V((2, t, f), bf), V((nu, piece, f), f32),
         DMA((2, 2)), DMA((2,)), DMA((2,)), DMA((2,))], "fwd_a")(x, y, w_in, w_out)

    slots = min(CORE_SLOTS, nu)
    bwd_scratch = [
        V((t, d), bf), V((t, d), bf), V((2, d, t), bf), V((2, t, f), bf), V((t, d), f32), V((2, t, f), bf), V((2, 2, d, f), bf),
        V((slots, d, f), f32), V((2, d, f), f32), V((2, d, f), f32),
        V((nu, d // 2, f), f32), V((nu, d // 4, f), f32), V((nu, d // 8, f), f32), V((nu, d // 16, f), f32), V((nu, piece, f), f32),
        DMA((2, 2)), DMA((4,)), DMA((2,)), DMA((nu, 4)), DMA((5, nu)), pltpu.SemaphoreType.REGULAR]
    (g,) = call(functools.partial(backward, dm, scale, False), 5, [w_s], bwd_scratch, "bwd_a", 0)(x, h1, q, z, v)

    z, v, h1, q, sq = call(
        functools.partial(second_forward, dm, scale, rho), 4, [z_s, v_s, a_s, a_s, sds((8, 128), f32)],
        [V((t, d), bf), V((t, d), bf), V((t, d), f32), V((nu, piece, f), f32), V((nu, piece, f), f32), V((nu, 2, d, f), bf), V((2, t, f), bf), V((11, 8, 128), f32),
         DMA((nu, 5)), DMA((nu, 5)), DMA((5,)), DMA((5,)), DMA((2,)), DMA((nu,)), DMA((4,))], "fwd_b", 1)(g, ws, x, y)

    w_new, sq = call(
        functools.partial(backward, dm, scale, True), 7, [sds((nu, 2, d, f), f32), sds((8, 128), f32)],
        bwd_scratch + [V((11, 8, 128), f32), DMA((nu, 5)), DMA((nu, 5)), DMA((nu,)), DMA((5,)), DMA((5,))], "bwd_b", 2)(x, h1, q, z, v, ws, sq)

    w_new = w_new.reshape(nl, nf, 2, d, f)
    new_in = w_new[:, :, 0].transpose(0, 2, 1, 3).reshape(nl, d, ff)
    new_out = w_new[:, :, 1].transpose(0, 1, 3, 2).reshape(nl, ff, d)
    loss = 0.5 * (jnp.sum(sq) * scale)
    return new_in, new_out, loss


def solution(mesh):
    step = functools.partial(local_step, mesh.shape["data"], TILE_F)
    return jax.shard_map(step, mesh=mesh, in_specs=(P("data"), P("data"), P(), P()), out_specs=(P(), P(), P()), check_vma=False)
```

```python
import math
import functools
import jax
import jax.numpy as jnp
from jax import lax
from jax.experimental import pallas as pl
from jax.experimental.pallas import tpu as pltpu
from jax.sharding import PartitionSpec as P

RHO_FRAC = 0.1
LEARN_RATE = 1.0
TILE_F = 256
MESH = pl.DeviceIdType.MESH
ANY = pl.BlockSpec(memory_space=pl.ANY)
NN = (((1,), (0,)), ((), ()))
NT = (((1,), (1,)), ((), ()))
GELU_C = math.sqrt(2.0 / math.pi)
GELU_K = 0.044715
VMEM_CAP = 67043328
CORE_SLOTS = 14
RS_LAG = (1, 4, 6, 9, 11)
AG_LAG = (13, 15, 17, 20, 22)
VG_LAG = (0, 2, 4, 6, 9, 10)


def dot(lhs, rhs, dims=NN):
    return lax.dot_general(lhs, rhs, dims, preferred_element_type=jnp.float32)


def gelu_parts(z):
    sq = z * z
    th = jnp.tanh(GELU_C * (z + GELU_K * (sq * z)))
    cdf = 0.5 * (1.0 + th)
    return sq, th, cdf


def gelu(z):
    return z * gelu_parts(z)[2]


def gelu_and_grad(z):
    sq, th, cdf = gelu_parts(z)
    slope = cdf + (0.5 * z) * ((1.0 - th * th) * (GELU_C + (3.0 * GELU_K * GELU_C) * sq))
    return z * cdf, slope


def place(axis="data"):
    me = lax.axis_index(axis)
    bits = [lax.rem(lax.div(me, 1 << k), 2) for k in range(5)]
    peers = [me + (1 << k) * (1 - 2 * bits[k]) for k in range(5)]
    return bits, peers


def route(bits, peers, parity, rows):
    _, bx, by, ba, bb = bits
    _, px, py, pa, pb = peers
    b1 = jnp.where(parity == 0, bx, by)
    b3 = jnp.where(parity == 0, by, bx)
    p1 = jnp.where(parity == 0, px, py)
    p3 = jnp.where(parity == 0, py, px)
    keep, send, base = [0], [], 0
    n = rows
    for bit in (b1, ba, b3, bb):
        n //= 2
        keep.append(pl.multiple_of(base + bit * n, 8))
        send.append(pl.multiple_of(base + (1 - bit) * n, 8))
        base = base + bit * n
    return (p1, pa, p3, pb), keep, send


def enter(peers):
    barrier = pltpu.get_barrier_semaphore()
    for peer in peers:
        pl.semaphore_signal(barrier, inc=1, device_id=(peer,), device_id_type=MESH)
    pl.semaphore_wait(barrier, len(peers))


def remote(src, dst, send_sem, recv_sem, peer):
    return pltpu.make_async_remote_copy(src_ref=src, dst_ref=dst, send_sem=send_sem, recv_sem=recv_sem, device_id=(peer,), device_id_type=MESH)


def local(src, dst, sem):
    return pltpu.make_async_copy(src, dst, sem)


def halves(t):
    return [(0, t // 2), (t // 2, t // 2)] if t % 32 == 0 else [(0, t)]


def transpose_into(dst, src, t):
    full = t // 128
    if full:
        @pl.loop(0, full)
        def _(i):
            lo = pl.multiple_of(i * 128, 128)
            dst[:, pl.ds(lo, 128)] = src[pl.ds(lo, 128), :].T
    if t % 128:
        dst[:, full * 128:t] = src[full * 128:t, :].T


def fwd_pair(h_ref, v_ref, acc_ref, a_ref, z_ref, t, f):
    for lo, n in halves(t):
        for j in range(2):
            z = dot(h_ref[lo:lo + n, :], v_ref[j, 0]).astype(jnp.bfloat16)
            z_ref[j, lo:lo + n, :] = z
            a_ref[lo:lo + n, j * f:(j + 1) * f] = gelu(z.astype(jnp.float32)).astype(jnp.bfloat16)
    v_out = jnp.concatenate([v_ref[0, 1], v_ref[1, 1]], axis=1)
    for lo, n in halves(t):
        acc_ref[lo:lo + n, :] += dot(a_ref[lo:lo + n, :], v_out, NT)


def fwd_close(h_ref, acc_ref, t):
    for lo, n in halves(t):
        h_ref[lo:lo + n, :] = acc_ref[lo:lo + n, :].astype(jnp.bfloat16)


def fwd_seed(h_ref, acc_ref, t):
    for lo, n in halves(t):
        acc_ref[lo:lo + n, :] = h_ref[lo:lo + n, :].astype(jnp.float32)


def first_forward(dm, x_hbm, y_hbm, wi_hbm, wo_hbm, z_out, v_out, ws_out, h_out, q_out,
                  h, yb, acc, ab, wi, wo, vb, zb, ws, load_sem, z_sem, v_sem, io_sem):
    t, d, f, nf, nl = dm
    nu = nf * nl
    bits, peers = place()
    piece = d // 16

    def loads(p, slot):
        layer, tile = p // (nf // 2), lax.rem(p, nf // 2)
        lo = pl.multiple_of(tile * 2 * f, 2 * f)
        return (local(wi_hbm.at[layer, :, pl.ds(lo, 2 * f)], wi.at[slot], load_sem.at[slot, 0]),
                local(wo_hbm.at[layer, pl.ds(lo, 2 * f), :], wo.at[slot], load_sem.at[slot, 1]))

    def stores(p, slot):
        two = pl.ds(2 * p, 2)
        return local(zb.at[slot], z_out.at[two], z_sem.at[slot]), local(vb.at[slot], v_out.at[two], v_sem.at[slot])

    x_in = local(x_hbm, h, io_sem.at[0])
    y_in = local(y_hbm, yb, io_sem.at[1])
    x_in.start()
    for cp in loads(0, 0):
        cp.start()
    y_in.start()
    x_in.wait()
    fwd_seed(h, acc, t)

    @pl.loop(0, nu // 2)
    def _(p):
        slot = lax.rem(p, 2)
        for cp in loads(p, slot):
            cp.wait()

        @pl.when(p + 1 < nu // 2)
        def _():
            for cp in loads(p + 1, 1 - slot):
                cp.start()

        @pl.when(p >= 2)
        def _():
            for cp in stores(p - 2, slot):
                cp.wait()
        for j in range(2):
            cols = slice(j * f, (j + 1) * f)
            wot = wo[slot, cols, :].T
            _, keep, _ = route(bits, peers, j, d)
            rows = pl.ds(keep[4], piece)
            vb[slot, j, 0] = wi[slot, :, cols].astype(jnp.bfloat16)
            vb[slot, j, 1] = wot.astype(jnp.bfloat16)

            @pl.when(bits[0] == 0)
            def _():
                ws[2 * p + j] = wi[slot, rows, cols]

            @pl.when(bits[0] == 1)
            def _():
                wi[slot, :, cols] = wot
                ws[2 * p + j] = wi[slot, rows, cols]

        fwd_pair(h, vb.at[slot], acc, ab, zb.at[slot], t, f)
        for cp in stores(p, slot):
            cp.start()

        @pl.when(p == nf // 2 - 1)
        def _():
            fwd_close(h, acc, t)
            fwd_seed(h, acc, t)
            out = local(h, h_out, io_sem.at[0])
            out.start()
            out.wait()

    y_in.wait()
    for lo, n in halves(t):
        hl = acc[lo:lo + n, :].astype(jnp.bfloat16).astype(jnp.float32)
        h[lo:lo + n, :] = (hl - yb[lo:lo + n, :].astype(jnp.float32)).astype(jnp.bfloat16)
    out = local(h, q_out, io_sem.at[0])
    out.start()
    ws_cp = local(ws, ws_out, io_sem.at[1])
    ws_cp.start()
    for p in range(max(nu // 2 - 2, 0), nu // 2):
        for cp in stores(p, p % 2):
            cp.wait()
    out.wait()
    ws_cp.wait()


def second_forward(dm, scale, rho, gs_hbm, ws_hbm, x_hbm, y_hbm, z_out, v_out, h_out, q_out, sq_out,
                   h, yb, acc, ab, gs, ws, vb, zb, nb, send_sem, recv_sem, nsend_sem, nrecv_sem, z_sem, v_sem, io_sem):
    t, d, f, nf, nl = dm
    nu = nf * nl
    bits, peers = place()
    core = bits[0]
    piece = d // 16
    enter(peers)
    ins = (local(gs_hbm, gs, io_sem.at[0]), local(ws_hbm, ws, io_sem.at[1]), local(x_hbm, h, io_sem.at[2]), local(y_hbm, yb, io_sem.at[3]))
    for cp in ins:
        cp.start()
    ins[0].wait()

    def square(u, total):
        g = gs[u] * scale
        return total + jnp.sum((g * g).reshape(piece // 8, 8, f // 128, 128), axis=(0, 2))
    nb[0] = lax.fori_loop(0, nu, square, jnp.zeros((8, 128), jnp.float32))
    for k in range(5):
        cp = remote(nb.at[2 * k], nb.at[2 * k + 1], nsend_sem.at[k], nrecv_sem.at[k], peers[k])
        cp.start()
        cp.wait()
        nb[2 * k + 2] = nb[2 * k] + nb[2 * k + 1]
    coef = rho / jnp.sqrt(jnp.sum(nb[10], keepdims=True))
    ins[1].wait()

    def hop(u, k):
        ps, keep, _ = route(bits, peers, lax.rem(u, 2), d)
        if k == 4:
            ref = vb.at[u, core]
            return remote(ref, ref, send_sem.at[u, 4], recv_sem.at[u, 4], peers[0])
        n = piece << k
        ref = vb.at[u, core, pl.ds(pl.multiple_of(keep[4 - k], 16), n), :]
        return remote(ref, ref, send_sem.at[u, k], recv_sem.at[u, k], ps[3 - k])

    ins[2].wait()
    fwd_seed(h, acc, t)

    def z_store(p, slot):
        return local(zb.at[slot], z_out.at[pl.ds(2 * p, 2)], z_sem.at[slot])

    @pl.loop(0, nu + VG_LAG[5])
    def _(it):
        @pl.when(it < nu)
        def _():
            _, keep, _ = route(bits, peers, lax.rem(it, 2), d)
            new = ws[it] + coef * (gs[it] * scale)
            vb[it, core, pl.ds(pl.multiple_of(keep[4], 16), piece), :] = new.astype(jnp.bfloat16)
            hop(it, 0).start()
        for k in range(1, 5):
            u = it - VG_LAG[k]

            @pl.when((u >= 0) & (u < nu))
            def _():
                hop(u, k - 1).wait_recv()
                hop(u, k).start()
        u = it - VG_LAG[5]

        @pl.when(u >= 0)
        def _():
            hop(u, 4).wait_recv()
            local(vb.at[u], v_out.at[u], v_sem.at[u]).start()

        @pl.when((u >= 0) & (lax.rem(u, 2) == 1))
        def _():
            p = u // 2
            slot = lax.rem(p, 2)

            @pl.when(p >= 2)
            def _():
                z_store(p - 2, slot).wait()
            fwd_pair(h, vb.at[pl.ds(2 * p, 2)], acc, ab, zb.at[slot], t, f)
            z_store(p, slot).start()

            @pl.when(p == nf // 2 - 1)
            def _():
                fwd_close(h, acc, t)
                fwd_seed(h, acc, t)
                out = local(h, h_out, io_sem.at[0])
                out.start()
                out.wait()

    ins[3].wait()
    total = jnp.zeros((8, 128), jnp.float32)
    for lo, n in halves(t):
        hl = acc[lo:lo + n, :].astype(jnp.bfloat16).astype(jnp.float32)
        e = hl - yb[lo:lo + n, :].astype(jnp.float32)
        h[lo:lo + n, :] = e.astype(jnp.bfloat16)
        total = total + jnp.sum((e * e).reshape(n // 8, 8, d // 128, 128), axis=(0, 2))
    nb[0] = total
    out = local(h, q_out, io_sem.at[0])
    sq = local(nb.at[0], sq_out, io_sem.at[1])
    out.start()
    sq.start()

    @pl.loop(0, nu)
    def _(u):
        local(vb.at[u], v_out.at[u], v_sem.at[u]).wait()
        for k in range(5):
            hop(u, k).wait_send()
    for p in range(max(nu // 2 - 2, 0), nu // 2):
        z_store(p, p % 2).wait()
    out.wait()
    sq.wait()


def backward(dm, scale, final, *refs):
    t, d, f, nf, nl = dm
    nu = nf * nl
    if final:
        (x_hbm, h_hbm, q_hbm, z_hbm, v_hbm, ws_hbm, sq_hbm, w_out, sq_out, *scr) = refs
    else:
        (x_hbm, h_hbm, q_hbm, z_hbm, v_hbm, g_out, *scr) = refs
    (q, tmp, tb, eb, acc, zb, vb, cbuf, obuf, sbuf, r1, r2, r3, r4, gs,
     load_sem, io_sem, csend_sem, send_sem, recv_sem, credit, *more) = scr
    if final:
        nb, ag_send, ag_recv, ag_loc, nsend_sem, nrecv_sem = more
    rbuf = (r1, r2, r3, r4)
    bits, peers = place()
    core = bits[0]
    piece = d // 16
    slots = cbuf.shape[0]
    enter(peers)

    def unit_of(it):
        return (nl - 1 - it // nf) * nf + lax.rem(it, nf)

    def loads(it, slot):
        u = unit_of(it)
        return local(z_hbm.at[u], zb.at[slot], load_sem.at[slot, 0]), local(v_hbm.at[u], vb.at[slot], load_sem.at[slot, 1])

    q_in = local(q_hbm, q, io_sem.at[0])
    h_in = local(h_hbm, tmp, io_sem.at[1])
    q_in.start()
    for cp in loads(0, 0):
        cp.start()
    h_in.start()
    if final:
        ws_in = local(ws_hbm, gs, io_sem.at[2])
        sq_in = local(sq_hbm, nb.at[0], io_sem.at[3])
        ws_in.start()
        sq_in.start()
        ws_in.wait()
        sq_in.wait()
    q_in.wait()
    fwd_seed(q, acc, t)
    transpose_into(tb.at[1], q, t)
    h_in.wait()
    transpose_into(tb.at[0], tmp, t)
    x_in = local(x_hbm, tmp, io_sem.at[1])
    x_in.start()

    def core_copy(it):
        slot = lax.rem(it, 2)
        return remote(sbuf.at[slot], cbuf.at[lax.rem(it, slots)], csend_sem.at[slot], recv_sem.at[0, it], peers[0])

    def rs_copy(it, k):
        ps, _, send = route(bits, peers, lax.rem(it, 2), d)
        n = d >> (k + 1)
        return remote(cbuf.at[lax.rem(it, slots), pl.ds(send[k], n), :], rbuf[k].at[it], send_sem.at[it, k], recv_sem.at[k + 1, it], ps[k])

    def ag_copy(it, k):
        ps, keep, _ = route(bits, peers, lax.rem(it, 2), d)
        u = unit_of(it)
        if k == 4:
            ref = w_out.at[u, core]
            return remote(ref, ref, ag_send.at[it, 4], ag_recv.at[it, 4], peers[0])
        n = piece << k
        ref = w_out.at[u, core, pl.ds(keep[4 - k], n), :]
        src = gs.at[u] if k == 0 else ref
        return remote(src, ref, ag_send.at[it, k], ag_recv.at[it, k], ps[3 - k])

    def ag_local(it):
        _, keep, _ = route(bits, peers, lax.rem(it, 2), d)
        u = unit_of(it)
        return local(gs.at[u], w_out.at[u, core, pl.ds(keep[4], piece), :], ag_loc.at[it])

    n_it = nu + (AG_LAG[4] if final else RS_LAG[4])

    @pl.loop(0, n_it)
    def _(it):
        @pl.when(it == nf)
        def _():
            fwd_close(q, acc, t)
            transpose_into(tb.at[1], q, t)
            x_in.wait()
            transpose_into(tb.at[0], tmp, t)

        @pl.when(it < nu)
        def _():
            slot = lax.rem(it, 2)
            for cp in loads(it, slot):
                cp.wait()

            @pl.when(it + 1 < nu)
            def _():
                for cp in loads(it + 1, 1 - slot):
                    cp.start()
            for lo, n in halves(t):
                back = dot(q[lo:lo + n, :], vb[slot, 1])
                a, slope = gelu_and_grad(zb[slot, lo:lo + n, :].astype(jnp.float32))
                eb[1, lo:lo + n, :] = a.astype(jnp.bfloat16)
                eb[0, lo:lo + n, :] = (back * slope).astype(jnp.bfloat16)

            @pl.when(it >= 2)
            def _():
                core_copy(it - 2).wait_send()
            other = 1 - core
            sbuf[slot] = dot(tb[other], eb[other])

            @pl.when(it >= slots)
            def _():
                pl.semaphore_wait(credit, 1)
            core_copy(it).start()
            obuf[slot] = dot(tb[core], eb[core])

            @pl.when(it < nf)
            def _():
                for lo, n in halves(t):
                    acc[lo:lo + n, :] += dot(eb[0, lo:lo + n, :], vb[slot, 0], NT)

        j0 = it - RS_LAG[0]

        @pl.when((j0 >= 0) & (j0 < nu))
        def _():
            cs = lax.rem(j0, slots)
            core_copy(j0).wait_recv()
            cbuf[cs] = cbuf[cs] + obuf[lax.rem(j0, 2)]
            rs_copy(j0, 0).start()

        for k in range(4):
            j = it - RS_LAG[k + 1]

            @pl.when((j >= 0) & (j < nu))
            def _():
                cs = lax.rem(j, slots)
                _, keep, _ = route(bits, peers, lax.rem(j, 2), d)
                n = d >> (k + 1)
                rows = pl.ds(keep[k + 1], n)
                rs_copy(j, k).wait_recv()
                if k < 3:
                    cbuf[cs, rows, :] = cbuf[cs, rows, :] + rbuf[k][j]
                    rs_copy(j, k + 1).start()
                else:
                    total = cbuf[cs, rows, :] + rbuf[k][j]
                    u = unit_of(j)
                    gs[u] = gs[u] - LEARN_RATE * (total * scale) if final else total
                    for kk in range(4):
                        rs_copy(j, kk).wait_send()

                    @pl.when(j + slots < nu)
                    def _():
                        pl.semaphore_signal(credit, inc=1, device_id=(peers[0],), device_id_type=MESH)
                    if final:
                        ag_local(j).start()
                        ag_copy(j, 0).start()
        if final:
            for k in range(4):
                j = it - AG_LAG[k]

                @pl.when((j >= 0) & (j < nu))
                def _():
                    ag_copy(j, k).wait_recv()
                    if k == 0:
                        ag_local(j).wait()
                    ag_copy(j, k + 1).start()

            @pl.when(it < 5)
            def _():
                for k in range(5):
                    @pl.when(it == k)
                    def _():
                        cp = remote(nb.at[2 * k], nb.at[2 * k + 1], nsend_sem.at[k], nrecv_sem.at[k], peers[k])
                        cp.start()
                        cp.wait()
                        nb[2 * k + 2] = nb[2 * k] + nb[2 * k + 1]

    core_copy(nu - 2).wait_send()
    core_copy(nu - 1).wait_send()
    if final:
        sq_cp = local(nb.at[10], sq_out, io_sem.at[3])
        sq_cp.start()

        @pl.loop(0, nu)
        def _(it):
            ag_copy(it, 4).wait_recv()
            for k in range(5):
                ag_copy(it, k).wait_send()
        sq_cp.wait()
    else:
        g_cp = local(gs, g_out, io_sem.at[0])
        g_cp.start()
        g_cp.wait()


def finish(scale, f, w_ref, sq_ref, in_ref, out_ref, loss_ref):
    for j in range(2):
        in_ref[0, :, j * f:(j + 1) * f] = w_ref[j, 0]
        out_ref[0, j * f:(j + 1) * f, :] = w_ref[j, 1].T
    loss_ref[0, 0] = 0.5 * (jnp.sum(sq_ref[...]) * scale)


def sds(shape, dtype):
    return jax.ShapeDtypeStruct(shape, dtype)


def call(kernel, n_in, outs, scratch, name, collective_id=None):
    params = dict(vmem_limit_bytes=VMEM_CAP)
    if collective_id is not None:
        params.update(collective_id=collective_id, has_side_effects=True)
    return pl.pallas_call(
        kernel,
        out_shape=outs,
        in_specs=[ANY] * n_in,
        out_specs=[ANY] * len(outs),
        scratch_shapes=scratch,
        compiler_params=pltpu.CompilerParams(**params),
        name=name,
    )


def local_step(n_dev, tile_f, x_loc, y_loc, w_in, w_out):
    nl, d, ff = w_in.shape
    f = tile_f
    nf = ff // f
    nu = nl * nf
    t = x_loc.shape[0] * x_loc.shape[1]
    piece = d // 16
    dm = (t, d, f, nf, nl)
    scale = 1.0 / (t * n_dev * d)
    rho = RHO_FRAC * math.sqrt(nl * (d + ff))
    bf, f32 = jnp.bfloat16, jnp.float32
    V, DMA = pltpu.VMEM, pltpu.SemaphoreType.DMA
    x = x_loc.transpose(1, 0, 2).reshape(t, d)
    y = y_loc.transpose(1, 0, 2).reshape(t, d)
    z_s, v_s, w_s, a_s = sds((nu, t, f), bf), sds((nu, 2, d, f), bf), sds((nu, piece, f), f32), sds((t, d), bf)

    z, v, ws, h1, q = call(
        functools.partial(first_forward, dm), 4, [z_s, v_s, w_s, a_s, a_s],
        [V((t, d), bf), V((t, d), bf), V((t, d), f32), V((t, 2 * f), bf), V((2, d, 2 * f), f32), V((2, 2 * f, d), f32), V((2, 2, 2, d, f), bf), V((2, 2, t, f), bf),
         V((nu, piece, f), f32),
         DMA((2, 2)), DMA((2,)), DMA((2,)), DMA((2,))], "fwd_a")(x, y, w_in, w_out)

    slots = min(CORE_SLOTS, nu)
    bwd_scratch = [
        V((t, d), bf), V((t, d), bf), V((2, d, t), bf), V((2, t, f), bf), V((t, d), f32), V((2, t, f), bf), V((2, 2, d, f), bf),
        V((slots, d, f), f32), V((2, d, f), f32), V((2, d, f), f32),
        V((nu, d // 2, f), f32), V((nu, d // 4, f), f32), V((nu, d // 8, f), f32), V((nu, d // 16, f), f32), V((nu, piece, f), f32),
        DMA((2, 2)), DMA((4,)), DMA((2,)), DMA((nu, 4)), DMA((5, nu)), pltpu.SemaphoreType.REGULAR]
    (g,) = call(functools.partial(backward, dm, scale, False), 5, [w_s], bwd_scratch, "bwd_a", 0)(x, h1, q, z, v)

    z, v, h1, q, sq = call(
        functools.partial(second_forward, dm, scale, rho), 4, [z_s, v_s, a_s, a_s, sds((8, 128), f32)],
        [V((t, d), bf), V((t, d), bf), V((t, d), f32), V((t, 2 * f), bf), V((nu, piece, f), f32), V((nu, piece, f), f32), V((nu, 2, d, f), bf), V((2, 2, t, f), bf),
         V((11, 8, 128), f32),
         DMA((nu, 5)), DMA((nu, 5)), DMA((5,)), DMA((5,)), DMA((2,)), DMA((nu,)), DMA((4,))], "fwd_b", 1)(g, ws, x, y)

    w_new, sq = call(
        functools.partial(backward, dm, scale, True), 7, [sds((nu, 2, d, f), f32), sds((8, 128), f32)],
        bwd_scratch + [V((11, 8, 128), f32), DMA((nu, 5)), DMA((nu, 5)), DMA((nu,)), DMA((5,)), DMA((5,))], "bwd_b", 2)(x, h1, q, z, v, ws, sq)

    new_in, new_out, loss = pl.pallas_call(
        functools.partial(finish, scale, f),
        grid=(nl, nf // 2),
        in_specs=[pl.BlockSpec((2, 2, d, f), lambda i, j: (i * (nf // 2) + j, 0, 0, 0)), pl.BlockSpec((8, 128), lambda i, j: (0, 0))],
        out_specs=[pl.BlockSpec((1, d, 2 * f), lambda i, j: (i, 0, j)), pl.BlockSpec((1, 2 * f, d), lambda i, j: (i, j, 0)),
                   pl.BlockSpec((1, 1), lambda i, j: (0, 0), memory_space=pltpu.SMEM)],
        out_shape=[sds((nl, d, ff), f32), sds((nl, ff, d), f32), sds((1, 1), f32)],
        compiler_params=pltpu.CompilerParams(vmem_limit_bytes=VMEM_CAP),
        name="finish")(w_new, sq)
    return new_in, new_out, loss.reshape(())


def solution(mesh):
    step = functools.partial(local_step, mesh.shape["data"], TILE_F)
    return jax.shard_map(step, mesh=mesh, in_specs=(P("data"), P("data"), P(), P()), out_specs=(P(), P(), P()), check_vma=False)
```

```python
import math
import functools
import jax
import jax.numpy as jnp
from jax import lax
from jax.experimental import pallas as pl
from jax.experimental.pallas import tpu as pltpu
from jax.sharding import PartitionSpec as P

RHO_FRAC = 0.1
LEARN_RATE = 1.0
TILE_F = 256
MESH = pl.DeviceIdType.MESH
ANY = pl.BlockSpec(memory_space=pl.ANY)
NN = (((1,), (0,)), ((), ()))
NT = (((1,), (1,)), ((), ()))
GELU_C = math.sqrt(2.0 / math.pi)
GELU_K = 0.044715
VMEM_CAP = 67043328
CORE_SLOTS = 14
RS_LAG = (1, 4, 6, 9, 11)
AG_LAG = (13, 15, 17, 20, 22)
VG_LAG = (0, 2, 4, 6, 9, 10)


def dot(lhs, rhs, dims=NN):
    return lax.dot_general(lhs, rhs, dims, preferred_element_type=jnp.float32)


def gelu_parts(z):
    sq = z * z
    th = jnp.tanh(GELU_C * (z + GELU_K * (sq * z)))
    cdf = 0.5 * (1.0 + th)
    return sq, th, cdf


def gelu(z):
    return z * gelu_parts(z)[2]


def gelu_and_grad(z):
    sq, th, cdf = gelu_parts(z)
    slope = cdf + (0.5 * z) * ((1.0 - th * th) * (GELU_C + (3.0 * GELU_K * GELU_C) * sq))
    return z * cdf, slope


def place(axis="data"):
    me = lax.axis_index(axis)
    bits = [lax.rem(lax.div(me, 1 << k), 2) for k in range(5)]
    peers = [me + (1 << k) * (1 - 2 * bits[k]) for k in range(5)]
    return bits, peers


def route(bits, peers, unit, rows):
    core, bx, by, ba, bb = bits
    parity = lax.rem(unit + core, 2)
    _, px, py, pa, pb = peers
    b1 = jnp.where(parity == 0, bx, by)
    b3 = jnp.where(parity == 0, by, bx)
    p1 = jnp.where(parity == 0, px, py)
    p3 = jnp.where(parity == 0, py, px)
    keep, send, base = [0], [], 0
    n = rows
    for bit in (b1, ba, b3, bb):
        n //= 2
        keep.append(pl.multiple_of(base + bit * n, 8))
        send.append(pl.multiple_of(base + (1 - bit) * n, 8))
        base = base + bit * n
    return (p1, pa, p3, pb), keep, send


def enter(peers):
    barrier = pltpu.get_barrier_semaphore()
    for peer in peers:
        pl.semaphore_signal(barrier, inc=1, device_id=(peer,), device_id_type=MESH)
    pl.semaphore_wait(barrier, len(peers))


def remote(src, dst, send_sem, recv_sem, peer):
    return pltpu.make_async_remote_copy(src_ref=src, dst_ref=dst, send_sem=send_sem, recv_sem=recv_sem, device_id=(peer,), device_id_type=MESH)


def local(src, dst, sem):
    return pltpu.make_async_copy(src, dst, sem)


def halves(t):
    return [(0, t // 2), (t // 2, t // 2)] if t % 32 == 0 else [(0, t)]


def transpose_into(dst, src, t):
    full = t // 128
    if full:
        @pl.loop(0, full)
        def _(i):
            lo = pl.multiple_of(i * 128, 128)
            dst[:, pl.ds(lo, 128)] = src[pl.ds(lo, 128), :].T
    if t % 128:
        dst[:, full * 128:t] = src[full * 128:t, :].T


def fwd_pair(h_ref, v_ref, acc_ref, a_ref, z_ref, t, f):
    for lo, n in halves(t):
        for j in range(2):
            z = dot(h_ref[lo:lo + n, :], v_ref[j, 0]).astype(jnp.bfloat16)
            z_ref[j, lo:lo + n, :] = z
            a_ref[lo:lo + n, j * f:(j + 1) * f] = gelu(z.astype(jnp.float32)).astype(jnp.bfloat16)
    v_out = jnp.concatenate([v_ref[0, 1], v_ref[1, 1]], axis=1)
    for lo, n in halves(t):
        acc_ref[lo:lo + n, :] += dot(a_ref[lo:lo + n, :], v_out, NT)


def fwd_close(h_ref, acc_ref, t):
    for lo, n in halves(t):
        h_ref[lo:lo + n, :] = acc_ref[lo:lo + n, :].astype(jnp.bfloat16)


def fwd_seed(h_ref, acc_ref, t):
    for lo, n in halves(t):
        acc_ref[lo:lo + n, :] = h_ref[lo:lo + n, :].astype(jnp.float32)


def first_forward(dm, x_hbm, y_hbm, wi_hbm, wo_hbm, z_out, v_out, ws_out, h_out, q_out,
                  h, yb, acc, ab, wi, wo, vb, zb, ws, load_sem, z_sem, v_sem, io_sem):
    t, d, f, nf, nl = dm
    nu = nf * nl
    bits, peers = place()
    piece = d // 16

    def loads(p, slot):
        layer, tile = p // (nf // 2), lax.rem(p, nf // 2)
        lo = pl.multiple_of(tile * 2 * f, 2 * f)
        return (local(wi_hbm.at[layer, :, pl.ds(lo, 2 * f)], wi.at[slot], load_sem.at[slot, 0]),
                local(wo_hbm.at[layer, pl.ds(lo, 2 * f), :], wo.at[slot], load_sem.at[slot, 1]))

    def stores(p, slot):
        two = pl.ds(2 * p, 2)
        return local(zb.at[slot], z_out.at[two], z_sem.at[slot]), local(vb.at[slot], v_out.at[two], v_sem.at[slot])

    x_in = local(x_hbm, h, io_sem.at[0])
    y_in = local(y_hbm, yb, io_sem.at[1])
    x_in.start()
    for cp in loads(0, 0):
        cp.start()
    y_in.start()
    x_in.wait()
    fwd_seed(h, acc, t)

    @pl.loop(0, nu // 2)
    def _(p):
        slot = lax.rem(p, 2)
        for cp in loads(p, slot):
            cp.wait()

        @pl.when(p + 1 < nu // 2)
        def _():
            for cp in loads(p + 1, 1 - slot):
                cp.start()

        @pl.when(p >= 2)
        def _():
            for cp in stores(p - 2, slot):
                cp.wait()
        for j in range(2):
            cols = slice(j * f, (j + 1) * f)
            wot = wo[slot, cols, :].T
            _, keep, _ = route(bits, peers, j, d)
            rows = pl.ds(keep[4], piece)
            vb[slot, j, 0] = wi[slot, :, cols].astype(jnp.bfloat16)
            vb[slot, j, 1] = wot.astype(jnp.bfloat16)

            @pl.when(bits[0] == 0)
            def _():
                ws[2 * p + j] = wi[slot, rows, cols]

            @pl.when(bits[0] == 1)
            def _():
                wi[slot, :, cols] = wot
                ws[2 * p + j] = wi[slot, rows, cols]

        fwd_pair(h, vb.at[slot], acc, ab, zb.at[slot], t, f)
        for cp in stores(p, slot):
            cp.start()

        @pl.when(p == nf // 2 - 1)
        def _():
            fwd_close(h, acc, t)
            fwd_seed(h, acc, t)
            out = local(h, h_out, io_sem.at[0])
            out.start()
            out.wait()

    y_in.wait()
    for lo, n in halves(t):
        hl = acc[lo:lo + n, :].astype(jnp.bfloat16).astype(jnp.float32)
        h[lo:lo + n, :] = (hl - yb[lo:lo + n, :].astype(jnp.float32)).astype(jnp.bfloat16)
    out = local(h, q_out, io_sem.at[0])
    out.start()
    ws_cp = local(ws, ws_out, io_sem.at[1])
    ws_cp.start()
    for p in range(max(nu // 2 - 2, 0), nu // 2):
        for cp in stores(p, p % 2):
            cp.wait()
    out.wait()
    ws_cp.wait()


def second_forward(dm, scale, rho, gs_hbm, ws_hbm, x_hbm, y_hbm, z_out, v_out, h_out, q_out, sq_out,
                   h, yb, acc, ab, gs, ws, vb, zb, nb, send_sem, recv_sem, nsend_sem, nrecv_sem, z_sem, v_sem, io_sem):
    t, d, f, nf, nl = dm
    nu = nf * nl
    bits, peers = place()
    core = bits[0]
    piece = d // 16
    enter(peers)
    ins = (local(gs_hbm, gs, io_sem.at[0]), local(ws_hbm, ws, io_sem.at[1]), local(x_hbm, h, io_sem.at[2]), local(y_hbm, yb, io_sem.at[3]))
    for cp in ins:
        cp.start()
    ins[0].wait()

    def square(u, total):
        g = gs[u] * scale
        return total + jnp.sum((g * g).reshape(piece // 8, 8, f // 128, 128), axis=(0, 2))
    nb[0] = lax.fori_loop(0, nu, square, jnp.zeros((8, 128), jnp.float32))
    for k in range(5):
        cp = remote(nb.at[2 * k], nb.at[2 * k + 1], nsend_sem.at[k], nrecv_sem.at[k], peers[k])
        cp.start()
        cp.wait()
        nb[2 * k + 2] = nb[2 * k] + nb[2 * k + 1]
    coef = rho / jnp.sqrt(jnp.sum(nb[10], keepdims=True))
    ins[1].wait()

    def hop(u, k):
        ps, keep, _ = route(bits, peers, u, d)
        if k == 4:
            ref = vb.at[u, core]
            return remote(ref, ref, send_sem.at[u, 4], recv_sem.at[u, 4], peers[0])
        n = piece << k
        ref = vb.at[u, core, pl.ds(pl.multiple_of(keep[4 - k], 16), n), :]
        return remote(ref, ref, send_sem.at[u, k], recv_sem.at[u, k], ps[3 - k])

    ins[2].wait()
    fwd_seed(h, acc, t)

    def z_store(p, slot):
        return local(zb.at[slot], z_out.at[pl.ds(2 * p, 2)], z_sem.at[slot])

    @pl.loop(0, nu + VG_LAG[5])
    def _(it):
        @pl.when(it < nu)
        def _():
            _, keep, _ = route(bits, peers, it, d)
            new = ws[it] + coef * (gs[it] * scale)
            vb[it, core, pl.ds(pl.multiple_of(keep[4], 16), piece), :] = new.astype(jnp.bfloat16)
            hop(it, 0).start()
        for k in range(1, 5):
            u = it - VG_LAG[k]

            @pl.when((u >= 0) & (u < nu))
            def _():
                hop(u, k - 1).wait_recv()
                hop(u, k).start()
        u = it - VG_LAG[5]

        @pl.when(u >= 0)
        def _():
            hop(u, 4).wait_recv()
            local(vb.at[u], v_out.at[u], v_sem.at[u]).start()

        @pl.when((u >= 0) & (lax.rem(u, 2) == 1))
        def _():
            p = u // 2
            slot = lax.rem(p, 2)

            @pl.when(p >= 2)
            def _():
                z_store(p - 2, slot).wait()
            fwd_pair(h, vb.at[pl.ds(2 * p, 2)], acc, ab, zb.at[slot], t, f)
            z_store(p, slot).start()

            @pl.when(p == nf // 2 - 1)
            def _():
                fwd_close(h, acc, t)
                fwd_seed(h, acc, t)
                out = local(h, h_out, io_sem.at[0])
                out.start()
                out.wait()

    ins[3].wait()
    total = jnp.zeros((8, 128), jnp.float32)
    for lo, n in halves(t):
        hl = acc[lo:lo + n, :].astype(jnp.bfloat16).astype(jnp.float32)
        e = hl - yb[lo:lo + n, :].astype(jnp.float32)
        h[lo:lo + n, :] = e.astype(jnp.bfloat16)
        total = total + jnp.sum((e * e).reshape(n // 8, 8, d // 128, 128), axis=(0, 2))
    nb[0] = total
    out = local(h, q_out, io_sem.at[0])
    sq = local(nb.at[0], sq_out, io_sem.at[1])
    out.start()
    sq.start()

    @pl.loop(0, nu)
    def _(u):
        local(vb.at[u], v_out.at[u], v_sem.at[u]).wait()
        for k in range(5):
            hop(u, k).wait_send()
    for p in range(max(nu // 2 - 2, 0), nu // 2):
        z_store(p, p % 2).wait()
    out.wait()
    sq.wait()


def backward(dm, scale, final, *refs):
    t, d, f, nf, nl = dm
    nu = nf * nl
    if final:
        (x_hbm, h_hbm, q_hbm, z_hbm, v_hbm, ws_hbm, sq_hbm, w_out, sq_out, *scr) = refs
    else:
        (x_hbm, h_hbm, q_hbm, z_hbm, v_hbm, g_out, *scr) = refs
    (q, tmp, tb, eb, acc, zb, vb, cbuf, obuf, sbuf, r1, r2, r3, r4, gs,
     load_sem, io_sem, csend_sem, send_sem, recv_sem, credit, *more) = scr
    if final:
        nb, ag_send, ag_recv, ag_loc, nsend_sem, nrecv_sem = more
    rbuf = (r1, r2, r3, r4)
    bits, peers = place()
    core = bits[0]
    piece = d // 16
    slots = cbuf.shape[0]
    enter(peers)

    def unit_of(it):
        return (nl - 1 - it // nf) * nf + lax.rem(it, nf)

    def loads(it, slot):
        u = unit_of(it)
        return local(z_hbm.at[u], zb.at[slot], load_sem.at[slot, 0]), local(v_hbm.at[u], vb.at[slot], load_sem.at[slot, 1])

    q_in = local(q_hbm, q, io_sem.at[0])
    h_in = local(h_hbm, tmp, io_sem.at[1])
    q_in.start()
    for cp in loads(0, 0):
        cp.start()
    h_in.start()
    if final:
        ws_in = local(ws_hbm, gs, io_sem.at[2])
        sq_in = local(sq_hbm, nb.at[0], io_sem.at[3])
        ws_in.start()
        sq_in.start()
        ws_in.wait()
        sq_in.wait()
    q_in.wait()
    fwd_seed(q, acc, t)
    transpose_into(tb.at[1], q, t)
    h_in.wait()
    transpose_into(tb.at[0], tmp, t)
    x_in = local(x_hbm, tmp, io_sem.at[1])
    x_in.start()

    def core_copy(it):
        slot = lax.rem(it, 2)
        return remote(sbuf.at[slot], cbuf.at[lax.rem(it, slots)], csend_sem.at[slot], recv_sem.at[0, it], peers[0])

    def rs_copy(it, k):
        ps, _, send = route(bits, peers, it, d)
        n = d >> (k + 1)
        return remote(cbuf.at[lax.rem(it, slots), pl.ds(send[k], n), :], rbuf[k].at[it], send_sem.at[it, k], recv_sem.at[k + 1, it], ps[k])

    def ag_copy(it, k):
        ps, keep, _ = route(bits, peers, it, d)
        u = unit_of(it)
        if k == 4:
            ref = w_out.at[u, core]
            return remote(ref, ref, ag_send.at[it, 4], ag_recv.at[it, 4], peers[0])
        n = piece << k
        ref = w_out.at[u, core, pl.ds(keep[4 - k], n), :]
        src = gs.at[u] if k == 0 else ref
        return remote(src, ref, ag_send.at[it, k], ag_recv.at[it, k], ps[3 - k])

    def ag_local(it):
        _, keep, _ = route(bits, peers, it, d)
        u = unit_of(it)
        return local(gs.at[u], w_out.at[u, core, pl.ds(keep[4], piece), :], ag_loc.at[it])

    n_it = nu + (AG_LAG[4] if final else RS_LAG[4])

    @pl.loop(0, n_it)
    def _(it):
        @pl.when(it == nf)
        def _():
            fwd_close(q, acc, t)
            transpose_into(tb.at[1], q, t)
            x_in.wait()
            transpose_into(tb.at[0], tmp, t)

        @pl.when(it < nu)
        def _():
            slot = lax.rem(it, 2)
            for cp in loads(it, slot):
                cp.wait()

            @pl.when(it + 1 < nu)
            def _():
                for cp in loads(it + 1, 1 - slot):
                    cp.start()
            for lo, n in halves(t):
                back = dot(q[lo:lo + n, :], vb[slot, 1])
                a, slope = gelu_and_grad(zb[slot, lo:lo + n, :].astype(jnp.float32))
                eb[1, lo:lo + n, :] = a.astype(jnp.bfloat16)
                eb[0, lo:lo + n, :] = (back * slope).astype(jnp.bfloat16)

            @pl.when(it >= 2)
            def _():
                core_copy(it - 2).wait_send()
            other = 1 - core
            sbuf[slot] = dot(tb[other], eb[other])

            @pl.when(it >= slots)
            def _():
                pl.semaphore_wait(credit, 1)
            core_copy(it).start()
            obuf[slot] = dot(tb[core], eb[core])

            @pl.when(it < nf)
            def _():
                for lo, n in halves(t):
                    acc[lo:lo + n, :] += dot(eb[0, lo:lo + n, :], vb[slot, 0], NT)

        j0 = it - RS_LAG[0]

        @pl.when((j0 >= 0) & (j0 < nu))
        def _():
            cs = lax.rem(j0, slots)
            core_copy(j0).wait_recv()
            cbuf[cs] = cbuf[cs] + obuf[lax.rem(j0, 2)]
            rs_copy(j0, 0).start()

        for k in range(4):
            j = it - RS_LAG[k + 1]

            @pl.when((j >= 0) & (j < nu))
            def _():
                cs = lax.rem(j, slots)
                _, keep, _ = route(bits, peers, j, d)
                n = d >> (k + 1)
                rows = pl.ds(keep[k + 1], n)
                rs_copy(j, k).wait_recv()
                if k < 3:
                    cbuf[cs, rows, :] = cbuf[cs, rows, :] + rbuf[k][j]
                    rs_copy(j, k + 1).start()
                else:
                    total = cbuf[cs, rows, :] + rbuf[k][j]
                    u = unit_of(j)
                    gs[u] = gs[u] - LEARN_RATE * (total * scale) if final else total
                    for kk in range(4):
                        rs_copy(j, kk).wait_send()

                    @pl.when(j + slots < nu)
                    def _():
                        pl.semaphore_signal(credit, inc=1, device_id=(peers[0],), device_id_type=MESH)
                    if final:
                        ag_local(j).start()
                        ag_copy(j, 0).start()
        if final:
            for k in range(4):
                j = it - AG_LAG[k]

                @pl.when((j >= 0) & (j < nu))
                def _():
                    ag_copy(j, k).wait_recv()
                    if k == 0:
                        ag_local(j).wait()
                    ag_copy(j, k + 1).start()

            @pl.when(it < 5)
            def _():
                for k in range(5):
                    @pl.when(it == k)
                    def _():
                        cp = remote(nb.at[2 * k], nb.at[2 * k + 1], nsend_sem.at[k], nrecv_sem.at[k], peers[k])
                        cp.start()
                        cp.wait()
                        nb[2 * k + 2] = nb[2 * k] + nb[2 * k + 1]

    core_copy(nu - 2).wait_send()
    core_copy(nu - 1).wait_send()
    if final:
        sq_cp = local(nb.at[10], sq_out, io_sem.at[3])
        sq_cp.start()

        @pl.loop(0, nu)
        def _(it):
            ag_copy(it, 4).wait_recv()
            for k in range(5):
                ag_copy(it, k).wait_send()
        sq_cp.wait()
    else:
        g_cp = local(gs, g_out, io_sem.at[0])
        g_cp.start()
        g_cp.wait()


def finish(scale, f, w_ref, sq_ref, in_ref, out_ref, loss_ref):
    for j in range(2):
        in_ref[0, :, j * f:(j + 1) * f] = w_ref[j, 0]
        out_ref[0, j * f:(j + 1) * f, :] = w_ref[j, 1].T
    loss_ref[0, 0] = 0.5 * (jnp.sum(sq_ref[...]) * scale)


def sds(shape, dtype):
    return jax.ShapeDtypeStruct(shape, dtype)


def call(kernel, n_in, outs, scratch, name, collective_id=None):
    params = dict(vmem_limit_bytes=VMEM_CAP)
    if collective_id is not None:
        params.update(collective_id=collective_id, has_side_effects=True)
    return pl.pallas_call(
        kernel,
        out_shape=outs,
        in_specs=[ANY] * n_in,
        out_specs=[ANY] * len(outs),
        scratch_shapes=scratch,
        compiler_params=pltpu.CompilerParams(**params),
        name=name,
    )


def local_step(n_dev, tile_f, x_loc, y_loc, w_in, w_out):
    nl, d, ff = w_in.shape
    f = tile_f
    nf = ff // f
    nu = nl * nf
    t = x_loc.shape[0] * x_loc.shape[1]
    piece = d // 16
    dm = (t, d, f, nf, nl)
    scale = 1.0 / (t * n_dev * d)
    rho = RHO_FRAC * math.sqrt(nl * (d + ff))
    bf, f32 = jnp.bfloat16, jnp.float32
    V, DMA = pltpu.VMEM, pltpu.SemaphoreType.DMA
    x = x_loc.transpose(1, 0, 2).reshape(t, d)
    y = y_loc.transpose(1, 0, 2).reshape(t, d)
    z_s, v_s, w_s, a_s = sds((nu, t, f), bf), sds((nu, 2, d, f), bf), sds((nu, piece, f), f32), sds((t, d), bf)

    z, v, ws, h1, q = call(
        functools.partial(first_forward, dm), 4, [z_s, v_s, w_s, a_s, a_s],
        [V((t, d), bf), V((t, d), bf), V((t, d), f32), V((t, 2 * f), bf), V((2, d, 2 * f), f32), V((2, 2 * f, d), f32), V((2, 2, 2, d, f), bf), V((2, 2, t, f), bf),
         V((nu, piece, f), f32),
         DMA((2, 2)), DMA((2,)), DMA((2,)), DMA((2,))], "fwd_a")(x, y, w_in, w_out)

    slots = min(CORE_SLOTS, nu)
    bwd_scratch = [
        V((t, d), bf), V((t, d), bf), V((2, d, t), bf), V((2, t, f), bf), V((t, d), f32), V((2, t, f), bf), V((2, 2, d, f), bf),
        V((slots, d, f), f32), V((2, d, f), f32), V((2, d, f), f32),
        V((nu, d // 2, f), f32), V((nu, d // 4, f), f32), V((nu, d // 8, f), f32), V((nu, d // 16, f), f32), V((nu, piece, f), f32),
        DMA((2, 2)), DMA((4,)), DMA((2,)), DMA((nu, 4)), DMA((5, nu)), pltpu.SemaphoreType.REGULAR]
    (g,) = call(functools.partial(backward, dm, scale, False), 5, [w_s], bwd_scratch, "bwd_a", 0)(x, h1, q, z, v)

    z, v, h1, q, sq = call(
        functools.partial(second_forward, dm, scale, rho), 4, [z_s, v_s, a_s, a_s, sds((8, 128), f32)],
        [V((t, d), bf), V((t, d), bf), V((t, d), f32), V((t, 2 * f), bf), V((nu, piece, f), f32), V((nu, piece, f), f32), V((nu, 2, d, f), bf), V((2, 2, t, f), bf),
         V((11, 8, 128), f32),
         DMA((nu, 5)), DMA((nu, 5)), DMA((5,)), DMA((5,)), DMA((2,)), DMA((nu,)), DMA((4,))], "fwd_b", 1)(g, ws, x, y)

    w_new, sq = call(
        functools.partial(backward, dm, scale, True), 7, [sds((nu, 2, d, f), f32), sds((8, 128), f32)],
        bwd_scratch + [V((11, 8, 128), f32), DMA((nu, 5)), DMA((nu, 5)), DMA((nu,)), DMA((5,)), DMA((5,))], "bwd_b", 2)(x, h1, q, z, v, ws, sq)

    new_in, new_out, loss = pl.pallas_call(
        functools.partial(finish, scale, f),
        grid=(nl, nf // 2),
        in_specs=[pl.BlockSpec((2, 2, d, f), lambda i, j: (i * (nf // 2) + j, 0, 0, 0)), pl.BlockSpec((8, 128), lambda i, j: (0, 0))],
        out_specs=[pl.BlockSpec((1, d, 2 * f), lambda i, j: (i, 0, j)), pl.BlockSpec((1, 2 * f, d), lambda i, j: (i, j, 0)),
                   pl.BlockSpec((1, 1), lambda i, j: (0, 0), memory_space=pltpu.SMEM)],
        out_shape=[sds((nl, d, ff), f32), sds((nl, ff, d), f32), sds((1, 1), f32)],
        compiler_params=pltpu.CompilerParams(vmem_limit_bytes=VMEM_CAP),
        name="finish")(w_new, sq)
    return new_in, new_out, loss.reshape(())


def solution(mesh):
    step = functools.partial(local_step, mesh.shape["data"], TILE_F)
    return jax.shard_map(step, mesh=mesh, in_specs=(P("data"), P("data"), P(), P()), out_specs=(P(), P(), P()), check_vma=False)
```

```python
import math
import functools
import jax
import jax.numpy as jnp
from jax import lax
from jax.experimental import pallas as pl
from jax.experimental.pallas import tpu as pltpu
from jax.sharding import PartitionSpec as P

RHO_FRAC = 0.1
LEARN_RATE = 1.0
TILE_F = 256
MESH = pl.DeviceIdType.MESH
ANY = pl.BlockSpec(memory_space=pl.ANY)
NN = (((1,), (0,)), ((), ()))
NT = (((1,), (1,)), ((), ()))
GELU_C = math.sqrt(2.0 / math.pi)
GELU_K = 0.044715
VMEM_CAP = 67043328
CORE_SLOTS = 9
RS_LAG = (0, 1, 4, 5, 6)
AG_LAG = (1, 2, 4, 5)
VG_LAG = (0, 2, 3, 5, 7, 9)


def dot(lhs, rhs, dims=NN):
    return lax.dot_general(lhs, rhs, dims, preferred_element_type=jnp.float32)


def gelu_parts(z):
    sq = z * z
    th = jnp.tanh(GELU_C * (z + GELU_K * (sq * z)))
    cdf = 0.5 * (1.0 + th)
    return sq, th, cdf


def gelu(z):
    return z * gelu_parts(z)[2]


def gelu_and_grad(z):
    sq, th, cdf = gelu_parts(z)
    slope = cdf + (0.5 * z) * ((1.0 - th * th) * (GELU_C + (3.0 * GELU_K * GELU_C) * sq))
    return z * cdf, slope


def place(axis="data"):
    me = lax.axis_index(axis)
    bits = [lax.rem(lax.div(me, 1 << k), 2) for k in range(5)]
    peers = [me + (1 << k) * (1 - 2 * bits[k]) for k in range(5)]
    return bits, peers


def route(bits, peers, unit, rows):
    core, bx, by, ba, bb = bits
    parity = lax.rem(unit + core, 2)
    _, px, py, pa, pb = peers
    b1 = jnp.where(parity == 0, bx, by)
    b3 = jnp.where(parity == 0, by, bx)
    p1 = jnp.where(parity == 0, px, py)
    p3 = jnp.where(parity == 0, py, px)
    step = rows // 16
    keep, send, base = [0], [], 0
    n = rows
    for bit in (b1, ba, b3, bb):
        n //= 2
        keep.append(pl.multiple_of(base + bit * n, step))
        send.append(pl.multiple_of(base + (1 - bit) * n, step))
        base = base + bit * n
    return (p1, pa, p3, pb), keep, send, (b1, ba, b3, bb)


def arrive(peers):
    barrier = pltpu.get_barrier_semaphore()
    for peer in peers:
        pl.semaphore_signal(barrier, inc=1, device_id=(peer,), device_id_type=MESH)
    return functools.partial(pl.semaphore_wait, barrier, len(peers))


def others(bits, me_bits):
    me = lax.axis_index("data")
    out = []
    for mask in range(1, 1 << len(me_bits)):
        peer = me
        for i, k in enumerate(me_bits):
            if mask >> i & 1:
                peer = peer + (1 << k) * (1 - 2 * bits[k])
        out.append(peer)
    return out


def exchange_sum(buf, first, peers, send_sem, recv_sem, sem0):
    copies = [remote(buf.at[first], buf.at[first + 1 + i], send_sem.at[sem0 + i], recv_sem.at[sem0 + i], peer) for i, peer in enumerate(peers)]
    for cp in copies:
        cp.start()
    total = buf[first]
    for i, cp in enumerate(copies):
        cp.wait()
        total = total + buf[first + 1 + i]
    buf[first + len(peers) + 1] = total


def gather_hops(bits, peers, unit, d, full, piece_src=None):
    ps, keep, send, _ = route(bits, peers, unit, d)
    piece = d // 16

    def rows(base, n):
        return full.at[pl.ds(base, n), :]

    def hop(k, part, sem_s, sem_r):
        peer = ps[3 - k] if k < 4 else peers[0]
        if k == 0:
            ref = rows(keep[4], piece)
        elif part == 0:
            ref = rows(keep[5 - k], piece << (k - 1))
        else:
            ref = rows(send[4 - k], piece << (k - 1))
        src = piece_src if piece_src is not None and part == 0 and k <= 1 else ref
        return remote(src, ref, sem_s, sem_r, peer)

    def arrived(k, sem_s, sem_r):
        ref = rows(send[3 - k], piece << k)
        return remote(ref, ref, sem_s, sem_r, ps[3 - k])

    def sent(sem_s, sem_r):
        ref = rows(0, 15 * piece)
        return remote(ref, ref, sem_s, sem_r, ps[0])
    return hop, arrived, sent


def remote(src, dst, send_sem, recv_sem, peer):
    return pltpu.make_async_remote_copy(src_ref=src, dst_ref=dst, send_sem=send_sem, recv_sem=recv_sem, device_id=(peer,), device_id_type=MESH)


def local(src, dst, sem):
    return pltpu.make_async_copy(src, dst, sem)


def halves(t):
    return [(0, t // 2), (t // 2, t // 2)] if t % 32 == 0 else [(0, t)]


def transpose_into(dst, src, t):
    full = t // 128
    if full:
        @pl.loop(0, full)
        def _(i):
            lo = pl.multiple_of(i * 128, 128)
            dst[:, pl.ds(lo, 128)] = src[pl.ds(lo, 128), :].T
    if t % 128:
        dst[:, full * 128:t] = src[full * 128:t, :].T


def fwd_pair(h_ref, v_ref, acc_ref, a_ref, z_ref, t, f):
    for lo, n in halves(t):
        for j in range(2):
            z = dot(h_ref[lo:lo + n, :], v_ref[j, 0]).astype(jnp.bfloat16)
            z_ref[j, lo:lo + n, :] = z
            a_ref[lo:lo + n, j * f:(j + 1) * f] = gelu(z.astype(jnp.float32)).astype(jnp.bfloat16)
    v_out = jnp.concatenate([v_ref[0, 1], v_ref[1, 1]], axis=1)
    for lo, n in halves(t):
        acc_ref[lo:lo + n, :] += dot(a_ref[lo:lo + n, :], v_out, NT)


def fwd_close(h_ref, acc_ref, t):
    for lo, n in halves(t):
        h_ref[lo:lo + n, :] = acc_ref[lo:lo + n, :].astype(jnp.bfloat16)


def fwd_seed(h_ref, acc_ref, t):
    for lo, n in halves(t):
        acc_ref[lo:lo + n, :] = h_ref[lo:lo + n, :].astype(jnp.float32)


def first_forward(dm, x_hbm, y_hbm, wi_hbm, wo_hbm, z_out, v_out, ws_out, h_out, q_out,
                  h, yb, acc, ab, wi, wo, wt, vb, zb, ws, load_sem, z_sem, v_sem, io_sem):
    t, d, f, nf, nl = dm
    nu = nf * nl
    bits, peers = place()
    piece = d // 16

    def loads(p, slot):
        layer, tile = p // (nf // 2), lax.rem(p, nf // 2)
        lo = pl.multiple_of(tile * 2 * f, 2 * f)
        return (local(wi_hbm.at[layer, :, pl.ds(lo, 2 * f)], wi.at[slot], load_sem.at[slot, 0]),
                local(wo_hbm.at[layer, pl.ds(lo, 2 * f), :], wo.at[slot], load_sem.at[slot, 1]))

    def stores(p, slot):
        two = pl.ds(2 * p, 2)
        return local(zb.at[slot], z_out.at[two], z_sem.at[slot]), local(vb.at[slot], v_out.at[two], v_sem.at[slot])

    x_in = local(x_hbm, h, io_sem.at[0])
    y_in = local(y_hbm, yb, io_sem.at[1])
    x_in.start()
    for cp in loads(0, 0):
        cp.start()
    y_in.start()
    x_in.wait()
    fwd_seed(h, acc, t)

    @pl.loop(0, nu // 2)
    def _(p):
        slot = lax.rem(p, 2)
        for cp in loads(p, slot):
            cp.wait()

        @pl.when(p + 1 < nu // 2)
        def _():
            for cp in loads(p + 1, 1 - slot):
                cp.start()

        @pl.when(p >= 2)
        def _():
            for cp in stores(p - 2, slot):
                cp.wait()
        for j in range(2):
            cols = slice(j * f, (j + 1) * f)
            wot = wo[slot, cols, :].T
            _, keep, _, _ = route(bits, peers, j, d)
            rows = pl.ds(keep[4], piece)
            vb[slot, j, 0] = wi[slot, :, cols].astype(jnp.bfloat16)
            vb[slot, j, 1] = wot.astype(jnp.bfloat16)
            wt[...] = wot
            ws[2 * p + j] = jnp.where(bits[0] == 0, wi[slot, rows, cols], wt[rows, :])

        fwd_pair(h, vb.at[slot], acc, ab, zb.at[slot], t, f)
        for cp in stores(p, slot):
            cp.start()

        @pl.when(p == nf // 2 - 1)
        def _():
            fwd_close(h, acc, t)
            fwd_seed(h, acc, t)
            out = local(h, h_out, io_sem.at[0])
            out.start()
            out.wait()

    y_in.wait()
    for lo, n in halves(t):
        hl = acc[lo:lo + n, :].astype(jnp.bfloat16).astype(jnp.float32)
        h[lo:lo + n, :] = (hl - yb[lo:lo + n, :].astype(jnp.float32)).astype(jnp.bfloat16)
    out = local(h, q_out, io_sem.at[0])
    out.start()
    ws_cp = local(ws, ws_out, io_sem.at[1])
    ws_cp.start()
    for p in range(max(nu // 2 - 2, 0), nu // 2):
        for cp in stores(p, p % 2):
            cp.wait()
    out.wait()
    ws_cp.wait()


def second_forward(dm, scale, rho, gs_hbm, ws_hbm, x_hbm, y_hbm, z_out, v_out, h_out, q_out, sq_out,
                   h, yb, acc, ab, gs, ws, vb, zb, nb, send_sem, recv_sem, nsend_sem, nrecv_sem, z_sem, v_sem, io_sem):
    t, d, f, nf, nl = dm
    nu = nf * nl
    bits, peers = place()
    core = bits[0]
    piece = d // 16
    near, far = others(bits, (0, 1, 2)), others(bits, (3, 4))
    wait_all = arrive(near + far)
    ins = (local(gs_hbm, gs, io_sem.at[0]), local(ws_hbm, ws, io_sem.at[1]), local(x_hbm, h, io_sem.at[2]), local(y_hbm, yb, io_sem.at[3]))
    for cp in ins:
        cp.start()
    ins[0].wait()

    def square(u, total):
        g = gs[u] * scale
        return total + jnp.sum((g * g).reshape(piece // 8, 8, f // 128, 128), axis=(0, 2))
    nb[0] = lax.fori_loop(0, nu, square, jnp.zeros((8, 128), jnp.float32))
    wait_all()
    exchange_sum(nb, 0, near, nsend_sem, nrecv_sem, 0)
    exchange_sum(nb, 8, far, nsend_sem, nrecv_sem, 7)
    coef = rho / jnp.sqrt(jnp.sum(nb[12], keepdims=True))
    ins[1].wait()

    def hops(u):
        return gather_hops(bits, peers, u, d, vb.at[u, core])

    def sems(u, k):
        return send_sem.at[u, 0 if k < 4 else 1], recv_sem.at[u, k]

    def core_arrived(u):
        ref = vb.at[u, 1 - core]
        return remote(ref, ref, *sems(u, 4), peers[0])

    ins[2].wait()
    fwd_seed(h, acc, t)

    def z_store(p, slot):
        return local(zb.at[slot], z_out.at[pl.ds(2 * p, 2)], z_sem.at[slot])

    @pl.loop(0, nu + VG_LAG[5])
    def _(it):
        @pl.when(it < nu)
        def _():
            _, keep, _, _ = route(bits, peers, it, d)
            new = ws[it] + coef * (gs[it] * scale)
            vb[it, core, pl.ds(keep[4], piece), :] = new.astype(jnp.bfloat16)
            hop, _, _ = hops(it)
            hop(0, 0, *sems(it, 0)).start()
            hop(1, 0, *sems(it, 1)).start()
        for k in range(1, 5):
            u = it - VG_LAG[k]

            @pl.when((u >= 0) & (u < nu))
            def _():
                hop, arrived, _ = hops(u)
                arrived(k - 1, *sems(u, k - 1)).wait_recv()
                hop(k, 1, *sems(u, k)).start()
                if k < 4:
                    hop(k + 1, 0, *sems(u, k + 1)).start()
        u = it - VG_LAG[5]

        @pl.when(u >= 0)
        def _():
            core_arrived(u).wait_recv()
            local(vb.at[u], v_out.at[u], v_sem.at[u]).start()

        @pl.when((u >= 0) & (lax.rem(u, 2) == 1))
        def _():
            p = u // 2
            slot = lax.rem(p, 2)

            @pl.when(p >= 2)
            def _():
                z_store(p - 2, slot).wait()
            fwd_pair(h, vb.at[pl.ds(2 * p, 2)], acc, ab, zb.at[slot], t, f)
            z_store(p, slot).start()

            @pl.when(p == nf // 2 - 1)
            def _():
                fwd_close(h, acc, t)
                fwd_seed(h, acc, t)
                out = local(h, h_out, io_sem.at[0])
                out.start()
                out.wait()

    ins[3].wait()
    total = jnp.zeros((8, 128), jnp.float32)
    for lo, n in halves(t):
        hl = acc[lo:lo + n, :].astype(jnp.bfloat16).astype(jnp.float32)
        e = hl - yb[lo:lo + n, :].astype(jnp.float32)
        h[lo:lo + n, :] = e.astype(jnp.bfloat16)
        total = total + jnp.sum((e * e).reshape(n // 8, 8, d // 128, 128), axis=(0, 2))
    nb[0] = total
    out = local(h, q_out, io_sem.at[0])
    sq = local(nb.at[0], sq_out, io_sem.at[1])
    out.start()
    sq.start()

    @pl.loop(0, nu)
    def _(u):
        local(vb.at[u], v_out.at[u], v_sem.at[u]).wait()
        hops(u)[2](*sems(u, 0)).wait_send()
        core_arrived(u).wait_send()
    for p in range(max(nu // 2 - 2, 0), nu // 2):
        z_store(p, p % 2).wait()
    out.wait()
    sq.wait()


def backward(dm, scale, final, *refs):
    t, d, f, nf, nl = dm
    nu = nf * nl
    if final:
        (x_hbm, h_hbm, q_hbm, z_hbm, v_hbm, ws_hbm, sq_hbm, w_out, sq_out, *scr) = refs
    else:
        (x_hbm, h_hbm, q_hbm, z_hbm, v_hbm, g_out, *scr) = refs
    (q, tmp, tb, eb, acc, zb, vb, cbuf, obuf, sbuf, r1, r2, r3, r4, gs,
     load_sem, io_sem, csend_sem, send_sem, recv_sem, credit, *more) = scr
    if final:
        nb, ag_send, ag_recv, ag_loc, nsend_sem, nrecv_sem = more
    rbuf = (r1, r2, r3, r4)
    bits, peers = place()
    core = bits[0]
    piece = d // 16
    slots = cbuf.shape[0]
    near, far = others(bits, (0, 1, 2)), others(bits, (3, 4))
    wait_all = arrive(near + far if final else peers)

    def unit_of(it):
        return (nl - 1 - it // nf) * nf + lax.rem(it, nf)

    def loads(it, slot):
        u = unit_of(it)
        return local(z_hbm.at[u], zb.at[slot], load_sem.at[slot, 0]), local(v_hbm.at[u], vb.at[slot], load_sem.at[slot, 1])

    q_in = local(q_hbm, q, io_sem.at[0])
    h_in = local(h_hbm, tmp, io_sem.at[1])
    q_in.start()
    for cp in loads(0, 0):
        cp.start()
    h_in.start()
    if final:
        ws_in = local(ws_hbm, gs, io_sem.at[2])
        sq_in = local(sq_hbm, nb.at[0], io_sem.at[3])
        ws_in.start()
        sq_in.start()
        ws_in.wait()
        sq_in.wait()
    q_in.wait()
    fwd_seed(q, acc, t)
    transpose_into(tb.at[1], q, t)
    h_in.wait()
    transpose_into(tb.at[0], tmp, t)
    x_in = local(x_hbm, tmp, io_sem.at[1])
    x_in.start()
    wait_all()

    def core_copy(it):
        slot = lax.rem(it, 2)
        return remote(sbuf.at[slot], cbuf.at[lax.rem(it, slots)], csend_sem.at[slot], recv_sem.at[0, it, 0], peers[0])

    def rs_sends(it, k):
        ps, _, send, on = route(bits, peers, it, d)
        n = d >> (k + 1)
        cs = lax.rem(it, slots)

        def part(off, m, sem):
            return remote(cbuf.at[cs, pl.ds(send[k] + off, m), :], rbuf[k].at[it, pl.ds(off, m), :], send_sem.at[it], sem, ps[k])
        if k == 3:
            return [part(0, n, recv_sem.at[1, it, k])]
        m = n // 2
        step = d // 16
        return [part(pl.multiple_of((1 - on[k + 1]) * m, step), m, recv_sem.at[1, it, k]),
                part(pl.multiple_of(on[k + 1] * m, step), m, recv_sem.at[2, it, k])]

    def rs_add(it, k, kept):
        ps, keep, send, _ = route(bits, peers, it, d)
        cs = lax.rem(it, slots)
        if k == 3:
            base, m = keep[4], d >> 4
        else:
            base, m = (keep[k + 2] if kept else send[k + 1]), d >> (k + 2)
        here = rbuf[k].at[it, pl.ds(pl.multiple_of(base - keep[k + 1], d // 16), m), :]
        mine = cbuf.at[cs, pl.ds(base, m), :]
        remote(mine, here, send_sem.at[it], recv_sem.at[2 if kept else 1, it, k], ps[k]).wait_recv()
        total = mine[...] + here[...]
        if k == 3:
            return total
        mine[...] = total

    def rs_sent(it):
        ref = cbuf.at[lax.rem(it, slots), pl.ds(0, 15 * piece), :]
        return remote(ref, ref, send_sem.at[it], recv_sem.at[1, it, 3], peers[0])

    if final:
        def hops(it):
            u = unit_of(it)
            return gather_hops(bits, peers, it, d, w_out.at[u, core], gs.at[u])

        def sems(it, k):
            return ag_send.at[it, 0 if k < 4 else 1], ag_recv.at[it, k]

        def core_arrived(it):
            ref = w_out.at[unit_of(it), 1 - core]
            return remote(ref, ref, *sems(it, 4), peers[0])

        def ag_local(it):
            _, keep, _, _ = route(bits, peers, it, d)
            u = unit_of(it)
            return local(gs.at[u], w_out.at[u, core, pl.ds(keep[4], piece), :], ag_loc.at[it])

    n_it = nu + RS_LAG[4] + (AG_LAG[3] if final else 0)

    @pl.loop(0, n_it)
    def _(it):
        @pl.when(it == nf)
        def _():
            fwd_close(q, acc, t)
            transpose_into(tb.at[1], q, t)
            x_in.wait()
            transpose_into(tb.at[0], tmp, t)

        @pl.when(it < nu)
        def _():
            slot = lax.rem(it, 2)
            for cp in loads(it, slot):
                cp.wait()

            @pl.when(it + 1 < nu)
            def _():
                for cp in loads(it + 1, 1 - slot):
                    cp.start()
            for lo, n in halves(t):
                back = dot(q[lo:lo + n, :], vb[slot, 1])
                a, slope = gelu_and_grad(zb[slot, lo:lo + n, :].astype(jnp.float32))
                eb[1, lo:lo + n, :] = a.astype(jnp.bfloat16)
                eb[0, lo:lo + n, :] = (back * slope).astype(jnp.bfloat16)

            @pl.when(it >= 2)
            def _():
                core_copy(it - 2).wait_send()
            other = 1 - core
            sbuf[slot] = dot(tb[other], eb[other])

            @pl.when(it >= slots)
            def _():
                pl.semaphore_wait(credit, 1)
            core_copy(it).start()
            obuf[slot] = dot(tb[core], eb[core])

            @pl.when(it < nf)
            def _():
                for lo, n in halves(t):
                    acc[lo:lo + n, :] += dot(eb[0, lo:lo + n, :], vb[slot, 0], NT)

        j0 = it - RS_LAG[0]

        @pl.when((j0 >= 0) & (j0 < nu))
        def _():
            cs = lax.rem(j0, slots)
            core_copy(j0).wait_recv()
            cbuf[cs] = cbuf[cs] + obuf[lax.rem(j0, 2)]
            for cp in rs_sends(j0, 0):
                cp.start()

        for k in range(4):
            j = it - RS_LAG[k + 1]

            @pl.when((j >= 0) & (j < nu))
            def _():
                if k > 0:
                    rs_add(j, k - 1, True)
                if k < 3:
                    rs_add(j, k, False)
                    for cp in rs_sends(j, k + 1):
                        cp.start()
                else:
                    total = rs_add(j, k, False)
                    u = unit_of(j)
                    gs[u] = gs[u] - LEARN_RATE * (total * scale) if final else total
                    rs_sent(j).wait_send()

                    @pl.when(j + slots < nu)
                    def _():
                        pl.semaphore_signal(credit, inc=1, device_id=(peers[0],), device_id_type=MESH)
                    if final:
                        ag_local(j).start()
                        hop, _, _ = hops(j)
                        hop(0, 0, *sems(j, 0)).start()
                        hop(1, 0, *sems(j, 1)).start()
        if final:
            for k in range(1, 5):
                j = it - RS_LAG[4] - AG_LAG[k - 1]

                @pl.when((j >= 0) & (j < nu))
                def _():
                    hop, arrived, _ = hops(j)
                    if k == 1:
                        ag_local(j).wait()
                    arrived(k - 1, *sems(j, k - 1)).wait_recv()
                    hop(k, 1, *sems(j, k)).start()
                    if k < 4:
                        hop(k + 1, 0, *sems(j, k + 1)).start()

            @pl.when(it == 1)
            def _():
                exchange_sum(nb, 0, near, nsend_sem, nrecv_sem, 0)

            @pl.when(it == 2)
            def _():
                exchange_sum(nb, 8, far, nsend_sem, nrecv_sem, 7)

    core_copy(nu - 2).wait_send()
    core_copy(nu - 1).wait_send()
    if final:
        sq_cp = local(nb.at[12], sq_out, io_sem.at[3])
        sq_cp.start()

        @pl.loop(0, nu)
        def _(it):
            core_arrived(it).wait_recv()
            hops(it)[2](*sems(it, 0)).wait_send()
            core_arrived(it).wait_send()
        sq_cp.wait()
    else:
        g_cp = local(gs, g_out, io_sem.at[0])
        g_cp.start()
        g_cp.wait()


def finish(scale, f, w_ref, sq_ref, in_ref, out_ref, loss_ref):
    for j in range(2):
        in_ref[0, :, j * f:(j + 1) * f] = w_ref[j, 0]
        out_ref[0, j * f:(j + 1) * f, :] = w_ref[j, 1].T
    loss_ref[0, 0] = 0.5 * (jnp.sum(sq_ref[...]) * scale)


def sds(shape, dtype):
    return jax.ShapeDtypeStruct(shape, dtype)


def call(kernel, n_in, outs, scratch, name, collective_id=None):
    params = dict(vmem_limit_bytes=VMEM_CAP)
    if collective_id is not None:
        params.update(collective_id=collective_id, has_side_effects=True)
    return pl.pallas_call(
        kernel,
        out_shape=outs,
        in_specs=[ANY] * n_in,
        out_specs=[ANY] * len(outs),
        scratch_shapes=scratch,
        compiler_params=pltpu.CompilerParams(**params),
        name=name,
    )


def local_step(n_dev, tile_f, x_loc, y_loc, w_in, w_out):
    nl, d, ff = w_in.shape
    f = tile_f
    nf = ff // f
    nu = nl * nf
    t = x_loc.shape[0] * x_loc.shape[1]
    piece = d // 16
    dm = (t, d, f, nf, nl)
    scale = 1.0 / (t * n_dev * d)
    rho = RHO_FRAC * math.sqrt(nl * (d + ff))
    bf, f32 = jnp.bfloat16, jnp.float32
    V, DMA = pltpu.VMEM, pltpu.SemaphoreType.DMA
    x = x_loc.transpose(1, 0, 2).reshape(t, d)
    y = y_loc.transpose(1, 0, 2).reshape(t, d)
    z_s, v_s, w_s, a_s = sds((nu, t, f), bf), sds((nu, 2, d, f), bf), sds((nu, piece, f), f32), sds((t, d), bf)

    z, v, ws, h1, q = call(
        functools.partial(first_forward, dm), 4, [z_s, v_s, w_s, a_s, a_s],
        [V((t, d), bf), V((t, d), bf), V((t, d), f32), V((t, 2 * f), bf), V((2, d, 2 * f), f32), V((2, 2 * f, d), f32), V((d, f), f32), V((2, 2, 2, d, f), bf), V((2, 2, t, f), bf),
         V((nu, piece, f), f32),
         DMA((2, 2)), DMA((2,)), DMA((2,)), DMA((2,))], "fwd_a")(x, y, w_in, w_out)

    slots = min(CORE_SLOTS, nu)
    bwd_scratch = [
        V((t, d), bf), V((t, d), bf), V((2, d, t), bf), V((2, t, f), bf), V((t, d), f32), V((2, t, f), bf), V((2, 2, d, f), bf),
        V((slots, d, f), f32), V((2, d, f), f32), V((2, d, f), f32),
        V((nu, d // 2, f), f32), V((nu, d // 4, f), f32), V((nu, d // 8, f), f32), V((nu, d // 16, f), f32), V((nu, piece, f), f32),
        DMA((2, 2)), DMA((4,)), DMA((2,)), DMA((nu,)), DMA((3, nu, 4)), pltpu.SemaphoreType.REGULAR]
    (g,) = call(functools.partial(backward, dm, scale, False), 5, [w_s], bwd_scratch, "bwd_a", 0)(x, h1, q, z, v)

    z, v, h1, q, sq = call(
        functools.partial(second_forward, dm, scale, rho), 4, [z_s, v_s, a_s, a_s, sds((8, 128), f32)],
        [V((t, d), bf), V((t, d), bf), V((t, d), f32), V((t, 2 * f), bf), V((nu, piece, f), f32), V((nu, piece, f), f32), V((nu, 2, d, f), bf), V((2, 2, t, f), bf),
         V((13, 8, 128), f32),
         DMA((nu, 2)), DMA((nu, 5)), DMA((10,)), DMA((10,)), DMA((2,)), DMA((nu,)), DMA((4,))], "fwd_b", 1)(g, ws, x, y)

    w_new, sq = call(
        functools.partial(backward, dm, scale, True), 7, [sds((nu, 2, d, f), f32), sds((8, 128), f32)],
        bwd_scratch + [V((13, 8, 128), f32), DMA((nu, 2)), DMA((nu, 5)), DMA((nu,)), DMA((10,)), DMA((10,))], "bwd_b", 2)(x, h1, q, z, v, ws, sq)

    new_in, new_out, loss = pl.pallas_call(
        functools.partial(finish, scale, f),
        grid=(nl, nf // 2),
        in_specs=[pl.BlockSpec((2, 2, d, f), lambda i, j: (i * (nf // 2) + j, 0, 0, 0)), pl.BlockSpec((8, 128), lambda i, j: (0, 0))],
        out_specs=[pl.BlockSpec((1, d, 2 * f), lambda i, j: (i, 0, j)), pl.BlockSpec((1, 2 * f, d), lambda i, j: (i, j, 0)),
                   pl.BlockSpec((1, 1), lambda i, j: (0, 0), memory_space=pltpu.SMEM)],
        out_shape=[sds((nl, d, ff), f32), sds((nl, ff, d), f32), sds((1, 1), f32)],
        compiler_params=pltpu.CompilerParams(vmem_limit_bytes=VMEM_CAP),
        name="finish")(w_new, sq)
    return new_in, new_out, loss.reshape(())


def solution(mesh):
    step = functools.partial(local_step, mesh.shape["data"], TILE_F)
    return jax.shard_map(step, mesh=mesh, in_specs=(P("data"), P("data"), P(), P()), out_specs=(P(), P(), P()), check_vma=False)
```

```python
import math
import functools
import jax
import jax.numpy as jnp
from jax import lax
from jax.experimental import pallas as pl
from jax.experimental.pallas import tpu as pltpu
from jax.sharding import PartitionSpec as P

RHO_FRAC = 0.1
LEARN_RATE = 1.0
TILE_F = 256
MESH = pl.DeviceIdType.MESH
ANY = pl.BlockSpec(memory_space=pl.ANY)
NN = (((1,), (0,)), ((), ()))
NT = (((1,), (1,)), ((), ()))
GELU_C = math.sqrt(2.0 / math.pi)
GELU_K = 0.044715
VMEM_CAP = 67043328
CORE_SLOTS = 9
RS_LAG = (0, 1, 4, 5, 6)
AG_LAG = (1, 2, 4, 5)
VG_LAG = (0, 2, 3, 5, 7, 9)


def dot(lhs, rhs, dims=NN):
    return lax.dot_general(lhs, rhs, dims, preferred_element_type=jnp.float32)


def gelu_parts(z):
    sq = z * z
    th = jnp.tanh(GELU_C * (z + GELU_K * (sq * z)))
    cdf = 0.5 * (1.0 + th)
    return sq, th, cdf


def gelu(z):
    return z * gelu_parts(z)[2]


def gelu_and_grad(z):
    sq, th, cdf = gelu_parts(z)
    slope = cdf + (0.5 * z) * ((1.0 - th * th) * (GELU_C + (3.0 * GELU_K * GELU_C) * sq))
    return z * cdf, slope


def place(axis="data"):
    me = lax.axis_index(axis)
    bits = [lax.rem(lax.div(me, 1 << k), 2) for k in range(5)]
    peers = [me + (1 << k) * (1 - 2 * bits[k]) for k in range(5)]
    return bits, peers


def route(bits, peers, unit, rows):
    core, bx, by, ba, bb = bits
    parity = lax.rem(unit + core, 2)
    _, px, py, pa, pb = peers
    b1 = jnp.where(parity == 0, bx, by)
    b3 = jnp.where(parity == 0, by, bx)
    p1 = jnp.where(parity == 0, px, py)
    p3 = jnp.where(parity == 0, py, px)
    step = rows // 16
    keep, send, base = [0], [], 0
    n = rows
    for bit in (b1, ba, b3, bb):
        n //= 2
        keep.append(pl.multiple_of(base + bit * n, step))
        send.append(pl.multiple_of(base + (1 - bit) * n, step))
        base = base + bit * n
    return (p1, pa, p3, pb), keep, send, (b1, ba, b3, bb)


def arrive(peers):
    barrier = pltpu.get_barrier_semaphore()
    for peer in peers:
        pl.semaphore_signal(barrier, inc=1, device_id=(peer,), device_id_type=MESH)
    return functools.partial(pl.semaphore_wait, barrier, len(peers))


def others(bits, me_bits):
    me = lax.axis_index("data")
    out = []
    for mask in range(1, 1 << len(me_bits)):
        peer = me
        for i, k in enumerate(me_bits):
            if mask >> i & 1:
                peer = peer + (1 << k) * (1 - 2 * bits[k])
        out.append(peer)
    return out


def exchange_sum(buf, first, peers, send_sem, recv_sem, sem0):
    copies = [remote(buf.at[first], buf.at[first + 1 + i], send_sem.at[sem0 + i], recv_sem.at[sem0 + i], peer) for i, peer in enumerate(peers)]
    for cp in copies:
        cp.start()
    total = buf[first]
    for i, cp in enumerate(copies):
        cp.wait()
        total = total + buf[first + 1 + i]
    buf[first + len(peers) + 1] = total


def gather_hops(bits, peers, unit, d, full, piece_src=None):
    ps, keep, send, _ = route(bits, peers, unit, d)
    piece = d // 16

    def rows(base, n):
        return full.at[pl.ds(base, n), :]

    def hop(k, part, sem_s, sem_r):
        peer = ps[3 - k] if k < 4 else peers[0]
        if k == 0:
            ref = rows(keep[4], piece)
        elif part == 0:
            ref = rows(keep[5 - k], piece << (k - 1))
        else:
            ref = rows(send[4 - k], piece << (k - 1))
        src = piece_src if piece_src is not None and part == 0 and k <= 1 else ref
        return remote(src, ref, sem_s, sem_r, peer)

    def arrived(k, sem_s, sem_r):
        ref = rows(send[3 - k], piece << k)
        return remote(ref, ref, sem_s, sem_r, ps[3 - k])

    def sent(sem_s, sem_r):
        ref = rows(0, 15 * piece)
        return remote(ref, ref, sem_s, sem_r, ps[0])
    return hop, arrived, sent


def remote(src, dst, send_sem, recv_sem, peer):
    return pltpu.make_async_remote_copy(src_ref=src, dst_ref=dst, send_sem=send_sem, recv_sem=recv_sem, device_id=(peer,), device_id_type=MESH)


def local(src, dst, sem):
    return pltpu.make_async_copy(src, dst, sem)


def halves(t):
    return [(0, t // 2), (t // 2, t // 2)] if t % 32 == 0 else [(0, t)]


def transpose_into(dst, src, t):
    full = t // 128
    if full:
        @pl.loop(0, full)
        def _(i):
            lo = pl.multiple_of(i * 128, 128)
            dst[:, pl.ds(lo, 128)] = src[pl.ds(lo, 128), :].T
    if t % 128:
        dst[:, full * 128:t] = src[full * 128:t, :].T


def fwd_pair(h_ref, v_ref, acc_ref, a_ref, z_ref, t, f):
    for lo, n in halves(t):
        for j in range(2):
            z = dot(h_ref[lo:lo + n, :], v_ref[j, 0]).astype(jnp.bfloat16)
            z_ref[j, lo:lo + n, :] = z
            a_ref[j, lo:lo + n, :] = gelu(z.astype(jnp.float32)).astype(jnp.bfloat16)
    v_out = jnp.concatenate([v_ref[0, 1], v_ref[1, 1]], axis=1)
    for lo, n in halves(t):
        acc_ref[lo:lo + n, :] += dot(jnp.concatenate([a_ref[0, lo:lo + n, :], a_ref[1, lo:lo + n, :]], axis=1), v_out, NT)


def fwd_close(h_ref, acc_ref, t):
    for lo, n in halves(t):
        h_ref[lo:lo + n, :] = acc_ref[lo:lo + n, :].astype(jnp.bfloat16)


def fwd_seed(h_ref, acc_ref, t):
    for lo, n in halves(t):
        acc_ref[lo:lo + n, :] = h_ref[lo:lo + n, :].astype(jnp.float32)


def fold(v):
    r, c = v.shape
    return jnp.sum(v.reshape(r // 8, 8, c // 128, 128), axis=(0, 2))


def loss_close(h_ref, y_ref, acc_ref, t, total_ref):
    n = 112 if t % 112 == 0 else t
    total_ref[...] = jnp.zeros((8, 128), jnp.float32)

    @pl.loop(0, t // n)
    def _(i):
        rows = pl.ds(pl.multiple_of(i * n, n), n)
        e = acc_ref[rows, :].astype(jnp.bfloat16).astype(jnp.float32) - y_ref[rows, :].astype(jnp.float32)
        q = e.astype(jnp.bfloat16)
        h_ref[rows, :] = q
        acc_ref[rows, :] = q.astype(jnp.float32)
        total_ref[...] += fold(e * e)


def unit_of(it, nf, nl):
    return (nl - 1 - it // nf) * nf + lax.rem(it, nf)


def first_pass(dm, scale, x_hbm, y_hbm, wi_hbm, wo_hbm, z_out, v_out, ws_out, g_out, n_out,
               h, tmp, tb, eb, acc, wi, wo, wt, zb, vb, ws, cbuf, obuf, sbuf, r1, r2, r3, r4, gs, nb,
               load_sem, z_sem, v_sem, io_sem, csend_sem, send_sem, recv_sem, credit, nsend_sem, nrecv_sem):
    t, d, f, nf, nl = dm
    nu = nf * nl
    bits, peers = place()
    piece = d // 16
    near, far = others(bits, (0, 1, 2)), others(bits, (3, 4))
    wait_all = arrive(near + far)

    def loads(p, slot):
        layer, tile = p // (nf // 2), lax.rem(p, nf // 2)
        lo = pl.multiple_of(tile * 2 * f, 2 * f)
        return (local(wi_hbm.at[layer, :, pl.ds(lo, 2 * f)], wi.at[slot], load_sem.at[slot, 0]),
                local(wo_hbm.at[layer, pl.ds(lo, 2 * f), :], wo.at[slot], load_sem.at[slot, 1]))

    def stores(p, slot):
        two = pl.ds(2 * p, 2)
        return local(zb.at[slot], z_out.at[two], z_sem.at[slot]), local(vb.at[slot], v_out.at[two], v_sem.at[slot])

    x_in = local(x_hbm, h, io_sem.at[0])
    y_in = local(y_hbm, tmp, io_sem.at[1])
    x_in.start()
    for cp in loads(0, 0):
        cp.start()
    y_in.start()
    x_in.wait()
    fwd_seed(h, acc, t)

    @pl.loop(0, nu // 2)
    def _(p):
        slot = lax.rem(p, 2)
        for cp in loads(p, slot):
            cp.wait()

        @pl.when(p + 1 < nu // 2)
        def _():
            for cp in loads(p + 1, 1 - slot):
                cp.start()

        @pl.when(p >= 2)
        def _():
            for cp in stores(p - 2, slot):
                cp.wait()
        for j in range(2):
            cols = slice(j * f, (j + 1) * f)
            wot = wo[slot, cols, :].T
            _, keep, _, _ = route(bits, peers, j, d)
            rows = pl.ds(keep[4], piece)
            vb[slot, j, 0] = wi[slot, :, cols].astype(jnp.bfloat16)
            vb[slot, j, 1] = wot.astype(jnp.bfloat16)
            wt[...] = wot
            ws[2 * p + j] = jnp.where(bits[0] == 0, wi[slot, rows, cols], wt[rows, :])

        fwd_pair(h, vb.at[slot], acc, eb, zb.at[slot], t, f)
        for cp in stores(p, slot):
            cp.start()

        @pl.when(p == nf // 2 - 1)
        def _():
            fwd_close(h, acc, t)
            fwd_seed(h, acc, t)
            transpose_into(tb.at[0], h, t)

    np_ = nu // 2
    if np_ >= 2:
        for cp in stores(np_ - 2, np_ % 2):
            cp.wait()
    spare = np_ % 2

    def tiles(it, slot):
        u = unit_of(it, nf, nl)
        return (local(z_out.at[u], zb.at[spare, slot], load_sem.at[slot, 0]), local(v_out.at[u], vb.at[spare, slot], load_sem.at[slot, 1]))
    for cp in tiles(0, 0):
        cp.start()
    ws_cp = local(ws, ws_out, io_sem.at[2])
    ws_cp.start()
    y_in.wait()
    loss_close(h, tmp, acc, t, nb.at[0])
    transpose_into(tb.at[1], h, t)
    x_again = local(x_hbm, tmp, io_sem.at[1])
    x_again.start()
    for cp in stores(np_ - 1, (np_ - 1) % 2):
        cp.wait()
    wait_all()
    nb[0] = jnp.zeros((8, 128), jnp.float32)

    def on_total(j, u, total):
        gs[u] = total
        g = total * scale
        nb[0] += fold(g * g)

    backward_phase(dm, bits, peers, h, tmp, tb, eb, acc, zb.at[spare], vb.at[spare], cbuf, obuf, sbuf, (r1, r2, r3, r4),
                   csend_sem, send_sem, recv_sem, credit, tiles, x_again.wait, on_total)
    g_cp = local(gs, g_out, io_sem.at[0])
    g_cp.start()
    exchange_sum(nb, 0, near, nsend_sem, nrecv_sem, 0)
    exchange_sum(nb, 8, far, nsend_sem, nrecv_sem, 7)
    n_cp = local(nb.at[12], n_out, io_sem.at[1])
    n_cp.start()
    ws_cp.wait()
    g_cp.wait()
    n_cp.wait()


def second_forward(dm, scale, rho, gs_hbm, ws_hbm, n_hbm, x_hbm, y_hbm, z_out, v_out, h_out, q_out, sq_out,
                   h, yb, acc, ab, gs, ws, vb, zb, nb, send_sem, recv_sem, z_sem, v_sem, io_sem):
    t, d, f, nf, nl = dm
    nu = nf * nl
    bits, peers = place()
    core = bits[0]
    piece = d // 16
    wait_all = arrive(peers)
    ins = (local(gs_hbm, gs, io_sem.at[0]), local(ws_hbm, ws, io_sem.at[1]), local(x_hbm, h, io_sem.at[2]), local(y_hbm, yb, io_sem.at[3]))
    n_in = local(n_hbm, nb, io_sem.at[4])
    n_in.start()
    for cp in ins:
        cp.start()
    n_in.wait()
    coef = rho / jnp.sqrt(jnp.sum(nb[...], keepdims=True))
    ins[0].wait()
    ins[1].wait()
    wait_all()

    def hops(u):
        return gather_hops(bits, peers, u, d, vb.at[u, core])

    def sems(u, k):
        return send_sem.at[u, 0 if k < 4 else 1], recv_sem.at[u, k]

    def core_arrived(u):
        ref = vb.at[u, 1 - core]
        return remote(ref, ref, *sems(u, 4), peers[0])

    ins[2].wait()
    fwd_seed(h, acc, t)

    def z_store(p, slot):
        return local(zb.at[slot], z_out.at[pl.ds(2 * p, 2)], z_sem.at[slot])

    @pl.loop(0, nu + VG_LAG[5])
    def _(it):
        @pl.when(it < nu)
        def _():
            _, keep, _, _ = route(bits, peers, it, d)
            new = ws[it] + coef * (gs[it] * scale)
            vb[it, core, pl.ds(keep[4], piece), :] = new.astype(jnp.bfloat16)
            hop, _, _ = hops(it)
            hop(0, 0, *sems(it, 0)).start()
            hop(1, 0, *sems(it, 1)).start()
        for k in range(1, 5):
            u = it - VG_LAG[k]

            @pl.when((u >= 0) & (u < nu))
            def _():
                hop, arrived, _ = hops(u)
                arrived(k - 1, *sems(u, k - 1)).wait_recv()
                hop(k, 1, *sems(u, k)).start()
                if k < 4:
                    hop(k + 1, 0, *sems(u, k + 1)).start()
        u = it - VG_LAG[5]

        @pl.when(u >= 0)
        def _():
            core_arrived(u).wait_recv()
            local(vb.at[u], v_out.at[u], v_sem.at[u]).start()

        @pl.when((u >= 0) & (lax.rem(u, 2) == 1))
        def _():
            p = u // 2
            slot = lax.rem(p, 2)

            @pl.when(p >= 2)
            def _():
                z_store(p - 2, slot).wait()
            fwd_pair(h, vb.at[pl.ds(2 * p, 2)], acc, ab, zb.at[slot], t, f)
            z_store(p, slot).start()

            @pl.when(p == nf // 2 - 1)
            def _():
                fwd_close(h, acc, t)
                fwd_seed(h, acc, t)
                out = local(h, h_out, io_sem.at[0])
                out.start()
                out.wait()

    ins[3].wait()
    loss_close(h, yb, acc, t, nb)
    out = local(h, q_out, io_sem.at[0])
    sq = local(nb, sq_out, io_sem.at[1])
    out.start()
    sq.start()

    @pl.loop(0, nu)
    def _(u):
        local(vb.at[u], v_out.at[u], v_sem.at[u]).wait()
        hops(u)[2](*sems(u, 0)).wait_send()
        core_arrived(u).wait_send()
    for p in range(max(nu // 2 - 2, 0), nu // 2):
        z_store(p, p % 2).wait()
    out.wait()
    sq.wait()


def backward_phase(dm, bits, peers, q, tmp, tb, eb, acc, zb, vb, cbuf, obuf, sbuf, rbuf, csend_sem, send_sem, recv_sem, credit,
                   tiles, x_ready, on_total, extra_its=0, extra=None):
    t, d, f, nf, nl = dm
    nu = nf * nl
    core = bits[0]
    piece = d // 16
    slots = cbuf.shape[0]

    def core_copy(it):
        slot = lax.rem(it, 2)
        return remote(sbuf.at[slot], cbuf.at[lax.rem(it, slots)], csend_sem.at[slot], recv_sem.at[0, it, 0], peers[0])

    def rs_sends(it, k):
        ps, _, send, on = route(bits, peers, it, d)
        n = d >> (k + 1)
        cs = lax.rem(it, slots)

        def part(off, m, sem):
            return remote(cbuf.at[cs, pl.ds(send[k] + off, m), :], rbuf[k].at[it, pl.ds(off, m), :], send_sem.at[it], sem, ps[k])
        if k == 3:
            return [part(0, n, recv_sem.at[1, it, k])]
        m = n // 2
        return [part(pl.multiple_of((1 - on[k + 1]) * m, piece), m, recv_sem.at[1, it, k]),
                part(pl.multiple_of(on[k + 1] * m, piece), m, recv_sem.at[2, it, k])]

    def rs_add(it, k, kept):
        ps, keep, send, _ = route(bits, peers, it, d)
        cs = lax.rem(it, slots)
        if k == 3:
            base, m = keep[4], d >> 4
        else:
            base, m = (keep[k + 2] if kept else send[k + 1]), d >> (k + 2)
        here = rbuf[k].at[it, pl.ds(pl.multiple_of(base - keep[k + 1], piece), m), :]
        mine = cbuf.at[cs, pl.ds(base, m), :]
        remote(mine, here, send_sem.at[it], recv_sem.at[2 if kept else 1, it, k], ps[k]).wait_recv()
        total = mine[...] + here[...]
        if k == 3:
            return total
        mine[...] = total

    def rs_sent(it):
        ref = cbuf.at[lax.rem(it, slots), pl.ds(0, 15 * piece), :]
        return remote(ref, ref, send_sem.at[it], recv_sem.at[1, it, 3], peers[0])

    @pl.loop(0, nu + RS_LAG[4] + extra_its)
    def _(it):
        @pl.when(it == nf)
        def _():
            fwd_close(q, acc, t)
            transpose_into(tb.at[1], q, t)
            x_ready()
            transpose_into(tb.at[0], tmp, t)

        @pl.when(it < nu)
        def _():
            slot = lax.rem(it, 2)
            for cp in tiles(it, slot):
                cp.wait()

            @pl.when(it + 1 < nu)
            def _():
                for cp in tiles(it + 1, 1 - slot):
                    cp.start()
            for lo, n in halves(t):
                back = dot(q[lo:lo + n, :], vb[slot, 1])
                a, slope = gelu_and_grad(zb[slot, lo:lo + n, :].astype(jnp.float32))
                eb[1, lo:lo + n, :] = a.astype(jnp.bfloat16)
                eb[0, lo:lo + n, :] = (back * slope).astype(jnp.bfloat16)

            @pl.when(it >= 2)
            def _():
                core_copy(it - 2).wait_send()
            sbuf[slot] = dot(tb[1 - core], eb[1 - core])

            @pl.when(it >= slots)
            def _():
                pl.semaphore_wait(credit, 1)
            core_copy(it).start()
            obuf[slot] = dot(tb[core], eb[core])

            @pl.when(it < nf)
            def _():
                for lo, n in halves(t):
                    acc[lo:lo + n, :] += dot(eb[0, lo:lo + n, :], vb[slot, 0], NT)

        j0 = it - RS_LAG[0]

        @pl.when((j0 >= 0) & (j0 < nu))
        def _():
            cs = lax.rem(j0, slots)
            core_copy(j0).wait_recv()
            cbuf[cs] = cbuf[cs] + obuf[lax.rem(j0, 2)]
            for cp in rs_sends(j0, 0):
                cp.start()

        for k in range(4):
            j = it - RS_LAG[k + 1]

            @pl.when((j >= 0) & (j < nu))
            def _():
                if k > 0:
                    rs_add(j, k - 1, True)
                total = rs_add(j, k, False)
                if k < 3:
                    for cp in rs_sends(j, k + 1):
                        cp.start()
                else:
                    on_total(j, unit_of(j, nf, nl), total)
                    rs_sent(j).wait_send()

                    @pl.when(j + slots < nu)
                    def _():
                        pl.semaphore_signal(credit, inc=1, device_id=(peers[0],), device_id_type=MESH)
        if extra is not None:
            extra(it)

    core_copy(nu - 2).wait_send()
    core_copy(nu - 1).wait_send()


def second_backward(dm, scale, x_hbm, h_hbm, q_hbm, z_hbm, v_hbm, ws_hbm, sq_hbm, w_out, sq_out,
                    q, tmp, tb, eb, acc, zb, vb, cbuf, obuf, sbuf, r1, r2, r3, r4, gs,
                    load_sem, io_sem, csend_sem, send_sem, recv_sem, credit, nb, ag_send, ag_recv, ag_loc, nsend_sem, nrecv_sem):
    t, d, f, nf, nl = dm
    nu = nf * nl
    bits, peers = place()
    core = bits[0]
    piece = d // 16
    near, far = others(bits, (0, 1, 2)), others(bits, (3, 4))
    wait_all = arrive(near + far)

    def tiles(it, slot):
        u = unit_of(it, nf, nl)
        return local(z_hbm.at[u], zb.at[slot], load_sem.at[slot, 0]), local(v_hbm.at[u], vb.at[slot], load_sem.at[slot, 1])

    q_in = local(q_hbm, q, io_sem.at[0])
    h_in = local(h_hbm, tmp, io_sem.at[1])
    ws_in = local(ws_hbm, gs, io_sem.at[2])
    sq_in = local(sq_hbm, nb.at[0], io_sem.at[3])
    q_in.start()
    for cp in tiles(0, 0):
        cp.start()
    for cp in (h_in, ws_in, sq_in):
        cp.start()
    q_in.wait()
    fwd_seed(q, acc, t)
    transpose_into(tb.at[1], q, t)
    h_in.wait()
    transpose_into(tb.at[0], tmp, t)
    x_in = local(x_hbm, tmp, io_sem.at[1])
    x_in.start()
    ws_in.wait()
    sq_in.wait()
    wait_all()

    def hops(it):
        return gather_hops(bits, peers, it, d, w_out.at[unit_of(it, nf, nl), core], gs.at[unit_of(it, nf, nl)])

    def sems(it, k):
        return ag_send.at[it, 0 if k < 4 else 1], ag_recv.at[it, k]

    def core_arrived(it):
        ref = w_out.at[unit_of(it, nf, nl), 1 - core]
        return remote(ref, ref, *sems(it, 4), peers[0])

    def ag_local(it):
        _, keep, _, _ = route(bits, peers, it, d)
        u = unit_of(it, nf, nl)
        return local(gs.at[u], w_out.at[u, core, pl.ds(keep[4], piece), :], ag_loc.at[it])

    def on_total(j, u, total):
        gs[u] = gs[u] - LEARN_RATE * (total * scale)
        ag_local(j).start()
        hop, _, _ = hops(j)
        hop(0, 0, *sems(j, 0)).start()
        hop(1, 0, *sems(j, 1)).start()

    def extra(it):
        for k in range(1, 5):
            j = it - RS_LAG[4] - AG_LAG[k - 1]

            @pl.when((j >= 0) & (j < nu))
            def _():
                hop, arrived, _ = hops(j)
                if k == 1:
                    ag_local(j).wait()
                arrived(k - 1, *sems(j, k - 1)).wait_recv()
                hop(k, 1, *sems(j, k)).start()
                if k < 4:
                    hop(k + 1, 0, *sems(j, k + 1)).start()

        @pl.when(it == 1)
        def _():
            exchange_sum(nb, 0, near, nsend_sem, nrecv_sem, 0)

        @pl.when(it == 2)
        def _():
            exchange_sum(nb, 8, far, nsend_sem, nrecv_sem, 7)

    backward_phase(dm, bits, peers, q, tmp, tb, eb, acc, zb, vb, cbuf, obuf, sbuf, (r1, r2, r3, r4),
                   csend_sem, send_sem, recv_sem, credit, tiles, x_in.wait, on_total, AG_LAG[3], extra)
    sq_cp = local(nb.at[12], sq_out, io_sem.at[3])
    sq_cp.start()

    @pl.loop(0, nu)
    def _(it):
        core_arrived(it).wait_recv()
        hops(it)[2](*sems(it, 0)).wait_send()
        core_arrived(it).wait_send()
    sq_cp.wait()


def finish(scale, w_ref, sq_ref, in_ref, out_ref, loss_ref):
    in_ref[0] = w_ref[0, 0]
    out_ref[0] = w_ref[0, 1].T
    loss_ref[0, 0] = 0.5 * (jnp.sum(sq_ref[...]) * scale)


def sds(shape, dtype):
    return jax.ShapeDtypeStruct(shape, dtype)


def call(kernel, n_in, outs, scratch, name, collective_id=None):
    params = dict(vmem_limit_bytes=VMEM_CAP)
    if collective_id is not None:
        params.update(collective_id=collective_id, has_side_effects=True)
    return pl.pallas_call(
        kernel,
        out_shape=outs,
        in_specs=[ANY] * n_in,
        out_specs=[ANY] * len(outs),
        scratch_shapes=scratch,
        compiler_params=pltpu.CompilerParams(**params),
        name=name,
    )


def local_step(n_dev, tile_f, x_loc, y_loc, w_in, w_out):
    nl, d, ff = w_in.shape
    f = tile_f
    nf = ff // f
    nu = nl * nf
    t = x_loc.shape[0] * x_loc.shape[1]
    piece = d // 16
    dm = (t, d, f, nf, nl)
    scale = 1.0 / (t * n_dev * d)
    rho = RHO_FRAC * math.sqrt(nl * (d + ff))
    bf, f32 = jnp.bfloat16, jnp.float32
    V, DMA = pltpu.VMEM, pltpu.SemaphoreType.DMA
    x = x_loc.transpose(1, 0, 2).reshape(t, d)
    y = y_loc.transpose(1, 0, 2).reshape(t, d)
    z_s, v_s, w_s, a_s = sds((nu, t, f), bf), sds((nu, 2, d, f), bf), sds((nu, piece, f), f32), sds((t, d), bf)

    REG = pltpu.SemaphoreType.REGULAR
    slots = min(CORE_SLOTS, nu)
    n_s = sds((8, 128), f32)
    reduce_bufs = [V((slots, d, f), f32), V((2, d, f), f32), V((2, d, f), f32),
                   V((nu, d // 2, f), f32), V((nu, d // 4, f), f32), V((nu, d // 8, f), f32), V((nu, d // 16, f), f32), V((nu, piece, f), f32)]
    acts = [V((t, d), bf), V((t, d), bf), V((2, d, t), bf), V((2, t, f), bf), V((t, d), f32)]

    z, v, ws, g, norm = call(
        functools.partial(first_pass, dm, scale), 4, [z_s, v_s, w_s, w_s, n_s],
        acts + [V((2, d, 2 * f), f32), V((2, 2 * f, d), f32), V((d, f), f32), V((2, 2, t, f), bf), V((2, 2, 2, d, f), bf), V((nu, piece, f), f32)]
        + reduce_bufs + [V((13, 8, 128), f32), DMA((2, 2)), DMA((2,)), DMA((2,)), DMA((3,)), DMA((2,)), DMA((nu,)), DMA((3, nu, 4)), REG, DMA((10,)), DMA((10,))],
        "pass_a", 0)(x, y, w_in, w_out)

    z, v, h1, q, sq = call(
        functools.partial(second_forward, dm, scale, rho), 5, [z_s, v_s, a_s, a_s, n_s],
        [V((t, d), bf), V((t, d), bf), V((t, d), f32), V((2, t, f), bf), V((nu, piece, f), f32), V((nu, piece, f), f32), V((nu, 2, d, f), bf), V((2, 2, t, f), bf),
         V((8, 128), f32), DMA((nu, 2)), DMA((nu, 5)), DMA((2,)), DMA((nu,)), DMA((5,))], "fwd_b", 1)(g, ws, norm, x, y)

    w_new, sq = call(
        functools.partial(second_backward, dm, scale), 7, [sds((nu, 2, d, f), f32), n_s],
        acts + [V((2, t, f), bf), V((2, 2, d, f), bf)] + reduce_bufs + [DMA((2, 2)), DMA((4,)), DMA((2,)), DMA((nu,)), DMA((3, nu, 4)), REG,
         V((13, 8, 128), f32), DMA((nu, 2)), DMA((nu, 5)), DMA((nu,)), DMA((10,)), DMA((10,))], "bwd_b", 2)(x, h1, q, z, v, ws, sq)

    new_in, new_out, loss = pl.pallas_call(
        functools.partial(finish, scale),
        grid=(nl, nf),
        in_specs=[pl.BlockSpec((1, 2, d, f), lambda i, j: (i * nf + j, 0, 0, 0)), pl.BlockSpec((8, 128), lambda i, j: (0, 0))],
        out_specs=[pl.BlockSpec((1, d, f), lambda i, j: (i, 0, j)), pl.BlockSpec((1, f, d), lambda i, j: (i, j, 0)),
                   pl.BlockSpec((1, 1), lambda i, j: (0, 0), memory_space=pltpu.SMEM)],
        out_shape=[sds((nl, d, ff), f32), sds((nl, ff, d), f32), sds((1, 1), f32)],
        compiler_params=pltpu.CompilerParams(vmem_limit_bytes=VMEM_CAP),
        name="finish")(w_new, sq)
    return new_in, new_out, loss.reshape(())


def solution(mesh):
    step = functools.partial(local_step, mesh.shape["data"], TILE_F)
    return jax.shard_map(step, mesh=mesh, in_specs=(P("data"), P("data"), P(), P()), out_specs=(P(), P(), P()), check_vma=False)
```

```python
import math
import functools
import jax
import jax.numpy as jnp
from jax import lax
from jax.experimental import pallas as pl
from jax.experimental.pallas import tpu as pltpu
from jax.sharding import PartitionSpec as P

RHO_FRAC = 0.1
LEARN_RATE = 1.0
TILE_F = 256
MESH = pl.DeviceIdType.MESH
ANY = pl.BlockSpec(memory_space=pl.ANY)
NN = (((1,), (0,)), ((), ()))
NT = (((1,), (1,)), ((), ()))
GELU_C = math.sqrt(2.0 / math.pi)
GELU_K = 0.044715
VMEM_CAP = 67043328
CORE_SLOTS = 9
LAG_A = (0, 1, 4, 5, 7)
LAG_B = (0, 1, 4, 6, 7)
AG_LAG = (2, 3, 5, 6)
VG_LAG = (0, 2, 3, 5, 7, 9)


def dot(lhs, rhs, dims=NN):
    return lax.dot_general(lhs, rhs, dims, preferred_element_type=jnp.float32)


def gelu_parts(z):
    sq = z * z
    th = jnp.tanh(GELU_C * (z + GELU_K * (sq * z)))
    cdf = 0.5 * (1.0 + th)
    return sq, th, cdf


def gelu(z):
    return z * gelu_parts(z)[2]


def gelu_and_grad(z):
    sq, th, cdf = gelu_parts(z)
    slope = cdf + (0.5 * z) * ((1.0 - th * th) * (GELU_C + (3.0 * GELU_K * GELU_C) * sq))
    return z * cdf, slope


def place(axis="data"):
    me = lax.axis_index(axis)
    bits = [lax.rem(lax.div(me, 1 << k), 2) for k in range(5)]
    peers = [me + (1 << k) * (1 - 2 * bits[k]) for k in range(5)]
    return bits, peers


def route(bits, peers, unit, rows):
    core, bx, by, ba, bb = bits
    _, px, py, pa, pb = peers
    swap = lax.rem(unit + core, 2) == 1
    b1, p1 = jnp.where(swap, by, bx), jnp.where(swap, py, px)
    b3, p3 = jnp.where(swap, bx, by), jnp.where(swap, px, py)
    axes = (b1, ba, b3, bb)
    step = rows // 16
    keep, send, base = [0], [], 0
    n = rows
    for bit in axes:
        n //= 2
        keep.append(pl.multiple_of(base + bit * n, step))
        send.append(pl.multiple_of(base + (1 - bit) * n, step))
        base = base + bit * n
    return (p1, pa, p3, pb), keep, send, axes


def arrive(peers):
    barrier = pltpu.get_barrier_semaphore()
    for peer in peers:
        pl.semaphore_signal(barrier, inc=1, device_id=(peer,), device_id_type=MESH)
    return functools.partial(pl.semaphore_wait, barrier, len(peers))


def others(bits, me_bits):
    me = lax.axis_index("data")
    out = []
    for mask in range(1, 1 << len(me_bits)):
        peer = me
        for i, k in enumerate(me_bits):
            if mask >> i & 1:
                peer = peer + (1 << k) * (1 - 2 * bits[k])
        out.append(peer)
    return out


def exchange_sum(buf, first, peers, send_sem, recv_sem, sem0):
    copies = [remote(buf.at[first], buf.at[first + 1 + i], send_sem.at[sem0 + i], recv_sem.at[sem0 + i], peer) for i, peer in enumerate(peers)]
    for cp in copies:
        cp.start()
    total = buf[first]
    for i, cp in enumerate(copies):
        cp.wait()
        total = total + buf[first + 1 + i]
    buf[first + len(peers) + 1] = total


def gather_hops(bits, peers, unit, d, full, piece_src=None):
    ps, keep, send, _ = route(bits, peers, unit, d)
    piece = d // 16

    def rows(base, n):
        return full.at[pl.ds(base, n), :]

    def hop(k, part, sem_s, sem_r):
        peer = ps[3 - k] if k < 4 else peers[0]
        if k == 0:
            ref = rows(keep[4], piece)
        elif part == 0:
            ref = rows(keep[5 - k], piece << (k - 1))
        else:
            ref = rows(send[4 - k], piece << (k - 1))
        src = piece_src if piece_src is not None and part == 0 and k <= 1 else ref
        return remote(src, ref, sem_s, sem_r, peer)

    def arrived(k, sem_s, sem_r):
        ref = rows(send[3 - k], piece << k)
        return remote(ref, ref, sem_s, sem_r, ps[3 - k])

    def sent(sem_s, sem_r):
        ref = rows(0, 15 * piece)
        return remote(ref, ref, sem_s, sem_r, ps[0])
    return hop, arrived, sent


def remote(src, dst, send_sem, recv_sem, peer):
    return pltpu.make_async_remote_copy(src_ref=src, dst_ref=dst, send_sem=send_sem, recv_sem=recv_sem, device_id=(peer,), device_id_type=MESH)


def local(src, dst, sem):
    return pltpu.make_async_copy(src, dst, sem)


def halves(t):
    return [(0, t // 2), (t // 2, t // 2)] if t % 32 == 0 else [(0, t)]


def transpose_into(dst, src, t):
    full = t // 128
    if full:
        @pl.loop(0, full)
        def _(i):
            lo = pl.multiple_of(i * 128, 128)
            dst[:, pl.ds(lo, 128)] = src[pl.ds(lo, 128), :].T
    if t % 128:
        dst[:, full * 128:t] = src[full * 128:t, :].T


def fwd_pair(h_ref, v_ref, acc_ref, a_ref, z_ref, t, f):
    for lo, n in halves(t):
        for j in range(2):
            z = dot(h_ref[lo:lo + n, :], v_ref[j, 0]).astype(jnp.bfloat16)
            z_ref[j, lo:lo + n, :] = z
            a_ref[lo:lo + n, j * f:(j + 1) * f] = gelu(z.astype(jnp.float32)).astype(jnp.bfloat16)
    v_out = jnp.concatenate([v_ref[0, 1], v_ref[1, 1]], axis=1)
    for lo, n in halves(t):
        acc_ref[lo:lo + n, :] += dot(a_ref[lo:lo + n, :], v_out, NT)


def fwd_close(h_ref, acc_ref, t):
    for lo, n in halves(t):
        h_ref[lo:lo + n, :] = acc_ref[lo:lo + n, :].astype(jnp.bfloat16)


def fwd_seed(h_ref, acc_ref, t):
    for lo, n in halves(t):
        acc_ref[lo:lo + n, :] = h_ref[lo:lo + n, :].astype(jnp.float32)


def fold(v):
    r, c = v.shape
    rows = jnp.sum(v.reshape(r // 8, 8, c), axis=0)
    return sum(rows[:, lo:lo + 128] for lo in range(0, c, 128))


def loss_close(h_ref, y_ref, acc_ref, t, d, total_ref=None):
    def rows_of(rows):
        e = acc_ref[rows, :].astype(jnp.bfloat16).astype(jnp.float32) - y_ref[rows, :].astype(jnp.float32)
        q = e.astype(jnp.bfloat16)
        h_ref[rows, :] = q
        acc_ref[rows, :] = q.astype(jnp.float32)
        return e
    if total_ref is None:
        for lo, n in halves(t):
            rows_of(slice(lo, lo + n))
        return
    n = 112 if t % 112 == 0 else t
    total_ref[...] = jnp.zeros((8, 128), jnp.float32)

    @pl.loop(0, t // n)
    def _(i):
        e = rows_of(pl.ds(pl.multiple_of(i * n, n), n))
        total_ref[...] += fold(e * e)


def unit_of(it, nf, nl):
    return (nl - 1 - it // nf) * nf + lax.rem(it, nf)


def first_pass(dm, scale, x_hbm, y_hbm, wi_hbm, wo_hbm, z_out, v_out, ws_out, g_out, n_out,
               h, tmp, tb, eb, acc, ab, wi, wo, zb, vb, ws, cbuf, obuf, sbuf, r1, r2, r3, r4, gs, nb,
               load_sem, z_sem, v_sem, io_sem, csend_sem, send_sem, recv_sem, credit, nsend_sem, nrecv_sem):
    t, d, f, nf, nl = dm
    nu = nf * nl
    bits, peers = place()
    piece = d // 16
    near, far = others(bits, (0, 1, 2)), others(bits, (3, 4))
    wait_all = arrive(near + far)

    def loads(p, slot):
        layer, tile = p // (nf // 2), lax.rem(p, nf // 2)
        lo = pl.multiple_of(tile * 2 * f, 2 * f)
        return (local(wi_hbm.at[layer, :, pl.ds(lo, 2 * f)], wi.at[slot], load_sem.at[slot, 0]),
                local(wo_hbm.at[layer, pl.ds(lo, 2 * f), :], wo.at[slot], load_sem.at[slot, 1]))

    def stores(p, slot):
        two = pl.ds(2 * p, 2)
        return local(zb.at[slot], z_out.at[two], z_sem.at[slot]), local(vb.at[slot], v_out.at[two], v_sem.at[slot])

    x_in = local(x_hbm, h, io_sem.at[0])
    y_in = local(y_hbm, tmp, io_sem.at[1])
    x_in.start()
    for cp in loads(0, 0):
        cp.start()
    y_in.start()
    x_in.wait()
    fwd_seed(h, acc, t)

    @pl.loop(0, nu // 2)
    def _(p):
        slot = lax.rem(p, 2)
        for cp in loads(p, slot):
            cp.wait()

        @pl.when(p + 1 < nu // 2)
        def _():
            for cp in loads(p + 1, 1 - slot):
                cp.start()

        @pl.when(p >= 2)
        def _():
            for cp in stores(p - 2, slot):
                cp.wait()
        for j in range(2):
            cols = slice(j * f, (j + 1) * f)
            wot = wo[slot, cols, :].T
            _, keep, _, _ = route(bits, peers, 2 * p + j, d)
            rows = pl.ds(keep[4], piece)
            vb[slot, j, 0] = wi[slot, :, cols].astype(jnp.bfloat16)
            vb[slot, j, 1] = wot.astype(jnp.bfloat16)
            obuf[j] = wot
            ws[2 * p + j] = jnp.where(bits[0] == 0, wi[slot, rows, cols], obuf[j, rows, :])

        fwd_pair(h, vb.at[slot], acc, ab, zb.at[slot], t, f)
        for cp in stores(p, slot):
            cp.start()

        @pl.when(p == nf // 2 - 1)
        def _():
            fwd_close(h, acc, t)
            fwd_seed(h, acc, t)
            transpose_into(tb.at[0], h, t)

    np_ = nu // 2
    if np_ >= 2:
        for cp in stores(np_ - 2, np_ % 2):
            cp.wait()
    spare = np_ % 2

    def tiles(it, slot):
        u = unit_of(it, nf, nl)
        return (local(z_out.at[u], zb.at[spare, slot], load_sem.at[slot, 0]), local(v_out.at[u], vb.at[spare, slot], load_sem.at[slot, 1]))
    for cp in tiles(0, 0):
        cp.start()
    ws_cp = local(ws, ws_out, io_sem.at[2])
    ws_cp.start()
    y_in.wait()
    loss_close(h, tmp, acc, t, d)
    transpose_into(tb.at[1], h, t)
    x_again = local(x_hbm, tmp, io_sem.at[1])
    x_again.start()
    for cp in stores(np_ - 1, (np_ - 1) % 2):
        cp.wait()
    wait_all()
    nb[0] = jnp.zeros((8, 128), jnp.float32)

    def on_total(j, u, total):
        gs[u] = total
        g = total * scale
        nb[0] += fold(g * g)

    backward_phase(dm, bits, peers, h, tmp, tb, eb, acc, zb.at[spare], vb.at[spare], cbuf, obuf, sbuf, (r1, r2, r3, r4),
                   csend_sem, send_sem, recv_sem, credit, tiles, x_again.wait, on_total, LAG_A)
    g_cp = local(gs, g_out, io_sem.at[0])
    g_cp.start()
    exchange_sum(nb, 0, near, nsend_sem, nrecv_sem, 0)
    exchange_sum(nb, 8, far, nsend_sem, nrecv_sem, 7)
    n_cp = local(nb.at[12], n_out, io_sem.at[1])
    n_cp.start()
    ws_cp.wait()
    g_cp.wait()
    n_cp.wait()


def second_forward(dm, scale, rho, gs_hbm, ws_hbm, n_hbm, x_hbm, y_hbm, z_out, v_out, h_out, q_out, sq_out,
                   h, yb, acc, ab, gs, ws, vb, zb, nb, send_sem, recv_sem, z_sem, v_sem, io_sem):
    t, d, f, nf, nl = dm
    nu = nf * nl
    bits, peers = place()
    core = bits[0]
    piece = d // 16
    wait_all = arrive(peers)
    ins = (local(gs_hbm, gs, io_sem.at[0]), local(ws_hbm, ws, io_sem.at[1]), local(x_hbm, h, io_sem.at[2]), local(y_hbm, yb, io_sem.at[3]))
    n_in = local(n_hbm, nb, io_sem.at[4])
    n_in.start()
    for cp in ins:
        cp.start()
    n_in.wait()
    coef = rho / jnp.sqrt(jnp.sum(nb[...], keepdims=True))
    ins[0].wait()
    ins[1].wait()
    wait_all()

    def hops(u):
        return gather_hops(bits, peers, u, d, vb.at[u, core])

    def sems(u, k):
        return send_sem.at[u, 0 if k < 4 else 1], recv_sem.at[u, k]

    def core_arrived(u):
        ref = vb.at[u, 1 - core]
        return remote(ref, ref, *sems(u, 4), peers[0])

    def z_store(p, slot):
        return local(zb.at[slot], z_out.at[pl.ds(2 * p, 2)], z_sem.at[slot])

    @pl.loop(0, nu + VG_LAG[5])
    def _(it):
        @pl.when(it < nu)
        def _():
            _, keep, _, _ = route(bits, peers, it, d)
            new = ws[it] + coef * (gs[it] * scale)
            vb[it, core, pl.ds(keep[4], piece), :] = new.astype(jnp.bfloat16)
            hop, _, _ = hops(it)
            hop(0, 0, *sems(it, 0)).start()
            hop(1, 0, *sems(it, 1)).start()
        for k in range(1, 5):
            u = it - VG_LAG[k]

            @pl.when((u >= 0) & (u < nu))
            def _():
                hop, arrived, _ = hops(u)
                arrived(k - 1, *sems(u, k - 1)).wait_recv()
                hop(k, 1, *sems(u, k)).start()
                if k < 4:
                    hop(k + 1, 0, *sems(u, k + 1)).start()
        u = it - VG_LAG[5]

        @pl.when(u >= 0)
        def _():
            core_arrived(u).wait_recv()
            local(vb.at[u], v_out.at[u], v_sem.at[u]).start()

        @pl.when((u >= 0) & (lax.rem(u, 2) == 1))
        def _():
            p = u // 2
            slot = lax.rem(p, 2)

            @pl.when(p >= 2)
            def _():
                z_store(p - 2, slot).wait()

            @pl.when(p == 0)
            def _():
                ins[2].wait()
                fwd_seed(h, acc, t)
            fwd_pair(h, vb.at[pl.ds(2 * p, 2)], acc, ab, zb.at[slot], t, f)
            z_store(p, slot).start()

            @pl.when(p == nf // 2 - 1)
            def _():
                fwd_close(h, acc, t)
                fwd_seed(h, acc, t)
                out = local(h, h_out, io_sem.at[0])
                out.start()
                out.wait()

    ins[3].wait()
    loss_close(h, yb, acc, t, d, nb)
    out = local(h, q_out, io_sem.at[0])
    sq = local(nb, sq_out, io_sem.at[1])
    out.start()
    sq.start()

    @pl.loop(0, nu)
    def _(u):
        local(vb.at[u], v_out.at[u], v_sem.at[u]).wait()
        hops(u)[2](*sems(u, 0)).wait_send()
        core_arrived(u).wait_send()
    for p in range(max(nu // 2 - 2, 0), nu // 2):
        z_store(p, p % 2).wait()
    out.wait()
    sq.wait()


def backward_phase(dm, bits, peers, q, tmp, tb, eb, acc, zb, vb, cbuf, obuf, sbuf, rbuf, csend_sem, send_sem, recv_sem, credit,
                   tiles, x_ready, on_total, lag, extra_its=0, extra=None):
    t, d, f, nf, nl = dm
    nu = nf * nl
    core = bits[0]
    piece = d // 16
    slots = cbuf.shape[0]

    def core_copy(it):
        slot = lax.rem(it, 2)
        return remote(sbuf.at[slot], cbuf.at[lax.rem(it, slots)], csend_sem.at[slot], recv_sem.at[0, it, 0], peers[0])

    def rs_sends(it, k):
        ps, _, send, on = route(bits, peers, unit_of(it, nf, nl), d)
        n = d >> (k + 1)
        cs = lax.rem(it, slots)

        def part(off, m, sem):
            return remote(cbuf.at[cs, pl.ds(send[k] + off, m), :], rbuf[k].at[it, pl.ds(off, m), :], send_sem.at[it], sem, ps[k])
        if k == 3:
            return [part(0, n, recv_sem.at[1, it, k])]
        m = n // 2
        return [part(pl.multiple_of((1 - on[k + 1]) * m, piece), m, recv_sem.at[1, it, k]),
                part(pl.multiple_of(on[k + 1] * m, piece), m, recv_sem.at[2, it, k])]

    def rs_add(it, k, kept):
        ps, keep, send, _ = route(bits, peers, unit_of(it, nf, nl), d)
        cs = lax.rem(it, slots)
        if k == 3:
            base, m = keep[4], d >> 4
        else:
            base, m = (keep[k + 2] if kept else send[k + 1]), d >> (k + 2)
        here = rbuf[k].at[it, pl.ds(pl.multiple_of(base - keep[k + 1], piece), m), :]
        mine = cbuf.at[cs, pl.ds(base, m), :]
        remote(mine, here, send_sem.at[it], recv_sem.at[2 if kept else 1, it, k], ps[k]).wait_recv()
        total = mine[...] + here[...]
        if k == 3:
            return total
        mine[...] = total

    def rs_sent(it):
        ref = cbuf.at[lax.rem(it, slots), pl.ds(0, 15 * piece), :]
        return remote(ref, ref, send_sem.at[it], recv_sem.at[1, it, 3], peers[0])

    @pl.loop(0, nu + lag[4] + extra_its)
    def _(it):
        @pl.when(it == nf)
        def _():
            fwd_close(q, acc, t)
            transpose_into(tb.at[1], q, t)
            x_ready()
            transpose_into(tb.at[0], tmp, t)

        @pl.when(it < nu)
        def _():
            slot = lax.rem(it, 2)
            for cp in tiles(it, slot):
                cp.wait()

            @pl.when(it + 1 < nu)
            def _():
                for cp in tiles(it + 1, 1 - slot):
                    cp.start()
            for lo, n in halves(t):
                back = dot(q[lo:lo + n, :], vb[slot, 1])
                a, slope = gelu_and_grad(zb[slot, lo:lo + n, :].astype(jnp.float32))
                eb[1, lo:lo + n, :] = a.astype(jnp.bfloat16)
                eb[0, lo:lo + n, :] = (back * slope).astype(jnp.bfloat16)

            @pl.when(it >= 2)
            def _():
                core_copy(it - 2).wait_send()
            sbuf[slot] = dot(tb[1 - core], eb[1 - core])

            @pl.when(it >= slots)
            def _():
                pl.semaphore_wait(credit, 1)
            core_copy(it).start()
            obuf[slot] = dot(tb[core], eb[core])

            @pl.when(it < nf)
            def _():
                for lo, n in halves(t):
                    acc[lo:lo + n, :] += dot(eb[0, lo:lo + n, :], vb[slot, 0], NT)

        j0 = it - lag[0]

        @pl.when((j0 >= 0) & (j0 < nu))
        def _():
            cs = lax.rem(j0, slots)
            core_copy(j0).wait_recv()
            cbuf[cs] = cbuf[cs] + obuf[lax.rem(j0, 2)]
            for cp in rs_sends(j0, 0):
                cp.start()

        for k in range(4):
            j = it - lag[k + 1]

            @pl.when((j >= 0) & (j < nu))
            def _():
                if k > 0:
                    rs_add(j, k - 1, True)
                total = rs_add(j, k, False)
                if k < 3:
                    for cp in rs_sends(j, k + 1):
                        cp.start()
                else:
                    on_total(j, unit_of(j, nf, nl), total)
                    rs_sent(j).wait_send()

                    @pl.when(j + slots < nu)
                    def _():
                        pl.semaphore_signal(credit, inc=1, device_id=(peers[0],), device_id_type=MESH)
        if extra is not None:
            extra(it)

    core_copy(nu - 2).wait_send()
    core_copy(nu - 1).wait_send()


def second_backward(dm, scale, x_hbm, h_hbm, q_hbm, z_hbm, v_hbm, ws_hbm, sq_hbm, w_out, sq_out,
                    q, tmp, tb, eb, acc, zb, vb, cbuf, obuf, sbuf, r1, r2, r3, r4, gs,
                    load_sem, io_sem, csend_sem, send_sem, recv_sem, credit, nb, ag_send, ag_recv, ag_loc, nsend_sem, nrecv_sem):
    t, d, f, nf, nl = dm
    nu = nf * nl
    bits, peers = place()
    core = bits[0]
    piece = d // 16
    near, far = others(bits, (0, 1, 2)), others(bits, (3, 4))
    wait_all = arrive(near + far)

    def tiles(it, slot):
        u = unit_of(it, nf, nl)
        return local(z_hbm.at[u], zb.at[slot], load_sem.at[slot, 0]), local(v_hbm.at[u], vb.at[slot], load_sem.at[slot, 1])

    q_in = local(q_hbm, q, io_sem.at[0])
    h_in = local(h_hbm, tmp, io_sem.at[1])
    ws_in = local(ws_hbm, gs, io_sem.at[2])
    sq_in = local(sq_hbm, nb.at[0], io_sem.at[3])
    q_in.start()
    for cp in tiles(0, 0):
        cp.start()
    for cp in (h_in, ws_in, sq_in):
        cp.start()
    q_in.wait()
    fwd_seed(q, acc, t)
    transpose_into(tb.at[1], q, t)
    h_in.wait()
    transpose_into(tb.at[0], tmp, t)
    x_in = local(x_hbm, tmp, io_sem.at[1])
    x_in.start()
    ws_in.wait()
    sq_in.wait()
    wait_all()

    def hops(it):
        return gather_hops(bits, peers, unit_of(it, nf, nl), d, w_out.at[unit_of(it, nf, nl), core], gs.at[unit_of(it, nf, nl)])

    def sems(it, k):
        return ag_send.at[it, 0 if k < 4 else 1], ag_recv.at[it, k]

    def core_arrived(it):
        ref = w_out.at[unit_of(it, nf, nl), 1 - core]
        return remote(ref, ref, *sems(it, 4), peers[0])

    def ag_local(it):
        _, keep, _, _ = route(bits, peers, unit_of(it, nf, nl), d)
        u = unit_of(it, nf, nl)
        return local(gs.at[u], w_out.at[u, core, pl.ds(keep[4], piece), :], ag_loc.at[it])

    def on_total(j, u, total):
        gs[u] = gs[u] - LEARN_RATE * (total * scale)
        ag_local(j).start()
        hop, _, _ = hops(j)
        hop(0, 0, *sems(j, 0)).start()
        hop(1, 0, *sems(j, 1)).start()

    def extra(it):
        for k in range(1, 5):
            j = it - LAG_B[4] - AG_LAG[k - 1]

            @pl.when((j >= 0) & (j < nu))
            def _():
                hop, arrived, _ = hops(j)
                if k == 1:
                    ag_local(j).wait()
                arrived(k - 1, *sems(j, k - 1)).wait_recv()
                hop(k, 1, *sems(j, k)).start()
                if k < 4:
                    hop(k + 1, 0, *sems(j, k + 1)).start()

        @pl.when(it == 1)
        def _():
            exchange_sum(nb, 0, near, nsend_sem, nrecv_sem, 0)

        @pl.when(it == 2)
        def _():
            exchange_sum(nb, 8, far, nsend_sem, nrecv_sem, 7)

    backward_phase(dm, bits, peers, q, tmp, tb, eb, acc, zb, vb, cbuf, obuf, sbuf, (r1, r2, r3, r4),
                   csend_sem, send_sem, recv_sem, credit, tiles, x_in.wait, on_total, LAG_B, AG_LAG[3], extra)
    sq_cp = local(nb.at[12], sq_out, io_sem.at[3])
    sq_cp.start()

    @pl.loop(0, nu)
    def _(it):
        core_arrived(it).wait_recv()
        hops(it)[2](*sems(it, 0)).wait_send()
        core_arrived(it).wait_send()
    sq_cp.wait()


def finish(scale, f, w_ref, sq_ref, in_ref, out_ref, loss_ref):
    for j in range(w_ref.shape[0]):
        in_ref[0, :, j * f:(j + 1) * f] = w_ref[j, 0]
        out_ref[0, j * f:(j + 1) * f, :] = w_ref[j, 1].T
    loss_ref[0, 0] = 0.5 * (jnp.sum(sq_ref[...]) * scale)


def sds(shape, dtype):
    return jax.ShapeDtypeStruct(shape, dtype)


def call(kernel, n_in, outs, scratch, name, collective_id=None):
    params = dict(vmem_limit_bytes=VMEM_CAP)
    if collective_id is not None:
        params.update(collective_id=collective_id, has_side_effects=True)
    return pl.pallas_call(
        kernel,
        out_shape=outs,
        in_specs=[ANY] * n_in,
        out_specs=[ANY] * len(outs),
        scratch_shapes=scratch,
        compiler_params=pltpu.CompilerParams(**params),
        name=name,
    )


def local_step(n_dev, tile_f, x_loc, y_loc, w_in, w_out):
    nl, d, ff = w_in.shape
    f = tile_f
    nf = ff // f
    nu = nl * nf
    t = x_loc.shape[0] * x_loc.shape[1]
    piece = d // 16
    dm = (t, d, f, nf, nl)
    scale = 1.0 / (t * n_dev * d)
    rho = RHO_FRAC * math.sqrt(nl * (d + ff))
    bf, f32 = jnp.bfloat16, jnp.float32
    V, DMA = pltpu.VMEM, pltpu.SemaphoreType.DMA
    x = x_loc.transpose(1, 0, 2).reshape(t, d)
    y = y_loc.transpose(1, 0, 2).reshape(t, d)
    z_s, v_s, w_s, a_s = sds((nu, t, f), bf), sds((nu, 2, d, f), bf), sds((nu, piece, f), f32), sds((t, d), bf)

    REG = pltpu.SemaphoreType.REGULAR
    slots = min(CORE_SLOTS, nu)
    n_s = sds((8, 128), f32)
    reduce_bufs = [V((slots, d, f), f32), V((2, d, f), f32), V((2, d, f), f32),
                   V((nu, d // 2, f), f32), V((nu, d // 4, f), f32), V((nu, d // 8, f), f32), V((nu, d // 16, f), f32), V((nu, piece, f), f32)]
    acts = [V((t, d), bf), V((t, d), bf), V((2, d, t), bf), V((2, t, f), bf), V((t, d), f32)]

    z, v, ws, g, norm = call(
        functools.partial(first_pass, dm, scale), 4, [z_s, v_s, w_s, w_s, n_s],
        acts + [V((t, 2 * f), bf), V((2, d, 2 * f), f32), V((2, 2 * f, d), f32), V((2, 2, t, f), bf), V((2, 2, 2, d, f), bf), V((nu, piece, f), f32)]
        + reduce_bufs + [V((13, 8, 128), f32), DMA((2, 2)), DMA((2,)), DMA((2,)), DMA((3,)), DMA((2,)), DMA((nu,)), DMA((3, nu, 4)), REG, DMA((10,)), DMA((10,))],
        "pass_a", 0)(x, y, w_in, w_out)

    z, v, h1, q, sq = call(
        functools.partial(second_forward, dm, scale, rho), 5, [z_s, v_s, a_s, a_s, n_s],
        [V((t, d), bf), V((t, d), bf), V((t, d), f32), V((t, 2 * f), bf), V((nu, piece, f), f32), V((nu, piece, f), f32), V((nu, 2, d, f), bf), V((2, 2, t, f), bf),
         V((8, 128), f32), DMA((nu, 2)), DMA((nu, 5)), DMA((2,)), DMA((nu,)), DMA((5,))], "fwd_b", 1)(g, ws, norm, x, y)

    w_new, sq = call(
        functools.partial(second_backward, dm, scale), 7, [sds((nu, 2, d, f), f32), n_s],
        acts + [V((2, t, f), bf), V((2, 2, d, f), bf)] + reduce_bufs + [DMA((2, 2)), DMA((4,)), DMA((2,)), DMA((nu,)), DMA((3, nu, 4)), REG,
         V((13, 8, 128), f32), DMA((nu, 2)), DMA((nu, 5)), DMA((nu,)), DMA((10,)), DMA((10,))], "bwd_b", 2)(x, h1, q, z, v, ws, sq)

    new_in, new_out, loss = pl.pallas_call(
        functools.partial(finish, scale, f),
        grid=(nl, nf // 4),
        in_specs=[pl.BlockSpec((4, 2, d, f), lambda i, j: (i * (nf // 4) + j, 0, 0, 0)), pl.BlockSpec((8, 128), lambda i, j: (0, 0))],
        out_specs=[pl.BlockSpec((1, d, 4 * f), lambda i, j: (i, 0, j)), pl.BlockSpec((1, 4 * f, d), lambda i, j: (i, j, 0)),
                   pl.BlockSpec((1, 1), lambda i, j: (0, 0), memory_space=pltpu.SMEM)],
        out_shape=[sds((nl, d, ff), f32), sds((nl, ff, d), f32), sds((1, 1), f32)],
        compiler_params=pltpu.CompilerParams(vmem_limit_bytes=VMEM_CAP),
        name="finish")(w_new, sq)
    return new_in, new_out, loss.reshape(())


def solution(mesh):
    step = functools.partial(local_step, mesh.shape["data"], TILE_F)
    return jax.shard_map(step, mesh=mesh, in_specs=(P("data"), P("data"), P(), P()), out_specs=(P(), P(), P()), check_vma=False)
```

```python
import math
import functools
import jax
import jax.numpy as jnp
from jax import lax
from jax.experimental import pallas as pl
from jax.experimental.pallas import tpu as pltpu
from jax.sharding import PartitionSpec as P

RHO_FRAC = 0.1
LEARN_RATE = 1.0
TILE_F = 256
MESH = pl.DeviceIdType.MESH
ANY = pl.BlockSpec(memory_space=pl.ANY)
NN = (((1,), (0,)), ((), ()))
NT = (((1,), (1,)), ((), ()))
GELU_C = math.sqrt(2.0 / math.pi)
GELU_K = 0.044715
VMEM_CAP = 67043328
CORE_SLOTS = 9
LAG_A = (0, 1, 4, 5, 7)
LAG_B = (0, 1, 2, 3, 4, 4, 5, 7, 8, 9, 12)
VG_LAG = (0, 2, 3, 5, 7, 9)


def dot(lhs, rhs, dims=NN):
    return lax.dot_general(lhs, rhs, dims, preferred_element_type=jnp.float32)


def gelu_parts(z):
    sq = z * z
    th = jnp.tanh(GELU_C * (z + GELU_K * (sq * z)))
    cdf = 0.5 * (1.0 + th)
    return sq, th, cdf


def gelu(z):
    return z * gelu_parts(z)[2]


def gelu_and_grad(z):
    sq, th, cdf = gelu_parts(z)
    slope = cdf + (0.5 * z) * ((1.0 - th * th) * (GELU_C + (3.0 * GELU_K * GELU_C) * sq))
    return z * cdf, slope


def place(axis="data"):
    me = lax.axis_index(axis)
    bits = [lax.rem(lax.div(me, 1 << k), 2) for k in range(5)]
    peers = [me + (1 << k) * (1 - 2 * bits[k]) for k in range(5)]
    return bits, peers


def route(bits, peers, unit, rows):
    core, bx, by, ba, bb = bits
    _, px, py, pa, pb = peers
    swap = lax.rem(unit + core, 2) == 1
    b1, p1 = jnp.where(swap, by, bx), jnp.where(swap, py, px)
    b3, p3 = jnp.where(swap, bx, by), jnp.where(swap, px, py)
    axes = (b1, ba, b3, bb)
    step = rows // 16
    keep, send, base = [0], [], 0
    n = rows
    for bit in axes:
        n //= 2
        keep.append(pl.multiple_of(base + bit * n, step))
        send.append(pl.multiple_of(base + (1 - bit) * n, step))
        base = base + bit * n
    return (p1, pa, p3, pb), keep, send, axes


def chain_route(bits, peers, unit, d):
    core, bx, by, ba, bb = bits
    _, px, py, pa, _ = peers
    swap = lax.rem(unit + core, 2) == 1
    b1, p1 = jnp.where(swap, by, bx), jnp.where(swap, py, px)
    b3, p3 = jnp.where(swap, bx, by), jnp.where(swap, px, py)
    piece, chunk, pair, half = d // 16, d // 8, d // 4, d // 2
    me = lax.axis_index("data")

    def rows(base, n):
        return pl.ds(pl.multiple_of(base, piece), n)
    kx = b1 * half
    own = kx + (2 * bb + ba) * chunk
    mate = 2 * (kx + bb * pair) + chunk - own
    r = dict(
        half=rows(kx, half), other_half=rows((1 - b1) * half, half),
        pair=rows(kx + bb * pair, pair), other_pair=rows(kx + (1 - bb) * pair, pair),
        own=rows(own, chunk), mate=rows(mate, chunk),
        far_end=rows(kx + (1 - bb) * 3 * chunk, chunk), far_mid=rows(kx + (2 - bb) * chunk, chunk),
        keep=rows(own + b3 * piece, piece), send=rows(own + (1 - b3) * piece, piece),
        x_send_first=(rows((1 - b1) * half + (1 - bb) * pair, pair), rows((1 - bb) * pair, pair)),
        x_send_second=(rows((1 - b1) * half + bb * pair, pair), rows(bb * pair, pair)),
    )
    return r, p1, pa, me + 8 * (1 - 2 * bb), p3


def arrive(peers):
    barrier = pltpu.get_barrier_semaphore()
    for peer in peers:
        pl.semaphore_signal(barrier, inc=1, device_id=(peer,), device_id_type=MESH)
    return functools.partial(pl.semaphore_wait, barrier, len(peers))


def others(bits, me_bits):
    me = lax.axis_index("data")
    out = []
    for mask in range(1, 1 << len(me_bits)):
        peer = me
        for i, k in enumerate(me_bits):
            if mask >> i & 1:
                peer = peer + (1 << k) * (1 - 2 * bits[k])
        out.append(peer)
    return out


def exchange_sum(buf, first, peers, send_sem, recv_sem, sem0):
    copies = [remote(buf.at[first], buf.at[first + 1 + i], send_sem.at[sem0 + i], recv_sem.at[sem0 + i], peer) for i, peer in enumerate(peers)]
    for cp in copies:
        cp.start()
    total = buf[first]
    for i, cp in enumerate(copies):
        cp.wait()
        total = total + buf[first + 1 + i]
    buf[first + len(peers) + 1] = total


def gather_hops(bits, peers, unit, d, full, piece_src=None):
    ps, keep, send, _ = route(bits, peers, unit, d)
    piece = d // 16

    def rows(base, n):
        return full.at[pl.ds(base, n), :]

    def hop(k, part, sem_s, sem_r):
        peer = ps[3 - k] if k < 4 else peers[0]
        if k == 0:
            ref = rows(keep[4], piece)
        elif part == 0:
            ref = rows(keep[5 - k], piece << (k - 1))
        else:
            ref = rows(send[4 - k], piece << (k - 1))
        src = piece_src if piece_src is not None and part == 0 and k <= 1 else ref
        return remote(src, ref, sem_s, sem_r, peer)

    def arrived(k, sem_s, sem_r):
        ref = rows(send[3 - k], piece << k)
        return remote(ref, ref, sem_s, sem_r, ps[3 - k])

    def sent(sem_s, sem_r):
        ref = rows(0, 15 * piece)
        return remote(ref, ref, sem_s, sem_r, ps[0])
    return hop, arrived, sent


def remote(src, dst, send_sem, recv_sem, peer):
    return pltpu.make_async_remote_copy(src_ref=src, dst_ref=dst, send_sem=send_sem, recv_sem=recv_sem, device_id=(peer,), device_id_type=MESH)


def local(src, dst, sem):
    return pltpu.make_async_copy(src, dst, sem)


def halves(t):
    return [(0, t // 2), (t // 2, t // 2)] if t % 32 == 0 else [(0, t)]


def transpose_into(dst, src, t):
    full = t // 128
    if full:
        @pl.loop(0, full)
        def _(i):
            lo = pl.multiple_of(i * 128, 128)
            dst[:, pl.ds(lo, 128)] = src[pl.ds(lo, 128), :].T
    if t % 128:
        dst[:, full * 128:t] = src[full * 128:t, :].T


def fwd_pair(h_ref, v_ref, acc_ref, a_ref, z_ref, t, f):
    for lo, n in halves(t):
        for j in range(2):
            z = dot(h_ref[lo:lo + n, :], v_ref[j, 0]).astype(jnp.bfloat16)
            z_ref[j, lo:lo + n, :] = z
            a_ref[lo:lo + n, j * f:(j + 1) * f] = gelu(z.astype(jnp.float32)).astype(jnp.bfloat16)
    v_out = jnp.concatenate([v_ref[0, 1], v_ref[1, 1]], axis=1)
    for lo, n in halves(t):
        acc_ref[lo:lo + n, :] += dot(a_ref[lo:lo + n, :], v_out, NT)


def fwd_close(h_ref, acc_ref, t):
    for lo, n in halves(t):
        h_ref[lo:lo + n, :] = acc_ref[lo:lo + n, :].astype(jnp.bfloat16)


def fwd_seed(h_ref, acc_ref, t):
    for lo, n in halves(t):
        acc_ref[lo:lo + n, :] = h_ref[lo:lo + n, :].astype(jnp.float32)


def fold(v):
    r, c = v.shape
    rows = jnp.sum(v.reshape(r // 8, 8, c), axis=0)
    return sum(rows[:, lo:lo + 128] for lo in range(0, c, 128))


def loss_close(h_ref, y_ref, acc_ref, t, d, total_ref=None):
    def rows_of(rows):
        e = acc_ref[rows, :].astype(jnp.bfloat16).astype(jnp.float32) - y_ref[rows, :].astype(jnp.float32)
        q = e.astype(jnp.bfloat16)
        h_ref[rows, :] = q
        acc_ref[rows, :] = q.astype(jnp.float32)
        return e
    if total_ref is None:
        for lo, n in halves(t):
            rows_of(slice(lo, lo + n))
        return
    n = 112 if t % 112 == 0 else t
    total_ref[...] = jnp.zeros((8, 128), jnp.float32)

    @pl.loop(0, t // n)
    def _(i):
        e = rows_of(pl.ds(pl.multiple_of(i * n, n), n))
        total_ref[...] += fold(e * e)


def unit_of(it, nf, nl):
    return (nl - 1 - it // nf) * nf + lax.rem(it, nf)


def first_pass(dm, scale, x_hbm, y_hbm, wi_hbm, wo_hbm, z_out, v_out, ws_out, wc_out, g_out, n_out,
               h, tmp, tb, eb, acc, ab, wi, wo, zb, vb, ws, wc, cbuf, obuf, sbuf, r1, r2, r3, r4, nb,
               load_sem, z_sem, v_sem, io_sem, csend_sem, core_sem, send_sem, recv_sem, credit, nsend_sem, nrecv_sem):
    t, d, f, nf, nl = dm
    nu = nf * nl
    bits, peers = place()
    piece = d // 16
    near, far = others(bits, (0, 1, 2)), others(bits, (3, 4))
    wait_all = arrive(near + far)

    def loads(p, slot):
        layer, tile = p // (nf // 2), lax.rem(p, nf // 2)
        lo = pl.multiple_of(tile * 2 * f, 2 * f)
        return (local(wi_hbm.at[layer, :, pl.ds(lo, 2 * f)], wi.at[slot], load_sem.at[slot, 0]),
                local(wo_hbm.at[layer, pl.ds(lo, 2 * f), :], wo.at[slot], load_sem.at[slot, 1]))

    def stores(p, slot):
        two = pl.ds(2 * p, 2)
        return local(zb.at[slot], z_out.at[two], z_sem.at[slot]), local(vb.at[slot], v_out.at[two], v_sem.at[slot])

    x_in = local(x_hbm, h, io_sem.at[0])
    y_in = local(y_hbm, tmp, io_sem.at[1])
    x_in.start()
    for cp in loads(0, 0):
        cp.start()
    y_in.start()
    x_in.wait()
    fwd_seed(h, acc, t)

    @pl.loop(0, nu // 2)
    def _(p):
        slot = lax.rem(p, 2)
        for cp in loads(p, slot):
            cp.wait()

        @pl.when(p + 1 < nu // 2)
        def _():
            for cp in loads(p + 1, 1 - slot):
                cp.start()

        @pl.when(p >= 2)
        def _():
            for cp in stores(p - 2, slot):
                cp.wait()
        for j in range(2):
            cols = slice(j * f, (j + 1) * f)
            wot = wo[slot, cols, :].T
            _, keep, _, _ = route(bits, peers, 2 * p + j, d)
            rows = pl.ds(keep[4], piece)
            vb[slot, j, 0] = wi[slot, :, cols].astype(jnp.bfloat16)
            vb[slot, j, 1] = wot.astype(jnp.bfloat16)
            obuf[j] = wot
            ws[2 * p + j] = jnp.where(bits[0] == 0, wi[slot, rows, cols], obuf[j, rows, :])
            rows = chain_route(bits, peers, j, d)[0]['keep']
            wc[2 * p + j] = jnp.where(bits[0] == 0, wi[slot, rows, cols], obuf[j, rows, :])

        fwd_pair(h, vb.at[slot], acc, ab, zb.at[slot], t, f)
        for cp in stores(p, slot):
            cp.start()

        @pl.when(p == nf // 2 - 1)
        def _():
            fwd_close(h, acc, t)
            fwd_seed(h, acc, t)
            transpose_into(tb.at[0], h, t)

    np_ = nu // 2
    if np_ >= 2:
        for cp in stores(np_ - 2, np_ % 2):
            cp.wait()
    spare = np_ % 2

    def tiles(it, slot):
        u = unit_of(it, nf, nl)
        return (local(z_out.at[u], zb.at[spare, slot], load_sem.at[slot, 0]), local(v_out.at[u], vb.at[spare, slot], load_sem.at[slot, 1]))
    for cp in tiles(0, 0):
        cp.start()
    ws_cp = local(ws, ws_out, io_sem.at[2])
    wc_cp = local(wc, wc_out, io_sem.at[3])
    ws_cp.start()
    wc_cp.start()
    y_in.wait()
    loss_close(h, tmp, acc, t, d)
    transpose_into(tb.at[1], h, t)
    x_again = local(x_hbm, tmp, io_sem.at[1])
    x_again.start()
    for cp in stores(np_ - 1, (np_ - 1) % 2):
        cp.wait()
    wait_all()
    nb[0] = jnp.zeros((8, 128), jnp.float32)

    ws_cp.wait()

    def on_total(u, total):
        ws[u] = total
        g = total * scale
        nb[0] += fold(g * g)

    start, events = halving(dm, bits, peers, cbuf, (r1, r2, r3, r4), send_sem, recv_sem, credit, LAG_A[1:], on_total)
    backward_phase(dm, bits, peers, h, tmp, tb, eb, acc, zb.at[spare], vb.at[spare], cbuf, obuf, sbuf,
                   csend_sem, core_sem, credit, tiles, x_again.wait, LAG_A[0], start, events)
    g_cp = local(ws, g_out, io_sem.at[0])
    g_cp.start()
    exchange_sum(nb, 0, near, nsend_sem, nrecv_sem, 0)
    exchange_sum(nb, 8, far, nsend_sem, nrecv_sem, 7)
    n_cp = local(nb.at[12], n_out, io_sem.at[1])
    n_cp.start()
    wc_cp.wait()
    g_cp.wait()
    n_cp.wait()


def second_forward(dm, scale, rho, gs_hbm, ws_hbm, n_hbm, x_hbm, y_hbm, z_out, v_out, h_out, q_out, sq_out,
                   h, yb, acc, ab, gs, ws, vb, zb, nb, send_sem, recv_sem, z_sem, v_sem, io_sem):
    t, d, f, nf, nl = dm
    nu = nf * nl
    bits, peers = place()
    core = bits[0]
    piece = d // 16
    wait_all = arrive(peers)
    ins = (local(gs_hbm, gs, io_sem.at[0]), local(ws_hbm, ws, io_sem.at[1]), local(x_hbm, h, io_sem.at[2]), local(y_hbm, yb, io_sem.at[3]))
    n_in = local(n_hbm, nb, io_sem.at[4])
    n_in.start()
    for cp in ins:
        cp.start()
    n_in.wait()
    coef = rho / jnp.sqrt(jnp.sum(nb[...], keepdims=True))
    ins[0].wait()
    ins[1].wait()
    wait_all()

    def hops(u):
        return gather_hops(bits, peers, u, d, vb.at[u, core])

    def sems(u, k):
        return send_sem.at[u, 0 if k < 4 else 1], recv_sem.at[u, k]

    def core_arrived(u):
        ref = vb.at[u, 1 - core]
        return remote(ref, ref, *sems(u, 4), peers[0])

    def z_store(p, slot):
        return local(zb.at[slot], z_out.at[pl.ds(2 * p, 2)], z_sem.at[slot])

    @pl.loop(0, nu + VG_LAG[5])
    def _(it):
        @pl.when(it < nu)
        def _():
            _, keep, _, _ = route(bits, peers, it, d)
            new = ws[it] + coef * (gs[it] * scale)
            vb[it, core, pl.ds(keep[4], piece), :] = new.astype(jnp.bfloat16)
            hop, _, _ = hops(it)
            hop(0, 0, *sems(it, 0)).start()
            hop(1, 0, *sems(it, 1)).start()
        for k in range(1, 5):
            u = it - VG_LAG[k]

            @pl.when((u >= 0) & (u < nu))
            def _():
                hop, arrived, _ = hops(u)
                arrived(k - 1, *sems(u, k - 1)).wait_recv()
                hop(k, 1, *sems(u, k)).start()
                if k < 4:
                    hop(k + 1, 0, *sems(u, k + 1)).start()
        u = it - VG_LAG[5]

        @pl.when(u >= 0)
        def _():
            core_arrived(u).wait_recv()
            local(vb.at[u], v_out.at[u], v_sem.at[u]).start()

        @pl.when((u >= 0) & (lax.rem(u, 2) == 1))
        def _():
            p = u // 2
            slot = lax.rem(p, 2)

            @pl.when(p >= 2)
            def _():
                z_store(p - 2, slot).wait()

            @pl.when(p == 0)
            def _():
                ins[2].wait()
                fwd_seed(h, acc, t)
            fwd_pair(h, vb.at[pl.ds(2 * p, 2)], acc, ab, zb.at[slot], t, f)
            z_store(p, slot).start()

            @pl.when(p == nf // 2 - 1)
            def _():
                fwd_close(h, acc, t)
                fwd_seed(h, acc, t)
                out = local(h, h_out, io_sem.at[0])
                out.start()
                out.wait()

    ins[3].wait()
    loss_close(h, yb, acc, t, d, nb)
    out = local(h, q_out, io_sem.at[0])
    sq = local(nb, sq_out, io_sem.at[1])
    out.start()
    sq.start()

    @pl.loop(0, nu)
    def _(u):
        local(vb.at[u], v_out.at[u], v_sem.at[u]).wait()
        hops(u)[2](*sems(u, 0)).wait_send()
        core_arrived(u).wait_send()
    for p in range(max(nu // 2 - 2, 0), nu // 2):
        z_store(p, p % 2).wait()
    out.wait()
    sq.wait()


def backward_phase(dm, bits, peers, q, tmp, tb, eb, acc, zb, vb, cbuf, obuf, sbuf, csend_sem, core_sem, credit,
                   tiles, x_ready, core_lag, after_core, events):
    t, d, f, nf, nl = dm
    nu = nf * nl
    core = bits[0]
    slots = cbuf.shape[0]

    def core_copy(it):
        slot = lax.rem(it, 2)
        return remote(sbuf.at[slot], cbuf.at[lax.rem(it, slots)], csend_sem.at[slot], core_sem.at[it], peers[0])

    def core_stage(j):
        cs = lax.rem(j, slots)
        core_copy(j).wait_recv()
        cbuf[cs] = cbuf[cs] + obuf[lax.rem(j, 2)]
        after_core(j)

    @pl.loop(0, nu + max(lag for lag, _ in events))
    def _(it):
        @pl.when(it == nf)
        def _():
            fwd_close(q, acc, t)
            transpose_into(tb.at[1], q, t)
            x_ready()
            transpose_into(tb.at[0], tmp, t)

        @pl.when(it < nu)
        def _():
            slot = lax.rem(it, 2)
            for cp in tiles(it, slot):
                cp.wait()

            @pl.when(it + 1 < nu)
            def _():
                for cp in tiles(it + 1, 1 - slot):
                    cp.start()
            for lo, n in halves(t):
                back = dot(q[lo:lo + n, :], vb[slot, 1])
                a, slope = gelu_and_grad(zb[slot, lo:lo + n, :].astype(jnp.float32))
                eb[1, lo:lo + n, :] = a.astype(jnp.bfloat16)
                eb[0, lo:lo + n, :] = (back * slope).astype(jnp.bfloat16)

            @pl.when(it >= 2)
            def _():
                core_copy(it - 2).wait_send()
            sbuf[slot] = dot(tb[1 - core], eb[1 - core])

            @pl.when(it >= slots)
            def _():
                pl.semaphore_wait(credit, 1)
            core_copy(it).start()
            obuf[slot] = dot(tb[core], eb[core])

            @pl.when(it < nf)
            def _():
                for lo, n in halves(t):
                    acc[lo:lo + n, :] += dot(eb[0, lo:lo + n, :], vb[slot, 0], NT)

        for lag, event in ((core_lag, core_stage), *events):
            j = it - lag

            @pl.when((j >= 0) & (j < nu))
            def _():
                event(j)

    core_copy(nu - 2).wait_send()
    core_copy(nu - 1).wait_send()


def free_slot(j, nu, slots, credit, peer):
    @pl.when(j + slots < nu)
    def _():
        pl.semaphore_signal(credit, inc=1, device_id=(peer,), device_id_type=MESH)


def halving(dm, bits, peers, cbuf, rbuf, send_sem, recv_sem, credit, lags, on_total):
    t, d, f, nf, nl = dm
    nu = nf * nl
    piece = d // 16
    slots = cbuf.shape[0]

    def rs_sends(it, k):
        ps, _, send, on = route(bits, peers, it, d)
        n = d >> (k + 1)
        cs = lax.rem(it, slots)

        def part(off, m, sem):
            return remote(cbuf.at[cs, pl.ds(send[k] + off, m), :], rbuf[k].at[it, pl.ds(off, m), :], send_sem.at[it], sem, ps[k])
        if k == 3:
            return [part(0, n, recv_sem.at[0, it, k])]
        m = n // 2
        return [part(pl.multiple_of((1 - on[k + 1]) * m, piece), m, recv_sem.at[0, it, k]),
                part(pl.multiple_of(on[k + 1] * m, piece), m, recv_sem.at[1, it, k])]

    def rs_add(it, k, kept):
        ps, keep, send, _ = route(bits, peers, it, d)
        cs = lax.rem(it, slots)
        if k == 3:
            base, m = keep[4], d >> 4
        else:
            base, m = (keep[k + 2] if kept else send[k + 1]), d >> (k + 2)
        here = rbuf[k].at[it, pl.ds(pl.multiple_of(base - keep[k + 1], piece), m), :]
        mine = cbuf.at[cs, pl.ds(base, m), :]
        remote(mine, here, send_sem.at[it], recv_sem.at[1 if kept else 0, it, k], ps[k]).wait_recv()
        total = mine[...] + here[...]
        if k == 3:
            return total
        mine[...] = total

    def start(j):
        for cp in rs_sends(j, 0):
            cp.start()

    def stage(k):
        def event(j):
            if k > 0:
                rs_add(j, k - 1, True)
            total = rs_add(j, k, False)
            if k < 3:
                for cp in rs_sends(j, k + 1):
                    cp.start()
            else:
                on_total(unit_of(j, nf, nl), total)
                ref = cbuf.at[lax.rem(j, slots), pl.ds(0, 15 * piece), :]
                remote(ref, ref, send_sem.at[j], recv_sem.at[0, j, 3], peers[0]).wait_send()
                free_slot(j, nu, slots, credit, peers[0])
        return event
    return start, [(lags[k], stage(k)) for k in range(4)]


def chain(dm, bits, peers, cbuf, rbuf, gs, w_out, send_sem, recv_sem, credit, ag_send, ag_recv, ag_loc, lags, on_total):
    t, d, f, nf, nl = dm
    nu = nf * nl
    core, _, _, ba, bb = bits
    piece = d // 16
    slots = cbuf.shape[0]
    r1, r2, r3, r4, r5 = rbuf
    at_end = ba == bb
    chunk = d // 8
    XU, XK, EU, EK, MU, MK, YY = range(7)

    def send(j, src, dst, sem, peer):
        remote(cbuf.at[lax.rem(j, slots), src, :], dst, send_sem.at[j], recv_sem.at[sem, j], peer).start()

    def add(j, rows, buf, sem):
        mine = cbuf.at[lax.rem(j, slots), rows, :]
        remote(mine, buf, send_sem.at[j], recv_sem.at[sem, j], peers[0]).wait_recv()
        mine[...] = mine[...] + buf[...]

    def at(j):
        return chain_route(bits, peers, unit_of(j, nf, nl), d)

    def start(j):
        r, p1, _, _, _ = at(j)
        for (src, dst), sem in ((r["x_send_first"], XU), (r["x_send_second"], XK)):
            send(j, src, r1.at[j, dst, :], sem, p1)

    def rel(first):
        return pl.ds(pl.multiple_of((1 - bb if first else bb) * (d // 4), piece), d // 4)

    def s1(j):
        r, _, pa, _, _ = at(j)
        add(j, r["other_pair"], r1.at[j, rel(True), :], XU)

        @pl.when(at_end)
        def _():
            send(j, r["other_pair"], r2.at[j], EU, pa)

    def s2(j):
        r, _, pa, pm, _ = at(j)
        add(j, r["pair"], r1.at[j, rel(False), :], XK)

        @pl.when(at_end)
        def _():
            send(j, r["mate"], r3.at[j], EK, pa)

        @pl.when(jnp.logical_not(at_end))
        def _():
            add(j, r["other_pair"], r2.at[j], EU)
            send(j, r["far_end"], r5.at[j, 0:chunk, :], MU, pm)
            send(j, r["far_mid"], r5.at[j, chunk:2 * chunk, :], MK, pm)

    def s3(j):
        r, _, pa, _, p3 = at(j)

        @pl.when(jnp.logical_not(at_end))
        def _():
            add(j, r["mate"], r5.at[j, 0:chunk, :], MU)
            send(j, r["mate"], r3.at[j], EK, pa)
            add(j, r["own"], r3.at[j], EK)
            add(j, r["own"], r5.at[j, chunk:2 * chunk, :], MK)
            send(j, r["send"], r4.at[j], YY, p3)

    def s4(j):
        r, _, _, _, p3 = at(j)

        @pl.when(at_end)
        def _():
            add(j, r["own"], r3.at[j], EK)
            send(j, r["send"], r4.at[j], YY, p3)

    def full(j):
        return w_out.at[unit_of(j, nf, nl), core]

    def give(j, rows, sem_s, sem_r, peer, src=None):
        ref = full(j).at[rows, :]
        return remote(ref if src is None else src, ref, ag_send.at[j, sem_s], ag_recv.at[j, sem_r], peer)

    def own_copy(j):
        u = unit_of(j, nf, nl)
        return local(gs.at[u], full(j).at[at(j)[0]["keep"], :], ag_loc.at[j])

    def s5(j):
        r, _, _, _, p3 = at(j)
        u = unit_of(j, nf, nl)
        mine = cbuf.at[lax.rem(j, slots), r["keep"], :]
        remote(mine, r4.at[j], send_sem.at[j], recv_sem.at[YY, j], p3).wait_recv()
        on_total(u, mine[...] + r4[j])
        own_copy(j).start()
        give(j, r["keep"], 0, 0, p3, gs.at[u]).start()
        ref = cbuf.at[lax.rem(j, slots), pl.ds(0, 15 * piece), :]
        remote(ref, ref, send_sem.at[j], recv_sem.at[YY, j], p3).wait_send()
        free_slot(j, nu, slots, credit, peers[0])

    def g1(j):
        r, p1, pa, pm, p3 = at(j)
        own_copy(j).wait()
        give(j, r["send"], 0, 0, p3).wait_recv()
        give(j, r["own"], 0, 1, pa).start()

        @pl.when(jnp.logical_not(at_end))
        def _():
            give(j, r["own"], 1, 2, pm).start()
        give(j, r["own"], 0, 3, p1).start()

    def g2(j):
        r, p1, pa, pm, _ = at(j)
        give(j, r["mate"], 0, 1, pa).wait_recv()

        @pl.when(jnp.logical_not(at_end))
        def _():
            give(j, r["mate"], 1, 2, pm).start()
        give(j, r["mate"], 0, 3, p1).start()

    def g3(j, r, p1, pa):
        give(j, r["other_pair"], 1, 2, pa).wait_recv()
        give(j, r["other_pair"], 0, 3, p1).start()
        give(j, r["half"], 2, 4, peers[0]).start()

    def g3_middle(j):
        r, p1, pa, _, _ = at(j)

        @pl.when(jnp.logical_not(at_end))
        def _():
            g3(j, r, p1, pa)
            give(j, r["other_pair"], 1, 2, pa).start()

    def g3_end(j):
        r, p1, pa, _, _ = at(j)

        @pl.when(at_end)
        def _():
            g3(j, r, p1, pa)

    def g4(j):
        r, p1, _, _, _ = at(j)
        give(j, r["other_half"], 0, 3, p1).wait_recv()
        give(j, r["other_half"], 2, 4, peers[0]).start()

    def finish_unit(j):
        ref = w_out.at[unit_of(j, nf, nl), 1 - core]
        last = remote(ref, ref, ag_send.at[j, 2], ag_recv.at[j, 4], peers[0])
        last.wait_recv()
        last.wait_send()
        ref = full(j).at[pl.ds(0, 11 * piece), :]
        remote(ref, ref, ag_send.at[j, 0], ag_recv.at[j, 3], peers[0]).wait_send()

        @pl.when(jnp.logical_not(at_end))
        def _():
            ref = full(j).at[pl.ds(0, 8 * piece), :]
            remote(ref, ref, ag_send.at[j, 1], ag_recv.at[j, 2], peers[0]).wait_send()

    steps = (s1, s2, s3, s4, s5, g1, g2, g3_middle, g3_end, g4)
    return start, list(zip(lags, steps)), finish_unit


def second_backward(dm, scale, x_hbm, h_hbm, q_hbm, z_hbm, v_hbm, ws_hbm, sq_hbm, w_out, sq_out,
                    q, tmp, tb, eb, acc, zb, vb, cbuf, obuf, sbuf, r1, r2, r3, r4, gs, r5,
                    load_sem, io_sem, csend_sem, core_sem, send_sem, recv_sem, credit, nb, ag_send, ag_recv, ag_loc, nsend_sem, nrecv_sem):
    t, d, f, nf, nl = dm
    nu = nf * nl
    bits, peers = place()
    near, far = others(bits, (0, 1, 2)), others(bits, (3, 4))
    wait_all = arrive(near + far)

    def tiles(it, slot):
        u = unit_of(it, nf, nl)
        return local(z_hbm.at[u], zb.at[slot], load_sem.at[slot, 0]), local(v_hbm.at[u], vb.at[slot], load_sem.at[slot, 1])

    q_in = local(q_hbm, q, io_sem.at[0])
    h_in = local(h_hbm, tmp, io_sem.at[1])
    ws_in = local(ws_hbm, gs, io_sem.at[2])
    sq_in = local(sq_hbm, nb.at[0], io_sem.at[3])
    q_in.start()
    for cp in tiles(0, 0):
        cp.start()
    for cp in (h_in, ws_in, sq_in):
        cp.start()
    q_in.wait()
    fwd_seed(q, acc, t)
    transpose_into(tb.at[1], q, t)
    h_in.wait()
    transpose_into(tb.at[0], tmp, t)
    x_in = local(x_hbm, tmp, io_sem.at[1])
    x_in.start()
    ws_in.wait()
    sq_in.wait()
    wait_all()

    def on_total(u, total):
        gs[u] = gs[u] - LEARN_RATE * (total * scale)

    def sums(j):
        @pl.when(j == 1)
        def _():
            exchange_sum(nb, 0, near, nsend_sem, nrecv_sem, 0)

        @pl.when(j == 2)
        def _():
            exchange_sum(nb, 8, far, nsend_sem, nrecv_sem, 7)

    start, events, finish_unit = chain(dm, bits, peers, cbuf, (r1, r2, r3, r4, r5), gs, w_out, send_sem, recv_sem, credit,
                                       ag_send, ag_recv, ag_loc, LAG_B[1:], on_total)
    backward_phase(dm, bits, peers, q, tmp, tb, eb, acc, zb, vb, cbuf, obuf, sbuf,
                   csend_sem, core_sem, credit, tiles, x_in.wait, LAG_B[0], start, [*events, (0, sums)])
    sq_cp = local(nb.at[12], sq_out, io_sem.at[3])
    sq_cp.start()

    @pl.loop(0, nu)
    def _(j):
        finish_unit(j)
    sq_cp.wait()


def finish(scale, f, w_ref, sq_ref, in_ref, out_ref, loss_ref):
    for j in range(w_ref.shape[0]):
        in_ref[0, :, j * f:(j + 1) * f] = w_ref[j, 0]
        out_ref[0, j * f:(j + 1) * f, :] = w_ref[j, 1].T
    loss_ref[0, 0] = 0.5 * (jnp.sum(sq_ref[...]) * scale)


def sds(shape, dtype):
    return jax.ShapeDtypeStruct(shape, dtype)


def call(kernel, n_in, outs, scratch, name, collective_id=None):
    params = dict(vmem_limit_bytes=VMEM_CAP)
    if collective_id is not None:
        params.update(collective_id=collective_id, has_side_effects=True)
    return pl.pallas_call(
        kernel,
        out_shape=outs,
        in_specs=[ANY] * n_in,
        out_specs=[ANY] * len(outs),
        scratch_shapes=scratch,
        compiler_params=pltpu.CompilerParams(**params),
        name=name,
    )


def local_step(n_dev, tile_f, x_loc, y_loc, w_in, w_out):
    nl, d, ff = w_in.shape
    f = tile_f
    nf = ff // f
    nu = nl * nf
    t = x_loc.shape[0] * x_loc.shape[1]
    piece = d // 16
    dm = (t, d, f, nf, nl)
    scale = 1.0 / (t * n_dev * d)
    rho = RHO_FRAC * math.sqrt(nl * (d + ff))
    bf, f32 = jnp.bfloat16, jnp.float32
    V, DMA = pltpu.VMEM, pltpu.SemaphoreType.DMA
    x = x_loc.transpose(1, 0, 2).reshape(t, d)
    y = y_loc.transpose(1, 0, 2).reshape(t, d)
    z_s, v_s, w_s, a_s = sds((nu, t, f), bf), sds((nu, 2, d, f), bf), sds((nu, piece, f), f32), sds((t, d), bf)

    REG = pltpu.SemaphoreType.REGULAR
    slots = min(CORE_SLOTS, nu)
    n_s = sds((8, 128), f32)
    reduce_bufs = [V((slots, d, f), f32), V((2, d, f), f32), V((2, d, f), f32),
                   V((nu, d // 2, f), f32), V((nu, d // 4, f), f32), V((nu, d // 8, f), f32), V((nu, d // 16, f), f32), V((nu, piece, f), f32)]
    acts = [V((t, d), bf), V((t, d), bf), V((2, d, t), bf), V((2, t, f), bf), V((t, d), f32)]

    z, v, ws, wc, g, norm = call(
        functools.partial(first_pass, dm, scale), 4, [z_s, v_s, w_s, w_s, w_s, n_s],
        acts + [V((t, 2 * f), bf), V((2, d, 2 * f), f32), V((2, 2 * f, d), f32), V((2, 2, t, f), bf), V((2, 2, 2, d, f), bf), V((nu, piece, f), f32), V((nu, piece, f), f32)]
        + reduce_bufs[:-1] + [V((13, 8, 128), f32), DMA((2, 2)), DMA((2,)), DMA((2,)), DMA((4,)), DMA((2,)), DMA((nu,)), DMA((nu,)), DMA((2, nu, 4)), REG, DMA((10,)), DMA((10,))],
        "pass_a", 0)(x, y, w_in, w_out)

    z, v, h1, q, sq = call(
        functools.partial(second_forward, dm, scale, rho), 5, [z_s, v_s, a_s, a_s, n_s],
        [V((t, d), bf), V((t, d), bf), V((t, d), f32), V((t, 2 * f), bf), V((nu, piece, f), f32), V((nu, piece, f), f32), V((nu, 2, d, f), bf), V((2, 2, t, f), bf),
         V((8, 128), f32), DMA((nu, 2)), DMA((nu, 5)), DMA((2,)), DMA((nu,)), DMA((5,))], "fwd_b", 1)(g, ws, norm, x, y)

    w_new, sq = call(
        functools.partial(second_backward, dm, scale), 7, [sds((nu, 2, d, f), f32), n_s],
        acts + [V((2, t, f), bf), V((2, 2, d, f), bf)] + reduce_bufs + [V((nu, d // 4, f), f32), DMA((2, 2)), DMA((4,)), DMA((2,)), DMA((nu,)), DMA((nu,)), DMA((7, nu)), REG,
         V((13, 8, 128), f32), DMA((nu, 3)), DMA((nu, 5)), DMA((nu,)), DMA((10,)), DMA((10,))], "bwd_b", 2)(x, h1, q, z, v, wc, sq)

    new_in, new_out, loss = pl.pallas_call(
        functools.partial(finish, scale, f),
        grid=(nl, nf // 4),
        in_specs=[pl.BlockSpec((4, 2, d, f), lambda i, j: (i * (nf // 4) + j, 0, 0, 0)), pl.BlockSpec((8, 128), lambda i, j: (0, 0))],
        out_specs=[pl.BlockSpec((1, d, 4 * f), lambda i, j: (i, 0, j)), pl.BlockSpec((1, 4 * f, d), lambda i, j: (i, j, 0)),
                   pl.BlockSpec((1, 1), lambda i, j: (0, 0), memory_space=pltpu.SMEM)],
        out_shape=[sds((nl, d, ff), f32), sds((nl, ff, d), f32), sds((1, 1), f32)],
        compiler_params=pltpu.CompilerParams(vmem_limit_bytes=VMEM_CAP),
        name="finish")(w_new, sq)
    return new_in, new_out, loss.reshape(())


def solution(mesh):
    step = functools.partial(local_step, mesh.shape["data"], TILE_F)
    return jax.shard_map(step, mesh=mesh, in_specs=(P("data"), P("data"), P(), P()), out_specs=(P(), P(), P()), check_vma=False)
```

```python
import math
import functools
import jax
import jax.numpy as jnp
from jax import lax
from jax.experimental import pallas as pl
from jax.experimental.pallas import tpu as pltpu
from jax.sharding import PartitionSpec as P

RHO_FRAC = 0.1
LEARN_RATE = 1.0
TILE_F = 256
MESH = pl.DeviceIdType.MESH
ANY = pl.BlockSpec(memory_space=pl.ANY)
NN = (((1,), (0,)), ((), ()))
NT = (((1,), (1,)), ((), ()))
GELU_C = math.sqrt(2.0 / math.pi)
GELU_K = 0.044715
VMEM_CAP = 67043328
TILE = (8, 128)
CORE_SLOTS = 9
LAG_A = (0, 1, 4, 5, 7)
LAG_B = (0, 1, 2, 3, 4, 4, 5, 7, 8, 9, 12)
VG_LAG = (0, 2, 3, 5, 7, 9)


steps = functools.partial(pl.loop, 0)


def odd(i):
    return lax.rem(i, 2)


def dot(lhs, rhs, dims=NN):
    return lax.dot_general(lhs, rhs, dims, preferred_element_type=jnp.float32)


def gelu_parts(z):
    sq = z * z
    th = jnp.tanh(GELU_C * (z + GELU_K * (sq * z)))
    cdf = 0.5 * (1.0 + th)
    return sq, th, cdf


def gelu(z):
    return z * gelu_parts(z)[2]


def gelu_and_grad(z):
    sq, th, cdf = gelu_parts(z)
    slope = cdf + (0.5 * z) * ((1.0 - th * th) * (GELU_C + (3.0 * GELU_K * GELU_C) * sq))
    return z * cdf, slope


def place(axis="data"):
    me = lax.axis_index(axis)
    bits = [lax.rem(lax.div(me, 1 << k), 2) for k in range(5)]
    peers = [me + (1 << k) * (1 - 2 * bits[k]) for k in range(5)]
    return bits, peers


def route(bits, peers, unit, rows):
    core, bx, by, ba, bb = bits
    _, px, py, pa, pb = peers
    swap = odd(unit + core) == 1
    b1, p1 = jnp.where(swap, by, bx), jnp.where(swap, py, px)
    b3, p3 = jnp.where(swap, bx, by), jnp.where(swap, px, py)
    axes = (b1, ba, b3, bb)
    step = rows // 16
    keep, send, base = [0], [], 0
    n = rows
    for bit in axes:
        n //= 2
        keep.append(pl.multiple_of(base + bit * n, step))
        send.append(pl.multiple_of(base + (1 - bit) * n, step))
        base = base + bit * n
    return (p1, pa, p3, pb), keep, send, axes


def chain_route(bits, peers, unit, d):
    core, bx, by, ba, bb = bits
    _, px, py, pa, _ = peers
    swap = odd(unit + core) == 1
    b1, p1 = jnp.where(swap, by, bx), jnp.where(swap, py, px)
    b3, p3 = jnp.where(swap, bx, by), jnp.where(swap, px, py)
    piece, chunk, pair, half = d // 16, d // 8, d // 4, d // 2
    me = lax.axis_index("data")

    def rows(base, n):
        return pl.ds(pl.multiple_of(base, piece), n)
    kx = b1 * half
    own = kx + (2 * bb + ba) * chunk
    mate = 2 * (kx + bb * pair) + chunk - own
    r = dict(
        half=rows(kx, half), other_half=rows((1 - b1) * half, half),
        pair=rows(kx + bb * pair, pair), other_pair=rows(kx + (1 - bb) * pair, pair),
        own=rows(own, chunk), mate=rows(mate, chunk),
        far_end=rows(kx + (1 - bb) * 3 * chunk, chunk), far_mid=rows(kx + (2 - bb) * chunk, chunk),
        keep=rows(own + b3 * piece, piece), send=rows(own + (1 - b3) * piece, piece),
        x_send_first=(rows((1 - b1) * half + (1 - bb) * pair, pair), rows((1 - bb) * pair, pair)),
        x_send_second=(rows((1 - b1) * half + bb * pair, pair), rows(bb * pair, pair)),
    )
    return r, p1, pa, me + 8 * (1 - 2 * bb), p3


def arrive(peers):
    barrier = pltpu.get_barrier_semaphore()
    for peer in peers:
        pl.semaphore_signal(barrier, device_id=(peer,), device_id_type=MESH)
    return functools.partial(pl.semaphore_wait, barrier, len(peers))


def others(bits, me_bits):
    me = lax.axis_index("data")
    out = []
    for mask in range(1, 1 << len(me_bits)):
        peer = me
        for i, k in enumerate(me_bits):
            if mask >> i & 1:
                peer = peer + (1 << k) * (1 - 2 * bits[k])
        out.append(peer)
    return out


def exchange_sum(buf, first, peers, send_sem, recv_sem, sem0):
    copies = [remote(buf.at[first], buf.at[first + 1 + i], send_sem.at[sem0 + i], recv_sem.at[sem0 + i], peer) for i, peer in enumerate(peers)]
    for cp in copies:
        cp.start()
    total = buf[first]
    for i, cp in enumerate(copies):
        cp.wait()
        total = total + buf[first + 1 + i]
    buf[first + len(peers) + 1] = total


def gather_hops(bits, peers, unit, d, full, piece_src=None):
    ps, keep, send, _ = route(bits, peers, unit, d)
    piece = d // 16

    def rows(base, n):
        return full.at[pl.ds(base, n), :]

    def hop(k, part, sem_s, sem_r):
        peer = ps[3 - k] if k < 4 else peers[0]
        if k == 0:
            ref = rows(keep[4], piece)
        elif part == 0:
            ref = rows(keep[5 - k], piece << (k - 1))
        else:
            ref = rows(send[4 - k], piece << (k - 1))
        src = piece_src if piece_src is not None and part == 0 and k <= 1 else ref
        return remote(src, ref, sem_s, sem_r, peer)

    def arrived(k, sem_s, sem_r):
        ref = rows(send[3 - k], piece << k)
        return remote(ref, ref, sem_s, sem_r, ps[3 - k])

    def sent(sem_s, sem_r):
        ref = rows(0, 15 * piece)
        return remote(ref, ref, sem_s, sem_r, ps[0])
    return hop, arrived, sent


def remote(src, dst, send_sem, recv_sem, peer):
    return pltpu.make_async_remote_copy(src_ref=src, dst_ref=dst, send_sem=send_sem, recv_sem=recv_sem, device_id=(peer,), device_id_type=MESH)


def local(src, dst, sem):
    return pltpu.make_async_copy(src, dst, sem)


def halves(t):
    return [(0, t // 2), (t // 2, t // 2)] if t % 32 == 0 else [(0, t)]


def transpose_into(dst, src, t):
    full = t // 128
    if full:
        @steps(full)
        def _(i):
            lo = pl.multiple_of(i * 128, 128)
            dst[:, pl.ds(lo, 128)] = src[pl.ds(lo, 128), :].T
    if t % 128:
        dst[:, full * 128:t] = src[full * 128:t, :].T


def fwd_pair(h_ref, v_ref, acc_ref, a_ref, z_ref, t, f):
    for lo, n in halves(t):
        for j in range(2):
            z = dot(h_ref[lo:lo + n, :], v_ref[j, 0]).astype(jnp.bfloat16)
            z_ref[j, lo:lo + n, :] = z
            a_ref[lo:lo + n, j * f:(j + 1) * f] = gelu(z.astype(jnp.float32)).astype(jnp.bfloat16)
    v_out = jnp.concatenate([v_ref[0, 1], v_ref[1, 1]], axis=1)
    for lo, n in halves(t):
        acc_ref[lo:lo + n, :] += dot(a_ref[lo:lo + n, :], v_out, NT)


def fwd_close(h_ref, acc_ref, t):
    for lo, n in halves(t):
        h_ref[lo:lo + n, :] = acc_ref[lo:lo + n, :].astype(jnp.bfloat16)


def fwd_seed(h_ref, acc_ref, t):
    for lo, n in halves(t):
        acc_ref[lo:lo + n, :] = h_ref[lo:lo + n, :].astype(jnp.float32)


def fold(v):
    r, c = v.shape
    rows = jnp.sum(v.reshape(r // 8, 8, c), axis=0)
    return sum(rows[:, lo:lo + 128] for lo in range(0, c, 128))


def loss_close(h_ref, y_ref, acc_ref, t, d, total_ref=None):
    def rows_of(rows):
        e = acc_ref[rows, :].astype(jnp.bfloat16).astype(jnp.float32) - y_ref[rows, :].astype(jnp.float32)
        q = e.astype(jnp.bfloat16)
        h_ref[rows, :] = q
        acc_ref[rows, :] = q.astype(jnp.float32)
        return e
    if total_ref is None:
        for lo, n in halves(t):
            rows_of(slice(lo, lo + n))
        return
    n = 112 if t % 112 == 0 else t
    total_ref[...] = jnp.zeros(TILE, jnp.float32)

    @steps(t // n)
    def _(i):
        e = rows_of(pl.ds(pl.multiple_of(i * n, n), n))
        total_ref[...] += fold(e * e)


def unit_of(it, nf, nl):
    return (nl - 1 - it // nf) * nf + lax.rem(it, nf)


def first_pass(dm, scale, x_hbm, y_hbm, wi_hbm, wo_hbm, z_out, v_out, ws_out, wc_out, g_out, n_out,
               h, tmp, tb, eb, acc, ab, wi, wo, zb, vb, ws, wc, cbuf, obuf, sbuf, r1, r2, r3, r4, nb,
               load_sem, z_sem, v_sem, io_sem, csend_sem, core_sem, send_sem, recv_sem, credit, nsend_sem, nrecv_sem):
    t, d, f, nf, nl = dm
    nu = nf * nl
    bits, peers = place()
    piece = d // 16
    near, far = others(bits, (0, 1, 2)), others(bits, (3, 4))
    wait_all = arrive(near + far)

    def loads(p, slot):
        layer, tile = p // (nf // 2), lax.rem(p, nf // 2)
        lo = pl.multiple_of(tile * 2 * f, 2 * f)
        return (local(wi_hbm.at[layer, :, pl.ds(lo, 2 * f)], wi.at[slot], load_sem.at[slot, 0]),
                local(wo_hbm.at[layer, pl.ds(lo, 2 * f), :], wo.at[slot], load_sem.at[slot, 1]))

    def stores(p, slot):
        two = pl.ds(2 * p, 2)
        return local(zb.at[slot], z_out.at[two], z_sem.at[slot]), local(vb.at[slot], v_out.at[two], v_sem.at[slot])

    x_in = local(x_hbm, h, io_sem.at[0])
    y_in = local(y_hbm, tmp, io_sem.at[1])
    x_in.start()
    for cp in loads(0, 0):
        cp.start()
    y_in.start()
    x_in.wait()
    fwd_seed(h, acc, t)

    @steps(nu // 2)
    def _(p):
        slot = odd(p)
        for cp in loads(p, slot):
            cp.wait()

        @pl.when(p + 1 < nu // 2)
        def _():
            for cp in loads(p + 1, 1 - slot):
                cp.start()

        @pl.when(p >= 2)
        def _():
            for cp in stores(p - 2, slot):
                cp.wait()
        for j in range(2):
            cols = slice(j * f, (j + 1) * f)
            wot = wo[slot, cols, :].T
            _, keep, _, _ = route(bits, peers, 2 * p + j, d)
            rows = pl.ds(keep[4], piece)
            vb[slot, j, 0] = wi[slot, :, cols].astype(jnp.bfloat16)
            vb[slot, j, 1] = wot.astype(jnp.bfloat16)
            obuf[j] = wot
            ws[2 * p + j] = jnp.where(bits[0] == 0, wi[slot, rows, cols], obuf[j, rows, :])
            rows = chain_route(bits, peers, j, d)[0]['keep']
            wc[2 * p + j] = jnp.where(bits[0] == 0, wi[slot, rows, cols], obuf[j, rows, :])

        fwd_pair(h, vb.at[slot], acc, ab, zb.at[slot], t, f)
        for cp in stores(p, slot):
            cp.start()

        @pl.when(p == nf // 2 - 1)
        def _():
            fwd_close(h, acc, t)
            fwd_seed(h, acc, t)
            transpose_into(tb.at[0], h, t)

    np_ = nu // 2
    if np_ >= 2:
        for cp in stores(np_ - 2, np_ % 2):
            cp.wait()
    spare = np_ % 2

    def tiles(it, slot):
        u = unit_of(it, nf, nl)
        return (local(z_out.at[u], zb.at[spare, slot], load_sem.at[slot, 0]), local(v_out.at[u], vb.at[spare, slot], load_sem.at[slot, 1]))
    for cp in tiles(0, 0):
        cp.start()
    ws_cp = local(ws, ws_out, io_sem.at[2])
    wc_cp = local(wc, wc_out, io_sem.at[3])
    ws_cp.start()
    wc_cp.start()
    y_in.wait()
    loss_close(h, tmp, acc, t, d)
    transpose_into(tb.at[1], h, t)
    x_again = local(x_hbm, tmp, io_sem.at[1])
    x_again.start()
    for cp in stores(np_ - 1, (np_ - 1) % 2):
        cp.wait()
    wait_all()
    nb[0] = jnp.zeros(TILE, jnp.float32)

    ws_cp.wait()

    def on_total(u, total):
        ws[u] = total
        g = total * scale
        nb[0] += fold(g * g)

    start, events = halving(dm, bits, peers, cbuf, (r1, r2, r3, r4), send_sem, recv_sem, credit, LAG_A[1:], on_total)
    backward_phase(dm, bits, peers, h, tmp, tb, eb, acc, zb.at[spare], vb.at[spare], cbuf, obuf, sbuf,
                   csend_sem, core_sem, credit, tiles, x_again.wait, LAG_A[0], start, events)
    g_cp = local(ws, g_out, io_sem.at[0])
    g_cp.start()
    exchange_sum(nb, 0, near, nsend_sem, nrecv_sem, 0)
    exchange_sum(nb, 8, far, nsend_sem, nrecv_sem, 7)
    n_cp = local(nb.at[12], n_out, io_sem.at[1])
    n_cp.start()
    wc_cp.wait()
    g_cp.wait()
    n_cp.wait()


def second_forward(dm, scale, rho, gs_hbm, ws_hbm, n_hbm, x_hbm, y_hbm, z_out, v_out, h_out, q_out, sq_out,
                   h, yb, acc, ab, gs, ws, vb, zb, nb, send_sem, recv_sem, z_sem, v_sem, io_sem):
    t, d, f, nf, nl = dm
    nu = nf * nl
    bits, peers = place()
    core = bits[0]
    piece = d // 16
    wait_all = arrive(peers)
    ins = (local(gs_hbm, gs, io_sem.at[0]), local(ws_hbm, ws, io_sem.at[1]), local(x_hbm, h, io_sem.at[2]), local(y_hbm, yb, io_sem.at[3]))
    n_in = local(n_hbm, nb, io_sem.at[4])
    n_in.start()
    for cp in ins:
        cp.start()
    n_in.wait()
    coef = rho / jnp.sqrt(jnp.sum(nb[...], keepdims=True))
    ins[0].wait()
    ins[1].wait()
    wait_all()

    def hops(u):
        return gather_hops(bits, peers, u, d, vb.at[u, core])

    def sems(u, k):
        return send_sem.at[u, 0 if k < 4 else 1], recv_sem.at[u, k]

    def core_arrived(u):
        ref = vb.at[u, 1 - core]
        return remote(ref, ref, *sems(u, 4), peers[0])

    def z_store(p, slot):
        return local(zb.at[slot], z_out.at[pl.ds(2 * p, 2)], z_sem.at[slot])

    @steps(nu + VG_LAG[5])
    def _(it):
        @pl.when(it < nu)
        def _():
            _, keep, _, _ = route(bits, peers, it, d)
            new = ws[it] + coef * (gs[it] * scale)
            vb[it, core, pl.ds(keep[4], piece), :] = new.astype(jnp.bfloat16)
            hop, _, _ = hops(it)
            hop(0, 0, *sems(it, 0)).start()
            hop(1, 0, *sems(it, 1)).start()
        for k in range(1, 5):
            u = it - VG_LAG[k]

            @pl.when((u >= 0) & (u < nu))
            def _():
                hop, arrived, _ = hops(u)
                arrived(k - 1, *sems(u, k - 1)).wait_recv()
                hop(k, 1, *sems(u, k)).start()
                if k < 4:
                    hop(k + 1, 0, *sems(u, k + 1)).start()
        u = it - VG_LAG[5]

        @pl.when(u >= 0)
        def _():
            core_arrived(u).wait_recv()
            local(vb.at[u], v_out.at[u], v_sem.at[u]).start()

        @pl.when((u >= 0) & (odd(u) == 1))
        def _():
            p = u // 2
            slot = odd(p)

            @pl.when(p >= 2)
            def _():
                z_store(p - 2, slot).wait()

            @pl.when(p == 0)
            def _():
                ins[2].wait()
                fwd_seed(h, acc, t)
            fwd_pair(h, vb.at[pl.ds(2 * p, 2)], acc, ab, zb.at[slot], t, f)
            z_store(p, slot).start()

            @pl.when(p == nf // 2 - 1)
            def _():
                fwd_close(h, acc, t)
                fwd_seed(h, acc, t)
                out = local(h, h_out, io_sem.at[0])
                out.start()
                out.wait()

    ins[3].wait()
    loss_close(h, yb, acc, t, d, nb)
    out = local(h, q_out, io_sem.at[0])
    sq = local(nb, sq_out, io_sem.at[1])
    out.start()
    sq.start()

    @steps(nu)
    def _(u):
        local(vb.at[u], v_out.at[u], v_sem.at[u]).wait()
        hops(u)[2](*sems(u, 0)).wait_send()
        core_arrived(u).wait_send()
    for p in range(max(nu // 2 - 2, 0), nu // 2):
        z_store(p, p % 2).wait()
    out.wait()
    sq.wait()


def backward_phase(dm, bits, peers, q, tmp, tb, eb, acc, zb, vb, cbuf, obuf, sbuf, csend_sem, core_sem, credit,
                   tiles, x_ready, core_lag, after_core, events):
    t, d, f, nf, nl = dm
    nu = nf * nl
    core = bits[0]
    slots = cbuf.shape[0]

    def core_copy(it):
        slot = odd(it)
        return remote(sbuf.at[slot], cbuf.at[lax.rem(it, slots)], csend_sem.at[slot], core_sem.at[it], peers[0])

    def core_stage(j):
        cs = lax.rem(j, slots)
        core_copy(j).wait_recv()
        cbuf[cs] = cbuf[cs] + obuf[odd(j)]
        after_core(j)

    @steps(nu + max(lag for lag, _ in events))
    def _(it):
        @pl.when(it == nf)
        def _():
            fwd_close(q, acc, t)
            transpose_into(tb.at[1], q, t)
            x_ready()
            transpose_into(tb.at[0], tmp, t)

        @pl.when(it < nu)
        def _():
            slot = odd(it)
            for cp in tiles(it, slot):
                cp.wait()

            @pl.when(it + 1 < nu)
            def _():
                for cp in tiles(it + 1, 1 - slot):
                    cp.start()
            for lo, n in halves(t):
                back = dot(q[lo:lo + n, :], vb[slot, 1])
                a, slope = gelu_and_grad(zb[slot, lo:lo + n, :].astype(jnp.float32))
                eb[1, lo:lo + n, :] = a.astype(jnp.bfloat16)
                eb[0, lo:lo + n, :] = (back * slope).astype(jnp.bfloat16)

            @pl.when(it >= 2)
            def _():
                core_copy(it - 2).wait_send()
            sbuf[slot] = dot(tb[1 - core], eb[1 - core])

            @pl.when(it >= slots)
            def _():
                pl.semaphore_wait(credit)
            core_copy(it).start()
            obuf[slot] = dot(tb[core], eb[core])

            @pl.when(it < nf)
            def _():
                for lo, n in halves(t):
                    acc[lo:lo + n, :] += dot(eb[0, lo:lo + n, :], vb[slot, 0], NT)

        for lag, event in ((core_lag, core_stage), *events):
            j = it - lag

            @pl.when((j >= 0) & (j < nu))
            def _():
                event(j)

    core_copy(nu - 2).wait_send()
    core_copy(nu - 1).wait_send()


def free_slot(j, nu, slots, credit, peer):
    @pl.when(j + slots < nu)
    def _():
        pl.semaphore_signal(credit, device_id=(peer,), device_id_type=MESH)


def halving(dm, bits, peers, cbuf, rbuf, send_sem, recv_sem, credit, lags, on_total):
    t, d, f, nf, nl = dm
    nu = nf * nl
    piece = d // 16
    slots = cbuf.shape[0]
    partner = peers[0]

    def rs_sends(it, k):
        ps, _, send, on = route(bits, peers, it, d)
        n = d >> (k + 1)
        cs = lax.rem(it, slots)

        def part(off, m, sem):
            return remote(cbuf.at[cs, pl.ds(send[k] + off, m), :], rbuf[k].at[it, pl.ds(off, m), :], send_sem.at[it], sem, ps[k])
        if k == 3:
            return [part(0, n, recv_sem.at[0, it, k])]
        m = n // 2
        return [part(pl.multiple_of((1 - on[k + 1]) * m, piece), m, recv_sem.at[0, it, k]),
                part(pl.multiple_of(on[k + 1] * m, piece), m, recv_sem.at[1, it, k])]

    def rs_add(it, k, kept):
        ps, keep, send, _ = route(bits, peers, it, d)
        cs = lax.rem(it, slots)
        if k == 3:
            base, m = keep[4], d >> 4
        else:
            base, m = (keep[k + 2] if kept else send[k + 1]), d >> (k + 2)
        here = rbuf[k].at[it, pl.ds(pl.multiple_of(base - keep[k + 1], piece), m), :]
        mine = cbuf.at[cs, pl.ds(base, m), :]
        remote(mine, here, send_sem.at[it], recv_sem.at[1 if kept else 0, it, k], ps[k]).wait_recv()
        total = mine[...] + here[...]
        if k == 3:
            return total
        mine[...] = total

    def start(j):
        for cp in rs_sends(j, 0):
            cp.start()

    def stage(k):
        def event(j):
            if k > 0:
                rs_add(j, k - 1, True)
            total = rs_add(j, k, False)
            if k < 3:
                for cp in rs_sends(j, k + 1):
                    cp.start()
            else:
                on_total(unit_of(j, nf, nl), total)
                ref = cbuf.at[lax.rem(j, slots), pl.ds(0, 15 * piece), :]
                remote(ref, ref, send_sem.at[j], recv_sem.at[0, j, 3], partner).wait_send()
                free_slot(j, nu, slots, credit, partner)
        return event
    return start, [(lags[k], stage(k)) for k in range(4)]


def chain(dm, bits, peers, cbuf, rbuf, gs, w_out, send_sem, recv_sem, credit, ag_send, ag_recv, ag_loc, lags, on_total):
    t, d, f, nf, nl = dm
    nu = nf * nl
    core, _, _, ba, bb = bits
    piece = d // 16
    slots = cbuf.shape[0]
    r1, r2, r3, r4, r5 = rbuf
    at_end = ba == bb
    chunk = d // 8
    XU, XK, EU, EK, MU, MK, YY = range(7)
    ALL, MIDDLE, CORE = range(3)
    HALF, MATE, PAIR, LAST, FULL = range(5)
    partner = peers[0]

    def send(j, src, dst, sem, peer):
        remote(cbuf.at[lax.rem(j, slots), src, :], dst, send_sem.at[j], recv_sem.at[sem, j], peer).start()

    def add(j, rows, buf, sem):
        mine = cbuf.at[lax.rem(j, slots), rows, :]
        remote(mine, buf, send_sem.at[j], recv_sem.at[sem, j], partner).wait_recv()
        mine[...] = mine[...] + buf[...]

    def at(j):
        return chain_route(bits, peers, unit_of(j, nf, nl), d)

    def start(j):
        r, p1, _, _, _ = at(j)
        for (src, dst), sem in ((r["x_send_first"], XU), (r["x_send_second"], XK)):
            send(j, src, r1.at[j, dst, :], sem, p1)

    def rel(first):
        return pl.ds(pl.multiple_of((1 - bb if first else bb) * (d // 4), piece), d // 4)

    def s1(j):
        r, _, pa, _, _ = at(j)
        add(j, r["other_pair"], r1.at[j, rel(True), :], XU)

        @pl.when(at_end)
        def _():
            send(j, r["other_pair"], r2.at[j], EU, pa)

    def s2(j):
        r, _, pa, pm, _ = at(j)
        add(j, r["pair"], r1.at[j, rel(False), :], XK)

        @pl.when(at_end)
        def _():
            send(j, r["mate"], r3.at[j], EK, pa)

        @pl.when(jnp.logical_not(at_end))
        def _():
            add(j, r["other_pair"], r2.at[j], EU)
            send(j, r["far_end"], r5.at[j, 0:chunk, :], MU, pm)
            send(j, r["far_mid"], r5.at[j, chunk:2 * chunk, :], MK, pm)

    def s3(j):
        r, _, pa, _, p3 = at(j)

        @pl.when(jnp.logical_not(at_end))
        def _():
            add(j, r["mate"], r5.at[j, 0:chunk, :], MU)
            send(j, r["mate"], r3.at[j], EK, pa)
            add(j, r["own"], r3.at[j], EK)
            add(j, r["own"], r5.at[j, chunk:2 * chunk, :], MK)
            send(j, r["send"], r4.at[j], YY, p3)

    def s4(j):
        r, _, _, _, p3 = at(j)

        @pl.when(at_end)
        def _():
            add(j, r["own"], r3.at[j], EK)
            send(j, r["send"], r4.at[j], YY, p3)

    def full(j):
        return w_out.at[unit_of(j, nf, nl), core]

    def give(j, rows, sem_s, sem_r, peer, src=None):
        ref = full(j).at[rows, :]
        return remote(ref if src is None else src, ref, ag_send.at[j, sem_s], ag_recv.at[j, sem_r], peer)

    def own_copy(j):
        u = unit_of(j, nf, nl)
        return local(gs.at[u], full(j).at[at(j)[0]["keep"], :], ag_loc.at[j])

    def s5(j):
        r, _, _, _, p3 = at(j)
        u = unit_of(j, nf, nl)
        mine = cbuf.at[lax.rem(j, slots), r["keep"], :]
        remote(mine, r4.at[j], send_sem.at[j], recv_sem.at[YY, j], p3).wait_recv()
        on_total(u, mine[...] + r4[j])
        own_copy(j).start()
        give(j, r["keep"], ALL, HALF, p3, gs.at[u]).start()
        ref = cbuf.at[lax.rem(j, slots), pl.ds(0, 15 * piece), :]
        remote(ref, ref, send_sem.at[j], recv_sem.at[YY, j], p3).wait_send()
        free_slot(j, nu, slots, credit, partner)

    def g1(j):
        r, p1, pa, pm, p3 = at(j)
        own_copy(j).wait()
        give(j, r["send"], ALL, HALF, p3).wait_recv()
        give(j, r["own"], ALL, MATE, pa).start()

        @pl.when(jnp.logical_not(at_end))
        def _():
            give(j, r["own"], MIDDLE, PAIR, pm).start()
        give(j, r["own"], ALL, LAST, p1).start()

    def g2(j):
        r, p1, pa, pm, _ = at(j)
        give(j, r["mate"], ALL, MATE, pa).wait_recv()

        @pl.when(jnp.logical_not(at_end))
        def _():
            give(j, r["mate"], MIDDLE, PAIR, pm).start()
        give(j, r["mate"], ALL, LAST, p1).start()

    def g3(j, r, p1, pa):
        give(j, r["other_pair"], MIDDLE, PAIR, pa).wait_recv()
        give(j, r["other_pair"], ALL, LAST, p1).start()
        give(j, r["half"], CORE, FULL, partner).start()

    def g3_middle(j):
        r, p1, pa, _, _ = at(j)

        @pl.when(jnp.logical_not(at_end))
        def _():
            g3(j, r, p1, pa)
            give(j, r["other_pair"], MIDDLE, PAIR, pa).start()

    def g3_end(j):
        r, p1, pa, _, _ = at(j)

        @pl.when(at_end)
        def _():
            g3(j, r, p1, pa)

    def g4(j):
        r, p1, _, _, _ = at(j)
        give(j, r["other_half"], ALL, LAST, p1).wait_recv()
        give(j, r["other_half"], CORE, FULL, partner).start()

    def finish_unit(j):
        ref = w_out.at[unit_of(j, nf, nl), 1 - core]
        last = remote(ref, ref, ag_send.at[j, CORE], ag_recv.at[j, FULL], partner)
        last.wait_recv()
        last.wait_send()
        ref = full(j).at[pl.ds(0, 11 * piece), :]
        remote(ref, ref, ag_send.at[j, ALL], ag_recv.at[j, LAST], partner).wait_send()

        @pl.when(jnp.logical_not(at_end))
        def _():
            ref = full(j).at[pl.ds(0, 8 * piece), :]
            remote(ref, ref, ag_send.at[j, MIDDLE], ag_recv.at[j, PAIR], partner).wait_send()

    steps = (s1, s2, s3, s4, s5, g1, g2, g3_middle, g3_end, g4)
    return start, list(zip(lags, steps)), finish_unit


def second_backward(dm, scale, x_hbm, h_hbm, q_hbm, z_hbm, v_hbm, ws_hbm, sq_hbm, w_out, sq_out,
                    q, tmp, tb, eb, acc, zb, vb, cbuf, obuf, sbuf, r1, r2, r3, r4, r5, gs,
                    load_sem, io_sem, csend_sem, core_sem, send_sem, recv_sem, credit, nb, ag_send, ag_recv, ag_loc, nsend_sem, nrecv_sem):
    t, d, f, nf, nl = dm
    nu = nf * nl
    bits, peers = place()
    near, far = others(bits, (0, 1, 2)), others(bits, (3, 4))
    wait_all = arrive(near + far)

    def tiles(it, slot):
        u = unit_of(it, nf, nl)
        return local(z_hbm.at[u], zb.at[slot], load_sem.at[slot, 0]), local(v_hbm.at[u], vb.at[slot], load_sem.at[slot, 1])

    q_in = local(q_hbm, q, io_sem.at[0])
    h_in = local(h_hbm, tmp, io_sem.at[1])
    ws_in = local(ws_hbm, gs, io_sem.at[2])
    sq_in = local(sq_hbm, nb.at[0], io_sem.at[3])
    q_in.start()
    for cp in tiles(0, 0):
        cp.start()
    for cp in (h_in, ws_in, sq_in):
        cp.start()
    q_in.wait()
    fwd_seed(q, acc, t)
    transpose_into(tb.at[1], q, t)
    h_in.wait()
    transpose_into(tb.at[0], tmp, t)
    x_in = local(x_hbm, tmp, io_sem.at[1])
    x_in.start()
    ws_in.wait()
    sq_in.wait()
    wait_all()

    def on_total(u, total):
        gs[u] = gs[u] - LEARN_RATE * (total * scale)

    def sums(j):
        @pl.when(j == 1)
        def _():
            exchange_sum(nb, 0, near, nsend_sem, nrecv_sem, 0)

        @pl.when(j == 2)
        def _():
            exchange_sum(nb, 8, far, nsend_sem, nrecv_sem, 7)

    start, events, finish_unit = chain(dm, bits, peers, cbuf, (r1, r2, r3, r4, r5), gs, w_out, send_sem, recv_sem, credit,
                                       ag_send, ag_recv, ag_loc, LAG_B[1:], on_total)
    backward_phase(dm, bits, peers, q, tmp, tb, eb, acc, zb, vb, cbuf, obuf, sbuf,
                   csend_sem, core_sem, credit, tiles, x_in.wait, LAG_B[0], start, [*events, (0, sums)])
    sq_cp = local(nb.at[12], sq_out, io_sem.at[3])
    sq_cp.start()

    @steps(nu)
    def _(j):
        finish_unit(j)
    sq_cp.wait()


def finish(scale, f, w_ref, sq_ref, in_ref, out_ref, loss_ref):
    for j in range(w_ref.shape[0]):
        in_ref[0, :, j * f:(j + 1) * f] = w_ref[j, 0]
        out_ref[0, j * f:(j + 1) * f, :] = w_ref[j, 1].T
    loss_ref[0, 0] = 0.5 * (jnp.sum(sq_ref[...]) * scale)


def sds(shape, dtype):
    return jax.ShapeDtypeStruct(shape, dtype)


def call(kernel, n_in, outs, scratch, name, collective_id=None):
    params = dict(vmem_limit_bytes=VMEM_CAP)
    if collective_id is not None:
        params.update(collective_id=collective_id, has_side_effects=True)
    return pl.pallas_call(
        kernel,
        out_shape=outs,
        in_specs=[ANY] * n_in,
        out_specs=[ANY] * len(outs),
        scratch_shapes=scratch,
        compiler_params=pltpu.CompilerParams(**params),
        name=name,
    )


def local_step(n_dev, tile_f, x_loc, y_loc, w_in, w_out):
    nl, d, ff = w_in.shape
    f = tile_f
    nf = ff // f
    nu = nl * nf
    t = x_loc.shape[0] * x_loc.shape[1]
    piece = d // 16
    dm = (t, d, f, nf, nl)
    scale = 1.0 / (t * n_dev * d)
    rho = RHO_FRAC * math.sqrt(nl * (d + ff))
    bf, f32 = jnp.bfloat16, jnp.float32
    V, DMA, REG = pltpu.VMEM, pltpu.SemaphoreType.DMA, pltpu.SemaphoreType.REGULAR
    x = x_loc.transpose(1, 0, 2).reshape(t, d)
    y = y_loc.transpose(1, 0, 2).reshape(t, d)
    z_s, v_s, w_s, a_s, n_s = sds((nu, t, f), bf), sds((nu, 2, d, f), bf), sds((nu, piece, f), f32), sds((t, d), bf), sds(TILE, f32)
    slots = min(CORE_SLOTS, nu)
    tile2, rows = V((2, d, f), f32), V((nu, piece, f), f32)
    reduce_bufs = [V((slots, d, f), f32), tile2, tile2, *(V((nu, d >> k, f), f32) for k in range(1, 5))]
    act, sums, both = V((t, d), bf), V((t, d), f32), V((t, 2 * f), bf)
    acts = [act, act, V((2, d, t), bf), V((2, t, f), bf), sums]
    norms, tens = V((13, *TILE), f32), DMA((10,))
    two, four, per_unit, loads = DMA((2,)), DMA((4,)), DMA((nu,)), DMA((2, 2))

    z, v, ws, wc, g, norm = call(
        functools.partial(first_pass, dm, scale), 4, [z_s, v_s, w_s, w_s, w_s, n_s],
        acts + [both, V((2, d, 2 * f), f32), V((2, 2 * f, d), f32), V((2, 2, t, f), bf), V((2, 2, 2, d, f), bf), rows, rows]
        + reduce_bufs + [norms, loads, two, two, four, two, per_unit, per_unit, DMA((2, nu, 4)), REG, tens, tens],
        "pass_a", 0)(x, y, w_in, w_out)

    z, v, h1, q, sq = call(
        functools.partial(second_forward, dm, scale, rho), 5, [z_s, v_s, a_s, a_s, n_s],
        [act, act, sums, both, rows, rows, V((nu, 2, d, f), bf), V((2, 2, t, f), bf), V(TILE, f32),
         DMA((nu, 2)), DMA((nu, 5)), two, per_unit, DMA((5,))], "fwd_b", 1)(g, ws, norm, x, y)

    w_new, sq = call(
        functools.partial(second_backward, dm, scale), 7, [sds((nu, 2, d, f), f32), n_s],
        acts + [V((2, t, f), bf), V((2, 2, d, f), bf)] + reduce_bufs
        + [V((nu, d // 4, f), f32), rows, loads, four, two, per_unit, per_unit, DMA((7, nu)), REG,
           norms, DMA((nu, 3)), DMA((nu, 5)), per_unit, tens, tens], "bwd_b", 2)(x, h1, q, z, v, wc, sq)

    new_in, new_out, loss = pl.pallas_call(
        functools.partial(finish, scale, f),
        grid=(nl, nf // 4),
        in_specs=[pl.BlockSpec((4, 2, d, f), lambda i, j: (i * (nf // 4) + j, 0, 0, 0)), pl.BlockSpec(TILE, lambda i, j: (0, 0))],
        out_specs=[pl.BlockSpec((1, d, 4 * f), lambda i, j: (i, 0, j)), pl.BlockSpec((1, 4 * f, d), lambda i, j: (i, j, 0)),
                   pl.BlockSpec((1, 1), lambda i, j: (0, 0), memory_space=pltpu.SMEM)],
        out_shape=[sds((nl, d, ff), f32), sds((nl, ff, d), f32), sds((1, 1), f32)],
        compiler_params=pltpu.CompilerParams(vmem_limit_bytes=VMEM_CAP),
        name="finish")(w_new, sq)
    return new_in, new_out, loss.reshape(())


def solution(mesh):
    step = functools.partial(local_step, mesh.shape["data"], TILE_F)
    return jax.shard_map(step, mesh=mesh, in_specs=(P("data"), P("data"), P(), P()), out_specs=(P(), P(), P()), check_vma=False)
```

```python
import math
import functools
import jax
import jax.numpy as jnp
from jax import lax
from jax.experimental import pallas as pl
from jax.experimental.pallas import tpu as pltpu
from jax.sharding import PartitionSpec as P

RHO_FRAC = 0.1
LEARN_RATE = 1.0
TILE_F = 256
MESH = pl.DeviceIdType.MESH
ANY = pl.BlockSpec(memory_space=pl.ANY)
NN = (((1,), (0,)), ((), ()))
NT = (((1,), (1,)), ((), ()))
GELU_C = math.sqrt(2.0 / math.pi)
GELU_K = 0.044715
VMEM_CAP = 67043328
TILE = (8, 128)
FINISH_TILES = 6
CORE_SLOTS = 9
LAG_A = (0, 1, 3, 5, 7)
LAG_B = (0, 2, 3, 4, 5, 6, 7, 8, 9, 11, 12)
VG_LAG = (0, 1, 2, 4, 6, 8)


steps = functools.partial(pl.loop, 0)


def odd(i):
    return lax.rem(i, 2)


def dot(lhs, rhs, dims=NN):
    return lax.dot_general(lhs, rhs, dims, preferred_element_type=jnp.float32)


def gelu_parts(z):
    sq = z * z
    th = jnp.tanh(GELU_C * (z + GELU_K * (sq * z)))
    cdf = 0.5 * (1.0 + th)
    return sq, th, cdf


def gelu(z):
    return z * gelu_parts(z)[2]


def gelu_and_grad(z):
    sq, th, cdf = gelu_parts(z)
    slope = cdf + (0.5 * z) * ((1.0 - th * th) * (GELU_C + (3.0 * GELU_K * GELU_C) * sq))
    return z * cdf, slope


def place(axis="data"):
    me = lax.axis_index(axis)
    bits = [lax.rem(lax.div(me, 1 << k), 2) for k in range(5)]
    peers = [me + (1 << k) * (1 - 2 * bits[k]) for k in range(5)]
    return bits, peers


def route(bits, peers, unit, rows):
    core, bx, by, ba, bb = bits
    _, px, py, pa, pb = peers
    swap = odd(unit + core) == 1
    b1, p1 = jnp.where(swap, by, bx), jnp.where(swap, py, px)
    b3, p3 = jnp.where(swap, bx, by), jnp.where(swap, px, py)
    axes = (b1, ba, b3, bb)
    step = rows // 16
    keep, send, base = [0], [], 0
    n = rows
    for bit in axes:
        n //= 2
        keep.append(pl.multiple_of(base + bit * n, step))
        send.append(pl.multiple_of(base + (1 - bit) * n, step))
        base = base + bit * n
    return (p1, pa, p3, pb), keep, send, axes


def chain_route(bits, peers, unit, d):
    core, bx, by, ba, bb = bits
    _, px, py, pa, _ = peers
    swap = odd(unit + core) == 1
    b1, p1 = jnp.where(swap, by, bx), jnp.where(swap, py, px)
    b3, p3 = jnp.where(swap, bx, by), jnp.where(swap, px, py)
    piece, chunk, pair, half = d // 16, d // 8, d // 4, d // 2
    me = lax.axis_index("data")

    def rows(base, n):
        return pl.ds(pl.multiple_of(base, piece), n)
    kx = b1 * half
    own = kx + (2 * bb + ba) * chunk
    mate = 2 * (kx + bb * pair) + chunk - own
    r = dict(
        half=rows(kx, half), other_half=rows((1 - b1) * half, half),
        pair=rows(kx + bb * pair, pair), other_pair=rows(kx + (1 - bb) * pair, pair),
        own=rows(own, chunk), mate=rows(mate, chunk),
        far_end=rows(kx + (1 - bb) * 3 * chunk, chunk), far_mid=rows(kx + (2 - bb) * chunk, chunk),
        keep=rows(own + b3 * piece, piece), send=rows(own + (1 - b3) * piece, piece),
        x_send_first=(rows((1 - b1) * half + (1 - bb) * pair, pair), rows((1 - bb) * pair, pair)),
        x_send_second=(rows((1 - b1) * half + bb * pair, pair), rows(bb * pair, pair)),
    )
    return r, p1, pa, me + 8 * (1 - 2 * bb), p3


def arrive(peers):
    barrier = pltpu.get_barrier_semaphore()
    for peer in peers:
        pl.semaphore_signal(barrier, device_id=(peer,), device_id_type=MESH)
    return functools.partial(pl.semaphore_wait, barrier, len(peers))


def others(bits, me_bits):
    me = lax.axis_index("data")
    out = []
    for mask in range(1, 1 << len(me_bits)):
        peer = me
        for i, k in enumerate(me_bits):
            if mask >> i & 1:
                peer = peer + (1 << k) * (1 - 2 * bits[k])
        out.append(peer)
    return out


def exchange_sum(buf, first, peers, send_sem, recv_sem, sem0):
    copies = [remote(buf.at[first], buf.at[first + 1 + i], send_sem.at[sem0 + i], recv_sem.at[sem0 + i], peer) for i, peer in enumerate(peers)]
    for cp in copies:
        cp.start()
    total = buf[first]
    for i, cp in enumerate(copies):
        cp.wait()
        total = total + buf[first + 1 + i]
    buf[first + len(peers) + 1] = total


def gather_hops(bits, peers, unit, d, full, piece_src=None):
    ps, keep, send, _ = route(bits, peers, unit, d)
    piece = d // 16

    def rows(base, n):
        return full.at[pl.ds(base, n), :]

    def hop(k, part, sem_s, sem_r):
        peer = ps[3 - k] if k < 4 else peers[0]
        if k == 0:
            ref = rows(keep[4], piece)
        elif part == 0:
            ref = rows(keep[5 - k], piece << (k - 1))
        else:
            ref = rows(send[4 - k], piece << (k - 1))
        src = piece_src if piece_src is not None and part == 0 and k <= 1 else ref
        return remote(src, ref, sem_s, sem_r, peer)

    def arrived(k, sem_s, sem_r):
        ref = rows(send[3 - k], piece << k)
        return remote(ref, ref, sem_s, sem_r, ps[3 - k])

    def sent(sem_s, sem_r):
        ref = rows(0, 15 * piece)
        return remote(ref, ref, sem_s, sem_r, ps[0])
    return hop, arrived, sent


def remote(src, dst, send_sem, recv_sem, peer):
    return pltpu.make_async_remote_copy(src_ref=src, dst_ref=dst, send_sem=send_sem, recv_sem=recv_sem, device_id=(peer,), device_id_type=MESH)


def local(src, dst, sem):
    return pltpu.make_async_copy(src, dst, sem)


def halves(t):
    return [(0, t // 2), (t // 2, t // 2)] if t % 32 == 0 else [(0, t)]


def transpose_into(dst, src, t):
    full = t // 128
    if full:
        @steps(full)
        def _(i):
            lo = pl.multiple_of(i * 128, 128)
            dst[:, pl.ds(lo, 128)] = src[pl.ds(lo, 128), :].T
    if t % 128:
        dst[:, full * 128:t] = src[full * 128:t, :].T


def fwd_pair(h_ref, v_ref, acc_ref, a_ref, z_ref, t, f):
    for lo, n in halves(t):
        for j in range(2):
            z = dot(h_ref[lo:lo + n, :], v_ref[j, 0]).astype(jnp.bfloat16)
            z_ref[j, lo:lo + n, :] = z
            a_ref[lo:lo + n, j * f:(j + 1) * f] = gelu(z.astype(jnp.float32)).astype(jnp.bfloat16)
    v_out = jnp.concatenate([v_ref[0, 1], v_ref[1, 1]], axis=1)
    for lo, n in halves(t):
        acc_ref[lo:lo + n, :] += dot(a_ref[lo:lo + n, :], v_out, NT)


def fwd_close(h_ref, acc_ref, t):
    for lo, n in halves(t):
        h_ref[lo:lo + n, :] = acc_ref[lo:lo + n, :].astype(jnp.bfloat16)


def fwd_seed(h_ref, acc_ref, t):
    for lo, n in halves(t):
        acc_ref[lo:lo + n, :] = h_ref[lo:lo + n, :].astype(jnp.float32)


def fold(v):
    r, c = v.shape
    rows = jnp.sum(v.reshape(r // 8, 8, c), axis=0)
    return sum(rows[:, lo:lo + 128] for lo in range(0, c, 128))


def loss_close(h_ref, y_ref, acc_ref, t, d, total_ref=None):
    def rows_of(rows):
        e = acc_ref[rows, :].astype(jnp.bfloat16).astype(jnp.float32) - y_ref[rows, :].astype(jnp.float32)
        q = e.astype(jnp.bfloat16)
        h_ref[rows, :] = q
        acc_ref[rows, :] = q.astype(jnp.float32)
        return e
    if total_ref is None:
        for lo, n in halves(t):
            rows_of(slice(lo, lo + n))
        return
    n = 112 if t % 112 == 0 else t
    total_ref[...] = jnp.zeros(TILE, jnp.float32)

    @steps(t // n)
    def _(i):
        e = rows_of(pl.ds(pl.multiple_of(i * n, n), n))
        total_ref[...] += fold(e * e)


def unit_of(it, nf, nl):
    return (nl - 1 - it // nf) * nf + lax.rem(it, nf)


def first_pass(dm, scale, x_hbm, y_hbm, wi_hbm, wo_hbm, z_out, v_out, ws_out, wc_out, g_out, n_out,
               h, tmp, tb, eb, acc, ab, wi, wo, zb, vb, ws, wc, cbuf, obuf, sbuf, r1, r2, r3, r4, nb,
               load_sem, z_sem, v_sem, io_sem, csend_sem, core_sem, send_sem, recv_sem, credit, nsend_sem, nrecv_sem):
    t, d, f, nf, nl = dm
    nu = nf * nl
    bits, peers = place()
    piece = d // 16
    near, far = others(bits, (0, 1, 2)), others(bits, (3, 4))
    wait_all = arrive(near + far)

    def loads(p, slot):
        layer, tile = p // (nf // 2), lax.rem(p, nf // 2)
        lo = pl.multiple_of(tile * 2 * f, 2 * f)
        return (local(wi_hbm.at[layer, :, pl.ds(lo, 2 * f)], wi.at[slot], load_sem.at[slot, 0]),
                local(wo_hbm.at[layer, pl.ds(lo, 2 * f), :], wo.at[slot], load_sem.at[slot, 1]))

    def stores(p, slot):
        two = pl.ds(2 * p, 2)
        return local(zb.at[slot], z_out.at[two], z_sem.at[slot]), local(vb.at[slot], v_out.at[two], v_sem.at[slot])

    x_in = local(x_hbm, h, io_sem.at[0])
    y_in = local(y_hbm, tmp, io_sem.at[1])
    x_in.start()
    for cp in loads(0, 0):
        cp.start()
    y_in.start()
    x_in.wait()
    fwd_seed(h, acc, t)

    @steps(nu // 2)
    def _(p):
        slot = odd(p)
        for cp in loads(p, slot):
            cp.wait()

        @pl.when(p + 1 < nu // 2)
        def _():
            for cp in loads(p + 1, 1 - slot):
                cp.start()

        @pl.when(p >= 2)
        def _():
            for cp in stores(p - 2, slot):
                cp.wait()
        for j in range(2):
            cols = slice(j * f, (j + 1) * f)
            wot = wo[slot, cols, :].T
            _, keep, _, _ = route(bits, peers, 2 * p + j, d)
            rows = pl.ds(keep[4], piece)
            vb[slot, j, 0] = wi[slot, :, cols].astype(jnp.bfloat16)
            vb[slot, j, 1] = wot.astype(jnp.bfloat16)
            obuf[j] = wot
            ws[2 * p + j] = jnp.where(bits[0] == 0, wi[slot, rows, cols], obuf[j, rows, :])
            rows = chain_route(bits, peers, j, d)[0]['keep']
            wc[2 * p + j] = jnp.where(bits[0] == 0, wi[slot, rows, cols], obuf[j, rows, :])

        fwd_pair(h, vb.at[slot], acc, ab, zb.at[slot], t, f)
        for cp in stores(p, slot):
            cp.start()

        @pl.when(p == nf // 2 - 1)
        def _():
            fwd_close(h, acc, t)
            fwd_seed(h, acc, t)
            transpose_into(tb.at[0], h, t)

    np_ = nu // 2
    if np_ >= 2:
        for cp in stores(np_ - 2, np_ % 2):
            cp.wait()
    spare = np_ % 2

    def tiles(it, slot):
        u = unit_of(it, nf, nl)
        return (local(z_out.at[u], zb.at[spare, slot], load_sem.at[slot, 0]), local(v_out.at[u], vb.at[spare, slot], load_sem.at[slot, 1]))
    for cp in tiles(0, 0):
        cp.start()
    ws_cp = local(ws, ws_out, io_sem.at[2])
    wc_cp = local(wc, wc_out, io_sem.at[3])
    ws_cp.start()
    wc_cp.start()
    y_in.wait()
    loss_close(h, tmp, acc, t, d)
    transpose_into(tb.at[1], h, t)
    x_again = local(x_hbm, tmp, io_sem.at[1])
    x_again.start()
    for cp in stores(np_ - 1, (np_ - 1) % 2):
        cp.wait()
    wait_all()
    nb[0] = jnp.zeros(TILE, jnp.float32)

    ws_cp.wait()

    def on_total(u, total):
        ws[u] = total
        g = total * scale
        nb[0] += fold(g * g)

    start, events = halving(dm, bits, peers, cbuf, (r1, r2, r3, r4), send_sem, recv_sem, credit, LAG_A[1:], on_total)
    backward_phase(dm, bits, peers, h, tmp, tb, eb, acc, zb.at[spare], vb.at[spare], cbuf, obuf, sbuf,
                   csend_sem, core_sem, credit, tiles, x_again.wait, LAG_A[0], start, events)
    g_cp = local(ws, g_out, io_sem.at[0])
    g_cp.start()
    exchange_sum(nb, 0, near, nsend_sem, nrecv_sem, 0)
    exchange_sum(nb, 8, far, nsend_sem, nrecv_sem, 7)
    n_cp = local(nb.at[12], n_out, io_sem.at[1])
    n_cp.start()
    wc_cp.wait()
    g_cp.wait()
    n_cp.wait()


def second_forward(dm, scale, rho, gs_hbm, ws_hbm, n_hbm, x_hbm, y_hbm, z_out, v_out, h_out, q_out, sq_out,
                   h, yb, acc, ab, gs, ws, vb, zb, nb, send_sem, recv_sem, z_sem, v_sem, io_sem):
    t, d, f, nf, nl = dm
    nu = nf * nl
    bits, peers = place()
    core = bits[0]
    piece = d // 16
    wait_all = arrive(peers)
    ins = (local(gs_hbm, gs, io_sem.at[0]), local(ws_hbm, ws, io_sem.at[1]), local(x_hbm, h, io_sem.at[2]), local(y_hbm, yb, io_sem.at[3]))
    n_in = local(n_hbm, nb, io_sem.at[4])
    n_in.start()
    for cp in ins:
        cp.start()
    n_in.wait()
    coef = rho / jnp.sqrt(jnp.sum(nb[...], keepdims=True))
    ins[0].wait()
    ins[1].wait()
    wait_all()

    def hops(u):
        return gather_hops(bits, peers, u, d, vb.at[u, core])

    def sems(u, k):
        return send_sem.at[u, 0 if k < 4 else 1], recv_sem.at[u, k]

    def core_arrived(u):
        ref = vb.at[u, 1 - core]
        return remote(ref, ref, *sems(u, 4), peers[0])

    def z_store(p, slot):
        return local(zb.at[slot], z_out.at[pl.ds(2 * p, 2)], z_sem.at[slot])

    @steps(nu + VG_LAG[5])
    def _(it):
        @pl.when(it < nu)
        def _():
            _, keep, _, _ = route(bits, peers, it, d)
            new = ws[it] + coef * (gs[it] * scale)
            vb[it, core, pl.ds(keep[4], piece), :] = new.astype(jnp.bfloat16)
            hop, _, _ = hops(it)
            hop(0, 0, *sems(it, 0)).start()
            hop(1, 0, *sems(it, 1)).start()
        for k in range(1, 5):
            u = it - VG_LAG[k]

            @pl.when((u >= 0) & (u < nu))
            def _():
                hop, arrived, _ = hops(u)
                arrived(k - 1, *sems(u, k - 1)).wait_recv()
                hop(k, 1, *sems(u, k)).start()
                if k < 4:
                    hop(k + 1, 0, *sems(u, k + 1)).start()
        u = it - VG_LAG[5]

        @pl.when(u >= 0)
        def _():
            core_arrived(u).wait_recv()
            local(vb.at[u], v_out.at[u], v_sem.at[u]).start()

        @pl.when((u >= 0) & (odd(u) == 1))
        def _():
            p = u // 2
            slot = odd(p)

            @pl.when(p >= 2)
            def _():
                z_store(p - 2, slot).wait()

            @pl.when(p == 0)
            def _():
                ins[2].wait()
                fwd_seed(h, acc, t)
            fwd_pair(h, vb.at[pl.ds(2 * p, 2)], acc, ab, zb.at[slot], t, f)
            z_store(p, slot).start()

            @pl.when(p == nf // 2 - 1)
            def _():
                fwd_close(h, acc, t)
                fwd_seed(h, acc, t)
                out = local(h, h_out, io_sem.at[0])
                out.start()
                out.wait()

    ins[3].wait()
    loss_close(h, yb, acc, t, d, nb)
    out = local(h, q_out, io_sem.at[0])
    sq = local(nb, sq_out, io_sem.at[1])
    out.start()
    sq.start()

    @steps(nu)
    def _(u):
        local(vb.at[u], v_out.at[u], v_sem.at[u]).wait()
        hops(u)[2](*sems(u, 0)).wait_send()
        core_arrived(u).wait_send()
    for p in range(max(nu // 2 - 2, 0), nu // 2):
        z_store(p, p % 2).wait()
    out.wait()
    sq.wait()


def backward_phase(dm, bits, peers, q, tmp, tb, eb, acc, zb, vb, cbuf, obuf, sbuf, csend_sem, core_sem, credit,
                   tiles, x_ready, core_lag, after_core, events):
    t, d, f, nf, nl = dm
    nu = nf * nl
    core = bits[0]
    slots = cbuf.shape[0]

    def core_copy(it):
        slot = odd(it)
        return remote(sbuf.at[slot], cbuf.at[lax.rem(it, slots)], csend_sem.at[slot], core_sem.at[it], peers[0])

    def core_stage(j):
        cs = lax.rem(j, slots)
        core_copy(j).wait_recv()
        cbuf[cs] = cbuf[cs] + obuf[odd(j)]
        after_core(j)

    @steps(nu + max(lag for lag, _ in events))
    def _(it):
        @pl.when(it == nf)
        def _():
            fwd_close(q, acc, t)
            transpose_into(tb.at[1], q, t)
            x_ready()
            transpose_into(tb.at[0], tmp, t)

        @pl.when(it < nu)
        def _():
            slot = odd(it)
            for cp in tiles(it, slot):
                cp.wait()

            @pl.when(it + 1 < nu)
            def _():
                for cp in tiles(it + 1, 1 - slot):
                    cp.start()
            for lo, n in halves(t):
                back = dot(q[lo:lo + n, :], vb[slot, 1])
                a, slope = gelu_and_grad(zb[slot, lo:lo + n, :].astype(jnp.float32))
                eb[1, lo:lo + n, :] = a.astype(jnp.bfloat16)
                eb[0, lo:lo + n, :] = (back * slope).astype(jnp.bfloat16)

            @pl.when(it >= 2)
            def _():
                core_copy(it - 2).wait_send()
            sbuf[slot] = dot(tb[1 - core], eb[1 - core])

            @pl.when(it >= slots)
            def _():
                pl.semaphore_wait(credit)
            core_copy(it).start()
            obuf[slot] = dot(tb[core], eb[core])

            @pl.when(it < nf)
            def _():
                for lo, n in halves(t):
                    acc[lo:lo + n, :] += dot(eb[0, lo:lo + n, :], vb[slot, 0], NT)

        for lag, event in ((core_lag, core_stage), *events):
            j = it - lag

            @pl.when((j >= 0) & (j < nu))
            def _():
                event(j)

    core_copy(nu - 2).wait_send()
    core_copy(nu - 1).wait_send()


def free_slot(j, nu, slots, credit, peer):
    @pl.when(j + slots < nu)
    def _():
        pl.semaphore_signal(credit, device_id=(peer,), device_id_type=MESH)


def halving(dm, bits, peers, cbuf, rbuf, send_sem, recv_sem, credit, lags, on_total):
    t, d, f, nf, nl = dm
    nu = nf * nl
    piece = d // 16
    slots = cbuf.shape[0]
    partner = peers[0]

    def rs_sends(it, k):
        ps, _, send, on = route(bits, peers, it, d)
        n = d >> (k + 1)
        cs = lax.rem(it, slots)

        def part(off, m, sem):
            return remote(cbuf.at[cs, pl.ds(send[k] + off, m), :], rbuf[k].at[it, pl.ds(off, m), :], send_sem.at[it], sem, ps[k])
        if k == 3:
            return [part(0, n, recv_sem.at[0, it, k])]
        m = n // 2
        return [part(pl.multiple_of((1 - on[k + 1]) * m, piece), m, recv_sem.at[0, it, k]),
                part(pl.multiple_of(on[k + 1] * m, piece), m, recv_sem.at[1, it, k])]

    def rs_add(it, k, kept):
        ps, keep, send, _ = route(bits, peers, it, d)
        cs = lax.rem(it, slots)
        if k == 3:
            base, m = keep[4], d >> 4
        else:
            base, m = (keep[k + 2] if kept else send[k + 1]), d >> (k + 2)
        here = rbuf[k].at[it, pl.ds(pl.multiple_of(base - keep[k + 1], piece), m), :]
        mine = cbuf.at[cs, pl.ds(base, m), :]
        remote(mine, here, send_sem.at[it], recv_sem.at[1 if kept else 0, it, k], ps[k]).wait_recv()
        total = mine[...] + here[...]
        if k == 3:
            return total
        mine[...] = total

    def start(j):
        for cp in rs_sends(j, 0):
            cp.start()

    def stage(k):
        def event(j):
            if k > 0:
                rs_add(j, k - 1, True)
            total = rs_add(j, k, False)
            if k < 3:
                for cp in rs_sends(j, k + 1):
                    cp.start()
            else:
                on_total(unit_of(j, nf, nl), total)
                ref = cbuf.at[lax.rem(j, slots), pl.ds(0, 15 * piece), :]
                remote(ref, ref, send_sem.at[j], recv_sem.at[0, j, 3], partner).wait_send()
                free_slot(j, nu, slots, credit, partner)
        return event
    return start, [(lags[k], stage(k)) for k in range(4)]


def chain(dm, bits, peers, cbuf, rbuf, gs, w_out, send_sem, recv_sem, credit, ag_send, ag_recv, ag_loc, lags, on_total):
    t, d, f, nf, nl = dm
    nu = nf * nl
    core, _, _, ba, bb = bits
    piece = d // 16
    slots = cbuf.shape[0]
    r1, r2, r3, r4, r5 = rbuf
    at_end = ba == bb
    chunk = d // 8
    XU, XK, EU, EK, MU, MK, YY = range(7)
    ALL, MIDDLE, CORE = range(3)
    HALF, MATE, PAIR, LAST, FULL = range(5)
    partner = peers[0]

    def send(j, src, dst, sem, peer):
        remote(cbuf.at[lax.rem(j, slots), src, :], dst, send_sem.at[j], recv_sem.at[sem, j], peer).start()

    def add(j, rows, buf, sem):
        mine = cbuf.at[lax.rem(j, slots), rows, :]
        remote(mine, buf, send_sem.at[j], recv_sem.at[sem, j], partner).wait_recv()
        mine[...] = mine[...] + buf[...]

    def at(j):
        return chain_route(bits, peers, unit_of(j, nf, nl), d)

    def start(j):
        r, p1, _, _, _ = at(j)
        for (src, dst), sem in ((r["x_send_first"], XU), (r["x_send_second"], XK)):
            send(j, src, r1.at[j, dst, :], sem, p1)

    def rel(first):
        return pl.ds(pl.multiple_of((1 - bb if first else bb) * (d // 4), piece), d // 4)

    def s1(j):
        r, _, pa, _, _ = at(j)
        add(j, r["other_pair"], r1.at[j, rel(True), :], XU)

        @pl.when(at_end)
        def _():
            send(j, r["other_pair"], r2.at[j], EU, pa)

    def s2(j):
        r, _, pa, pm, _ = at(j)
        add(j, r["pair"], r1.at[j, rel(False), :], XK)

        @pl.when(at_end)
        def _():
            send(j, r["mate"], r3.at[j], EK, pa)

        @pl.when(jnp.logical_not(at_end))
        def _():
            add(j, r["other_pair"], r2.at[j], EU)
            send(j, r["far_end"], r5.at[j, 0:chunk, :], MU, pm)
            send(j, r["far_mid"], r5.at[j, chunk:2 * chunk, :], MK, pm)

    def s3(j):
        r, _, pa, _, p3 = at(j)

        @pl.when(jnp.logical_not(at_end))
        def _():
            add(j, r["mate"], r5.at[j, 0:chunk, :], MU)
            send(j, r["mate"], r3.at[j], EK, pa)
            add(j, r["own"], r3.at[j], EK)
            add(j, r["own"], r5.at[j, chunk:2 * chunk, :], MK)
            send(j, r["send"], r4.at[j], YY, p3)

    def s4(j):
        r, _, _, _, p3 = at(j)

        @pl.when(at_end)
        def _():
            add(j, r["own"], r3.at[j], EK)
            send(j, r["send"], r4.at[j], YY, p3)

    def full(j):
        return w_out.at[unit_of(j, nf, nl), core]

    def give(j, rows, sem_s, sem_r, peer, src=None):
        ref = full(j).at[rows, :]
        return remote(ref if src is None else src, ref, ag_send.at[j, sem_s], ag_recv.at[j, sem_r], peer)

    def own_copy(j):
        u = unit_of(j, nf, nl)
        return local(gs.at[u], full(j).at[at(j)[0]["keep"], :], ag_loc.at[j])

    def s5(j):
        r, _, _, _, p3 = at(j)
        u = unit_of(j, nf, nl)
        mine = cbuf.at[lax.rem(j, slots), r["keep"], :]
        remote(mine, r4.at[j], send_sem.at[j], recv_sem.at[YY, j], p3).wait_recv()
        on_total(u, mine[...] + r4[j])
        own_copy(j).start()
        give(j, r["keep"], ALL, HALF, p3, gs.at[u]).start()
        ref = cbuf.at[lax.rem(j, slots), pl.ds(0, 15 * piece), :]
        remote(ref, ref, send_sem.at[j], recv_sem.at[YY, j], p3).wait_send()
        free_slot(j, nu, slots, credit, partner)

    def g1(j):
        r, p1, pa, pm, p3 = at(j)
        own_copy(j).wait()
        give(j, r["send"], ALL, HALF, p3).wait_recv()
        give(j, r["own"], ALL, MATE, pa).start()

        @pl.when(jnp.logical_not(at_end))
        def _():
            give(j, r["own"], MIDDLE, PAIR, pm).start()
        give(j, r["own"], ALL, LAST, p1).start()

    def g2(j):
        r, p1, pa, pm, _ = at(j)
        give(j, r["mate"], ALL, MATE, pa).wait_recv()

        @pl.when(jnp.logical_not(at_end))
        def _():
            give(j, r["mate"], MIDDLE, PAIR, pm).start()
        give(j, r["mate"], ALL, LAST, p1).start()

    def g3(j, r, p1, pa):
        give(j, r["other_pair"], MIDDLE, PAIR, pa).wait_recv()
        give(j, r["other_pair"], ALL, LAST, p1).start()
        give(j, r["half"], CORE, FULL, partner).start()

    def g3_middle(j):
        r, p1, pa, _, _ = at(j)

        @pl.when(jnp.logical_not(at_end))
        def _():
            g3(j, r, p1, pa)
            give(j, r["other_pair"], MIDDLE, PAIR, pa).start()

    def g3_end(j):
        r, p1, pa, _, _ = at(j)

        @pl.when(at_end)
        def _():
            g3(j, r, p1, pa)

    def g4(j):
        r, p1, _, _, _ = at(j)
        give(j, r["other_half"], ALL, LAST, p1).wait_recv()
        give(j, r["other_half"], CORE, FULL, partner).start()

    def finish_unit(j):
        ref = w_out.at[unit_of(j, nf, nl), 1 - core]
        last = remote(ref, ref, ag_send.at[j, CORE], ag_recv.at[j, FULL], partner)
        last.wait_recv()
        last.wait_send()
        ref = full(j).at[pl.ds(0, 11 * piece), :]
        remote(ref, ref, ag_send.at[j, ALL], ag_recv.at[j, LAST], partner).wait_send()

        @pl.when(jnp.logical_not(at_end))
        def _():
            ref = full(j).at[pl.ds(0, 8 * piece), :]
            remote(ref, ref, ag_send.at[j, MIDDLE], ag_recv.at[j, PAIR], partner).wait_send()

    steps = (s1, s2, s3, s4, s5, g1, g2, g3_middle, g3_end, g4)
    return start, list(zip(lags, steps)), finish_unit


def second_backward(dm, scale, x_hbm, h_hbm, q_hbm, z_hbm, v_hbm, ws_hbm, sq_hbm, w_out, sq_out,
                    q, tmp, tb, eb, acc, zb, vb, cbuf, obuf, sbuf, r1, r2, r3, r4, r5, gs,
                    load_sem, io_sem, csend_sem, core_sem, send_sem, recv_sem, credit, nb, ag_send, ag_recv, ag_loc, nsend_sem, nrecv_sem):
    t, d, f, nf, nl = dm
    nu = nf * nl
    bits, peers = place()
    near, far = others(bits, (0, 1, 2)), others(bits, (3, 4))
    wait_all = arrive(near + far)

    def tiles(it, slot):
        u = unit_of(it, nf, nl)
        return local(z_hbm.at[u], zb.at[slot], load_sem.at[slot, 0]), local(v_hbm.at[u], vb.at[slot], load_sem.at[slot, 1])

    q_in = local(q_hbm, q, io_sem.at[0])
    h_in = local(h_hbm, tmp, io_sem.at[1])
    ws_in = local(ws_hbm, gs, io_sem.at[2])
    sq_in = local(sq_hbm, nb.at[0], io_sem.at[3])
    q_in.start()
    for cp in tiles(0, 0):
        cp.start()
    for cp in (h_in, ws_in, sq_in):
        cp.start()
    q_in.wait()
    fwd_seed(q, acc, t)
    transpose_into(tb.at[1], q, t)
    h_in.wait()
    transpose_into(tb.at[0], tmp, t)
    x_in = local(x_hbm, tmp, io_sem.at[1])
    x_in.start()
    ws_in.wait()
    sq_in.wait()
    wait_all()

    def on_total(u, total):
        gs[u] = gs[u] - LEARN_RATE * (total * scale)

    def sums(j):
        @pl.when(j == 1)
        def _():
            exchange_sum(nb, 0, near, nsend_sem, nrecv_sem, 0)

        @pl.when(j == 2)
        def _():
            exchange_sum(nb, 8, far, nsend_sem, nrecv_sem, 7)

    start, events, finish_unit = chain(dm, bits, peers, cbuf, (r1, r2, r3, r4, r5), gs, w_out, send_sem, recv_sem, credit,
                                       ag_send, ag_recv, ag_loc, LAG_B[1:], on_total)
    backward_phase(dm, bits, peers, q, tmp, tb, eb, acc, zb, vb, cbuf, obuf, sbuf,
                   csend_sem, core_sem, credit, tiles, x_in.wait, LAG_B[0], start, [*events, (0, sums)])
    sq_cp = local(nb.at[12], sq_out, io_sem.at[3])
    sq_cp.start()

    @steps(nu)
    def _(j):
        finish_unit(j)
    sq_cp.wait()


def finish(scale, f, w_ref, sq_ref, in_ref, out_ref, loss_ref):
    for j in range(w_ref.shape[0]):
        in_ref[0, :, j * f:(j + 1) * f] = w_ref[j, 0]
        out_ref[0, j * f:(j + 1) * f, :] = w_ref[j, 1].T
    loss_ref[0, 0] = 0.5 * (jnp.sum(sq_ref[...]) * scale)


def sds(shape, dtype):
    return jax.ShapeDtypeStruct(shape, dtype)


def call(kernel, n_in, outs, scratch, name, collective_id=None):
    params = dict(vmem_limit_bytes=VMEM_CAP)
    if collective_id is not None:
        params.update(collective_id=collective_id, has_side_effects=True)
    return pl.pallas_call(
        kernel,
        out_shape=outs,
        in_specs=[ANY] * n_in,
        out_specs=[ANY] * len(outs),
        scratch_shapes=scratch,
        compiler_params=pltpu.CompilerParams(**params),
        name=name,
    )


def local_step(n_dev, tile_f, x_loc, y_loc, w_in, w_out):
    nl, d, ff = w_in.shape
    f = tile_f
    nf = ff // f
    nu = nl * nf
    t = x_loc.shape[0] * x_loc.shape[1]
    piece = d // 16
    dm = (t, d, f, nf, nl)
    scale = 1.0 / (t * n_dev * d)
    rho = RHO_FRAC * math.sqrt(nl * (d + ff))
    bf, f32 = jnp.bfloat16, jnp.float32
    V, DMA, REG = pltpu.VMEM, pltpu.SemaphoreType.DMA, pltpu.SemaphoreType.REGULAR
    x = x_loc.transpose(1, 0, 2).reshape(t, d)
    y = y_loc.transpose(1, 0, 2).reshape(t, d)
    z_s, v_s, w_s, a_s, n_s = sds((nu, t, f), bf), sds((nu, 2, d, f), bf), sds((nu, piece, f), f32), sds((t, d), bf), sds(TILE, f32)
    slots = min(CORE_SLOTS, nu)
    tile2, rows = V((2, d, f), f32), V((nu, piece, f), f32)
    reduce_bufs = [V((slots, d, f), f32), tile2, tile2, *(V((nu, d >> k, f), f32) for k in range(1, 5))]
    act, sums, both = V((t, d), bf), V((t, d), f32), V((t, 2 * f), bf)
    acts = [act, act, V((2, d, t), bf), V((2, t, f), bf), sums]
    norms, tens = V((13, *TILE), f32), DMA((10,))
    two, four, per_unit, loads = DMA((2,)), DMA((4,)), DMA((nu,)), DMA((2, 2))

    z, v, ws, wc, g, norm = call(
        functools.partial(first_pass, dm, scale), 4, [z_s, v_s, w_s, w_s, w_s, n_s],
        acts + [both, V((2, d, 2 * f), f32), V((2, 2 * f, d), f32), V((2, 2, t, f), bf), V((2, 2, 2, d, f), bf), rows, rows]
        + reduce_bufs + [norms, loads, two, two, four, two, per_unit, per_unit, DMA((2, nu, 4)), REG, tens, tens],
        "pass_a", 0)(x, y, w_in, w_out)

    z, v, h1, q, sq = call(
        functools.partial(second_forward, dm, scale, rho), 5, [z_s, v_s, a_s, a_s, n_s],
        [act, act, sums, both, rows, rows, V((nu, 2, d, f), bf), V((2, 2, t, f), bf), V(TILE, f32),
         DMA((nu, 2)), DMA((nu, 5)), two, per_unit, DMA((5,))], "fwd_b", 1)(g, ws, norm, x, y)

    w_new, sq = call(
        functools.partial(second_backward, dm, scale), 7, [sds((nu, 2, d, f), f32), n_s],
        acts + [V((2, t, f), bf), V((2, 2, d, f), bf)] + reduce_bufs
        + [V((nu, d // 4, f), f32), rows, loads, four, two, per_unit, per_unit, DMA((7, nu)), REG,
           norms, DMA((nu, 3)), DMA((nu, 5)), per_unit, tens, tens], "bwd_b", 2)(x, h1, q, z, v, wc, sq)

    per_step = min(FINISH_TILES, nf)
    new_in, new_out, loss = pl.pallas_call(
        functools.partial(finish, scale, f),
        grid=(nl, nf // per_step),
        in_specs=[pl.BlockSpec((per_step, 2, d, f), lambda i, j: (i * (nf // per_step) + j, 0, 0, 0)), pl.BlockSpec(TILE, lambda i, j: (0, 0))],
        out_specs=[pl.BlockSpec((1, d, per_step * f), lambda i, j: (i, 0, j)), pl.BlockSpec((1, per_step * f, d), lambda i, j: (i, j, 0)),
                   pl.BlockSpec((1, 1), lambda i, j: (0, 0), memory_space=pltpu.SMEM)],
        out_shape=[sds((nl, d, ff), f32), sds((nl, ff, d), f32), sds((1, 1), f32)],
        compiler_params=pltpu.CompilerParams(vmem_limit_bytes=VMEM_CAP),
        name="finish")(w_new, sq)
    return new_in, new_out, loss.reshape(())


def solution(mesh):
    step = functools.partial(local_step, mesh.shape["data"], TILE_F)
    return jax.shard_map(step, mesh=mesh, in_specs=(P("data"), P("data"), P(), P()), out_specs=(P(), P(), P()), check_vma=False)
```

```python
import math
import functools
import jax
import jax.numpy as jnp
from jax import lax
from jax.experimental import pallas as pl
from jax.experimental.pallas import tpu as pltpu
from jax.sharding import PartitionSpec as P

RHO_FRAC = 0.1
LEARN_RATE = 1.0
TILE_F = 256
MESH = pl.DeviceIdType.MESH
ANY = pl.BlockSpec(memory_space=pl.ANY)
NN = (((1,), (0,)), ((), ()))
NT = (((1,), (1,)), ((), ()))
GELU_C = math.sqrt(2.0 / math.pi)
GELU_K = 0.044715
VMEM_CAP = 67043328
TILE = (8, 128)
FINISH_TILES = 6
CORE_SLOTS = 9
LAG_A = (0, 1, 3, 5, 7)
LAG_B = (0, 2, 3, 4, 5, 6, 8, 9, 10, 12, 14)
VG_LAG = (0, 2, 4, 7, 9, 11)


steps = functools.partial(pl.loop, 0)


def odd(i):
    return lax.rem(i, 2)


def dot(lhs, rhs, dims=NN):
    return lax.dot_general(lhs, rhs, dims, preferred_element_type=jnp.float32)


def gelu_parts(z):
    sq = z * z
    th = jnp.tanh(GELU_C * (z + GELU_K * (sq * z)))
    cdf = 0.5 * (1.0 + th)
    return sq, th, cdf


def gelu(z):
    return z * gelu_parts(z)[2]


def gelu_and_grad(z):
    sq, th, cdf = gelu_parts(z)
    slope = cdf + (0.5 * z) * ((1.0 - th * th) * (GELU_C + (3.0 * GELU_K * GELU_C) * sq))
    return z * cdf, slope


def place(axis="data"):
    me = lax.axis_index(axis)
    bits = [lax.rem(lax.div(me, 1 << k), 2) for k in range(5)]
    peers = [me + (1 << k) * (1 - 2 * bits[k]) for k in range(5)]
    return bits, peers


def route(bits, peers, unit, rows):
    core, bx, by, ba, bb = bits
    _, px, py, pa, pb = peers
    swap = odd(unit + core) == 1
    b1, p1 = jnp.where(swap, by, bx), jnp.where(swap, py, px)
    b3, p3 = jnp.where(swap, bx, by), jnp.where(swap, px, py)
    axes = (b1, ba, b3, bb)
    step = rows // 16
    keep, send, base = [0], [], 0
    n = rows
    for bit in axes:
        n //= 2
        keep.append(pl.multiple_of(base + bit * n, step))
        send.append(pl.multiple_of(base + (1 - bit) * n, step))
        base = base + bit * n
    return (p1, pa, p3, pb), keep, send, axes


def chain_route(bits, peers, unit, d):
    core, bx, by, ba, bb = bits
    _, px, py, pa, _ = peers
    swap = odd(unit + core) == 1
    b1, p1 = jnp.where(swap, by, bx), jnp.where(swap, py, px)
    b3, p3 = jnp.where(swap, bx, by), jnp.where(swap, px, py)
    piece, chunk, pair, half = d // 16, d // 8, d // 4, d // 2
    me = lax.axis_index("data")

    def rows(base, n):
        return pl.ds(pl.multiple_of(base, piece), n)
    kx = b1 * half
    own = kx + (2 * bb + ba) * chunk
    mate = 2 * (kx + bb * pair) + chunk - own
    r = dict(
        half=rows(kx, half), other_half=rows((1 - b1) * half, half),
        pair=rows(kx + bb * pair, pair), other_pair=rows(kx + (1 - bb) * pair, pair),
        own=rows(own, chunk), mate=rows(mate, chunk),
        far_end=rows(kx + (1 - bb) * 3 * chunk, chunk), far_mid=rows(kx + (2 - bb) * chunk, chunk),
        keep=rows(own + b3 * piece, piece), send=rows(own + (1 - b3) * piece, piece),
        x_send_first=(rows((1 - b1) * half + (1 - bb) * pair, pair), rows((1 - bb) * pair, pair)),
        x_send_second=(rows((1 - b1) * half + bb * pair, pair), rows(bb * pair, pair)),
    )
    return r, p1, pa, me + 8 * (1 - 2 * bb), p3


def arrive(peers):
    barrier = pltpu.get_barrier_semaphore()
    for peer in peers:
        pl.semaphore_signal(barrier, device_id=(peer,), device_id_type=MESH)
    return functools.partial(pl.semaphore_wait, barrier, len(peers))


def others(bits, me_bits):
    me = lax.axis_index("data")
    out = []
    for mask in range(1, 1 << len(me_bits)):
        peer = me
        for i, k in enumerate(me_bits):
            if mask >> i & 1:
                peer = peer + (1 << k) * (1 - 2 * bits[k])
        out.append(peer)
    return out


def exchange_sum(buf, first, peers, send_sem, recv_sem, sem0):
    copies = [remote(buf.at[first], buf.at[first + 1 + i], send_sem.at[sem0 + i], recv_sem.at[sem0 + i], peer) for i, peer in enumerate(peers)]
    for cp in copies:
        cp.start()
    total = buf[first]
    for i, cp in enumerate(copies):
        cp.wait()
        total = total + buf[first + 1 + i]
    buf[first + len(peers) + 1] = total


def gather_hops(bits, peers, unit, d, full, piece_src=None):
    ps, keep, send, _ = route(bits, peers, unit, d)
    piece = d // 16

    def rows(base, n):
        return full.at[pl.ds(base, n), :]

    def hop(k, part, sem_s, sem_r):
        peer = ps[3 - k] if k < 4 else peers[0]
        if k == 0:
            ref = rows(keep[4], piece)
        elif part == 0:
            ref = rows(keep[5 - k], piece << (k - 1))
        else:
            ref = rows(send[4 - k], piece << (k - 1))
        src = piece_src if piece_src is not None and part == 0 and k <= 1 else ref
        return remote(src, ref, sem_s, sem_r, peer)

    def arrived(k, sem_s, sem_r):
        ref = rows(send[3 - k], piece << k)
        return remote(ref, ref, sem_s, sem_r, ps[3 - k])

    def sent(sem_s, sem_r):
        ref = rows(0, 15 * piece)
        return remote(ref, ref, sem_s, sem_r, ps[0])
    return hop, arrived, sent


def remote(src, dst, send_sem, recv_sem, peer):
    return pltpu.make_async_remote_copy(src_ref=src, dst_ref=dst, send_sem=send_sem, recv_sem=recv_sem, device_id=(peer,), device_id_type=MESH)


def local(src, dst, sem):
    return pltpu.make_async_copy(src, dst, sem)


def halves(t):
    return [(0, t // 2), (t // 2, t // 2)] if t % 32 == 0 else [(0, t)]


def transpose_into(dst, src, t):
    full = t // 128
    if full:
        @steps(full)
        def _(i):
            lo = pl.multiple_of(i * 128, 128)
            dst[:, pl.ds(lo, 128)] = src[pl.ds(lo, 128), :].T
    if t % 128:
        dst[:, full * 128:t] = src[full * 128:t, :].T


def fwd_pair(h_ref, v_ref, acc_ref, a_ref, z_ref, t, f):
    for lo, n in halves(t):
        for j in range(2):
            z = dot(h_ref[lo:lo + n, :], v_ref[j, 0]).astype(jnp.bfloat16)
            z_ref[j, lo:lo + n, :] = z
            a_ref[lo:lo + n, j * f:(j + 1) * f] = gelu(z.astype(jnp.float32)).astype(jnp.bfloat16)
    v_out = jnp.concatenate([v_ref[0, 1], v_ref[1, 1]], axis=1)
    for lo, n in halves(t):
        acc_ref[lo:lo + n, :] += dot(a_ref[lo:lo + n, :], v_out, NT)


def fwd_close(h_ref, acc_ref, t):
    for lo, n in halves(t):
        h_ref[lo:lo + n, :] = acc_ref[lo:lo + n, :].astype(jnp.bfloat16)


def fwd_seed(h_ref, acc_ref, t):
    for lo, n in halves(t):
        acc_ref[lo:lo + n, :] = h_ref[lo:lo + n, :].astype(jnp.float32)


def fold(v):
    r, c = v.shape
    rows = jnp.sum(v.reshape(r // 8, 8, c), axis=0)
    return sum(rows[:, lo:lo + 128] for lo in range(0, c, 128))


def loss_close(h_ref, y_ref, acc_ref, t, d, total_ref=None):
    def rows_of(rows):
        e = acc_ref[rows, :].astype(jnp.bfloat16).astype(jnp.float32) - y_ref[rows, :].astype(jnp.float32)
        q = e.astype(jnp.bfloat16)
        h_ref[rows, :] = q
        acc_ref[rows, :] = q.astype(jnp.float32)
        return e
    if total_ref is None:
        for lo, n in halves(t):
            rows_of(slice(lo, lo + n))
        return
    n = 112 if t % 112 == 0 else t
    total_ref[...] = jnp.zeros(TILE, jnp.float32)

    @steps(t // n)
    def _(i):
        e = rows_of(pl.ds(pl.multiple_of(i * n, n), n))
        total_ref[...] += fold(e * e)


def unit_of(it, nf, nl):
    return (nl - 1 - it // nf) * nf + lax.rem(it, nf)


def first_pass(dm, scale, x_hbm, y_hbm, wi_hbm, wo_hbm, z_out, v_out, ws_out, wc_out, g_out, n_out,
               h, tmp, tb, eb, acc, ab, wi, wo, zb, vb, ws, wc, cbuf, obuf, sbuf, r1, r2, r3, r4, nb,
               load_sem, z_sem, v_sem, io_sem, csend_sem, core_sem, send_sem, recv_sem, credit, nsend_sem, nrecv_sem):
    t, d, f, nf, nl = dm
    nu = nf * nl
    bits, peers = place()
    piece = d // 16
    near, far = others(bits, (0, 1, 2)), others(bits, (3, 4))
    wait_all = arrive(near + far)

    def loads(p, slot):
        layer, tile = p // (nf // 2), lax.rem(p, nf // 2)
        lo = pl.multiple_of(tile * 2 * f, 2 * f)
        return (local(wi_hbm.at[layer, :, pl.ds(lo, 2 * f)], wi.at[slot], load_sem.at[slot, 0]),
                local(wo_hbm.at[layer, pl.ds(lo, 2 * f), :], wo.at[slot], load_sem.at[slot, 1]))

    def stores(p, slot):
        two = pl.ds(2 * p, 2)
        return local(zb.at[slot], z_out.at[two], z_sem.at[slot]), local(vb.at[slot], v_out.at[two], v_sem.at[slot])

    x_in = local(x_hbm, h, io_sem.at[0])
    y_in = local(y_hbm, tmp, io_sem.at[1])
    x_in.start()
    for cp in loads(0, 0):
        cp.start()
    y_in.start()
    x_in.wait()
    fwd_seed(h, acc, t)

    @steps(nu // 2)
    def _(p):
        slot = odd(p)
        for cp in loads(p, slot):
            cp.wait()

        @pl.when(p + 1 < nu // 2)
        def _():
            for cp in loads(p + 1, 1 - slot):
                cp.start()

        @pl.when(p >= 2)
        def _():
            for cp in stores(p - 2, slot):
                cp.wait()
        for j in range(2):
            cols = slice(j * f, (j + 1) * f)
            wot = wo[slot, cols, :].T
            _, keep, _, _ = route(bits, peers, 2 * p + j, d)
            rows = pl.ds(keep[4], piece)
            vb[slot, j, 0] = wi[slot, :, cols].astype(jnp.bfloat16)
            vb[slot, j, 1] = wot.astype(jnp.bfloat16)
            obuf[j] = wot
            ws[2 * p + j] = jnp.where(bits[0] == 0, wi[slot, rows, cols], obuf[j, rows, :])
            rows = chain_route(bits, peers, j, d)[0]['keep']
            wc[2 * p + j] = jnp.where(bits[0] == 0, wi[slot, rows, cols], obuf[j, rows, :])

        fwd_pair(h, vb.at[slot], acc, ab, zb.at[slot], t, f)
        for cp in stores(p, slot):
            cp.start()

        @pl.when(p == nf // 2 - 1)
        def _():
            fwd_close(h, acc, t)
            fwd_seed(h, acc, t)
            transpose_into(tb.at[0], h, t)

    np_ = nu // 2
    if np_ >= 2:
        for cp in stores(np_ - 2, np_ % 2):
            cp.wait()
    spare = np_ % 2

    def tiles(it, slot):
        u = unit_of(it, nf, nl)
        return (local(z_out.at[u], zb.at[spare, slot], load_sem.at[slot, 0]), local(v_out.at[u], vb.at[spare, slot], load_sem.at[slot, 1]))
    for cp in tiles(0, 0):
        cp.start()
    ws_cp = local(ws, ws_out, io_sem.at[2])
    wc_cp = local(wc, wc_out, io_sem.at[3])
    ws_cp.start()
    wc_cp.start()
    y_in.wait()
    loss_close(h, tmp, acc, t, d)
    transpose_into(tb.at[1], h, t)
    x_again = local(x_hbm, tmp, io_sem.at[1])
    x_again.start()
    for cp in stores(np_ - 1, (np_ - 1) % 2):
        cp.wait()
    wait_all()
    nb[0] = jnp.zeros(TILE, jnp.float32)

    ws_cp.wait()

    def on_total(u, total):
        ws[u] = total
        g = total * scale
        nb[0] += fold(g * g)

    start, events = halving(dm, bits, peers, cbuf, (r1, r2, r3, r4), send_sem, recv_sem, credit, LAG_A[1:], on_total)
    backward_phase(dm, bits, peers, h, tmp, tb, eb, acc, zb.at[spare], vb.at[spare], cbuf, obuf, sbuf,
                   csend_sem, core_sem, credit, tiles, x_again.wait, LAG_A[0], start, events)
    g_cp = local(ws, g_out, io_sem.at[0])
    g_cp.start()
    exchange_sum(nb, 0, near, nsend_sem, nrecv_sem, 0)
    exchange_sum(nb, 8, far, nsend_sem, nrecv_sem, 7)
    n_cp = local(nb.at[12], n_out, io_sem.at[1])
    n_cp.start()
    wc_cp.wait()
    g_cp.wait()
    n_cp.wait()


def second_forward(dm, scale, rho, gs_hbm, ws_hbm, n_hbm, x_hbm, y_hbm, z_out, v_out, h_out, q_out, sq_out,
                   h, yb, acc, ab, gs, ws, vb, zb, nb, send_sem, recv_sem, z_sem, v_sem, io_sem):
    t, d, f, nf, nl = dm
    nu = nf * nl
    bits, peers = place()
    core = bits[0]
    piece = d // 16
    wait_all = arrive(peers)
    ins = (local(gs_hbm, gs, io_sem.at[0]), local(ws_hbm, ws, io_sem.at[1]), local(x_hbm, h, io_sem.at[2]), local(y_hbm, yb, io_sem.at[3]))
    n_in = local(n_hbm, nb, io_sem.at[4])
    n_in.start()
    for cp in ins:
        cp.start()
    n_in.wait()
    coef = rho / jnp.sqrt(jnp.sum(nb[...], keepdims=True))
    ins[0].wait()
    ins[1].wait()
    wait_all()

    def hops(u):
        return gather_hops(bits, peers, u, d, vb.at[u, core])

    def sems(u, k):
        return send_sem.at[u, 0 if k < 4 else 1], recv_sem.at[u, k]

    def core_arrived(u):
        ref = vb.at[u, 1 - core]
        return remote(ref, ref, *sems(u, 4), peers[0])

    def z_store(p, slot):
        return local(zb.at[slot], z_out.at[pl.ds(2 * p, 2)], z_sem.at[slot])

    @steps(nu + VG_LAG[5])
    def _(it):
        @pl.when(it < nu)
        def _():
            _, keep, _, _ = route(bits, peers, it, d)
            new = ws[it] + coef * (gs[it] * scale)
            vb[it, core, pl.ds(keep[4], piece), :] = new.astype(jnp.bfloat16)
            hop, _, _ = hops(it)
            hop(0, 0, *sems(it, 0)).start()
            hop(1, 0, *sems(it, 1)).start()
        for k in range(1, 5):
            u = it - VG_LAG[k]

            @pl.when((u >= 0) & (u < nu))
            def _():
                hop, arrived, _ = hops(u)
                arrived(k - 1, *sems(u, k - 1)).wait_recv()
                hop(k, 1, *sems(u, k)).start()
                if k < 4:
                    hop(k + 1, 0, *sems(u, k + 1)).start()
        u = it - VG_LAG[5]

        @pl.when(u >= 0)
        def _():
            core_arrived(u).wait_recv()
            local(vb.at[u], v_out.at[u], v_sem.at[u]).start()

        @pl.when((u >= 0) & (odd(u) == 1))
        def _():
            p = u // 2
            slot = odd(p)

            @pl.when(p >= 2)
            def _():
                z_store(p - 2, slot).wait()

            @pl.when(p == 0)
            def _():
                ins[2].wait()
                fwd_seed(h, acc, t)
            fwd_pair(h, vb.at[pl.ds(2 * p, 2)], acc, ab, zb.at[slot], t, f)
            z_store(p, slot).start()

            @pl.when(p == nf // 2 - 1)
            def _():
                fwd_close(h, acc, t)
                fwd_seed(h, acc, t)
                out = local(h, h_out, io_sem.at[0])
                out.start()
                out.wait()

    ins[3].wait()
    loss_close(h, yb, acc, t, d, nb)
    out = local(h, q_out, io_sem.at[0])
    sq = local(nb, sq_out, io_sem.at[1])
    out.start()
    sq.start()

    @steps(nu)
    def _(u):
        local(vb.at[u], v_out.at[u], v_sem.at[u]).wait()
        hops(u)[2](*sems(u, 0)).wait_send()
        core_arrived(u).wait_send()
    for p in range(max(nu // 2 - 2, 0), nu // 2):
        z_store(p, p % 2).wait()
    out.wait()
    sq.wait()


def backward_phase(dm, bits, peers, q, tmp, tb, eb, acc, zb, vb, cbuf, obuf, sbuf, csend_sem, core_sem, credit,
                   tiles, x_ready, core_lag, after_core, events):
    t, d, f, nf, nl = dm
    nu = nf * nl
    core = bits[0]
    slots = cbuf.shape[0]

    def core_copy(it):
        slot = odd(it)
        return remote(sbuf.at[slot], cbuf.at[lax.rem(it, slots)], csend_sem.at[slot], core_sem.at[it], peers[0])

    def core_stage(j):
        cs = lax.rem(j, slots)
        core_copy(j).wait_recv()
        cbuf[cs] = cbuf[cs] + obuf[odd(j)]
        after_core(j)

    @steps(nu + max(lag for lag, _ in events))
    def _(it):
        @pl.when(it == nf)
        def _():
            fwd_close(q, acc, t)
            transpose_into(tb.at[1], q, t)
            x_ready()
            transpose_into(tb.at[0], tmp, t)

        @pl.when(it < nu)
        def _():
            slot = odd(it)
            for cp in tiles(it, slot):
                cp.wait()

            @pl.when(it + 1 < nu)
            def _():
                for cp in tiles(it + 1, 1 - slot):
                    cp.start()
            for lo, n in halves(t):
                back = dot(q[lo:lo + n, :], vb[slot, 1])
                a, slope = gelu_and_grad(zb[slot, lo:lo + n, :].astype(jnp.float32))
                eb[1, lo:lo + n, :] = a.astype(jnp.bfloat16)
                eb[0, lo:lo + n, :] = (back * slope).astype(jnp.bfloat16)

            @pl.when(it >= 2)
            def _():
                core_copy(it - 2).wait_send()
            sbuf[slot] = dot(tb[1 - core], eb[1 - core])

            @pl.when(it >= slots)
            def _():
                pl.semaphore_wait(credit)
            core_copy(it).start()
            obuf[slot] = dot(tb[core], eb[core])

            @pl.when(it < nf)
            def _():
                for lo, n in halves(t):
                    acc[lo:lo + n, :] += dot(eb[0, lo:lo + n, :], vb[slot, 0], NT)

        for lag, event in ((core_lag, core_stage), *events):
            j = it - lag

            @pl.when((j >= 0) & (j < nu))
            def _():
                event(j)

    core_copy(nu - 2).wait_send()
    core_copy(nu - 1).wait_send()


def free_slot(j, nu, slots, credit, peer):
    @pl.when(j + slots < nu)
    def _():
        pl.semaphore_signal(credit, device_id=(peer,), device_id_type=MESH)


def halving(dm, bits, peers, cbuf, rbuf, send_sem, recv_sem, credit, lags, on_total):
    t, d, f, nf, nl = dm
    nu = nf * nl
    piece = d // 16
    slots = cbuf.shape[0]
    partner = peers[0]

    def rs_sends(it, k):
        ps, _, send, on = route(bits, peers, it, d)
        n = d >> (k + 1)
        cs = lax.rem(it, slots)

        def part(off, m, sem):
            return remote(cbuf.at[cs, pl.ds(send[k] + off, m), :], rbuf[k].at[it, pl.ds(off, m), :], send_sem.at[it], sem, ps[k])
        if k == 3:
            return [part(0, n, recv_sem.at[0, it, k])]
        m = n // 2
        return [part(pl.multiple_of((1 - on[k + 1]) * m, piece), m, recv_sem.at[0, it, k]),
                part(pl.multiple_of(on[k + 1] * m, piece), m, recv_sem.at[1, it, k])]

    def rs_add(it, k, kept):
        ps, keep, send, _ = route(bits, peers, it, d)
        cs = lax.rem(it, slots)
        if k == 3:
            base, m = keep[4], d >> 4
        else:
            base, m = (keep[k + 2] if kept else send[k + 1]), d >> (k + 2)
        here = rbuf[k].at[it, pl.ds(pl.multiple_of(base - keep[k + 1], piece), m), :]
        mine = cbuf.at[cs, pl.ds(base, m), :]
        remote(mine, here, send_sem.at[it], recv_sem.at[1 if kept else 0, it, k], ps[k]).wait_recv()
        total = mine[...] + here[...]
        if k == 3:
            return total
        mine[...] = total

    def start(j):
        for cp in rs_sends(j, 0):
            cp.start()

    def stage(k):
        def event(j):
            if k > 0:
                rs_add(j, k - 1, True)
            total = rs_add(j, k, False)
            if k < 3:
                for cp in rs_sends(j, k + 1):
                    cp.start()
            else:
                on_total(unit_of(j, nf, nl), total)
                ref = cbuf.at[lax.rem(j, slots), pl.ds(0, 15 * piece), :]
                remote(ref, ref, send_sem.at[j], recv_sem.at[0, j, 3], partner).wait_send()
                free_slot(j, nu, slots, credit, partner)
        return event
    return start, [(lags[k], stage(k)) for k in range(4)]


def chain(dm, bits, peers, cbuf, rbuf, gs, w_out, send_sem, recv_sem, credit, ag_send, ag_recv, ag_loc, lags, on_total):
    t, d, f, nf, nl = dm
    nu = nf * nl
    core, _, _, ba, bb = bits
    piece = d // 16
    slots = cbuf.shape[0]
    r1, r2, r3, r4, r5 = rbuf
    at_end = ba == bb
    chunk = d // 8
    XU, XK, EU, EK, MU, MK, YY = range(7)
    ALL, MIDDLE, CORE = range(3)
    HALF, MATE, PAIR, LAST, FULL = range(5)
    partner = peers[0]

    def send(j, src, dst, sem, peer):
        remote(cbuf.at[lax.rem(j, slots), src, :], dst, send_sem.at[j], recv_sem.at[sem, j], peer).start()

    def add(j, rows, buf, sem):
        mine = cbuf.at[lax.rem(j, slots), rows, :]
        remote(mine, buf, send_sem.at[j], recv_sem.at[sem, j], partner).wait_recv()
        mine[...] = mine[...] + buf[...]

    def at(j):
        return chain_route(bits, peers, unit_of(j, nf, nl), d)

    def start(j):
        r, p1, _, _, _ = at(j)
        for (src, dst), sem in ((r["x_send_first"], XU), (r["x_send_second"], XK)):
            send(j, src, r1.at[j, dst, :], sem, p1)

    def rel(first):
        return pl.ds(pl.multiple_of((1 - bb if first else bb) * (d // 4), piece), d // 4)

    def s1(j):
        r, _, pa, _, _ = at(j)
        add(j, r["other_pair"], r1.at[j, rel(True), :], XU)

        @pl.when(at_end)
        def _():
            send(j, r["other_pair"], r2.at[j], EU, pa)

    def s2(j):
        r, _, pa, pm, _ = at(j)
        add(j, r["pair"], r1.at[j, rel(False), :], XK)

        @pl.when(at_end)
        def _():
            send(j, r["mate"], r3.at[j], EK, pa)

        @pl.when(jnp.logical_not(at_end))
        def _():
            add(j, r["other_pair"], r2.at[j], EU)
            send(j, r["far_end"], r5.at[j, 0:chunk, :], MU, pm)
            send(j, r["far_mid"], r5.at[j, chunk:2 * chunk, :], MK, pm)

    def s3(j):
        r, _, pa, _, p3 = at(j)

        @pl.when(jnp.logical_not(at_end))
        def _():
            add(j, r["mate"], r5.at[j, 0:chunk, :], MU)
            send(j, r["mate"], r3.at[j], EK, pa)
            add(j, r["own"], r3.at[j], EK)
            add(j, r["own"], r5.at[j, chunk:2 * chunk, :], MK)
            send(j, r["send"], r4.at[j], YY, p3)

    def s4(j):
        r, _, _, _, p3 = at(j)

        @pl.when(at_end)
        def _():
            add(j, r["own"], r3.at[j], EK)
            send(j, r["send"], r4.at[j], YY, p3)

    def full(j):
        return w_out.at[unit_of(j, nf, nl), core]

    def give(j, rows, sem_s, sem_r, peer, src=None):
        ref = full(j).at[rows, :]
        return remote(ref if src is None else src, ref, ag_send.at[j, sem_s], ag_recv.at[j, sem_r], peer)

    def own_copy(j):
        u = unit_of(j, nf, nl)
        return local(gs.at[u], full(j).at[at(j)[0]["keep"], :], ag_loc.at[j])

    def s5(j):
        r, _, _, _, p3 = at(j)
        u = unit_of(j, nf, nl)
        mine = cbuf.at[lax.rem(j, slots), r["keep"], :]
        remote(mine, r4.at[j], send_sem.at[j], recv_sem.at[YY, j], p3).wait_recv()
        on_total(u, mine[...] + r4[j])
        own_copy(j).start()
        give(j, r["keep"], ALL, HALF, p3, gs.at[u]).start()
        ref = cbuf.at[lax.rem(j, slots), pl.ds(0, 15 * piece), :]
        remote(ref, ref, send_sem.at[j], recv_sem.at[YY, j], p3).wait_send()
        free_slot(j, nu, slots, credit, partner)

    def g1(j):
        r, p1, pa, pm, p3 = at(j)
        own_copy(j).wait()
        give(j, r["send"], ALL, HALF, p3).wait_recv()
        give(j, r["own"], ALL, MATE, pa).start()

        @pl.when(jnp.logical_not(at_end))
        def _():
            give(j, r["own"], MIDDLE, PAIR, pm).start()
        give(j, r["own"], ALL, LAST, p1).start()

    def g2(j):
        r, p1, pa, pm, _ = at(j)
        give(j, r["mate"], ALL, MATE, pa).wait_recv()

        @pl.when(jnp.logical_not(at_end))
        def _():
            give(j, r["mate"], MIDDLE, PAIR, pm).start()
        give(j, r["mate"], ALL, LAST, p1).start()

    def g3(j, r, p1, pa):
        give(j, r["other_pair"], MIDDLE, PAIR, pa).wait_recv()
        give(j, r["other_pair"], ALL, LAST, p1).start()
        give(j, r["half"], CORE, FULL, partner).start()

    def g3_middle(j):
        r, p1, pa, _, _ = at(j)

        @pl.when(jnp.logical_not(at_end))
        def _():
            g3(j, r, p1, pa)
            give(j, r["other_pair"], MIDDLE, PAIR, pa).start()

    def g3_end(j):
        r, p1, pa, _, _ = at(j)

        @pl.when(at_end)
        def _():
            g3(j, r, p1, pa)

    def g4(j):
        r, p1, _, _, _ = at(j)
        give(j, r["other_half"], ALL, LAST, p1).wait_recv()
        give(j, r["other_half"], CORE, FULL, partner).start()

    def finish_unit(j):
        ref = w_out.at[unit_of(j, nf, nl), 1 - core]
        last = remote(ref, ref, ag_send.at[j, CORE], ag_recv.at[j, FULL], partner)
        last.wait_recv()
        last.wait_send()
        ref = full(j).at[pl.ds(0, 11 * piece), :]
        remote(ref, ref, ag_send.at[j, ALL], ag_recv.at[j, LAST], partner).wait_send()

        @pl.when(jnp.logical_not(at_end))
        def _():
            ref = full(j).at[pl.ds(0, 8 * piece), :]
            remote(ref, ref, ag_send.at[j, MIDDLE], ag_recv.at[j, PAIR], partner).wait_send()

    steps = (s1, s2, s3, s4, s5, g1, g2, g3_middle, g3_end, g4)
    return start, list(zip(lags, steps)), finish_unit


def second_backward(dm, scale, x_hbm, h_hbm, q_hbm, z_hbm, v_hbm, ws_hbm, sq_hbm, w_out, sq_out,
                    q, tmp, tb, eb, acc, zb, vb, cbuf, obuf, sbuf, r1, r2, r3, r4, r5, gs,
                    load_sem, io_sem, csend_sem, core_sem, send_sem, recv_sem, credit, nb, ag_send, ag_recv, ag_loc, nsend_sem, nrecv_sem):
    t, d, f, nf, nl = dm
    nu = nf * nl
    bits, peers = place()
    near, far = others(bits, (0, 1, 2)), others(bits, (3, 4))
    wait_all = arrive(near + far)

    def tiles(it, slot):
        u = unit_of(it, nf, nl)
        return local(z_hbm.at[u], zb.at[slot], load_sem.at[slot, 0]), local(v_hbm.at[u], vb.at[slot], load_sem.at[slot, 1])

    q_in = local(q_hbm, q, io_sem.at[0])
    h_in = local(h_hbm, tmp, io_sem.at[1])
    ws_in = local(ws_hbm, gs, io_sem.at[2])
    sq_in = local(sq_hbm, nb.at[0], io_sem.at[3])
    q_in.start()
    for cp in tiles(0, 0):
        cp.start()
    for cp in (h_in, ws_in, sq_in):
        cp.start()
    q_in.wait()
    fwd_seed(q, acc, t)
    transpose_into(tb.at[1], q, t)
    h_in.wait()
    transpose_into(tb.at[0], tmp, t)
    x_in = local(x_hbm, tmp, io_sem.at[1])
    x_in.start()
    ws_in.wait()
    sq_in.wait()
    wait_all()

    def on_total(u, total):
        gs[u] = gs[u] - LEARN_RATE * (total * scale)

    def sums(j):
        @pl.when(j == 1)
        def _():
            exchange_sum(nb, 0, near, nsend_sem, nrecv_sem, 0)

        @pl.when(j == 2)
        def _():
            exchange_sum(nb, 8, far, nsend_sem, nrecv_sem, 7)

    start, events, finish_unit = chain(dm, bits, peers, cbuf, (r1, r2, r3, r4, r5), gs, w_out, send_sem, recv_sem, credit,
                                       ag_send, ag_recv, ag_loc, LAG_B[1:], on_total)
    backward_phase(dm, bits, peers, q, tmp, tb, eb, acc, zb, vb, cbuf, obuf, sbuf,
                   csend_sem, core_sem, credit, tiles, x_in.wait, LAG_B[0], start, [*events, (0, sums)])
    sq_cp = local(nb.at[12], sq_out, io_sem.at[3])
    sq_cp.start()

    @steps(nu)
    def _(j):
        finish_unit(j)
    sq_cp.wait()


def finish(scale, f, w_ref, sq_ref, in_ref, out_ref, loss_ref):
    for j in range(w_ref.shape[0]):
        in_ref[0, :, j * f:(j + 1) * f] = w_ref[j, 0]
        out_ref[0, j * f:(j + 1) * f, :] = w_ref[j, 1].T
    loss_ref[0, 0] = 0.5 * (jnp.sum(sq_ref[...]) * scale)


def sds(shape, dtype):
    return jax.ShapeDtypeStruct(shape, dtype)


def call(kernel, n_in, outs, scratch, name, collective_id=None):
    params = dict(vmem_limit_bytes=VMEM_CAP)
    if collective_id is not None:
        params.update(collective_id=collective_id, has_side_effects=True)
    return pl.pallas_call(
        kernel,
        out_shape=outs,
        in_specs=[ANY] * n_in,
        out_specs=[ANY] * len(outs),
        scratch_shapes=scratch,
        compiler_params=pltpu.CompilerParams(**params),
        name=name,
    )


def local_step(n_dev, tile_f, x_loc, y_loc, w_in, w_out):
    nl, d, ff = w_in.shape
    f = tile_f
    nf = ff // f
    nu = nl * nf
    t = x_loc.shape[0] * x_loc.shape[1]
    piece = d // 16
    dm = (t, d, f, nf, nl)
    scale = 1.0 / (t * n_dev * d)
    rho = RHO_FRAC * math.sqrt(nl * (d + ff))
    bf, f32 = jnp.bfloat16, jnp.float32
    V, DMA, REG = pltpu.VMEM, pltpu.SemaphoreType.DMA, pltpu.SemaphoreType.REGULAR
    x = x_loc.transpose(1, 0, 2).reshape(t, d)
    y = y_loc.transpose(1, 0, 2).reshape(t, d)
    z_s, v_s, w_s, a_s, n_s = sds((nu, t, f), bf), sds((nu, 2, d, f), bf), sds((nu, piece, f), f32), sds((t, d), bf), sds(TILE, f32)
    slots = min(CORE_SLOTS, nu)
    tile2, rows = V((2, d, f), f32), V((nu, piece, f), f32)
    reduce_bufs = [V((slots, d, f), f32), tile2, tile2, *(V((nu, d >> k, f), f32) for k in range(1, 5))]
    act, sums, both = V((t, d), bf), V((t, d), f32), V((t, 2 * f), bf)
    acts = [act, act, V((2, d, t), bf), V((2, t, f), bf), sums]
    norms, tens = V((13, *TILE), f32), DMA((10,))
    two, four, per_unit, loads = DMA((2,)), DMA((4,)), DMA((nu,)), DMA((2, 2))

    z, v, ws, wc, g, norm = call(
        functools.partial(first_pass, dm, scale), 4, [z_s, v_s, w_s, w_s, w_s, n_s],
        acts + [both, V((2, d, 2 * f), f32), V((2, 2 * f, d), f32), V((2, 2, t, f), bf), V((2, 2, 2, d, f), bf), rows, rows]
        + reduce_bufs + [norms, loads, two, two, four, two, per_unit, per_unit, DMA((2, nu, 4)), REG, tens, tens],
        "pass_a", 0)(x, y, w_in, w_out)

    z, v, h1, q, sq = call(
        functools.partial(second_forward, dm, scale, rho), 5, [z_s, v_s, a_s, a_s, n_s],
        [act, act, sums, both, rows, rows, V((nu, 2, d, f), bf), V((2, 2, t, f), bf), V(TILE, f32),
         DMA((nu, 2)), DMA((nu, 5)), two, per_unit, DMA((5,))], "fwd_b", 1)(g, ws, norm, x, y)

    w_new, sq = call(
        functools.partial(second_backward, dm, scale), 7, [sds((nu, 2, d, f), f32), n_s],
        acts + [V((2, t, f), bf), V((2, 2, d, f), bf)] + reduce_bufs
        + [V((nu, d // 4, f), f32), rows, loads, four, two, per_unit, per_unit, DMA((7, nu)), REG,
           norms, DMA((nu, 3)), DMA((nu, 5)), per_unit, tens, tens], "bwd_b", 2)(x, h1, q, z, v, wc, sq)

    per_step = min(FINISH_TILES, nf)
    new_in, new_out, loss = pl.pallas_call(
        functools.partial(finish, scale, f),
        grid=(nl, nf // per_step),
        in_specs=[pl.BlockSpec((per_step, 2, d, f), lambda i, j: (i * (nf // per_step) + j, 0, 0, 0)), pl.BlockSpec(TILE, lambda i, j: (0, 0))],
        out_specs=[pl.BlockSpec((1, d, per_step * f), lambda i, j: (i, 0, j)), pl.BlockSpec((1, per_step * f, d), lambda i, j: (i, j, 0)),
                   pl.BlockSpec((1, 1), lambda i, j: (0, 0), memory_space=pltpu.SMEM)],
        out_shape=[sds((nl, d, ff), f32), sds((nl, ff, d), f32), sds((1, 1), f32)],
        compiler_params=pltpu.CompilerParams(vmem_limit_bytes=VMEM_CAP),
        name="finish")(w_new, sq)
    return new_in, new_out, loss.reshape(())


def solution(mesh):
    step = functools.partial(local_step, mesh.shape["data"], TILE_F)
    return jax.shard_map(step, mesh=mesh, in_specs=(P("data"), P("data"), P(), P()), out_specs=(P(), P(), P()), check_vma=False)
```

```python
import math
import functools
import jax
import jax.numpy as jnp
from jax import lax
from jax.experimental import pallas as pl
from jax.experimental.pallas import tpu as pltpu
from jax.sharding import PartitionSpec as P

RHO_FRAC = 0.1
LEARN_RATE = 1.0
TILE_F = 256
MESH = pl.DeviceIdType.MESH
ANY = pl.BlockSpec(memory_space=pl.ANY)
NN = (((1,), (0,)), ((), ()))
NT = (((1,), (1,)), ((), ()))
GELU_C = math.sqrt(2.0 / math.pi)
GELU_K = 0.044715
VMEM_CAP = 67043328
TILE = (8, 128)
FINISH_TILES = 6
CORE_SLOTS = 9
LAG_A = (0, 1, 2, 3, 5)
LAG_B = (0, 2, 3, 4, 5, 6, 8, 9, 10, 14, 16)
VG_LAG = (0, 4, 6, 11, 14, 16)


steps = functools.partial(pl.loop, 0)


def odd(i):
    return lax.rem(i, 2)


def dot(lhs, rhs, dims=NN):
    return lax.dot_general(lhs, rhs, dims, preferred_element_type=jnp.float32)


def gelu_parts(z):
    sq = z * z
    th = jnp.tanh(GELU_C * (z + GELU_K * (sq * z)))
    cdf = 0.5 * (1.0 + th)
    return sq, th, cdf


def gelu(z):
    return z * gelu_parts(z)[2]


def gelu_and_grad(z):
    sq, th, cdf = gelu_parts(z)
    slope = cdf + (0.5 * z) * ((1.0 - th * th) * (GELU_C + (3.0 * GELU_K * GELU_C) * sq))
    return z * cdf, slope


def place(axis="data"):
    me = lax.axis_index(axis)
    bits = [lax.rem(lax.div(me, 1 << k), 2) for k in range(5)]
    peers = [me + (1 << k) * (1 - 2 * bits[k]) for k in range(5)]
    return bits, peers


def route(bits, peers, unit, rows):
    core, bx, by, ba, bb = bits
    _, px, py, pa, pb = peers
    swap = odd(unit + core) == 1
    b1, p1 = jnp.where(swap, by, bx), jnp.where(swap, py, px)
    b3, p3 = jnp.where(swap, bx, by), jnp.where(swap, px, py)
    axes = (b1, ba, b3, bb)
    step = rows // 16
    keep, send, base = [0], [], 0
    n = rows
    for bit in axes:
        n //= 2
        keep.append(pl.multiple_of(base + bit * n, step))
        send.append(pl.multiple_of(base + (1 - bit) * n, step))
        base = base + bit * n
    return (p1, pa, p3, pb), keep, send, axes


def chain_route(bits, peers, unit, d):
    core, bx, by, ba, bb = bits
    _, px, py, pa, _ = peers
    swap = odd(unit + core) == 1
    b1, p1 = jnp.where(swap, by, bx), jnp.where(swap, py, px)
    b3, p3 = jnp.where(swap, bx, by), jnp.where(swap, px, py)
    piece, chunk, pair, half = d // 16, d // 8, d // 4, d // 2
    me = lax.axis_index("data")

    def rows(base, n):
        return pl.ds(pl.multiple_of(base, piece), n)
    kx = b1 * half
    own = kx + (2 * bb + ba) * chunk
    mate = 2 * (kx + bb * pair) + chunk - own
    r = dict(
        half=rows(kx, half), other_half=rows((1 - b1) * half, half),
        pair=rows(kx + bb * pair, pair), other_pair=rows(kx + (1 - bb) * pair, pair),
        own=rows(own, chunk), mate=rows(mate, chunk),
        far_end=rows(kx + (1 - bb) * 3 * chunk, chunk), far_mid=rows(kx + (2 - bb) * chunk, chunk),
        keep=rows(own + b3 * piece, piece), send=rows(own + (1 - b3) * piece, piece),
        x_send_first=(rows((1 - b1) * half + (1 - bb) * pair, pair), rows((1 - bb) * pair, pair)),
        x_send_second=(rows((1 - b1) * half + bb * pair, pair), rows(bb * pair, pair)),
    )
    return r, p1, pa, me + 8 * (1 - 2 * bb), p3


def arrive(peers):
    barrier = pltpu.get_barrier_semaphore()
    for peer in peers:
        pl.semaphore_signal(barrier, device_id=(peer,), device_id_type=MESH)
    return functools.partial(pl.semaphore_wait, barrier, len(peers))


def others(bits, me_bits):
    me = lax.axis_index("data")
    out = []
    for mask in range(1, 1 << len(me_bits)):
        peer = me
        for i, k in enumerate(me_bits):
            if mask >> i & 1:
                peer = peer + (1 << k) * (1 - 2 * bits[k])
        out.append(peer)
    return out


def exchange_sum(buf, first, peers, send_sem, recv_sem, sem0):
    copies = [remote(buf.at[first], buf.at[first + 1 + i], send_sem.at[sem0 + i], recv_sem.at[sem0 + i], peer) for i, peer in enumerate(peers)]
    for cp in copies:
        cp.start()
    total = buf[first]
    for i, cp in enumerate(copies):
        cp.wait()
        total = total + buf[first + 1 + i]
    buf[first + len(peers) + 1] = total


def gather_hops(bits, peers, unit, d, full, piece_src=None):
    ps, keep, send, _ = route(bits, peers, unit, d)
    piece = d // 16

    def rows(base, n):
        return full.at[pl.ds(base, n), :]

    def hop(k, part, sem_s, sem_r):
        peer = ps[3 - k] if k < 4 else peers[0]
        if k == 0:
            ref = rows(keep[4], piece)
        elif part == 0:
            ref = rows(keep[5 - k], piece << (k - 1))
        else:
            ref = rows(send[4 - k], piece << (k - 1))
        src = piece_src if piece_src is not None and part == 0 and k <= 1 else ref
        return remote(src, ref, sem_s, sem_r, peer)

    def arrived(k, sem_s, sem_r):
        ref = rows(send[3 - k], piece << k)
        return remote(ref, ref, sem_s, sem_r, ps[3 - k])

    def sent(sem_s, sem_r):
        ref = rows(0, 15 * piece)
        return remote(ref, ref, sem_s, sem_r, ps[0])
    return hop, arrived, sent


def remote(src, dst, send_sem, recv_sem, peer):
    return pltpu.make_async_remote_copy(src_ref=src, dst_ref=dst, send_sem=send_sem, recv_sem=recv_sem, device_id=(peer,), device_id_type=MESH)


def local(src, dst, sem):
    return pltpu.make_async_copy(src, dst, sem)


def halves(t):
    return [(0, t // 2), (t // 2, t // 2)] if t % 32 == 0 else [(0, t)]


def transpose_into(dst, src, t):
    full = t // 128
    if full:
        @steps(full)
        def _(i):
            lo = pl.multiple_of(i * 128, 128)
            dst[:, pl.ds(lo, 128)] = src[pl.ds(lo, 128), :].T
    if t % 128:
        dst[:, full * 128:t] = src[full * 128:t, :].T


def fwd_pair(h_ref, v_ref, acc_ref, a_ref, z_ref, t, f):
    for lo, n in halves(t):
        for j in range(2):
            z = dot(h_ref[lo:lo + n, :], v_ref[j, 0]).astype(jnp.bfloat16)
            z_ref[j, lo:lo + n, :] = z
            a_ref[lo:lo + n, j * f:(j + 1) * f] = gelu(z.astype(jnp.float32)).astype(jnp.bfloat16)
    v_out = jnp.concatenate([v_ref[0, 1], v_ref[1, 1]], axis=1)
    for lo, n in halves(t):
        acc_ref[lo:lo + n, :] += dot(a_ref[lo:lo + n, :], v_out, NT)


def fwd_close(h_ref, acc_ref, t):
    for lo, n in halves(t):
        h_ref[lo:lo + n, :] = acc_ref[lo:lo + n, :].astype(jnp.bfloat16)


def fwd_seed(h_ref, acc_ref, t):
    for lo, n in halves(t):
        acc_ref[lo:lo + n, :] = h_ref[lo:lo + n, :].astype(jnp.float32)


def fold(v):
    r, c = v.shape
    rows = jnp.sum(v.reshape(r // 8, 8, c), axis=0)
    return sum(rows[:, lo:lo + 128] for lo in range(0, c, 128))


def loss_close(h_ref, y_ref, acc_ref, t, d, total_ref=None):
    def rows_of(rows):
        e = acc_ref[rows, :].astype(jnp.bfloat16).astype(jnp.float32) - y_ref[rows, :].astype(jnp.float32)
        q = e.astype(jnp.bfloat16)
        h_ref[rows, :] = q
        acc_ref[rows, :] = q.astype(jnp.float32)
        return e
    if total_ref is None:
        for lo, n in halves(t):
            rows_of(slice(lo, lo + n))
        return
    n = 112 if t % 112 == 0 else t
    total_ref[...] = jnp.zeros(TILE, jnp.float32)

    @steps(t // n)
    def _(i):
        e = rows_of(pl.ds(pl.multiple_of(i * n, n), n))
        total_ref[...] += fold(e * e)


def unit_of(it, nf, nl):
    return (nl - 1 - it // nf) * nf + lax.rem(it, nf)


def first_pass(dm, scale, x_hbm, y_hbm, wi_hbm, wo_hbm, z_out, v_out, ws_out, wc_out, g_out, n_out,
               h, tmp, tb, eb, acc, ab, wi, wo, zb, vb, ws, wc, cbuf, obuf, sbuf, r1, r2, r3, r4, nb,
               load_sem, z_sem, v_sem, io_sem, csend_sem, core_sem, send_sem, recv_sem, credit, nsend_sem, nrecv_sem):
    t, d, f, nf, nl = dm
    nu = nf * nl
    bits, peers = place()
    piece = d // 16
    near, far = others(bits, (0, 1, 2)), others(bits, (3, 4))
    wait_all = arrive(near + far)

    def loads(p, slot):
        layer, tile = p // (nf // 2), lax.rem(p, nf // 2)
        lo = pl.multiple_of(tile * 2 * f, 2 * f)
        return (local(wi_hbm.at[layer, :, pl.ds(lo, 2 * f)], wi.at[slot], load_sem.at[slot, 0]),
                local(wo_hbm.at[layer, pl.ds(lo, 2 * f), :], wo.at[slot], load_sem.at[slot, 1]))

    def stores(p, slot):
        two = pl.ds(2 * p, 2)
        return local(zb.at[slot], z_out.at[two], z_sem.at[slot]), local(vb.at[slot], v_out.at[two], v_sem.at[slot])

    x_in = local(x_hbm, h, io_sem.at[0])
    y_in = local(y_hbm, tmp, io_sem.at[1])
    x_in.start()
    for cp in loads(0, 0):
        cp.start()
    y_in.start()
    x_in.wait()
    fwd_seed(h, acc, t)

    @steps(nu // 2)
    def _(p):
        slot = odd(p)
        for cp in loads(p, slot):
            cp.wait()

        @pl.when(p + 1 < nu // 2)
        def _():
            for cp in loads(p + 1, 1 - slot):
                cp.start()

        @pl.when(p >= 2)
        def _():
            for cp in stores(p - 2, slot):
                cp.wait()
        for j in range(2):
            cols = slice(j * f, (j + 1) * f)
            wot = wo[slot, cols, :].T
            _, keep, _, _ = route(bits, peers, 2 * p + j, d)
            rows = pl.ds(keep[4], piece)
            vb[slot, j, 0] = wi[slot, :, cols].astype(jnp.bfloat16)
            vb[slot, j, 1] = wot.astype(jnp.bfloat16)
            obuf[j] = wot
            ws[2 * p + j] = jnp.where(bits[0] == 0, wi[slot, rows, cols], obuf[j, rows, :])
            rows = chain_route(bits, peers, j, d)[0]['keep']
            wc[2 * p + j] = jnp.where(bits[0] == 0, wi[slot, rows, cols], obuf[j, rows, :])

        fwd_pair(h, vb.at[slot], acc, ab, zb.at[slot], t, f)
        for cp in stores(p, slot):
            cp.start()

        @pl.when(p == nf // 2 - 1)
        def _():
            fwd_close(h, acc, t)
            fwd_seed(h, acc, t)
            transpose_into(tb.at[0], h, t)

    np_ = nu // 2
    if np_ >= 2:
        for cp in stores(np_ - 2, np_ % 2):
            cp.wait()
    spare = np_ % 2

    def tiles(it, slot):
        u = unit_of(it, nf, nl)
        return (local(z_out.at[u], zb.at[spare, slot], load_sem.at[slot, 0]), local(v_out.at[u], vb.at[spare, slot], load_sem.at[slot, 1]))
    for cp in tiles(0, 0):
        cp.start()
    ws_cp = local(ws, ws_out, io_sem.at[2])
    wc_cp = local(wc, wc_out, io_sem.at[3])
    ws_cp.start()
    wc_cp.start()
    y_in.wait()
    loss_close(h, tmp, acc, t, d)
    transpose_into(tb.at[1], h, t)
    x_again = local(x_hbm, tmp, io_sem.at[1])
    x_again.start()
    for cp in stores(np_ - 1, (np_ - 1) % 2):
        cp.wait()
    wait_all()
    nb[0] = jnp.zeros(TILE, jnp.float32)

    ws_cp.wait()

    def on_total(u, total):
        ws[u] = total
        g = total * scale
        nb[0] += fold(g * g)

    start, events = halving(dm, bits, peers, cbuf, (r1, r2, r3, r4), send_sem, recv_sem, credit, LAG_A[1:], on_total)
    backward_phase(dm, bits, peers, h, tmp, tb, eb, acc, zb.at[spare], vb.at[spare], cbuf, obuf, sbuf,
                   csend_sem, core_sem, credit, tiles, x_again.wait, LAG_A[0], start, events)
    g_cp = local(ws, g_out, io_sem.at[0])
    g_cp.start()
    exchange_sum(nb, 0, near, nsend_sem, nrecv_sem, 0)
    exchange_sum(nb, 8, far, nsend_sem, nrecv_sem, 7)
    n_cp = local(nb.at[12], n_out, io_sem.at[1])
    n_cp.start()
    wc_cp.wait()
    g_cp.wait()
    n_cp.wait()


def second_forward(dm, scale, rho, gs_hbm, ws_hbm, n_hbm, x_hbm, y_hbm, z_out, v_out, h_out, q_out, sq_out,
                   h, yb, acc, ab, gs, ws, vb, zb, nb, send_sem, recv_sem, z_sem, v_sem, io_sem):
    t, d, f, nf, nl = dm
    nu = nf * nl
    bits, peers = place()
    core = bits[0]
    piece = d // 16
    wait_all = arrive(peers)
    ins = (local(gs_hbm, gs, io_sem.at[0]), local(ws_hbm, ws, io_sem.at[1]), local(x_hbm, h, io_sem.at[2]), local(y_hbm, yb, io_sem.at[3]))
    n_in = local(n_hbm, nb, io_sem.at[4])
    n_in.start()
    for cp in ins:
        cp.start()
    n_in.wait()
    coef = rho / jnp.sqrt(jnp.sum(nb[...], keepdims=True))
    ins[0].wait()
    ins[1].wait()
    wait_all()

    def hops(u):
        return gather_hops(bits, peers, u, d, vb.at[u, core])

    def sems(u, k):
        return send_sem.at[u, 0 if k < 4 else 1], recv_sem.at[u, k]

    def core_arrived(u):
        ref = vb.at[u, 1 - core]
        return remote(ref, ref, *sems(u, 4), peers[0])

    def z_store(p, slot):
        return local(zb.at[slot], z_out.at[pl.ds(2 * p, 2)], z_sem.at[slot])

    @steps(nu + VG_LAG[5])
    def _(it):
        @pl.when(it < nu)
        def _():
            _, keep, _, _ = route(bits, peers, it, d)
            new = ws[it] + coef * (gs[it] * scale)
            vb[it, core, pl.ds(keep[4], piece), :] = new.astype(jnp.bfloat16)
            hop, _, _ = hops(it)
            hop(0, 0, *sems(it, 0)).start()
            hop(1, 0, *sems(it, 1)).start()
        for k in range(1, 5):
            u = it - VG_LAG[k]

            @pl.when((u >= 0) & (u < nu))
            def _():
                hop, arrived, _ = hops(u)
                arrived(k - 1, *sems(u, k - 1)).wait_recv()
                hop(k, 1, *sems(u, k)).start()
                if k < 4:
                    hop(k + 1, 0, *sems(u, k + 1)).start()
        u = it - VG_LAG[5]

        @pl.when(u >= 0)
        def _():
            core_arrived(u).wait_recv()
            local(vb.at[u], v_out.at[u], v_sem.at[u]).start()

        @pl.when((u >= 0) & (odd(u) == 1))
        def _():
            p = u // 2
            slot = odd(p)

            @pl.when(p >= 2)
            def _():
                z_store(p - 2, slot).wait()

            @pl.when(p == 0)
            def _():
                ins[2].wait()
                fwd_seed(h, acc, t)
            fwd_pair(h, vb.at[pl.ds(2 * p, 2)], acc, ab, zb.at[slot], t, f)
            z_store(p, slot).start()

            @pl.when(p == nf // 2 - 1)
            def _():
                fwd_close(h, acc, t)
                fwd_seed(h, acc, t)
                out = local(h, h_out, io_sem.at[0])
                out.start()
                out.wait()

    ins[3].wait()
    loss_close(h, yb, acc, t, d, nb)
    out = local(h, q_out, io_sem.at[0])
    sq = local(nb, sq_out, io_sem.at[1])
    out.start()
    sq.start()

    @steps(nu)
    def _(u):
        local(vb.at[u], v_out.at[u], v_sem.at[u]).wait()
        hops(u)[2](*sems(u, 0)).wait_send()
        core_arrived(u).wait_send()
    for p in range(max(nu // 2 - 2, 0), nu // 2):
        z_store(p, p % 2).wait()
    out.wait()
    sq.wait()


def backward_phase(dm, bits, peers, q, tmp, tb, eb, acc, zb, vb, cbuf, obuf, sbuf, csend_sem, core_sem, credit,
                   tiles, x_ready, core_lag, after_core, events):
    t, d, f, nf, nl = dm
    nu = nf * nl
    core = bits[0]
    slots = cbuf.shape[0]

    def core_copy(it):
        slot = odd(it)
        return remote(sbuf.at[slot], cbuf.at[lax.rem(it, slots)], csend_sem.at[slot], core_sem.at[it], peers[0])

    def core_stage(j):
        cs = lax.rem(j, slots)
        core_copy(j).wait_recv()
        cbuf[cs] = cbuf[cs] + obuf[odd(j)]
        after_core(j)

    @steps(nu + max(lag for lag, _ in events))
    def _(it):
        @pl.when(it == nf)
        def _():
            fwd_close(q, acc, t)
            transpose_into(tb.at[1], q, t)
            x_ready()
            transpose_into(tb.at[0], tmp, t)

        @pl.when(it < nu)
        def _():
            slot = odd(it)
            for cp in tiles(it, slot):
                cp.wait()

            @pl.when(it + 1 < nu)
            def _():
                for cp in tiles(it + 1, 1 - slot):
                    cp.start()
            for lo, n in halves(t):
                back = dot(q[lo:lo + n, :], vb[slot, 1])
                a, slope = gelu_and_grad(zb[slot, lo:lo + n, :].astype(jnp.float32))
                eb[1, lo:lo + n, :] = a.astype(jnp.bfloat16)
                eb[0, lo:lo + n, :] = (back * slope).astype(jnp.bfloat16)

            @pl.when(it >= 2)
            def _():
                core_copy(it - 2).wait_send()
            sbuf[slot] = dot(tb[1 - core], eb[1 - core])

            @pl.when(it >= slots)
            def _():
                pl.semaphore_wait(credit)
            core_copy(it).start()
            obuf[slot] = dot(tb[core], eb[core])

            @pl.when(it < nf)
            def _():
                for lo, n in halves(t):
                    acc[lo:lo + n, :] += dot(eb[0, lo:lo + n, :], vb[slot, 0], NT)

        for lag, event in ((core_lag, core_stage), *events):
            j = it - lag

            @pl.when((j >= 0) & (j < nu))
            def _():
                event(j)

    core_copy(nu - 2).wait_send()
    core_copy(nu - 1).wait_send()


def free_slot(j, nu, slots, credit, peer):
    @pl.when(j + slots < nu)
    def _():
        pl.semaphore_signal(credit, device_id=(peer,), device_id_type=MESH)


def halving(dm, bits, peers, cbuf, rbuf, send_sem, recv_sem, credit, lags, on_total):
    t, d, f, nf, nl = dm
    nu = nf * nl
    piece = d // 16
    slots = cbuf.shape[0]
    partner = peers[0]

    def rs_sends(it, k):
        ps, _, send, on = route(bits, peers, it, d)
        n = d >> (k + 1)
        cs = lax.rem(it, slots)

        def part(off, m, sem):
            return remote(cbuf.at[cs, pl.ds(send[k] + off, m), :], rbuf[k].at[it, pl.ds(off, m), :], send_sem.at[it], sem, ps[k])
        if k == 3:
            return [part(0, n, recv_sem.at[0, it, k])]
        m = n // 2
        return [part(pl.multiple_of((1 - on[k + 1]) * m, piece), m, recv_sem.at[0, it, k]),
                part(pl.multiple_of(on[k + 1] * m, piece), m, recv_sem.at[1, it, k])]

    def rs_add(it, k, kept):
        ps, keep, send, _ = route(bits, peers, it, d)
        cs = lax.rem(it, slots)
        if k == 3:
            base, m = keep[4], d >> 4
        else:
            base, m = (keep[k + 2] if kept else send[k + 1]), d >> (k + 2)
        here = rbuf[k].at[it, pl.ds(pl.multiple_of(base - keep[k + 1], piece), m), :]
        mine = cbuf.at[cs, pl.ds(base, m), :]
        remote(mine, here, send_sem.at[it], recv_sem.at[1 if kept else 0, it, k], ps[k]).wait_recv()
        total = mine[...] + here[...]
        if k == 3:
            return total
        mine[...] = total

    def start(j):
        for cp in rs_sends(j, 0):
            cp.start()

    def stage(k):
        def event(j):
            if k > 0:
                rs_add(j, k - 1, True)
            total = rs_add(j, k, False)
            if k < 3:
                for cp in rs_sends(j, k + 1):
                    cp.start()
            else:
                on_total(unit_of(j, nf, nl), total)
                ref = cbuf.at[lax.rem(j, slots), pl.ds(0, 15 * piece), :]
                remote(ref, ref, send_sem.at[j], recv_sem.at[0, j, 3], partner).wait_send()
                free_slot(j, nu, slots, credit, partner)
        return event
    return start, [(lags[k], stage(k)) for k in range(4)]


def chain(dm, bits, peers, cbuf, rbuf, gs, w_out, send_sem, recv_sem, credit, ag_send, ag_recv, ag_loc, lags, on_total):
    t, d, f, nf, nl = dm
    nu = nf * nl
    core, _, _, ba, bb = bits
    piece = d // 16
    slots = cbuf.shape[0]
    r1, r2, r3, r4, r5 = rbuf
    at_end = ba == bb
    chunk = d // 8
    XU, XK, EU, EK, MU, MK, YY = range(7)
    ALL, MIDDLE, CORE = range(3)
    HALF, MATE, PAIR, LAST, FULL = range(5)
    partner = peers[0]

    def send(j, src, dst, sem, peer):
        remote(cbuf.at[lax.rem(j, slots), src, :], dst, send_sem.at[j], recv_sem.at[sem, j], peer).start()

    def add(j, rows, buf, sem):
        mine = cbuf.at[lax.rem(j, slots), rows, :]
        remote(mine, buf, send_sem.at[j], recv_sem.at[sem, j], partner).wait_recv()
        mine[...] = mine[...] + buf[...]

    def at(j):
        return chain_route(bits, peers, unit_of(j, nf, nl), d)

    def start(j):
        r, p1, _, _, _ = at(j)
        for (src, dst), sem in ((r["x_send_first"], XU), (r["x_send_second"], XK)):
            send(j, src, r1.at[j, dst, :], sem, p1)

    def rel(first):
        return pl.ds(pl.multiple_of((1 - bb if first else bb) * (d // 4), piece), d // 4)

    def s1(j):
        r, _, pa, _, _ = at(j)
        add(j, r["other_pair"], r1.at[j, rel(True), :], XU)

        @pl.when(at_end)
        def _():
            send(j, r["other_pair"], r2.at[j], EU, pa)

    def s2(j):
        r, _, pa, pm, _ = at(j)
        add(j, r["pair"], r1.at[j, rel(False), :], XK)

        @pl.when(at_end)
        def _():
            send(j, r["mate"], r3.at[j], EK, pa)

        @pl.when(jnp.logical_not(at_end))
        def _():
            add(j, r["other_pair"], r2.at[j], EU)
            send(j, r["far_end"], r5.at[j, 0:chunk, :], MU, pm)
            send(j, r["far_mid"], r5.at[j, chunk:2 * chunk, :], MK, pm)

    def s3(j):
        r, _, pa, _, p3 = at(j)

        @pl.when(jnp.logical_not(at_end))
        def _():
            add(j, r["mate"], r5.at[j, 0:chunk, :], MU)
            send(j, r["mate"], r3.at[j], EK, pa)
            add(j, r["own"], r3.at[j], EK)
            add(j, r["own"], r5.at[j, chunk:2 * chunk, :], MK)
            send(j, r["send"], r4.at[j], YY, p3)

    def s4(j):
        r, _, _, _, p3 = at(j)

        @pl.when(at_end)
        def _():
            add(j, r["own"], r3.at[j], EK)
            send(j, r["send"], r4.at[j], YY, p3)

    def full(j):
        return w_out.at[unit_of(j, nf, nl), core]

    def give(j, rows, sem_s, sem_r, peer, src=None):
        ref = full(j).at[rows, :]
        return remote(ref if src is None else src, ref, ag_send.at[j, sem_s], ag_recv.at[j, sem_r], peer)

    def own_copy(j):
        u = unit_of(j, nf, nl)
        return local(gs.at[u], full(j).at[at(j)[0]["keep"], :], ag_loc.at[j])

    def s5(j):
        r, _, _, _, p3 = at(j)
        u = unit_of(j, nf, nl)
        mine = cbuf.at[lax.rem(j, slots), r["keep"], :]
        remote(mine, r4.at[j], send_sem.at[j], recv_sem.at[YY, j], p3).wait_recv()
        on_total(u, mine[...] + r4[j])
        own_copy(j).start()
        give(j, r["keep"], ALL, HALF, p3, gs.at[u]).start()
        ref = cbuf.at[lax.rem(j, slots), pl.ds(0, 15 * piece), :]
        remote(ref, ref, send_sem.at[j], recv_sem.at[YY, j], p3).wait_send()
        free_slot(j, nu, slots, credit, partner)

    def g1(j):
        r, p1, pa, pm, p3 = at(j)
        own_copy(j).wait()
        give(j, r["send"], ALL, HALF, p3).wait_recv()
        give(j, r["own"], ALL, MATE, pa).start()

        @pl.when(jnp.logical_not(at_end))
        def _():
            give(j, r["own"], MIDDLE, PAIR, pm).start()
        give(j, r["own"], ALL, LAST, p1).start()

    def g2(j):
        r, p1, pa, pm, _ = at(j)
        give(j, r["mate"], ALL, MATE, pa).wait_recv()

        @pl.when(jnp.logical_not(at_end))
        def _():
            give(j, r["mate"], MIDDLE, PAIR, pm).start()
        give(j, r["mate"], ALL, LAST, p1).start()

    def g3(j, r, p1, pa):
        give(j, r["other_pair"], MIDDLE, PAIR, pa).wait_recv()
        give(j, r["other_pair"], ALL, LAST, p1).start()
        give(j, r["half"], CORE, FULL, partner).start()

    def g3_middle(j):
        r, p1, pa, _, _ = at(j)

        @pl.when(jnp.logical_not(at_end))
        def _():
            g3(j, r, p1, pa)
            give(j, r["other_pair"], MIDDLE, PAIR, pa).start()

    def g3_end(j):
        r, p1, pa, _, _ = at(j)

        @pl.when(at_end)
        def _():
            g3(j, r, p1, pa)

    def g4(j):
        r, p1, _, _, _ = at(j)
        give(j, r["other_half"], ALL, LAST, p1).wait_recv()
        give(j, r["other_half"], CORE, FULL, partner).start()

    def finish_unit(j):
        ref = w_out.at[unit_of(j, nf, nl), 1 - core]
        last = remote(ref, ref, ag_send.at[j, CORE], ag_recv.at[j, FULL], partner)
        last.wait_recv()
        last.wait_send()
        ref = full(j).at[pl.ds(0, 11 * piece), :]
        remote(ref, ref, ag_send.at[j, ALL], ag_recv.at[j, LAST], partner).wait_send()

        @pl.when(jnp.logical_not(at_end))
        def _():
            ref = full(j).at[pl.ds(0, 8 * piece), :]
            remote(ref, ref, ag_send.at[j, MIDDLE], ag_recv.at[j, PAIR], partner).wait_send()

    steps = (s1, s2, s3, s4, s5, g1, g2, g3_middle, g3_end, g4)
    return start, list(zip(lags, steps)), finish_unit


def second_backward(dm, scale, x_hbm, h_hbm, q_hbm, z_hbm, v_hbm, ws_hbm, sq_hbm, w_out, sq_out,
                    q, tmp, tb, eb, acc, zb, vb, cbuf, obuf, sbuf, r1, r2, r3, r4, r5, gs,
                    load_sem, io_sem, csend_sem, core_sem, send_sem, recv_sem, credit, nb, ag_send, ag_recv, ag_loc, nsend_sem, nrecv_sem):
    t, d, f, nf, nl = dm
    nu = nf * nl
    bits, peers = place()
    near, far = others(bits, (0, 1, 2)), others(bits, (3, 4))
    wait_all = arrive(near + far)

    def tiles(it, slot):
        u = unit_of(it, nf, nl)
        return local(z_hbm.at[u], zb.at[slot], load_sem.at[slot, 0]), local(v_hbm.at[u], vb.at[slot], load_sem.at[slot, 1])

    q_in = local(q_hbm, q, io_sem.at[0])
    h_in = local(h_hbm, tmp, io_sem.at[1])
    ws_in = local(ws_hbm, gs, io_sem.at[2])
    sq_in = local(sq_hbm, nb.at[0], io_sem.at[3])
    q_in.start()
    for cp in tiles(0, 0):
        cp.start()
    for cp in (h_in, ws_in, sq_in):
        cp.start()
    q_in.wait()
    fwd_seed(q, acc, t)
    transpose_into(tb.at[1], q, t)
    h_in.wait()
    transpose_into(tb.at[0], tmp, t)
    x_in = local(x_hbm, tmp, io_sem.at[1])
    x_in.start()
    ws_in.wait()
    sq_in.wait()
    wait_all()

    def on_total(u, total):
        gs[u] = gs[u] - LEARN_RATE * (total * scale)

    def sums(j):
        @pl.when(j == 1)
        def _():
            exchange_sum(nb, 0, near, nsend_sem, nrecv_sem, 0)

        @pl.when(j == 2)
        def _():
            exchange_sum(nb, 8, far, nsend_sem, nrecv_sem, 7)

    start, events, finish_unit = chain(dm, bits, peers, cbuf, (r1, r2, r3, r4, r5), gs, w_out, send_sem, recv_sem, credit,
                                       ag_send, ag_recv, ag_loc, LAG_B[1:], on_total)
    backward_phase(dm, bits, peers, q, tmp, tb, eb, acc, zb, vb, cbuf, obuf, sbuf,
                   csend_sem, core_sem, credit, tiles, x_in.wait, LAG_B[0], start, [*events, (0, sums)])
    sq_cp = local(nb.at[12], sq_out, io_sem.at[3])
    sq_cp.start()

    @steps(nu)
    def _(j):
        finish_unit(j)
    sq_cp.wait()


def finish(scale, f, w_ref, sq_ref, in_ref, out_ref, loss_ref):
    for j in range(w_ref.shape[0]):
        in_ref[0, :, j * f:(j + 1) * f] = w_ref[j, 0]
        out_ref[0, j * f:(j + 1) * f, :] = w_ref[j, 1].T
    loss_ref[0, 0] = 0.5 * (jnp.sum(sq_ref[...]) * scale)


def sds(shape, dtype):
    return jax.ShapeDtypeStruct(shape, dtype)


def call(kernel, n_in, outs, scratch, name, collective_id=None):
    params = dict(vmem_limit_bytes=VMEM_CAP)
    if collective_id is not None:
        params.update(collective_id=collective_id, has_side_effects=True)
    return pl.pallas_call(
        kernel,
        out_shape=outs,
        in_specs=[ANY] * n_in,
        out_specs=[ANY] * len(outs),
        scratch_shapes=scratch,
        compiler_params=pltpu.CompilerParams(**params),
        name=name,
    )


def local_step(n_dev, tile_f, x_loc, y_loc, w_in, w_out):
    nl, d, ff = w_in.shape
    f = tile_f
    nf = ff // f
    nu = nl * nf
    t = x_loc.shape[0] * x_loc.shape[1]
    piece = d // 16
    dm = (t, d, f, nf, nl)
    scale = 1.0 / (t * n_dev * d)
    rho = RHO_FRAC * math.sqrt(nl * (d + ff))
    bf, f32 = jnp.bfloat16, jnp.float32
    V, DMA, REG = pltpu.VMEM, pltpu.SemaphoreType.DMA, pltpu.SemaphoreType.REGULAR
    x = x_loc.transpose(1, 0, 2).reshape(t, d)
    y = y_loc.transpose(1, 0, 2).reshape(t, d)
    z_s, v_s, w_s, a_s, n_s = sds((nu, t, f), bf), sds((nu, 2, d, f), bf), sds((nu, piece, f), f32), sds((t, d), bf), sds(TILE, f32)
    slots = min(CORE_SLOTS, nu)
    tile2, rows = V((2, d, f), f32), V((nu, piece, f), f32)
    reduce_bufs = [V((slots, d, f), f32), tile2, tile2, *(V((nu, d >> k, f), f32) for k in range(1, 5))]
    act, sums, both = V((t, d), bf), V((t, d), f32), V((t, 2 * f), bf)
    acts = [act, act, V((2, d, t), bf), V((2, t, f), bf), sums]
    norms, tens = V((13, *TILE), f32), DMA((10,))
    two, four, per_unit, loads = DMA((2,)), DMA((4,)), DMA((nu,)), DMA((2, 2))

    z, v, ws, wc, g, norm = call(
        functools.partial(first_pass, dm, scale), 4, [z_s, v_s, w_s, w_s, w_s, n_s],
        acts + [both, V((2, d, 2 * f), f32), V((2, 2 * f, d), f32), V((2, 2, t, f), bf), V((2, 2, 2, d, f), bf), rows, rows]
        + reduce_bufs + [norms, loads, two, two, four, two, per_unit, per_unit, DMA((2, nu, 4)), REG, tens, tens],
        "pass_a", 0)(x, y, w_in, w_out)

    z, v, h1, q, sq = call(
        functools.partial(second_forward, dm, scale, rho), 5, [z_s, v_s, a_s, a_s, n_s],
        [act, act, sums, both, rows, rows, V((nu, 2, d, f), bf), V((2, 2, t, f), bf), V(TILE, f32),
         DMA((nu, 2)), DMA((nu, 5)), two, per_unit, DMA((5,))], "fwd_b", 1)(g, ws, norm, x, y)

    w_new, sq = call(
        functools.partial(second_backward, dm, scale), 7, [sds((nu, 2, d, f), f32), n_s],
        acts + [V((2, t, f), bf), V((2, 2, d, f), bf)] + reduce_bufs
        + [V((nu, d // 4, f), f32), rows, loads, four, two, per_unit, per_unit, DMA((7, nu)), REG,
           norms, DMA((nu, 3)), DMA((nu, 5)), per_unit, tens, tens], "bwd_b", 2)(x, h1, q, z, v, wc, sq)

    per_step = min(FINISH_TILES, nf)
    new_in, new_out, loss = pl.pallas_call(
        functools.partial(finish, scale, f),
        grid=(nl, nf // per_step),
        in_specs=[pl.BlockSpec((per_step, 2, d, f), lambda i, j: (i * (nf // per_step) + j, 0, 0, 0)), pl.BlockSpec(TILE, lambda i, j: (0, 0))],
        out_specs=[pl.BlockSpec((1, d, per_step * f), lambda i, j: (i, 0, j)), pl.BlockSpec((1, per_step * f, d), lambda i, j: (i, j, 0)),
                   pl.BlockSpec((1, 1), lambda i, j: (0, 0), memory_space=pltpu.SMEM)],
        out_shape=[sds((nl, d, ff), f32), sds((nl, ff, d), f32), sds((1, 1), f32)],
        compiler_params=pltpu.CompilerParams(vmem_limit_bytes=VMEM_CAP),
        name="finish")(w_new, sq)
    return new_in, new_out, loss.reshape(())


def solution(mesh):
    step = functools.partial(local_step, mesh.shape["data"], TILE_F)
    return jax.shard_map(step, mesh=mesh, in_specs=(P("data"), P("data"), P(), P()), out_specs=(P(), P(), P()), check_vma=False)
```

```python
import math
import functools
import jax
import jax.numpy as jnp
from jax import lax
from jax.experimental import pallas as pl
from jax.experimental.pallas import tpu as pltpu
from jax.sharding import PartitionSpec as P

RHO_FRAC = 0.1
LEARN_RATE = 1.0
TILE_F = 256
MESH = pl.DeviceIdType.MESH
ANY = pl.BlockSpec(memory_space=pl.ANY)
NN = (((1,), (0,)), ((), ()))
NT = (((1,), (1,)), ((), ()))
GELU_C = math.sqrt(2.0 / math.pi)
GELU_K = 0.044715
VMEM_CAP = 67043328
TILE = (8, 128)
FINISH_TILES = 6
CORE_SLOTS = 9
LAG_A = (0, 1, 2, 3, 5)
LAG_B = (0, 2, 3, 4, 5, 6, 8, 9, 10, 14, 16)
VG_LAG = (0, 4, 6, 11, 14, 16)


steps = functools.partial(pl.loop, 0)


def odd(i):
    return lax.rem(i, 2)


def dot(lhs, rhs, dims=NN):
    return lax.dot_general(lhs, rhs, dims, preferred_element_type=jnp.float32)


def gelu_parts(z):
    sq = z * z
    th = jnp.tanh(GELU_C * (z + GELU_K * (sq * z)))
    cdf = 0.5 * (1.0 + th)
    return sq, th, cdf


def gelu(z):
    return z * gelu_parts(z)[2]


def gelu_and_grad(z):
    sq, th, cdf = gelu_parts(z)
    slope = cdf + (0.5 * z) * ((1.0 - th * th) * (GELU_C + (3.0 * GELU_K * GELU_C) * sq))
    return z * cdf, slope


def place(axis="data"):
    me = lax.axis_index(axis)
    bits = [lax.rem(lax.div(me, 1 << k), 2) for k in range(5)]
    peers = [me + (1 << k) * (1 - 2 * bits[k]) for k in range(5)]
    return bits, peers


def route(bits, peers, unit, rows):
    core, bx, by, ba, bb = bits
    _, px, py, pa, pb = peers
    swap = odd(unit + core) == 1
    b1, p1 = jnp.where(swap, by, bx), jnp.where(swap, py, px)
    b3, p3 = jnp.where(swap, bx, by), jnp.where(swap, px, py)
    axes = (b1, ba, b3, bb)
    step = rows // 16
    keep, send, base = [0], [], 0
    n = rows
    for bit in axes:
        n //= 2
        keep.append(pl.multiple_of(base + bit * n, step))
        send.append(pl.multiple_of(base + (1 - bit) * n, step))
        base = base + bit * n
    return (p1, pa, p3, pb), keep, send, axes


def chain_route(bits, peers, unit, d):
    core, bx, by, ba, bb = bits
    _, px, py, pa, _ = peers
    swap = odd(unit + core) == 1
    b1, p1 = jnp.where(swap, by, bx), jnp.where(swap, py, px)
    b3, p3 = jnp.where(swap, bx, by), jnp.where(swap, px, py)
    piece, chunk, pair, half = d // 16, d // 8, d // 4, d // 2
    me = lax.axis_index("data")

    def rows(base, n):
        return pl.ds(pl.multiple_of(base, piece), n)
    kx = b1 * half
    own = kx + (2 * bb + ba) * chunk
    mate = 2 * (kx + bb * pair) + chunk - own
    r = dict(
        half=rows(kx, half), other_half=rows((1 - b1) * half, half),
        pair=rows(kx + bb * pair, pair), other_pair=rows(kx + (1 - bb) * pair, pair),
        own=rows(own, chunk), mate=rows(mate, chunk),
        far_end=rows(kx + (1 - bb) * 3 * chunk, chunk), far_mid=rows(kx + (2 - bb) * chunk, chunk),
        keep=rows(own + b3 * piece, piece), send=rows(own + (1 - b3) * piece, piece),
        x_send_first=(rows((1 - b1) * half + (1 - bb) * pair, pair), rows((1 - bb) * pair, pair)),
        x_send_second=(rows((1 - b1) * half + bb * pair, pair), rows(bb * pair, pair)),
    )
    return r, p1, pa, me + 8 * (1 - 2 * bb), p3


def arrive(peers):
    barrier = pltpu.get_barrier_semaphore()
    for peer in peers:
        pl.semaphore_signal(barrier, device_id=(peer,), device_id_type=MESH)
    return functools.partial(pl.semaphore_wait, barrier, len(peers))


def others(bits, me_bits):
    me = lax.axis_index("data")
    out = []
    for mask in range(1, 1 << len(me_bits)):
        peer = me
        for i, k in enumerate(me_bits):
            if mask >> i & 1:
                peer = peer + (1 << k) * (1 - 2 * bits[k])
        out.append(peer)
    return out


def exchange(buf, first, peers, send_sem, recv_sem, sem0):
    copies = [remote(buf.at[first], buf.at[first + 1 + i], send_sem.at[sem0 + i], recv_sem.at[sem0 + i], peer) for i, peer in enumerate(peers)]

    def start():
        for cp in copies:
            cp.start()

    def close():
        total = buf[first]
        for i, cp in enumerate(copies):
            cp.wait()
            total = total + buf[first + 1 + i]
        buf[first + len(peers) + 1] = total
    return start, close


def gather_hops(bits, peers, unit, d, full, piece_src=None):
    ps, keep, send, _ = route(bits, peers, unit, d)
    piece = d // 16

    def rows(base, n):
        return full.at[pl.ds(base, n), :]

    def hop(k, part, sem_s, sem_r):
        peer = ps[3 - k] if k < 4 else peers[0]
        if k == 0:
            ref = rows(keep[4], piece)
        elif part == 0:
            ref = rows(keep[5 - k], piece << (k - 1))
        else:
            ref = rows(send[4 - k], piece << (k - 1))
        src = piece_src if piece_src is not None and part == 0 and k <= 1 else ref
        return remote(src, ref, sem_s, sem_r, peer)

    def arrived(k, sem_s, sem_r):
        ref = rows(send[3 - k], piece << k)
        return remote(ref, ref, sem_s, sem_r, ps[3 - k])

    def sent(sem_s, sem_r):
        ref = rows(0, 15 * piece)
        return remote(ref, ref, sem_s, sem_r, ps[0])
    return hop, arrived, sent


def remote(src, dst, send_sem, recv_sem, peer):
    return pltpu.make_async_remote_copy(src_ref=src, dst_ref=dst, send_sem=send_sem, recv_sem=recv_sem, device_id=(peer,), device_id_type=MESH)


def local(src, dst, sem):
    return pltpu.make_async_copy(src, dst, sem)


def halves(t):
    return [(0, t // 2), (t // 2, t // 2)] if t % 32 == 0 else [(0, t)]


def transpose_into(dst, src, t):
    full = t // 128
    if full:
        @steps(full)
        def _(i):
            lo = pl.multiple_of(i * 128, 128)
            dst[:, pl.ds(lo, 128)] = src[pl.ds(lo, 128), :].T
    if t % 128:
        dst[:, full * 128:t] = src[full * 128:t, :].T


def fwd_pair(h_ref, v_ref, acc_ref, a_ref, z_ref, t, f):
    for lo, n in halves(t):
        for j in range(2):
            z = dot(h_ref[lo:lo + n, :], v_ref[j, 0]).astype(jnp.bfloat16)
            z_ref[j, lo:lo + n, :] = z
            a_ref[lo:lo + n, j * f:(j + 1) * f] = gelu(z.astype(jnp.float32)).astype(jnp.bfloat16)
    v_out = jnp.concatenate([v_ref[0, 1], v_ref[1, 1]], axis=1)
    for lo, n in halves(t):
        acc_ref[lo:lo + n, :] += dot(a_ref[lo:lo + n, :], v_out, NT)


def fwd_close(h_ref, acc_ref, t):
    for lo, n in halves(t):
        h_ref[lo:lo + n, :] = acc_ref[lo:lo + n, :].astype(jnp.bfloat16)


def fwd_seed(h_ref, acc_ref, t):
    for lo, n in halves(t):
        acc_ref[lo:lo + n, :] = h_ref[lo:lo + n, :].astype(jnp.float32)


def fold(v):
    r, c = v.shape
    rows = jnp.sum(v.reshape(r // 8, 8, c), axis=0)
    return sum(rows[:, lo:lo + 128] for lo in range(0, c, 128))


def loss_close(h_ref, y_ref, acc_ref, t, d, total_ref=None):
    def rows_of(rows):
        e = acc_ref[rows, :].astype(jnp.bfloat16).astype(jnp.float32) - y_ref[rows, :].astype(jnp.float32)
        q = e.astype(jnp.bfloat16)
        h_ref[rows, :] = q
        acc_ref[rows, :] = q.astype(jnp.float32)
        return e
    if total_ref is None:
        for lo, n in halves(t):
            rows_of(slice(lo, lo + n))
        return
    n = 112 if t % 112 == 0 else t
    total_ref[...] = jnp.zeros(TILE, jnp.float32)

    @steps(t // n)
    def _(i):
        e = rows_of(pl.ds(pl.multiple_of(i * n, n), n))
        total_ref[...] += fold(e * e)


def unit_of(it, nf, nl):
    return (nl - 1 - it // nf) * nf + lax.rem(it, nf)


def first_pass(dm, scale, x_hbm, y_hbm, wi_hbm, wo_hbm, z_out, v_out, ws_out, wc_out, g_out, n_out,
               h, tmp, tb, eb, acc, ab, wi, wo, zb, vb, ws, wc, cbuf, obuf, sbuf, r1, r2, r3, r4, nb,
               load_sem, z_sem, v_sem, io_sem, csend_sem, core_sem, send_sem, recv_sem, credit, nsend_sem, nrecv_sem):
    t, d, f, nf, nl = dm
    nu = nf * nl
    bits, peers = place()
    piece = d // 16
    near, far = others(bits, (0, 1, 2)), others(bits, (3, 4))
    wait_all = arrive(near + far)

    def loads(p, slot):
        layer, tile = p // (nf // 2), lax.rem(p, nf // 2)
        lo = pl.multiple_of(tile * 2 * f, 2 * f)
        return (local(wi_hbm.at[layer, :, pl.ds(lo, 2 * f)], wi.at[slot], load_sem.at[slot, 0]),
                local(wo_hbm.at[layer, pl.ds(lo, 2 * f), :], wo.at[slot], load_sem.at[slot, 1]))

    def stores(p, slot):
        two = pl.ds(2 * p, 2)
        return local(zb.at[slot], z_out.at[two], z_sem.at[slot]), local(vb.at[slot], v_out.at[two], v_sem.at[slot])

    x_in = local(x_hbm, h, io_sem.at[0])
    y_in = local(y_hbm, tmp, io_sem.at[1])
    x_in.start()
    for cp in loads(0, 0):
        cp.start()
    y_in.start()
    x_in.wait()
    fwd_seed(h, acc, t)

    @steps(nu // 2)
    def _(p):
        slot = odd(p)
        for cp in loads(p, slot):
            cp.wait()

        @pl.when(p + 1 < nu // 2)
        def _():
            for cp in loads(p + 1, 1 - slot):
                cp.start()

        @pl.when(p >= 2)
        def _():
            for cp in stores(p - 2, slot):
                cp.wait()
        for j in range(2):
            cols = slice(j * f, (j + 1) * f)
            wot = wo[slot, cols, :].T
            _, keep, _, _ = route(bits, peers, 2 * p + j, d)
            rows = pl.ds(keep[4], piece)
            vb[slot, j, 0] = wi[slot, :, cols].astype(jnp.bfloat16)
            vb[slot, j, 1] = wot.astype(jnp.bfloat16)
            obuf[j] = wot
            ws[2 * p + j] = jnp.where(bits[0] == 0, wi[slot, rows, cols], obuf[j, rows, :])
            rows = chain_route(bits, peers, j, d)[0]['keep']
            wc[2 * p + j] = jnp.where(bits[0] == 0, wi[slot, rows, cols], obuf[j, rows, :])

        fwd_pair(h, vb.at[slot], acc, ab, zb.at[slot], t, f)
        for cp in stores(p, slot):
            cp.start()

        @pl.when(p == nf // 2 - 1)
        def _():
            fwd_close(h, acc, t)
            fwd_seed(h, acc, t)
            transpose_into(tb.at[0], h, t)

    np_ = nu // 2
    if np_ >= 2:
        for cp in stores(np_ - 2, np_ % 2):
            cp.wait()
    spare = np_ % 2

    def tiles(it, slot):
        u = unit_of(it, nf, nl)
        return (local(z_out.at[u], zb.at[spare, slot], load_sem.at[slot, 0]), local(v_out.at[u], vb.at[spare, slot], load_sem.at[slot, 1]))
    for cp in tiles(0, 0):
        cp.start()
    ws_cp = local(ws, ws_out, io_sem.at[2])
    wc_cp = local(wc, wc_out, io_sem.at[3])
    ws_cp.start()
    wc_cp.start()
    y_in.wait()
    loss_close(h, tmp, acc, t, d)
    transpose_into(tb.at[1], h, t)
    x_again = local(x_hbm, tmp, io_sem.at[1])
    x_again.start()
    for cp in stores(np_ - 1, (np_ - 1) % 2):
        cp.wait()
    wait_all()
    nb[0] = jnp.zeros(TILE, jnp.float32)

    ws_cp.wait()

    def on_total(u, total):
        ws[u] = total
        g = total * scale
        nb[0] += fold(g * g)

    start, events = halving(dm, bits, peers, cbuf, (r1, r2, r3, r4), send_sem, recv_sem, credit, LAG_A[1:], on_total)
    backward_phase(dm, bits, peers, h, tmp, tb, eb, acc, zb.at[spare], vb.at[spare], cbuf, obuf, sbuf,
                   csend_sem, core_sem, credit, tiles, x_again.wait, LAG_A[0], start, events)
    g_cp = local(ws, g_out, io_sem.at[0])
    g_cp.start()
    for start, close in (exchange(nb, 0, near, nsend_sem, nrecv_sem, 0), exchange(nb, 8, far, nsend_sem, nrecv_sem, 7)):
        start()
        close()
    n_cp = local(nb.at[12], n_out, io_sem.at[1])
    n_cp.start()
    wc_cp.wait()
    g_cp.wait()
    n_cp.wait()


def second_forward(dm, scale, rho, gs_hbm, ws_hbm, n_hbm, x_hbm, y_hbm, z_out, v_out, h_out, q_out, sq_out,
                   h, yb, acc, ab, gs, ws, vb, zb, nb, send_sem, recv_sem, z_sem, v_sem, io_sem):
    t, d, f, nf, nl = dm
    nu = nf * nl
    bits, peers = place()
    core = bits[0]
    piece = d // 16
    wait_all = arrive(peers)
    ins = (local(gs_hbm, gs, io_sem.at[0]), local(ws_hbm, ws, io_sem.at[1]), local(x_hbm, h, io_sem.at[2]), local(y_hbm, yb, io_sem.at[3]))
    n_in = local(n_hbm, nb, io_sem.at[4])
    n_in.start()
    for cp in ins:
        cp.start()
    n_in.wait()
    coef = rho / jnp.sqrt(jnp.sum(nb[...], keepdims=True))
    ins[0].wait()
    ins[1].wait()
    wait_all()

    def hops(u):
        return gather_hops(bits, peers, u, d, vb.at[u, core])

    def sems(u, k):
        return send_sem.at[u, 0 if k < 4 else 1], recv_sem.at[u, k]

    def core_arrived(u):
        ref = vb.at[u, 1 - core]
        return remote(ref, ref, *sems(u, 4), peers[0])

    def z_store(p, slot):
        return local(zb.at[slot], z_out.at[pl.ds(2 * p, 2)], z_sem.at[slot])

    @steps(nu + VG_LAG[5])
    def _(it):
        @pl.when(it < nu)
        def _():
            _, keep, _, _ = route(bits, peers, it, d)
            new = ws[it] + coef * (gs[it] * scale)
            vb[it, core, pl.ds(keep[4], piece), :] = new.astype(jnp.bfloat16)
            hop, _, _ = hops(it)
            hop(0, 0, *sems(it, 0)).start()
            hop(1, 0, *sems(it, 1)).start()
        for k in range(1, 5):
            u = it - VG_LAG[k]

            @pl.when((u >= 0) & (u < nu))
            def _():
                hop, arrived, _ = hops(u)
                arrived(k - 1, *sems(u, k - 1)).wait_recv()
                hop(k, 1, *sems(u, k)).start()
                if k < 4:
                    hop(k + 1, 0, *sems(u, k + 1)).start()
        u = it - VG_LAG[5]

        @pl.when(u >= 0)
        def _():
            core_arrived(u).wait_recv()
            local(vb.at[u], v_out.at[u], v_sem.at[u]).start()

        @pl.when((u >= 0) & (odd(u) == 1))
        def _():
            p = u // 2
            slot = odd(p)

            @pl.when(p >= 2)
            def _():
                z_store(p - 2, slot).wait()

            @pl.when(p == 0)
            def _():
                ins[2].wait()
                fwd_seed(h, acc, t)
            fwd_pair(h, vb.at[pl.ds(2 * p, 2)], acc, ab, zb.at[slot], t, f)
            z_store(p, slot).start()

            @pl.when(p == nf // 2 - 1)
            def _():
                fwd_close(h, acc, t)
                fwd_seed(h, acc, t)
                local(h, h_out, io_sem.at[0]).start()

    ins[3].wait()
    local(h, h_out, io_sem.at[0]).wait()
    loss_close(h, yb, acc, t, d, nb)
    out = local(h, q_out, io_sem.at[0])
    sq = local(nb, sq_out, io_sem.at[1])
    out.start()
    sq.start()

    @steps(nu)
    def _(u):
        local(vb.at[u], v_out.at[u], v_sem.at[u]).wait()
        hops(u)[2](*sems(u, 0)).wait_send()
        core_arrived(u).wait_send()
    for p in range(max(nu // 2 - 2, 0), nu // 2):
        z_store(p, p % 2).wait()
    out.wait()
    sq.wait()


def backward_phase(dm, bits, peers, q, tmp, tb, eb, acc, zb, vb, cbuf, obuf, sbuf, csend_sem, core_sem, credit,
                   tiles, x_ready, core_lag, after_core, events):
    t, d, f, nf, nl = dm
    nu = nf * nl
    core = bits[0]
    slots = cbuf.shape[0]

    def core_copy(it):
        slot = odd(it)
        return remote(sbuf.at[slot], cbuf.at[lax.rem(it, slots)], csend_sem.at[slot], core_sem.at[it], peers[0])

    def core_stage(j):
        cs = lax.rem(j, slots)
        core_copy(j).wait_recv()
        cbuf[cs] = cbuf[cs] + obuf[odd(j)]
        after_core(j)

    @steps(nu + max(lag for lag, _ in events))
    def _(it):
        @pl.when(it == nf)
        def _():
            fwd_close(q, acc, t)
            transpose_into(tb.at[1], q, t)
            x_ready()
            transpose_into(tb.at[0], tmp, t)

        @pl.when(it < nu)
        def _():
            slot = odd(it)
            for cp in tiles(it, slot):
                cp.wait()

            @pl.when(it + 1 < nu)
            def _():
                for cp in tiles(it + 1, 1 - slot):
                    cp.start()
            for lo, n in halves(t):
                back = dot(q[lo:lo + n, :], vb[slot, 1])
                a, slope = gelu_and_grad(zb[slot, lo:lo + n, :].astype(jnp.float32))
                eb[1, lo:lo + n, :] = a.astype(jnp.bfloat16)
                eb[0, lo:lo + n, :] = (back * slope).astype(jnp.bfloat16)

            @pl.when(it >= 2)
            def _():
                core_copy(it - 2).wait_send()
            sbuf[slot] = dot(tb[1 - core], eb[1 - core])

            @pl.when(it >= slots)
            def _():
                pl.semaphore_wait(credit)
            core_copy(it).start()
            obuf[slot] = dot(tb[core], eb[core])

            @pl.when(it < nf)
            def _():
                for lo, n in halves(t):
                    acc[lo:lo + n, :] += dot(eb[0, lo:lo + n, :], vb[slot, 0], NT)

        for lag, event in ((core_lag, core_stage), *events):
            j = it - lag

            @pl.when((j >= 0) & (j < nu))
            def _():
                event(j)

    core_copy(nu - 2).wait_send()
    core_copy(nu - 1).wait_send()


def free_slot(j, nu, slots, credit, peer):
    @pl.when(j + slots < nu)
    def _():
        pl.semaphore_signal(credit, device_id=(peer,), device_id_type=MESH)


def halving(dm, bits, peers, cbuf, rbuf, send_sem, recv_sem, credit, lags, on_total):
    t, d, f, nf, nl = dm
    nu = nf * nl
    piece = d // 16
    slots = cbuf.shape[0]
    partner = peers[0]

    def rs_sends(it, k):
        ps, _, send, on = route(bits, peers, it, d)
        n = d >> (k + 1)
        cs = lax.rem(it, slots)

        def part(off, m, sem):
            return remote(cbuf.at[cs, pl.ds(send[k] + off, m), :], rbuf[k].at[it, pl.ds(off, m), :], send_sem.at[it], sem, ps[k])
        if k == 3:
            return [part(0, n, recv_sem.at[0, it, k])]
        m = n // 2
        return [part(pl.multiple_of((1 - on[k + 1]) * m, piece), m, recv_sem.at[0, it, k]),
                part(pl.multiple_of(on[k + 1] * m, piece), m, recv_sem.at[1, it, k])]

    def rs_add(it, k, kept):
        ps, keep, send, _ = route(bits, peers, it, d)
        cs = lax.rem(it, slots)
        if k == 3:
            base, m = keep[4], d >> 4
        else:
            base, m = (keep[k + 2] if kept else send[k + 1]), d >> (k + 2)
        here = rbuf[k].at[it, pl.ds(pl.multiple_of(base - keep[k + 1], piece), m), :]
        mine = cbuf.at[cs, pl.ds(base, m), :]
        remote(mine, here, send_sem.at[it], recv_sem.at[1 if kept else 0, it, k], ps[k]).wait_recv()
        total = mine[...] + here[...]
        if k == 3:
            return total
        mine[...] = total

    def start(j):
        for cp in rs_sends(j, 0):
            cp.start()

    def stage(k):
        def event(j):
            if k > 0:
                rs_add(j, k - 1, True)
            total = rs_add(j, k, False)
            if k < 3:
                for cp in rs_sends(j, k + 1):
                    cp.start()
            else:
                on_total(unit_of(j, nf, nl), total)
                ref = cbuf.at[lax.rem(j, slots), pl.ds(0, 15 * piece), :]
                remote(ref, ref, send_sem.at[j], recv_sem.at[0, j, 3], partner).wait_send()
                free_slot(j, nu, slots, credit, partner)
        return event
    return start, [(lags[k], stage(k)) for k in range(4)]


def chain(dm, bits, peers, cbuf, rbuf, gs, w_out, send_sem, recv_sem, credit, ag_send, ag_recv, ag_loc, lags, on_total):
    t, d, f, nf, nl = dm
    nu = nf * nl
    core, _, _, ba, bb = bits
    piece = d // 16
    slots = cbuf.shape[0]
    r1, r2, r3, r4, r5 = rbuf
    at_end = ba == bb
    chunk = d // 8
    XU, XK, EU, EK, MU, MK, YY = range(7)
    ALL, MIDDLE, CORE = range(3)
    HALF, MATE, PAIR, LAST, FULL = range(5)
    partner = peers[0]

    def send(j, src, dst, sem, peer):
        remote(cbuf.at[lax.rem(j, slots), src, :], dst, send_sem.at[j], recv_sem.at[sem, j], peer).start()

    def add(j, rows, buf, sem):
        mine = cbuf.at[lax.rem(j, slots), rows, :]
        remote(mine, buf, send_sem.at[j], recv_sem.at[sem, j], partner).wait_recv()
        mine[...] = mine[...] + buf[...]

    def at(j):
        return chain_route(bits, peers, unit_of(j, nf, nl), d)

    def start(j):
        r, p1, _, _, _ = at(j)
        for (src, dst), sem in ((r["x_send_first"], XU), (r["x_send_second"], XK)):
            send(j, src, r1.at[j, dst, :], sem, p1)

    def rel(first):
        return pl.ds(pl.multiple_of((1 - bb if first else bb) * (d // 4), piece), d // 4)

    def s1(j):
        r, _, pa, _, _ = at(j)
        add(j, r["other_pair"], r1.at[j, rel(True), :], XU)

        @pl.when(at_end)
        def _():
            send(j, r["other_pair"], r2.at[j], EU, pa)

    def s2(j):
        r, _, pa, pm, _ = at(j)
        add(j, r["pair"], r1.at[j, rel(False), :], XK)

        @pl.when(at_end)
        def _():
            send(j, r["mate"], r3.at[j], EK, pa)

        @pl.when(jnp.logical_not(at_end))
        def _():
            add(j, r["other_pair"], r2.at[j], EU)
            send(j, r["far_end"], r5.at[j, 0:chunk, :], MU, pm)
            send(j, r["far_mid"], r5.at[j, chunk:2 * chunk, :], MK, pm)

    def s3(j):
        r, _, pa, _, p3 = at(j)

        @pl.when(jnp.logical_not(at_end))
        def _():
            add(j, r["mate"], r5.at[j, 0:chunk, :], MU)
            send(j, r["mate"], r3.at[j], EK, pa)
            add(j, r["own"], r3.at[j], EK)
            add(j, r["own"], r5.at[j, chunk:2 * chunk, :], MK)
            send(j, r["send"], r4.at[j], YY, p3)

    def s4(j):
        r, _, _, _, p3 = at(j)

        @pl.when(at_end)
        def _():
            add(j, r["own"], r3.at[j], EK)
            send(j, r["send"], r4.at[j], YY, p3)

    def full(j):
        return w_out.at[unit_of(j, nf, nl), core]

    def give(j, rows, sem_s, sem_r, peer, src=None):
        ref = full(j).at[rows, :]
        return remote(ref if src is None else src, ref, ag_send.at[j, sem_s], ag_recv.at[j, sem_r], peer)

    def own_copy(j):
        u = unit_of(j, nf, nl)
        return local(gs.at[u], full(j).at[at(j)[0]["keep"], :], ag_loc.at[j])

    def s5(j):
        r, _, _, _, p3 = at(j)
        u = unit_of(j, nf, nl)
        mine = cbuf.at[lax.rem(j, slots), r["keep"], :]
        remote(mine, r4.at[j], send_sem.at[j], recv_sem.at[YY, j], p3).wait_recv()
        on_total(u, mine[...] + r4[j])
        own_copy(j).start()
        give(j, r["keep"], ALL, HALF, p3, gs.at[u]).start()
        ref = cbuf.at[lax.rem(j, slots), pl.ds(0, 15 * piece), :]
        remote(ref, ref, send_sem.at[j], recv_sem.at[YY, j], p3).wait_send()
        free_slot(j, nu, slots, credit, partner)

    def g1(j):
        r, p1, pa, pm, p3 = at(j)
        own_copy(j).wait()
        give(j, r["send"], ALL, HALF, p3).wait_recv()
        give(j, r["own"], ALL, MATE, pa).start()

        @pl.when(jnp.logical_not(at_end))
        def _():
            give(j, r["own"], MIDDLE, PAIR, pm).start()
        give(j, r["own"], ALL, LAST, p1).start()

    def g2(j):
        r, p1, pa, pm, _ = at(j)
        give(j, r["mate"], ALL, MATE, pa).wait_recv()

        @pl.when(jnp.logical_not(at_end))
        def _():
            give(j, r["mate"], MIDDLE, PAIR, pm).start()
        give(j, r["mate"], ALL, LAST, p1).start()

    def g3(j, r, p1, pa):
        give(j, r["other_pair"], MIDDLE, PAIR, pa).wait_recv()
        give(j, r["other_pair"], ALL, LAST, p1).start()
        give(j, r["half"], CORE, FULL, partner).start()

    def g3_middle(j):
        r, p1, pa, _, _ = at(j)

        @pl.when(jnp.logical_not(at_end))
        def _():
            g3(j, r, p1, pa)
            give(j, r["other_pair"], MIDDLE, PAIR, pa).start()

    def g3_end(j):
        r, p1, pa, _, _ = at(j)

        @pl.when(at_end)
        def _():
            g3(j, r, p1, pa)

    def g4(j):
        r, p1, _, _, _ = at(j)
        give(j, r["other_half"], ALL, LAST, p1).wait_recv()
        give(j, r["other_half"], CORE, FULL, partner).start()

    def finish_unit(j):
        ref = w_out.at[unit_of(j, nf, nl), 1 - core]
        last = remote(ref, ref, ag_send.at[j, CORE], ag_recv.at[j, FULL], partner)
        last.wait_recv()
        last.wait_send()
        ref = full(j).at[pl.ds(0, 11 * piece), :]
        remote(ref, ref, ag_send.at[j, ALL], ag_recv.at[j, LAST], partner).wait_send()

        @pl.when(jnp.logical_not(at_end))
        def _():
            ref = full(j).at[pl.ds(0, 8 * piece), :]
            remote(ref, ref, ag_send.at[j, MIDDLE], ag_recv.at[j, PAIR], partner).wait_send()

    steps = (s1, s2, s3, s4, s5, g1, g2, g3_middle, g3_end, g4)
    return start, list(zip(lags, steps)), finish_unit


def second_backward(dm, scale, x_hbm, h_hbm, q_hbm, z_hbm, v_hbm, ws_hbm, sq_hbm, w_out, sq_out,
                    q, tmp, tb, eb, acc, zb, vb, cbuf, obuf, sbuf, r1, r2, r3, r4, r5, gs,
                    load_sem, io_sem, csend_sem, core_sem, send_sem, recv_sem, credit, nb, ag_send, ag_recv, ag_loc, nsend_sem, nrecv_sem):
    t, d, f, nf, nl = dm
    nu = nf * nl
    bits, peers = place()
    near, far = others(bits, (0, 1, 2)), others(bits, (3, 4))
    wait_all = arrive(near + far)

    def tiles(it, slot):
        u = unit_of(it, nf, nl)
        return local(z_hbm.at[u], zb.at[slot], load_sem.at[slot, 0]), local(v_hbm.at[u], vb.at[slot], load_sem.at[slot, 1])

    q_in = local(q_hbm, q, io_sem.at[0])
    h_in = local(h_hbm, tmp, io_sem.at[1])
    ws_in = local(ws_hbm, gs, io_sem.at[2])
    sq_in = local(sq_hbm, nb.at[0], io_sem.at[3])
    for cp in (q_in, h_in, *tiles(0, 0), ws_in, sq_in):
        cp.start()
    q_in.wait()
    fwd_seed(q, acc, t)
    transpose_into(tb.at[1], q, t)
    h_in.wait()
    transpose_into(tb.at[0], tmp, t)
    x_in = local(x_hbm, tmp, io_sem.at[1])
    x_in.start()
    ws_in.wait()
    sq_in.wait()
    wait_all()

    def on_total(u, total):
        gs[u] = gs[u] - LEARN_RATE * (total * scale)

    start_near, close_near = exchange(nb, 0, near, nsend_sem, nrecv_sem, 0)
    start_far, close_far = exchange(nb, 8, far, nsend_sem, nrecv_sem, 7)

    def start_far_after():
        close_near()
        start_far()

    def sums(j):
        for at, step in ((1, start_near), (nf // 2, start_far_after), (nf, close_far)):
            @pl.when(j == at)
            def _():
                step()

    start, events, finish_unit = chain(dm, bits, peers, cbuf, (r1, r2, r3, r4, r5), gs, w_out, send_sem, recv_sem, credit,
                                       ag_send, ag_recv, ag_loc, LAG_B[1:], on_total)
    backward_phase(dm, bits, peers, q, tmp, tb, eb, acc, zb, vb, cbuf, obuf, sbuf,
                   csend_sem, core_sem, credit, tiles, x_in.wait, LAG_B[0], start, [*events, (0, sums)])
    sq_cp = local(nb.at[12], sq_out, io_sem.at[3])
    sq_cp.start()

    @steps(nu)
    def _(j):
        finish_unit(j)
    sq_cp.wait()


def finish(scale, f, w_ref, sq_ref, in_ref, out_ref, loss_ref):
    for j in range(w_ref.shape[0]):
        in_ref[0, :, j * f:(j + 1) * f] = w_ref[j, 0]
        out_ref[0, j * f:(j + 1) * f, :] = w_ref[j, 1].T
    loss_ref[0, 0] = 0.5 * (jnp.sum(sq_ref[...]) * scale)


def sds(shape, dtype):
    return jax.ShapeDtypeStruct(shape, dtype)


def call(kernel, n_in, outs, scratch, name, collective_id=None):
    params = dict(vmem_limit_bytes=VMEM_CAP)
    if collective_id is not None:
        params.update(collective_id=collective_id, has_side_effects=True)
    return pl.pallas_call(
        kernel,
        out_shape=outs,
        in_specs=[ANY] * n_in,
        out_specs=[ANY] * len(outs),
        scratch_shapes=scratch,
        compiler_params=pltpu.CompilerParams(**params),
        name=name,
    )


def local_step(n_dev, tile_f, x_loc, y_loc, w_in, w_out):
    nl, d, ff = w_in.shape
    f = tile_f
    nf = ff // f
    nu = nl * nf
    t = x_loc.shape[0] * x_loc.shape[1]
    piece = d // 16
    dm = (t, d, f, nf, nl)
    scale = 1.0 / (t * n_dev * d)
    rho = RHO_FRAC * math.sqrt(nl * (d + ff))
    bf, f32 = jnp.bfloat16, jnp.float32
    V, DMA, REG = pltpu.VMEM, pltpu.SemaphoreType.DMA, pltpu.SemaphoreType.REGULAR
    x = x_loc.transpose(1, 0, 2).reshape(t, d)
    y = y_loc.transpose(1, 0, 2).reshape(t, d)
    z_s, v_s, w_s, a_s, n_s = sds((nu, t, f), bf), sds((nu, 2, d, f), bf), sds((nu, piece, f), f32), sds((t, d), bf), sds(TILE, f32)
    slots = min(CORE_SLOTS, nu)
    tile2, rows = V((2, d, f), f32), V((nu, piece, f), f32)
    reduce_bufs = [V((slots, d, f), f32), tile2, tile2, *(V((nu, d >> k, f), f32) for k in range(1, 5))]
    act, sums, both = V((t, d), bf), V((t, d), f32), V((t, 2 * f), bf)
    acts = [act, act, V((2, d, t), bf), V((2, t, f), bf), sums]
    norms, tens = V((13, *TILE), f32), DMA((10,))
    two, four, per_unit, loads = DMA((2,)), DMA((4,)), DMA((nu,)), DMA((2, 2))

    z, v, ws, wc, g, norm = call(
        functools.partial(first_pass, dm, scale), 4, [z_s, v_s, w_s, w_s, w_s, n_s],
        acts + [both, V((2, d, 2 * f), f32), V((2, 2 * f, d), f32), V((2, 2, t, f), bf), V((2, 2, 2, d, f), bf), rows, rows]
        + reduce_bufs + [norms, loads, two, two, four, two, per_unit, per_unit, DMA((2, nu, 4)), REG, tens, tens],
        "pass_a", 0)(x, y, w_in, w_out)

    z, v, h1, q, sq = call(
        functools.partial(second_forward, dm, scale, rho), 5, [z_s, v_s, a_s, a_s, n_s],
        [act, act, sums, both, rows, rows, V((nu, 2, d, f), bf), V((2, 2, t, f), bf), V(TILE, f32),
         DMA((nu, 2)), DMA((nu, 5)), two, per_unit, DMA((5,))], "fwd_b", 1)(g, ws, norm, x, y)

    w_new, sq = call(
        functools.partial(second_backward, dm, scale), 7, [sds((nu, 2, d, f), f32), n_s],
        acts + [V((2, t, f), bf), V((2, 2, d, f), bf)] + reduce_bufs
        + [V((nu, d // 4, f), f32), rows, loads, four, two, per_unit, per_unit, DMA((7, nu)), REG,
           norms, DMA((nu, 3)), DMA((nu, 5)), per_unit, tens, tens], "bwd_b", 2)(x, h1, q, z, v, wc, sq)

    per_step = min(FINISH_TILES, nf)
    new_in, new_out, loss = pl.pallas_call(
        functools.partial(finish, scale, f),
        grid=(nl, nf // per_step),
        in_specs=[pl.BlockSpec((per_step, 2, d, f), lambda i, j: (i * (nf // per_step) + j, 0, 0, 0)), pl.BlockSpec(TILE, lambda i, j: (0, 0))],
        out_specs=[pl.BlockSpec((1, d, per_step * f), lambda i, j: (i, 0, j)), pl.BlockSpec((1, per_step * f, d), lambda i, j: (i, j, 0)),
                   pl.BlockSpec((1, 1), lambda i, j: (0, 0), memory_space=pltpu.SMEM)],
        out_shape=[sds((nl, d, ff), f32), sds((nl, ff, d), f32), sds((1, 1), f32)],
        compiler_params=pltpu.CompilerParams(vmem_limit_bytes=VMEM_CAP),
        name="finish")(w_new, sq)
    return new_in, new_out, loss.reshape(())


def solution(mesh):
    step = functools.partial(local_step, mesh.shape["data"], TILE_F)
    return jax.shard_map(step, mesh=mesh, in_specs=(P("data"), P("data"), P(), P()), out_specs=(P(), P(), P()), check_vma=False)
```

```python
import math
import functools
import jax
import jax.numpy as jnp
from jax import lax
from jax.experimental import pallas as pl
from jax.experimental.pallas import tpu as pltpu
from jax.sharding import PartitionSpec as P

RHO_FRAC = 0.1
LEARN_RATE = 1.0
TILE_F = 256
MESH = pl.DeviceIdType.MESH
ANY = pl.BlockSpec(memory_space=pl.ANY)
NN = (((1,), (0,)), ((), ()))
NT = (((1,), (1,)), ((), ()))
GELU_C = math.sqrt(2.0 / math.pi)
GELU_K = 0.044715
VMEM_CAP = 67043328
TILE = (8, 128)
FINISH_TILES = 6
CORE_SLOTS = 9
LAG_A = (0, 1, 3, 5, 7)
LAG_B = (0, 2, 4, 5, 6, 7, 9, 10, 11, 14, 16)
VG_LAG = (0, 4, 6, 11, 14, 16)


steps = functools.partial(pl.loop, 0)


def odd(i):
    return lax.rem(i, 2)


def dot(lhs, rhs, dims=NN):
    return lax.dot_general(lhs, rhs, dims, preferred_element_type=jnp.float32)


def gelu_parts(z):
    sq = z * z
    th = jnp.tanh(GELU_C * (z + GELU_K * (sq * z)))
    cdf = 0.5 * (1.0 + th)
    return sq, th, cdf


def gelu(z):
    return z * gelu_parts(z)[2]


def gelu_and_grad(z):
    sq, th, cdf = gelu_parts(z)
    slope = cdf + (0.5 * z) * ((1.0 - th * th) * (GELU_C + (3.0 * GELU_K * GELU_C) * sq))
    return z * cdf, slope


def place(axis="data"):
    me = lax.axis_index(axis)
    bits = [lax.rem(lax.div(me, 1 << k), 2) for k in range(5)]
    peers = [me + (1 << k) * (1 - 2 * bits[k]) for k in range(5)]
    return bits, peers


def route(bits, peers, unit, rows):
    core, bx, by, ba, bb = bits
    _, px, py, pa, pb = peers
    swap = odd(unit + core) == 1
    b1, p1 = jnp.where(swap, by, bx), jnp.where(swap, py, px)
    b3, p3 = jnp.where(swap, bx, by), jnp.where(swap, px, py)
    axes = (b1, ba, b3, bb)
    step = rows // 16
    keep, send, base = [0], [], 0
    n = rows
    for bit in axes:
        n //= 2
        keep.append(pl.multiple_of(base + bit * n, step))
        send.append(pl.multiple_of(base + (1 - bit) * n, step))
        base = base + bit * n
    return (p1, pa, p3, pb), keep, send, axes


def chain_route(bits, peers, unit, d):
    core, bx, by, ba, bb = bits
    _, px, py, pa, _ = peers
    swap = odd(unit + core) == 1
    b1, p1 = jnp.where(swap, by, bx), jnp.where(swap, py, px)
    b3, p3 = jnp.where(swap, bx, by), jnp.where(swap, px, py)
    piece, chunk, pair, half = d // 16, d // 8, d // 4, d // 2
    me = lax.axis_index("data")

    def rows(base, n):
        return pl.ds(pl.multiple_of(base, piece), n)
    kx = b1 * half
    own = kx + (2 * bb + ba) * chunk
    mate = 2 * (kx + bb * pair) + chunk - own
    r = dict(
        half=rows(kx, half), other_half=rows((1 - b1) * half, half),
        pair=rows(kx + bb * pair, pair), other_pair=rows(kx + (1 - bb) * pair, pair),
        own=rows(own, chunk), mate=rows(mate, chunk),
        far_end=rows(kx + (1 - bb) * 3 * chunk, chunk), far_mid=rows(kx + (2 - bb) * chunk, chunk),
        keep=rows(own + b3 * piece, piece), send=rows(own + (1 - b3) * piece, piece),
        x_send_first=(rows((1 - b1) * half + (1 - bb) * pair, pair), rows((1 - bb) * pair, pair)),
        x_send_second=(rows((1 - b1) * half + bb * pair, pair), rows(bb * pair, pair)),
    )
    return r, p1, pa, me + 8 * (1 - 2 * bb), p3


def arrive(peers):
    barrier = pltpu.get_barrier_semaphore()
    for peer in peers:
        pl.semaphore_signal(barrier, device_id=(peer,), device_id_type=MESH)
    return functools.partial(pl.semaphore_wait, barrier, len(peers))


def others(bits, me_bits):
    me = lax.axis_index("data")
    out = []
    for mask in range(1, 1 << len(me_bits)):
        peer = me
        for i, k in enumerate(me_bits):
            if mask >> i & 1:
                peer = peer + (1 << k) * (1 - 2 * bits[k])
        out.append(peer)
    return out


def exchange(buf, first, peers, send_sem, recv_sem, sem0):
    copies = [remote(buf.at[first], buf.at[first + 1 + i], send_sem.at[sem0 + i], recv_sem.at[sem0 + i], peer) for i, peer in enumerate(peers)]

    def start():
        for cp in copies:
            cp.start()

    def close():
        total = buf[first]
        for i, cp in enumerate(copies):
            cp.wait()
            total = total + buf[first + 1 + i]
        buf[first + len(peers) + 1] = total
    return start, close


def gather_hops(bits, peers, unit, d, full, piece_src=None):
    ps, keep, send, _ = route(bits, peers, unit, d)
    piece = d // 16

    def rows(base, n):
        return full.at[pl.ds(base, n), :]

    def hop(k, part, sem_s, sem_r):
        peer = ps[3 - k] if k < 4 else peers[0]
        if k == 0:
            ref = rows(keep[4], piece)
        elif part == 0:
            ref = rows(keep[5 - k], piece << (k - 1))
        else:
            ref = rows(send[4 - k], piece << (k - 1))
        src = piece_src if piece_src is not None and part == 0 and k <= 1 else ref
        return remote(src, ref, sem_s, sem_r, peer)

    def arrived(k, sem_s, sem_r):
        ref = rows(send[3 - k], piece << k)
        return remote(ref, ref, sem_s, sem_r, ps[3 - k])

    def sent(sem_s, sem_r):
        ref = rows(0, 15 * piece)
        return remote(ref, ref, sem_s, sem_r, ps[0])
    return hop, arrived, sent


def remote(src, dst, send_sem, recv_sem, peer):
    return pltpu.make_async_remote_copy(src_ref=src, dst_ref=dst, send_sem=send_sem, recv_sem=recv_sem, device_id=(peer,), device_id_type=MESH)


def local(src, dst, sem):
    return pltpu.make_async_copy(src, dst, sem)


def halves(t):
    return [(0, t // 2), (t // 2, t // 2)] if t % 32 == 0 else [(0, t)]


def transpose_into(dst, src, t):
    full = t // 128
    if full:
        @steps(full)
        def _(i):
            lo = pl.multiple_of(i * 128, 128)
            dst[:, pl.ds(lo, 128)] = src[pl.ds(lo, 128), :].T
    if t % 128:
        dst[:, full * 128:t] = src[full * 128:t, :].T


def fwd_pair(h_ref, v_ref, acc_ref, a_ref, z_ref, t, f):
    for lo, n in halves(t):
        for j in range(2):
            z = dot(h_ref[lo:lo + n, :], v_ref[j, 0]).astype(jnp.bfloat16)
            z_ref[j, lo:lo + n, :] = z
            a_ref[lo:lo + n, j * f:(j + 1) * f] = gelu(z.astype(jnp.float32)).astype(jnp.bfloat16)
    v_out = jnp.concatenate([v_ref[0, 1], v_ref[1, 1]], axis=1)
    for lo, n in halves(t):
        acc_ref[lo:lo + n, :] += dot(a_ref[lo:lo + n, :], v_out, NT)


def fwd_close(h_ref, acc_ref, t):
    for lo, n in halves(t):
        h_ref[lo:lo + n, :] = acc_ref[lo:lo + n, :].astype(jnp.bfloat16)


def fwd_seed(h_ref, acc_ref, t):
    for lo, n in halves(t):
        acc_ref[lo:lo + n, :] = h_ref[lo:lo + n, :].astype(jnp.float32)


def fold(v):
    r, c = v.shape
    rows = jnp.sum(v.reshape(r // 8, 8, c), axis=0)
    return sum(rows[:, lo:lo + 128] for lo in range(0, c, 128))


def loss_close(h_ref, y_ref, acc_ref, t, d, total_ref=None):
    def rows_of(rows):
        e = acc_ref[rows, :].astype(jnp.bfloat16).astype(jnp.float32) - y_ref[rows, :].astype(jnp.float32)
        q = e.astype(jnp.bfloat16)
        h_ref[rows, :] = q
        acc_ref[rows, :] = q.astype(jnp.float32)
        return e
    if total_ref is None:
        for lo, n in halves(t):
            rows_of(slice(lo, lo + n))
        return
    n = 112 if t % 112 == 0 else t
    total_ref[...] = jnp.zeros(TILE, jnp.float32)

    @steps(t // n)
    def _(i):
        e = rows_of(pl.ds(pl.multiple_of(i * n, n), n))
        total_ref[...] += fold(e * e)


def unit_of(it, nf, nl):
    return (nl - 1 - it // nf) * nf + lax.rem(it, nf)


def first_pass(dm, scale, x_hbm, y_hbm, wi_hbm, wo_hbm, z_out, v_out, ws_out, wc_out, g_out, n_out,
               h, tmp, tb, eb, acc, ab, wi, wo, zb, vb, ws, wc, cbuf, obuf, sbuf, r1, r2, r3, r4, nb,
               load_sem, z_sem, v_sem, io_sem, csend_sem, core_sem, send_sem, recv_sem, credit, nsend_sem, nrecv_sem):
    t, d, f, nf, nl = dm
    nu = nf * nl
    bits, peers = place()
    piece = d // 16
    near, far = others(bits, (0, 1, 2)), others(bits, (3, 4))
    wait_all = arrive(near + far)

    def loads(p, slot):
        layer, tile = p // (nf // 2), lax.rem(p, nf // 2)
        lo = pl.multiple_of(tile * 2 * f, 2 * f)
        return (local(wi_hbm.at[layer, :, pl.ds(lo, 2 * f)], wi.at[slot], load_sem.at[slot, 0]),
                local(wo_hbm.at[layer, pl.ds(lo, 2 * f), :], wo.at[slot], load_sem.at[slot, 1]))

    def stores(p, slot):
        two = pl.ds(2 * p, 2)
        return local(zb.at[slot], z_out.at[two], z_sem.at[slot]), local(vb.at[slot], v_out.at[two], v_sem.at[slot])

    x_in = local(x_hbm, h, io_sem.at[0])
    y_in = local(y_hbm, tmp, io_sem.at[1])
    x_in.start()
    for cp in loads(0, 0):
        cp.start()
    y_in.start()
    x_in.wait()
    fwd_seed(h, acc, t)

    @steps(nu // 2)
    def _(p):
        slot = odd(p)
        for cp in loads(p, slot):
            cp.wait()

        @pl.when(p + 1 < nu // 2)
        def _():
            for cp in loads(p + 1, 1 - slot):
                cp.start()

        @pl.when(p >= 2)
        def _():
            for cp in stores(p - 2, slot):
                cp.wait()
        for j in range(2):
            cols = slice(j * f, (j + 1) * f)
            wot = wo[slot, cols, :].T
            _, keep, _, _ = route(bits, peers, 2 * p + j, d)
            rows = pl.ds(keep[4], piece)
            vb[slot, j, 0] = wi[slot, :, cols].astype(jnp.bfloat16)
            vb[slot, j, 1] = wot.astype(jnp.bfloat16)
            obuf[j] = wot
            ws[2 * p + j] = jnp.where(bits[0] == 0, wi[slot, rows, cols], obuf[j, rows, :])
            rows = chain_route(bits, peers, j, d)[0]['keep']
            wc[2 * p + j] = jnp.where(bits[0] == 0, wi[slot, rows, cols], obuf[j, rows, :])

        fwd_pair(h, vb.at[slot], acc, ab, zb.at[slot], t, f)
        for cp in stores(p, slot):
            cp.start()

        @pl.when(p == nf // 2 - 1)
        def _():
            fwd_close(h, acc, t)
            fwd_seed(h, acc, t)
            transpose_into(tb.at[0], h, t)

    np_ = nu // 2
    if np_ >= 2:
        for cp in stores(np_ - 2, np_ % 2):
            cp.wait()
    spare = np_ % 2

    def tiles(it, slot):
        u = unit_of(it, nf, nl)
        return (local(z_out.at[u], zb.at[spare, slot], load_sem.at[slot, 0]), local(v_out.at[u], vb.at[spare, slot], load_sem.at[slot, 1]))
    for cp in tiles(0, 0):
        cp.start()
    ws_cp = local(ws, ws_out, io_sem.at[2])
    wc_cp = local(wc, wc_out, io_sem.at[3])
    ws_cp.start()
    wc_cp.start()
    y_in.wait()
    loss_close(h, tmp, acc, t, d)
    transpose_into(tb.at[1], h, t)
    x_again = local(x_hbm, tmp, io_sem.at[1])
    x_again.start()
    for cp in stores(np_ - 1, (np_ - 1) % 2):
        cp.wait()
    wait_all()
    nb[0] = jnp.zeros(TILE, jnp.float32)

    ws_cp.wait()

    def on_total(u, total):
        ws[u] = total
        g = total * scale
        nb[0] += fold(g * g)

    start, events = halving(dm, bits, peers, cbuf, (r1, r2, r3, r4), send_sem, recv_sem, credit, LAG_A[1:], on_total)
    backward_phase(dm, bits, peers, h, tmp, tb, eb, acc, zb.at[spare], vb.at[spare], cbuf, obuf, sbuf,
                   csend_sem, core_sem, credit, tiles, x_again.wait, LAG_A[0], start, events)
    g_cp = local(ws, g_out, io_sem.at[0])
    g_cp.start()
    for start, close in (exchange(nb, 0, near, nsend_sem, nrecv_sem, 0), exchange(nb, 8, far, nsend_sem, nrecv_sem, 7)):
        start()
        close()
    n_cp = local(nb.at[12], n_out, io_sem.at[1])
    n_cp.start()
    wc_cp.wait()
    g_cp.wait()
    n_cp.wait()


def second_forward(dm, scale, rho, gs_hbm, ws_hbm, n_hbm, x_hbm, y_hbm, z_out, v_out, h_out, q_out, sq_out,
                   h, yb, acc, ab, gs, ws, vb, zb, nb, send_sem, recv_sem, z_sem, v_sem, io_sem):
    t, d, f, nf, nl = dm
    nu = nf * nl
    bits, peers = place()
    core = bits[0]
    piece = d // 16
    wait_all = arrive(peers)
    ins = (local(gs_hbm, gs, io_sem.at[0]), local(ws_hbm, ws, io_sem.at[1]), local(x_hbm, h, io_sem.at[2]), local(y_hbm, yb, io_sem.at[3]))
    n_in = local(n_hbm, nb, io_sem.at[4])
    n_in.start()
    for cp in ins:
        cp.start()
    n_in.wait()
    coef = rho / jnp.sqrt(jnp.sum(nb[...], keepdims=True))
    ins[0].wait()
    ins[1].wait()
    wait_all()

    def hops(u):
        return gather_hops(bits, peers, u, d, vb.at[u, core])

    def sems(u, k):
        return send_sem.at[u, 0 if k < 4 else 1], recv_sem.at[u, k]

    def core_arrived(u):
        ref = vb.at[u, 1 - core]
        return remote(ref, ref, *sems(u, 4), peers[0])

    def z_store(p, slot):
        return local(zb.at[slot], z_out.at[pl.ds(2 * p, 2)], z_sem.at[slot])

    @steps(nu + VG_LAG[5])
    def _(it):
        @pl.when(it < nu)
        def _():
            _, keep, _, _ = route(bits, peers, it, d)
            new = ws[it] + coef * (gs[it] * scale)
            vb[it, core, pl.ds(keep[4], piece), :] = new.astype(jnp.bfloat16)
            hop, _, _ = hops(it)
            hop(0, 0, *sems(it, 0)).start()
            hop(1, 0, *sems(it, 1)).start()
        for k in range(1, 5):
            u = it - VG_LAG[k]

            @pl.when((u >= 0) & (u < nu))
            def _():
                hop, arrived, _ = hops(u)
                arrived(k - 1, *sems(u, k - 1)).wait_recv()
                hop(k, 1, *sems(u, k)).start()
                if k < 4:
                    hop(k + 1, 0, *sems(u, k + 1)).start()
        u = it - VG_LAG[5]

        @pl.when(u >= 0)
        def _():
            core_arrived(u).wait_recv()
            local(vb.at[u], v_out.at[u], v_sem.at[u]).start()

        @pl.when((u >= 0) & (odd(u) == 1))
        def _():
            p = u // 2
            slot = odd(p)

            @pl.when(p >= 2)
            def _():
                z_store(p - 2, slot).wait()

            @pl.when(p == 0)
            def _():
                ins[2].wait()
                fwd_seed(h, acc, t)
            fwd_pair(h, vb.at[pl.ds(2 * p, 2)], acc, ab, zb.at[slot], t, f)
            z_store(p, slot).start()

            @pl.when(p == nf // 2 - 1)
            def _():
                fwd_close(h, acc, t)
                fwd_seed(h, acc, t)
                local(h, h_out, io_sem.at[0]).start()

    ins[3].wait()
    local(h, h_out, io_sem.at[0]).wait()
    loss_close(h, yb, acc, t, d, nb)
    out = local(h, q_out, io_sem.at[0])
    sq = local(nb, sq_out, io_sem.at[1])
    out.start()
    sq.start()

    @steps(nu)
    def _(u):
        local(vb.at[u], v_out.at[u], v_sem.at[u]).wait()
        hops(u)[2](*sems(u, 0)).wait_send()
        core_arrived(u).wait_send()
    for p in range(max(nu // 2 - 2, 0), nu // 2):
        z_store(p, p % 2).wait()
    out.wait()
    sq.wait()


def backward_phase(dm, bits, peers, q, tmp, tb, eb, acc, zb, vb, cbuf, obuf, sbuf, csend_sem, core_sem, credit,
                   tiles, x_ready, core_lag, after_core, events):
    t, d, f, nf, nl = dm
    nu = nf * nl
    core = bits[0]
    slots = cbuf.shape[0]

    def core_copy(it):
        slot = odd(it)
        return remote(sbuf.at[slot], cbuf.at[lax.rem(it, slots)], csend_sem.at[slot], core_sem.at[it], peers[0])

    def core_stage(j):
        cs = lax.rem(j, slots)
        core_copy(j).wait_recv()
        cbuf[cs] = cbuf[cs] + obuf[odd(j)]
        after_core(j)

    @steps(nu + max(lag for lag, _ in events))
    def _(it):
        @pl.when(it == nf)
        def _():
            fwd_close(q, acc, t)
            transpose_into(tb.at[1], q, t)
            x_ready()
            transpose_into(tb.at[0], tmp, t)

        @pl.when(it < nu)
        def _():
            slot = odd(it)
            for cp in tiles(it, slot):
                cp.wait()

            @pl.when(it + 1 < nu)
            def _():
                for cp in tiles(it + 1, 1 - slot):
                    cp.start()
            for lo, n in halves(t):
                back = dot(q[lo:lo + n, :], vb[slot, 1])
                a, slope = gelu_and_grad(zb[slot, lo:lo + n, :].astype(jnp.float32))
                eb[1, lo:lo + n, :] = a.astype(jnp.bfloat16)
                eb[0, lo:lo + n, :] = (back * slope).astype(jnp.bfloat16)

            @pl.when(it >= 2)
            def _():
                core_copy(it - 2).wait_send()
            sbuf[slot] = dot(tb[1 - core], eb[1 - core])

            @pl.when(it >= slots)
            def _():
                pl.semaphore_wait(credit)
            core_copy(it).start()
            obuf[slot] = dot(tb[core], eb[core])

            @pl.when(it < nf)
            def _():
                for lo, n in halves(t):
                    acc[lo:lo + n, :] += dot(eb[0, lo:lo + n, :], vb[slot, 0], NT)

        for lag, event in (*reversed(events), (core_lag, core_stage)):
            j = it - lag

            @pl.when((j >= 0) & (j < nu))
            def _():
                event(j)

    core_copy(nu - 2).wait_send()
    core_copy(nu - 1).wait_send()


def free_slot(j, nu, slots, credit, peer):
    @pl.when(j + slots < nu)
    def _():
        pl.semaphore_signal(credit, device_id=(peer,), device_id_type=MESH)


def halving(dm, bits, peers, cbuf, rbuf, send_sem, recv_sem, credit, lags, on_total):
    t, d, f, nf, nl = dm
    nu = nf * nl
    piece = d // 16
    slots = cbuf.shape[0]
    partner = peers[0]

    def rs_sends(it, k):
        ps, _, send, on = route(bits, peers, it, d)
        n = d >> (k + 1)
        cs = lax.rem(it, slots)

        def part(off, m, sem):
            return remote(cbuf.at[cs, pl.ds(send[k] + off, m), :], rbuf[k].at[it, pl.ds(off, m), :], send_sem.at[it], sem, ps[k])
        if k == 3:
            return [part(0, n, recv_sem.at[0, it, k])]
        m = n // 2
        return [part(pl.multiple_of((1 - on[k + 1]) * m, piece), m, recv_sem.at[0, it, k]),
                part(pl.multiple_of(on[k + 1] * m, piece), m, recv_sem.at[1, it, k])]

    def rs_add(it, k, kept):
        ps, keep, send, _ = route(bits, peers, it, d)
        cs = lax.rem(it, slots)
        if k == 3:
            base, m = keep[4], d >> 4
        else:
            base, m = (keep[k + 2] if kept else send[k + 1]), d >> (k + 2)
        here = rbuf[k].at[it, pl.ds(pl.multiple_of(base - keep[k + 1], piece), m), :]
        mine = cbuf.at[cs, pl.ds(base, m), :]
        remote(mine, here, send_sem.at[it], recv_sem.at[1 if kept else 0, it, k], ps[k]).wait_recv()
        total = mine[...] + here[...]
        if k == 3:
            return total
        mine[...] = total

    def start(j):
        for cp in rs_sends(j, 0):
            cp.start()

    def stage(k):
        def event(j):
            if k > 0:
                rs_add(j, k - 1, True)
            total = rs_add(j, k, False)
            if k < 3:
                for cp in rs_sends(j, k + 1):
                    cp.start()
            else:
                on_total(unit_of(j, nf, nl), total)
                ref = cbuf.at[lax.rem(j, slots), pl.ds(0, 15 * piece), :]
                remote(ref, ref, send_sem.at[j], recv_sem.at[0, j, 3], partner).wait_send()
                free_slot(j, nu, slots, credit, partner)
        return event
    return start, [(lags[k], stage(k)) for k in range(4)]


def chain(dm, bits, peers, cbuf, rbuf, gs, w_out, send_sem, recv_sem, credit, ag_send, ag_recv, ag_loc, lags, on_total):
    t, d, f, nf, nl = dm
    nu = nf * nl
    core, _, _, ba, bb = bits
    piece = d // 16
    slots = cbuf.shape[0]
    r1, r2, r3, r4, r5 = rbuf
    at_end = ba == bb
    chunk = d // 8
    XU, XK, EU, EK, MU, MK, YY = range(7)
    ALL, MIDDLE, CORE = range(3)
    HALF, MATE, PAIR, LAST, FULL = range(5)
    partner = peers[0]

    def send(j, src, dst, sem, peer):
        remote(cbuf.at[lax.rem(j, slots), src, :], dst, send_sem.at[j], recv_sem.at[sem, j], peer).start()

    def add(j, rows, buf, sem):
        mine = cbuf.at[lax.rem(j, slots), rows, :]
        remote(mine, buf, send_sem.at[j], recv_sem.at[sem, j], partner).wait_recv()
        mine[...] = mine[...] + buf[...]

    def at(j):
        return chain_route(bits, peers, unit_of(j, nf, nl), d)

    def start(j):
        r, p1, _, _, _ = at(j)
        for (src, dst), sem in ((r["x_send_first"], XU), (r["x_send_second"], XK)):
            send(j, src, r1.at[j, dst, :], sem, p1)

    def rel(first):
        return pl.ds(pl.multiple_of((1 - bb if first else bb) * (d // 4), piece), d // 4)

    def s1(j):
        r, _, pa, _, _ = at(j)
        add(j, r["other_pair"], r1.at[j, rel(True), :], XU)

        @pl.when(at_end)
        def _():
            send(j, r["other_pair"], r2.at[j], EU, pa)

    def s2(j):
        r, _, pa, pm, _ = at(j)
        add(j, r["pair"], r1.at[j, rel(False), :], XK)

        @pl.when(at_end)
        def _():
            send(j, r["mate"], r3.at[j], EK, pa)

        @pl.when(jnp.logical_not(at_end))
        def _():
            add(j, r["other_pair"], r2.at[j], EU)
            send(j, r["far_end"], r5.at[j, 0:chunk, :], MU, pm)
            send(j, r["far_mid"], r5.at[j, chunk:2 * chunk, :], MK, pm)

    def s3(j):
        r, _, pa, _, p3 = at(j)

        @pl.when(jnp.logical_not(at_end))
        def _():
            add(j, r["mate"], r5.at[j, 0:chunk, :], MU)
            send(j, r["mate"], r3.at[j], EK, pa)
            add(j, r["own"], r3.at[j], EK)
            add(j, r["own"], r5.at[j, chunk:2 * chunk, :], MK)
            send(j, r["send"], r4.at[j], YY, p3)

    def s4(j):
        r, _, _, _, p3 = at(j)

        @pl.when(at_end)
        def _():
            add(j, r["own"], r3.at[j], EK)
            send(j, r["send"], r4.at[j], YY, p3)

    def full(j):
        return w_out.at[unit_of(j, nf, nl), core]

    def give(j, rows, sem_s, sem_r, peer, src=None):
        ref = full(j).at[rows, :]
        return remote(ref if src is None else src, ref, ag_send.at[j, sem_s], ag_recv.at[j, sem_r], peer)

    def own_copy(j):
        u = unit_of(j, nf, nl)
        return local(gs.at[u], full(j).at[at(j)[0]["keep"], :], ag_loc.at[j])

    def s5(j):
        r, _, _, _, p3 = at(j)
        u = unit_of(j, nf, nl)
        mine = cbuf.at[lax.rem(j, slots), r["keep"], :]
        remote(mine, r4.at[j], send_sem.at[j], recv_sem.at[YY, j], p3).wait_recv()
        on_total(u, mine[...] + r4[j])
        own_copy(j).start()
        give(j, r["keep"], ALL, HALF, p3, gs.at[u]).start()
        ref = cbuf.at[lax.rem(j, slots), pl.ds(0, 15 * piece), :]
        remote(ref, ref, send_sem.at[j], recv_sem.at[YY, j], p3).wait_send()
        free_slot(j, nu, slots, credit, partner)

    def g1(j):
        r, p1, pa, pm, p3 = at(j)
        own_copy(j).wait()
        give(j, r["send"], ALL, HALF, p3).wait_recv()
        give(j, r["own"], ALL, MATE, pa).start()

        @pl.when(jnp.logical_not(at_end))
        def _():
            give(j, r["own"], MIDDLE, PAIR, pm).start()
        give(j, r["own"], ALL, LAST, p1).start()

    def g2(j):
        r, p1, pa, pm, _ = at(j)
        give(j, r["mate"], ALL, MATE, pa).wait_recv()

        @pl.when(jnp.logical_not(at_end))
        def _():
            give(j, r["mate"], MIDDLE, PAIR, pm).start()
        give(j, r["mate"], ALL, LAST, p1).start()

    def g3(j, r, p1, pa):
        give(j, r["other_pair"], MIDDLE, PAIR, pa).wait_recv()
        give(j, r["other_pair"], ALL, LAST, p1).start()
        give(j, r["half"], CORE, FULL, partner).start()

    def g3_middle(j):
        r, p1, pa, _, _ = at(j)

        @pl.when(jnp.logical_not(at_end))
        def _():
            g3(j, r, p1, pa)
            give(j, r["other_pair"], MIDDLE, PAIR, pa).start()

    def g3_end(j):
        r, p1, pa, _, _ = at(j)

        @pl.when(at_end)
        def _():
            g3(j, r, p1, pa)

    def g4(j):
        r, p1, _, _, _ = at(j)
        give(j, r["other_half"], ALL, LAST, p1).wait_recv()
        give(j, r["other_half"], CORE, FULL, partner).start()

    def finish_unit(j):
        ref = w_out.at[unit_of(j, nf, nl), 1 - core]
        last = remote(ref, ref, ag_send.at[j, CORE], ag_recv.at[j, FULL], partner)
        last.wait_recv()
        last.wait_send()
        ref = full(j).at[pl.ds(0, 11 * piece), :]
        remote(ref, ref, ag_send.at[j, ALL], ag_recv.at[j, LAST], partner).wait_send()

        @pl.when(jnp.logical_not(at_end))
        def _():
            ref = full(j).at[pl.ds(0, 8 * piece), :]
            remote(ref, ref, ag_send.at[j, MIDDLE], ag_recv.at[j, PAIR], partner).wait_send()

    steps = (s1, s2, s3, s4, s5, g1, g2, g3_middle, g3_end, g4)
    return start, list(zip(lags, steps)), finish_unit


def second_backward(dm, scale, x_hbm, h_hbm, q_hbm, z_hbm, v_hbm, ws_hbm, sq_hbm, w_out, sq_out,
                    q, tmp, tb, eb, acc, zb, vb, cbuf, obuf, sbuf, r1, r2, r3, r4, r5, gs,
                    load_sem, io_sem, csend_sem, core_sem, send_sem, recv_sem, credit, nb, ag_send, ag_recv, ag_loc, nsend_sem, nrecv_sem):
    t, d, f, nf, nl = dm
    nu = nf * nl
    bits, peers = place()
    near, far = others(bits, (0, 1, 2)), others(bits, (3, 4))
    wait_all = arrive(near + far)

    def tiles(it, slot):
        u = unit_of(it, nf, nl)
        return local(z_hbm.at[u], zb.at[slot], load_sem.at[slot, 0]), local(v_hbm.at[u], vb.at[slot], load_sem.at[slot, 1])

    q_in = local(q_hbm, q, io_sem.at[0])
    h_in = local(h_hbm, tmp, io_sem.at[1])
    ws_in = local(ws_hbm, gs, io_sem.at[2])
    sq_in = local(sq_hbm, nb.at[0], io_sem.at[3])
    for cp in (q_in, h_in, *tiles(0, 0), ws_in, sq_in):
        cp.start()
    q_in.wait()
    fwd_seed(q, acc, t)
    transpose_into(tb.at[1], q, t)
    h_in.wait()
    transpose_into(tb.at[0], tmp, t)
    x_in = local(x_hbm, tmp, io_sem.at[1])
    x_in.start()
    ws_in.wait()
    sq_in.wait()
    wait_all()

    def on_total(u, total):
        gs[u] = gs[u] - LEARN_RATE * (total * scale)

    start_near, close_near = exchange(nb, 0, near, nsend_sem, nrecv_sem, 0)
    start_far, close_far = exchange(nb, 8, far, nsend_sem, nrecv_sem, 7)

    def start_far_after():
        close_near()
        start_far()

    def sums(j):
        for at, step in ((1, start_near), (nf // 2, start_far_after), (nf, close_far)):
            @pl.when(j == at)
            def _():
                step()

    start, events, finish_unit = chain(dm, bits, peers, cbuf, (r1, r2, r3, r4, r5), gs, w_out, send_sem, recv_sem, credit,
                                       ag_send, ag_recv, ag_loc, LAG_B[1:], on_total)
    backward_phase(dm, bits, peers, q, tmp, tb, eb, acc, zb, vb, cbuf, obuf, sbuf,
                   csend_sem, core_sem, credit, tiles, x_in.wait, LAG_B[0], start, [*events, (0, sums)])
    sq_cp = local(nb.at[12], sq_out, io_sem.at[3])
    sq_cp.start()

    @steps(nu)
    def _(j):
        finish_unit(j)
    sq_cp.wait()


def finish(scale, f, w_ref, sq_ref, in_ref, out_ref, loss_ref):
    for j in range(w_ref.shape[0]):
        in_ref[0, :, j * f:(j + 1) * f] = w_ref[j, 0]
        out_ref[0, j * f:(j + 1) * f, :] = w_ref[j, 1].T
    loss_ref[0, 0] = 0.5 * (jnp.sum(sq_ref[...]) * scale)


def sds(shape, dtype):
    return jax.ShapeDtypeStruct(shape, dtype)


def call(kernel, n_in, outs, scratch, name, collective_id=None):
    params = dict(vmem_limit_bytes=VMEM_CAP)
    if collective_id is not None:
        params.update(collective_id=collective_id, has_side_effects=True)
    return pl.pallas_call(
        kernel,
        out_shape=outs,
        in_specs=[ANY] * n_in,
        out_specs=[ANY] * len(outs),
        scratch_shapes=scratch,
        compiler_params=pltpu.CompilerParams(**params),
        name=name,
    )


def local_step(n_dev, tile_f, x_loc, y_loc, w_in, w_out):
    nl, d, ff = w_in.shape
    f = tile_f
    nf = ff // f
    nu = nl * nf
    t = x_loc.shape[0] * x_loc.shape[1]
    piece = d // 16
    dm = (t, d, f, nf, nl)
    scale = 1.0 / (t * n_dev * d)
    rho = RHO_FRAC * math.sqrt(nl * (d + ff))
    bf, f32 = jnp.bfloat16, jnp.float32
    V, DMA, REG = pltpu.VMEM, pltpu.SemaphoreType.DMA, pltpu.SemaphoreType.REGULAR
    x = x_loc.transpose(1, 0, 2).reshape(t, d)
    y = y_loc.transpose(1, 0, 2).reshape(t, d)
    z_s, v_s, w_s, a_s, n_s = sds((nu, t, f), bf), sds((nu, 2, d, f), bf), sds((nu, piece, f), f32), sds((t, d), bf), sds(TILE, f32)
    slots = min(CORE_SLOTS, nu)
    tile2, rows = V((2, d, f), f32), V((nu, piece, f), f32)
    reduce_bufs = [V((slots, d, f), f32), tile2, tile2, *(V((nu, d >> k, f), f32) for k in range(1, 5))]
    act, sums, both = V((t, d), bf), V((t, d), f32), V((t, 2 * f), bf)
    acts = [act, act, V((2, d, t), bf), V((2, t, f), bf), sums]
    norms, tens = V((13, *TILE), f32), DMA((10,))
    two, four, per_unit, loads = DMA((2,)), DMA((4,)), DMA((nu,)), DMA((2, 2))

    z, v, ws, wc, g, norm = call(
        functools.partial(first_pass, dm, scale), 4, [z_s, v_s, w_s, w_s, w_s, n_s],
        acts + [both, V((2, d, 2 * f), f32), V((2, 2 * f, d), f32), V((2, 2, t, f), bf), V((2, 2, 2, d, f), bf), rows, rows]
        + reduce_bufs + [norms, loads, two, two, four, two, per_unit, per_unit, DMA((2, nu, 4)), REG, tens, tens],
        "pass_a", 0)(x, y, w_in, w_out)

    z, v, h1, q, sq = call(
        functools.partial(second_forward, dm, scale, rho), 5, [z_s, v_s, a_s, a_s, n_s],
        [act, act, sums, both, rows, rows, V((nu, 2, d, f), bf), V((2, 2, t, f), bf), V(TILE, f32),
         DMA((nu, 2)), DMA((nu, 5)), two, per_unit, DMA((5,))], "fwd_b", 1)(g, ws, norm, x, y)

    w_new, sq = call(
        functools.partial(second_backward, dm, scale), 7, [sds((nu, 2, d, f), f32), n_s],
        acts + [V((2, t, f), bf), V((2, 2, d, f), bf)] + reduce_bufs
        + [V((nu, d // 4, f), f32), rows, loads, four, two, per_unit, per_unit, DMA((7, nu)), REG,
           norms, DMA((nu, 3)), DMA((nu, 5)), per_unit, tens, tens], "bwd_b", 2)(x, h1, q, z, v, wc, sq)

    per_step = min(FINISH_TILES, nf)
    new_in, new_out, loss = pl.pallas_call(
        functools.partial(finish, scale, f),
        grid=(nl, nf // per_step),
        in_specs=[pl.BlockSpec((per_step, 2, d, f), lambda i, j: (i * (nf // per_step) + j, 0, 0, 0)), pl.BlockSpec(TILE, lambda i, j: (0, 0))],
        out_specs=[pl.BlockSpec((1, d, per_step * f), lambda i, j: (i, 0, j)), pl.BlockSpec((1, per_step * f, d), lambda i, j: (i, j, 0)),
                   pl.BlockSpec((1, 1), lambda i, j: (0, 0), memory_space=pltpu.SMEM)],
        out_shape=[sds((nl, d, ff), f32), sds((nl, ff, d), f32), sds((1, 1), f32)],
        compiler_params=pltpu.CompilerParams(vmem_limit_bytes=VMEM_CAP),
        name="finish")(w_new, sq)
    return new_in, new_out, loss.reshape(())


def solution(mesh):
    step = functools.partial(local_step, mesh.shape["data"], TILE_F)
    return jax.shard_map(step, mesh=mesh, in_specs=(P("data"), P("data"), P(), P()), out_specs=(P(), P(), P()), check_vma=False)
```
